32 devices in a mesh: section: 2 (over core), dp: 4 (over z), mp: 4 (over y, x).
Axes of the slice: x: 2, y: 2, z: 4, core: 2. Of those that a mesh axis runs over, the one named last changes fastest.
Arguments:
- block_input: bfloat16 [8, 1024, 1024], P('dp', None, 'mp'), may hold values from -6 to 6
- cotangent: bfloat16 [8, 1024, 1024], P('dp', None, 'mp'), may hold values from -6 to 6
- lengths: int32 [8], P('dp'), may hold values from 1 to 1024, 5120 in all
- ln_gain: float32 [2, 1024], P('section'), may hold values from 0.5 to 1.5
- ln_bias: float32 [2, 1024], P('section'), may hold values from -2 to 2
- w_qkv: bfloat16 [2, 3, 1024, 1024], P('section', None, None, 'mp'), may hold values from -0.1875 to 0.1875
- w_out: bfloat16 [2, 1024, 1024], P('section', 'mp'), may hold values from -1.5 to 1.5
- w_up: bfloat16 [2, 1024, 4096], P('section', None, 'mp'), may hold values from -0.1875 to 0.1875
- w_down: bfloat16 [2, 4096, 1024], P('section', 'mp'), may hold values from -0.09375 to 0.09375
- freq_table: bfloat16 [2, 16, 64, 64], P('section', 'mp'), may hold values from -0.75 to 0.75
- feat_weight: float32 [2, 16, 64], P('section', 'mp'), may hold values from 0.5 to 2
Outputs:
- boundary: float32 [2, 8, 1024, 1024], P('section', 'dp', None, 'mp')
- gain_grad: float32 [2, 1024], P('section', 'mp')
- bias_grad: float32 [2, 1024], P('section', 'mp')
- qkv_grad: float32 [2, 3, 1024, 1024], P('section', None, 'dp', 'mp')
- out_grad: float32 [2, 1024, 1024], P('section', 'mp', 'dp')
- up_grad: float32 [2, 1024, 4096], P('section', 'dp', 'mp')
- down_grad: float32 [2, 4096, 1024], P('section', 'mp', 'dp')
- freq_grad: float32 [2, 16, 64, 64], P('section', 'mp')
- feat_grad: float32 [2, 16, 64], P('section', 'mp')
The draws below stay inside these ranges and needn't reach their ends.
Inputs may be any that keep to these rules, and one draw needn't show every extreme that they name: Slot n holds lengths[n] real tokens at its start; later positions are padding.
All inputs are finite; a program needn't handle non-finite values. No bound on the sum of `lengths` on one device may be relied on, other than what follows from the above.
Results may differ from the reference program's by a relative error of at most 0.03.
Values may be sent and summed in bfloat16 or wider, within the bound.
No kernel may reach another device: no remote copies, remote signals or barrier semaphores. Data moves between devices by JAX's collectives and lax.ppermute only.
A program may use at most 384 MiB of HBM per device.

```python
import math
import jax
import jax.numpy as jnp
import numpy as np
from jax import lax

D = 1024
FF = 4096
HEADS = 16
HD = 64
ROT = 16
FEAT = 64
GROUP = 64
SEQ = 1024
SLOTS = 8


def raised(values, stream_key, source, target, blocks, factor):
    def block_of(position):
        return (jnp.arange(values.shape[position]) // (values.shape[position] // blocks)).reshape((-1,) + (1,) * (values.ndim - 1 - position))

    first = jax.random.permutation(stream_key, blocks)[block_of(target)]
    second = (block_of(target) + blocks // 2) % blocks
    return jnp.where((block_of(source) == first) | (block_of(source) == second), factor * values, values)


def block_scale(rng, dims, shards, low, high):
    level = 1.0
    for dim, parts in shards:
        steps = jax.random.uniform(jax.random.fold_in(jax.random.fold_in(rng, 6), dim), (parts,), jnp.float32, low / len(shards), high / len(shards))
        level = level * jnp.repeat(jnp.exp(steps), dims[dim] // parts).reshape((-1,) + (1,) * (len(dims) - 1 - dim))
    return level


def profile(amount, total, most, skew):
    portions = [(1 << 20) // math.isqrt(grade ** skew) + 1 for grade in range(2, amount + 1)]
    surplus, holding = total - most - (amount - 1), [1] * (amount - 1)
    while surplus > 0:
        free = [i for i in range(amount - 1) if holding[i] < most]
        pool, budget = sum([portions[i] for i in free]), surplus
        for i in free:
            extra = min(most - holding[i], max(1, budget * portions[i] // pool), surplus)
            holding[i] = holding[i] + extra
            surplus = surplus - extra
    return np.array([most] + holding)


def ragged_sizes(own_key, count, total, bound, skew):
    if count == 2:
        one = jax.random.randint(own_key, (), max(1, total - bound), min(bound, total - 1) + 1)
        return jnp.stack([one, total - one])
    sizes = jnp.asarray(profile(count, total, bound, skew), jnp.int32)
    couples = (count - 1) // 2
    donor, taker = sizes[1:1 + 2 * couples:2], sizes[2:2 + 2 * couples:2]
    margin = jnp.minimum(donor - 1, bound - taker)
    passed = jax.random.randint(jax.random.fold_in(own_key, 1), (couples,), 0, 1 << 20) % (margin + 1)
    sizes = sizes.at[1:1 + 2 * couples:2].set(donor - passed).at[2:2 + 2 * couples:2].set(taker + passed)
    return sizes[jax.random.permutation(jax.random.fold_in(own_key, 2), count)]


def centred(rng, shape, spread, most, pieces=(), kind=jnp.bfloat16):
    values = jax.random.normal(rng, shape, jnp.float32) * spread
    if len(pieces) > 0:
        values = block_scale(rng, shape, pieces, -0.22, 0.18) * values
    return jnp.clip(values, min=-most, max=most).astype(kind)


def heavy_noise(key, dims, spread, limit, cuts, heavy, kind=jnp.bfloat16):
    entries = spread * jax.random.normal(key, dims, jnp.float32)
    if cuts:
        entries = entries * block_scale(key, dims, cuts, -0.22, 0.18)
    return jnp.clip(raised(entries, jax.random.fold_in(key, 3), *heavy), -limit, limit).astype(kind)


def setup_inputs(seed: int = 0) -> dict:
    key_of = jax.random.split(jax.random.key(seed), 12)
    return {
        "block_input": heavy_noise(key_of[0], (SLOTS, SEQ, D), 1.0, 6.0, ((0, 4), (2, 4)), (0, 2, 4, 2.0)),
        "cotangent": heavy_noise(key_of[1], (SLOTS, SEQ, D), 1.0, 6.0, ((0, 4), (2, 4)), (0, 2, 4, 2.0)),
        "lengths": ragged_sizes(key_of[2], SLOTS, SLOTS * SEQ * 5 // 8, SEQ, 1).astype(jnp.int32),
        "ln_gain": jnp.clip(1.0 + 0.1 * jax.random.normal(key_of[3], (2, D), jnp.float32), 0.5, 1.5),
        "ln_bias": centred(key_of[4], (2, D), 0.3, 2.0, ((0, 2),), jnp.float32),
        "w_qkv": centred(key_of[5], (2, 3, D, D), D ** -0.5, 0.1875, ((0, 2), (3, 4))),
        "w_out": centred(key_of[6], (2, D, D), (max(D // 64, 4)) ** -0.5, 1.5, ((0, 2), (1, 4))),
        "w_up": centred(key_of[7], (2, D, FF), D ** -0.5, 0.1875, ((0, 2), (2, 4))),
        "w_down": centred(key_of[8], (2, FF, D), FF ** -0.5, 0.09375, ((0, 2), (1, 4))),
        "freq_table": centred(key_of[9], (2, HEADS, HD, FEAT), HD ** -0.5, 0.75, ((0, 2), (1, 4))),
        "feat_weight": jnp.clip(jnp.exp(math.log(2.0) - 1.3862944 * jax.random.uniform(key_of[10], (2, HEADS, FEAT), jnp.float32) ** block_scale(key_of[10], (2, HEADS, FEAT), ((0, 2), (1, 4)), -0.2, 0.2)), 0.5, 2.0),
    }


@jax.custom_vjp
def low(v):
    return lax.optimization_barrier(v.astype(jnp.bfloat16)).astype(jnp.float32)

@jax.custom_vjp
def low_back(v):
    return v

def low_keep(v):
    return (low(v), None)

def low_pass(kept, grad):
    return (grad,)

def back_keep(v):
    return (v, None)

def back_low(kept, grad):
    return (low(grad),)
low.defvjp(low_keep, low_pass)
low_back.defvjp(back_keep, back_low)
highest = lax.Precision.HIGHEST
eps_norm = 1e-05

def dct_table(order):
    row_index = jnp.arange(order, dtype=jnp.float32)[:, None]
    col_index = jnp.arange(order, dtype=jnp.float32)[None, :]
    cosines = jnp.sqrt(2.0 / order) * jnp.cos(math.pi * (row_index + 0.5) * col_index / order)
    return cosines * jnp.where(col_index == 0, math.sqrt(0.5), 1.0)

def rotate(values, rot_dims):
    half_dims = rot_dims // 2
    inverse = 10000.0 ** (-jnp.arange(half_dims, dtype=jnp.float32) * 2.0 / rot_dims)
    angles = jnp.arange(values.shape[0], dtype=jnp.float32)[:, None] * inverse[None, :]
    cosine = jnp.cos(angles)[:, None, :]
    sine_part = jnp.sin(angles)[:, None, :]
    lower_half = values[..., :half_dims]
    upper_half = values[..., half_dims:rot_dims]
    return jnp.concatenate([lower_half * cosine - upper_half * sine_part, upper_half * cosine + lower_half * sine_part, values[..., rot_dims:]], axis=-1)

def linear_attention(query, key, value, valid_mask, freq_values, feat_values):
    length, head_count, head_size = query.shape
    mixed = jnp.einsum('nk,hkm->hnm', dct_table(head_size), freq_values, precision=highest)
    query_logit = jnp.einsum('shn,hnm->shm', rotate(query, ROT), mixed, precision=highest)
    key_logit = jnp.einsum('shn,hnm->shm', rotate(key, ROT), mixed, precision=highest)
    query_feat = low(feat_values * jnp.exp(query_logit))
    key_feat = low(feat_values * jnp.exp(key_logit) * valid_mask[:, None, None])
    value_low = low(value)
    blocks = length // GROUP
    query_feat = query_feat.reshape(blocks, GROUP, head_count, -1)
    key_feat = key_feat.reshape(blocks, GROUP, head_count, -1)
    value_low = value_low.reshape(blocks, GROUP, head_count, head_size)
    scores = jnp.einsum('cihm,cjhm->chij', query_feat, key_feat, precision=highest)
    causal = jnp.arange(GROUP)[:, None] >= jnp.arange(GROUP)[None, :]
    scores = jnp.where(causal, scores, 0.0)
    denominator = lax.optimization_barrier(jnp.sum(scores, axis=-1))
    numerator = jnp.einsum('chij,cjhd->cihd', low(scores), value_low, precision=highest)
    states = jnp.einsum('cjhm,cjhd->chmd', key_feat, value_low, precision=highest)
    key_sums = lax.optimization_barrier(jnp.sum(key_feat, axis=1))
    prior_states = jnp.concatenate([jnp.zeros_like(states[:1]), jnp.cumsum(states, axis=0)[:-1]], axis=0)
    prior_sums = jnp.concatenate([jnp.zeros_like(key_sums[:1]), jnp.cumsum(key_sums, axis=0)[:-1]], axis=0)
    numerator = numerator + jnp.einsum('cihm,chmd->cihd', query_feat, prior_states, precision=highest)
    denominator = jnp.transpose(denominator, (0, 2, 1)) + jnp.einsum('cihm,chm->cih', query_feat, prior_sums, precision=highest)
    result = numerator / denominator[..., None]
    return result.reshape(length, head_count * head_size)

def residual_layer(inputs, valid_mask, gain, bias, qkv_weight, out_weight, up_weight, down_weight, freq_values, feat_values):
    row_mean = lax.optimization_barrier(jnp.mean(inputs, axis=-1, keepdims=True))
    centered = inputs - row_mean
    variance = lax.optimization_barrier(jnp.mean(centered * centered, axis=-1, keepdims=True))
    normed = low(centered * lax.rsqrt(variance + eps_norm) * gain + bias)
    projected = low_back(jnp.einsum('sd,tde->tse', normed, qkv_weight, precision=highest))
    up_proj = low_back(jnp.dot(normed, up_weight, precision=highest))
    length = inputs.shape[0]
    shaped = projected.reshape(3, length, HEADS, HD)
    attended = linear_attention(shaped[0], shaped[1], shaped[2], valid_mask, freq_values, feat_values)
    attended = low(low_back(attended))
    active = low(jax.nn.gelu(up_proj, approximate=False))
    return inputs + jnp.dot(attended, out_weight, precision=highest) + jnp.dot(active, down_weight, precision=highest)

def two_layers(sample, valid_mask, weights):
    lower_layer = tuple((values[0] for values in weights))
    upper_layer = tuple((values[1] for values in weights))
    hidden = low_back(low(residual_layer(sample, valid_mask, *lower_layer)))
    return residual_layer(hidden, valid_mask, *upper_layer)

def reference(block_input, cotangent, lengths, ln_gain, ln_bias, w_qkv, w_out, w_up, w_down, freq_table, feat_weight):
    inputs = block_input.astype(jnp.float32)
    weights = (ln_gain.astype(jnp.float32), ln_bias.astype(jnp.float32), w_qkv.astype(jnp.float32), w_out.astype(jnp.float32), w_up.astype(jnp.float32), w_down.astype(jnp.float32), freq_table.astype(jnp.float32), feat_weight.astype(jnp.float32))
    positions = jnp.arange(SEQ, dtype=jnp.int32)
    valid_all = (positions[None, :] < lengths[:, None]).astype(jnp.float32)

    def forward(values, params):

        def per_slot(sample):
            return two_layers(sample[0], sample[1], params)
        return lax.map(jax.checkpoint(per_slot), (values, valid_all))
    outputs, pullback = jax.vjp(forward, inputs, weights)
    input_grad, weight_grads = pullback(cotangent.astype(jnp.float32))
    boundary = jnp.stack([input_grad, outputs], axis=0)
    return (boundary, weight_grads[0], weight_grads[1], weight_grads[2], weight_grads[3], weight_grads[4], weight_grads[5], weight_grads[6], weight_grads[7])
```

```python
import functools
import math

import jax
import jax.numpy as jnp
from jax import lax
from jax.experimental import pallas as pl
from jax.experimental.pallas import tpu as pltpu
from jax.sharding import PartitionSpec as P

ROT = 16
TILE = 256
HEAD = 64
LANES = 256
EPS = 1e-05
F32 = jnp.float32
BF16 = jnp.bfloat16
RSQRT2 = math.sqrt(0.5)
RSQRT2PI = 1.0 / math.sqrt(2.0 * math.pi)
SAVED = 14


def dot_nn(a, b):
    return lax.dot_general(a, b, (((1,), (0,)), ((), ())), preferred_element_type=F32)


def dot_nt(a, b):
    return lax.dot_general(a, b, (((1,), (1,)), ((), ())), preferred_element_type=F32)


def dot_tn(a, b):
    return lax.dot_general(a, b, (((0,), (0,)), ((), ())), preferred_element_type=F32)


def split(values):
    high = values.astype(BF16)
    return high, (values - high.astype(F32)).astype(BF16)


def iota(shape, dim):
    return lax.broadcasted_iota(jnp.int32, shape, dim)


def partner(values):
    later = pltpu.roll(values, LANES - ROT // 2, 1)
    earlier = pltpu.roll(values, ROT // 2, 1)
    lower = iota(values.shape, 1) % HEAD < ROT // 2
    return jnp.where(lower, later, earlier)


def twice(table):
    return jnp.concatenate([table, table], axis=1)


def head_of(shape, dim):
    return iota(shape, dim) // HEAD


def weight_copies(refs, w_in, w_out, sems, which):
    qkv, up, out, down = refs
    ends = [(qkv.at[0, t], w_in.at[:, t * LANES:(t + 1) * LANES]) for t in range(3)] + [
        (up.at[0], w_in.at[:, 3 * LANES:]), (out.at[0], w_out.at[0:LANES, :]), (down.at[0], w_out.at[LANES:, :])]
    return [pltpu.make_async_copy(*ends[i], sems.at[i]) for i in which]


def start_weights(meta, mine, other, w_in, w_out, sems, order):
    def start(refs):
        for copy in weight_copies(refs, w_in, w_out, sems, order):
            copy.start()

    @pl.when(meta[1] == 1)
    def _():
        start(mine)

    @pl.when(meta[1] != 1)
    def _():
        start(other)


def wait_weights(step, refs, w_in, w_out, sems, which):
    @pl.when(step == 0)
    def _():
        for copy in weight_copies(refs, w_in, w_out, sems, which):
            copy.wait()


def forward_kernel(carried, phased, *refs):
    refs = list(refs)
    take = lambda n: [refs.pop(0) for _ in range(n)]
    meta, lens = take(2)
    p0, p1, p2, p3a, p3b, gain, bias, mix_hi, mix_lo, feat_w, cos_t, sin_t = take(12)
    mine, other = take(4), take(4)
    if carried:
        state_in, ksum_in = take(2)
        take(SAVED)
    parts = take(5 if phased else 4)
    normed, xhat, rstd, rq_o, rk_o, qf_o, kf_o, v_o, hcat, dgelu, invz, att_o, prior_s, prior_k = take(SAVED)
    state, ksum, w_in, w_out, sems = take(5)
    tile = pl.program_id(0)
    rank = meta[0]
    half = LANES // 2

    @pl.when(tile == 0)
    def _():
        start_weights(meta, mine, other, w_in, w_out, sems, (0, 1, 2, 3, 4, 5))
        if carried:
            state[...] = state_in[...]
            ksum[...] = ksum_in[...]
        else:
            state[...] = jnp.zeros_like(state)
            ksum[...] = jnp.zeros_like(ksum)

    pieces = [p0[...].astype(F32), p1[...].astype(F32), p2[...].astype(F32),
              jnp.concatenate([p3a[...], p3b[...]], axis=1).astype(F32)]
    width = 4 * LANES
    mean = jnp.sum(pieces[0] + pieces[1] + pieces[2] + pieces[3], axis=1, keepdims=True) * (1.0 / width)
    pieces = [piece - mean for piece in pieces]
    squares = sum(piece * piece for piece in pieces)
    factor = lax.rsqrt(jnp.sum(squares, axis=1, keepdims=True) * (1.0 / width) + EPS)
    for r in range(4):
        at = pl.ds(pl.multiple_of((rank ^ r) * LANES, LANES), LANES)
        hat = pieces[r] * factor
        if r == 0:
            xhat[...] = hat
        normed[:, at] = (hat * gain[:, at] + bias[:, at]).astype(BF16)
    rstd[...] = jnp.broadcast_to(factor, (TILE, half))
    tokens = normed[...]

    wait_weights(tile, mine, w_in, w_out, sems, (0, 1, 2))
    cosine, sine = twice(cos_t[...]), twice(sin_t[...])
    query = dot_nn(tokens, w_in[:, 0:LANES])
    key = dot_nn(tokens, w_in[:, LANES:2 * LANES])
    value = dot_nn(tokens, w_in[:, 2 * LANES:3 * LANES]).astype(BF16)
    rq = query * cosine + partner(query) * sine
    rk = key * cosine + partner(key) * sine
    weight = feat_w[...]

    def logits(rows):
        high, low = split(rows)
        return dot_nn(high, mix_hi[...]) + dot_nn(low, mix_hi[...]) + dot_nn(high, mix_lo[...])

    positions = lens[1] + tile * TILE + iota((TILE, LANES), 0)
    real = (positions < lens[0]).astype(F32)
    qf = (weight * jnp.exp(logits(rq))).astype(BF16)
    kf = (weight * jnp.exp(logits(rk)) * real).astype(BF16)
    rq_o[...] = rq.astype(BF16)
    rk_o[...] = rk.astype(BF16)
    qf_o[...] = qf
    kf_o[...] = kf
    v_o[...] = value

    square = (TILE, TILE)
    lower = iota(square, 0) >= iota(square, 1)
    same = head_of(square, 0) == head_of(square, 1)
    cumulative = dot_nn(lower.astype(BF16), kf) + ksum[0:1, :]
    high, low = split(qf.astype(F32) * cumulative)
    ones = same.astype(BF16)
    inverse = 1.0 / (dot_nn(high, ones) + dot_nn(low, ones))
    prior = jnp.where(same, state[...], 0.0)
    prior_hi, prior_lo = split(prior)
    numer = dot_nn(qf, prior_hi) + dot_nn(qf, prior_lo)
    lane_head = head_of((TILE, LANES), 1)
    zero = jnp.zeros((TILE, LANES), BF16)
    for h in range(LANES // HEAD):
        here = lane_head == h
        scores = dot_nt(qf, jnp.where(here, kf, zero))
        scores = jnp.where(lower, scores, 0.0).astype(BF16)
        numer = numer + dot_nn(scores, jnp.where(here, value, zero))
    prior_s[0] = prior
    prior_k[0] = ksum[...]
    state[...] = state[...] + dot_tn(kf, value)
    ksum[...] = jnp.broadcast_to(cumulative[TILE - 1:TILE, :], ksum.shape)
    invz[...] = inverse
    attended = numer * inverse
    att_o[...] = attended
    hcat[:, 0:LANES] = attended.astype(BF16)

    wait_weights(tile, mine, w_in, w_out, sems, (3,))
    for c in range(4):
        cols = slice(c * LANES, (c + 1) * LANES)
        up = dot_nn(tokens, w_in[:, (3 + c) * LANES:(4 + c) * LANES])
        cdf = 0.5 * (1.0 + lax.erf(up * RSQRT2))
        hcat[:, (1 + c) * LANES:(2 + c) * LANES] = (up * cdf).astype(BF16)
        dgelu[:, cols] = (cdf + up * (RSQRT2PI * jnp.exp(-0.5 * up * up))).astype(BF16)

    wait_weights(tile, mine, w_in, w_out, sems, (4, 5))
    hidden = hcat[...]
    emit(rank, lambda at: dot_nn(hidden, w_out[:, at]), parts)


def emit(rank, product, parts):
    half = LANES // 2
    for r in range(4):
        at = pl.ds(pl.multiple_of((rank ^ r) * LANES, LANES), LANES)
        part = product(at)
        if len(parts) == 4:
            parts[r][...] = part.astype(parts[r].dtype)
            continue
        sx, sy, k0, ka, kb = parts
        if r == 0:
            k0[...] = part
        elif r == 1:
            sx[0] = part[:, :half].astype(BF16)
            kb[...] = part[:, half:]
        elif r == 2:
            ka[...] = part[:, :half]
            sy[0] = part[:, half:].astype(BF16)
        else:
            sx[1] = part[:, :half].astype(BF16)
            sy[1] = part[:, half:].astype(BF16)


def backward_kernel(carried, phased, *refs):
    refs = list(refs)
    take = lambda n: [refs.pop(0) for _ in range(n)]
    meta, = take(1)
    grad, normed, rq, rk, qf_i, kf_i, v_i, att_i, dgelu, invz, prior_s, prior_k, gain, bias, mix_hi, cos_t, sin_t = take(17)
    mine, other = take(4), take(4)
    if carried:
        state_in, gsum_in, dmix_in, fsum_in = take(4)
        take(2)
    parts = take(5 if phased else 4)
    stats, dcat, state, gsum, dmix, fsum = take(6)
    w_in, w_out, sems = take(3)
    step = pl.program_id(0)
    rank = meta[0]

    @pl.when(step == 0)
    def _():
        start_weights(meta, mine, other, w_in, w_out, sems, (4, 5, 0, 1, 2, 3))
        if carried:
            state[...] = state_in[...]
            gsum[...] = gsum_in[...]
            dmix[...] = dmix_in[...]
            fsum[...] = fsum_in[...]
        else:
            state[...] = jnp.zeros_like(state)
            gsum[...] = jnp.zeros_like(gsum)
            dmix[...] = jnp.zeros_like(dmix)
            fsum[...] = jnp.zeros_like(fsum)

    wait_weights(step, mine, w_in, w_out, sems, (4, 5))
    g = grad[...]
    d_att = dot_nt(g, w_out[0:LANES, :]).astype(BF16).astype(F32)
    square = (TILE, TILE)
    same = head_of(square, 0) == head_of(square, 1)
    ones = same.astype(BF16)
    inverse = invz[...]
    dn = (d_att * inverse).astype(BF16)
    dn32 = dn.astype(F32)
    high, low = split(dn32 * att_i[...])
    dden = -(dot_nn(high, ones) + dot_nn(low, ones))
    den_hi = dden.astype(BF16).astype(F32)
    roll_hi = pltpu.roll(den_hi, HEAD, 1)
    roll_lo = pltpu.roll(dden - den_hi, HEAD, 1)
    qf, kf, value = qf_i[...], kf_i[...], v_i[...]
    zero = jnp.zeros((TILE, LANES), BF16)
    one = jnp.ones((TILE, LANES), BF16)
    lane = iota((TILE, LANES), 1)
    lane_head = lane // HEAD
    below = iota(square, 0) >= iota(square, 1)
    above = iota(square, 0) <= iota(square, 1)
    prior_hi, prior_lo = split(prior_s[0])
    later_hi, later_lo = split(jnp.where(same, state[...], 0.0))
    d_qf = dot_nt(dn, prior_hi) + dot_nt(dn, prior_lo) + prior_k[0, 0:1, :] * dden
    d_kf = dot_nt(value, later_hi) + dot_nt(value, later_lo) + gsum[0:1, :]
    d_v = dot_nn(kf, later_hi)
    heads = LANES // HEAD
    for h in range(heads):
        here = lane_head == h
        spare = HEAD * ((h + 1) % heads)
        left = jnp.where(lane == spare, roll_hi, jnp.where(lane == spare + 1, roll_lo, dn32)).astype(BF16)
        right = jnp.where(here, value, jnp.where((lane == spare) | (lane == spare + 1), one, zero))
        k_here = jnp.where(here, kf, zero)
        q_here = jnp.where(here, qf, zero)
        d_here = jnp.where(here, dn, zero)
        scores_t = jnp.where(above, dot_nt(k_here, qf), 0.0).astype(BF16)
        ds = jnp.where(below, dot_nt(left, right), 0.0).astype(BF16)
        ds_t = jnp.where(above, dot_nt(right, left), 0.0).astype(BF16)
        d_qf = d_qf + dot_nn(ds, k_here)
        d_kf = d_kf + dot_nn(ds_t, q_here)
        d_v = d_v + dot_nn(scores_t, d_here)
    state[...] = state[...] + dot_tn(qf, dn)
    gsum[...] = gsum[...] + jnp.sum(qf.astype(F32) * dden, axis=0, keepdims=True)
    dlq = d_qf * qf.astype(F32)
    dlk = d_kf * kf.astype(F32)
    fsum[...] = fsum[...] + jnp.sum(dlq + dlk, axis=0, keepdims=True)
    dlq, dlk = dlq.astype(BF16), dlk.astype(BF16)
    dmix[...] = dmix[...] + dot_tn(rq[...], dlq) + dot_tn(rk[...], dlk)
    cosine, sine = twice(cos_t[...]), twice(sin_t[...])
    for c, dl in ((0, dlq), (1, dlk)):
        dr = dot_nt(dl, mix_hi[...])
        dcat[:, c * LANES:(c + 1) * LANES] = (dr * cosine - partner(dr) * sine).astype(BF16)
    dcat[:, 2 * LANES:3 * LANES] = d_v.astype(BF16)
    for c in range(4):
        cols = slice(c * LANES, (c + 1) * LANES)
        d_act = dot_nt(g, w_out[(1 + c) * LANES:(2 + c) * LANES, :])
        dcat[:, (3 + c) * LANES:(4 + c) * LANES] = (d_act * dgelu[:, cols].astype(F32)).astype(BF16)
    wait_weights(step, mine, w_in, w_out, sems, (0, 1, 2, 3))
    wide = dcat[...]
    row = iota((8, LANES), 0)
    first, second = (row == 0).astype(BF16), (row == 1).astype(BF16)
    totals = []

    def product(at):
        part = dot_nt(wide, w_in[at, :])
        one_side = (part * gain[:, at]).astype(BF16)
        other = (part * (normed[:, at].astype(F32) - bias[:, at])).astype(BF16)
        totals.append(dot_nt(first, one_side) + dot_nt(second, other))
        return part

    emit(rank, product, parts)
    stats[...] = totals[0] + totals[1] + totals[2] + totals[3]


def join_kernel(meta, p0, p1, p2, p3a, p3b, whole):
    half = LANES // 2
    for r, piece in enumerate((p0, p1, p2)):
        whole[:, pl.ds(pl.multiple_of((meta[0] ^ r) * LANES, LANES), LANES)] = piece[...]
    at = pl.multiple_of((meta[0] ^ 3) * LANES, LANES)
    whole[:, pl.ds(at, half)] = p3a[...]
    whole[:, pl.ds(pl.multiple_of(at + half, half), half)] = p3b[...]


def partial_outs(rows, phased, row_of):
    half = LANES // 2
    if not phased:
        shapes = [jax.ShapeDtypeStruct((rows, LANES), F32)] + [jax.ShapeDtypeStruct((rows, LANES), BF16)] * 3
        return shapes, [pl.BlockSpec((TILE, LANES), lambda *i: (row_of(*i), 0))] * 4
    shapes = [jax.ShapeDtypeStruct((2, rows, half), BF16)] * 2 + [
        jax.ShapeDtypeStruct((rows, LANES), F32), jax.ShapeDtypeStruct((rows, half), F32),
        jax.ShapeDtypeStruct((rows, half), F32)]
    specs = [pl.BlockSpec((2, TILE, half), lambda *i: (0, row_of(*i), 0))] * 2 + [
        pl.BlockSpec((TILE, width), lambda *i: (row_of(*i), 0)) for width in (LANES, half, half)]
    return shapes, specs


def fixed(shape):
    return pl.BlockSpec(shape, lambda *i: (0,) * len(shape))


def outside(count):
    return [pl.BlockSpec(memory_space=pl.ANY)] * count


def params(axes=1):
    return pltpu.CompilerParams(dimension_semantics=("arbitrary",) * axes, vmem_limit_bytes=56 << 20)


def weight_scratch(width):
    return [pltpu.VMEM((width, 3 * LANES + width), BF16), pltpu.VMEM((LANES + width, width), BF16),
            pltpu.SemaphoreType.DMA((6,))]


def forward_layer(meta, lens, pieces, weights, tables, length, first_row, phased, carry=None):
    rows = pieces[0].shape[0]
    tiles, before = rows // TILE, first_row // TILE
    half, width = LANES // 2, 4 * LANES
    local = lambda t, *_: t
    there = lambda t, *_: before + t
    by_row = lambda n, row_of: pl.BlockSpec((TILE, n), lambda *i: (row_of(*i), 0))
    (gain, bias, mix_hi, mix_lo, feat_w), mine, other = weights
    small = (gain, bias, mix_hi, mix_lo, feat_w)
    shapes, specs = partial_outs(rows, phased, local)
    extra = [(width, BF16), (LANES, F32), (half, F32)] + [(LANES, BF16)] * 5 + [
        (LANES + width, BF16), (width, BF16), (LANES, F32), (LANES, F32)]
    shapes += [jax.ShapeDtypeStruct((length, n), d) for n, d in extra]
    specs += [by_row(n, there) for n, _ in extra]
    shapes += [jax.ShapeDtypeStruct((length // TILE, LANES, LANES), F32), jax.ShapeDtypeStruct((length // TILE, 8, LANES), F32)]
    specs += [pl.BlockSpec((1, n, LANES), lambda *i: (there(*i), 0, 0)) for n in (LANES, 8)]
    states = [(LANES, LANES), (8, LANES)]
    shapes += [jax.ShapeDtypeStruct(s, F32) for s in states]
    specs += [fixed(s) for s in states]
    operands = [meta, jnp.stack([lens[0], jnp.int32(first_row)]), *pieces, *small, *tables, *mine, *other]
    in_specs = [by_row(p.shape[1], local) for p in pieces] + [fixed(w.shape) for w in small] + [by_row(half, there)] * 2 + outside(8)
    aliases = {}
    if carry is not None:
        state, saved = carry
        operands += [*state, *saved]
        in_specs += [fixed(s) for s in states] + outside(SAVED)
        aliases = {len(operands) - SAVED + i: len(shapes) - 2 - SAVED + i for i in range(SAVED)}
    outs = pl.pallas_call(
        functools.partial(forward_kernel, carry is not None, phased),
        name="layer_forward",
        out_shape=shapes,
        grid_spec=pltpu.PrefetchScalarGridSpec(
            num_scalar_prefetch=2, grid=(tiles,), in_specs=in_specs, out_specs=specs, scratch_shapes=weight_scratch(width)),
        input_output_aliases=aliases,
        compiler_params=params(),
        cost_estimate=pl.CostEstimate(flops=rows * 20_000_000, transcendentals=rows * 5000, bytes_accessed=24 << 20),
    )(*operands)
    count = 5 if phased else 4
    return outs[:count], outs[count:count + SAVED], outs[count + SAVED:]


def backward_layer(meta, grad, saved, weights, tables, length, first_row, phased, carry=None):
    rows = grad.shape[0]
    tiles, before = rows // TILE, first_row // TILE
    half, width = LANES // 2, 4 * LANES
    local = lambda t, *_: tiles - 1 - t
    there = lambda t, *_: before + tiles - 1 - t
    by_row = lambda n, row_of=there: pl.BlockSpec((TILE, n), lambda *i: (row_of(*i), 0))
    normed, rq, rk, qf, kf, value, hcat, dgelu, invz, attended, prior_s, prior_k = saved
    (gain, bias, mix_hi, mix_lo, feat_w), mine, other = weights
    shapes, specs = partial_outs(rows, phased, local)
    shapes += [jax.ShapeDtypeStruct((8, length), F32), jax.ShapeDtypeStruct((length, 3 * LANES + width), BF16)]
    specs += [pl.BlockSpec((8, TILE), lambda *i: (0, there(*i))), by_row(3 * LANES + width)]
    states = [(LANES, LANES), (8, LANES)] * 2
    shapes += [jax.ShapeDtypeStruct(s, F32) for s in states]
    specs += [fixed(s) for s in states]
    operands = [meta, grad, normed, rq, rk, qf, kf, value, attended, dgelu, invz, prior_s, prior_k, gain, bias, mix_hi, *tables,
                *mine, *other]
    in_specs = [by_row(width, local), by_row(width)] + [by_row(LANES)] * 6 + [by_row(width), by_row(LANES)] + [
        pl.BlockSpec((1, n, LANES), lambda *i: (there(*i), 0, 0)) for n in (LANES, 8)] + [
        fixed(w.shape) for w in (gain, bias, mix_hi)] + [by_row(half)] * 2 + outside(8)
    aliases = {}
    if carry is not None:
        state, arrays = carry
        operands += [*state, *arrays]
        in_specs += [fixed(s) for s in states] + outside(2)
        aliases = {len(operands) - 2 + i: len(shapes) - 6 + i for i in range(2)}
    outs = pl.pallas_call(
        functools.partial(backward_kernel, carry is not None, phased),
        name="layer_backward",
        out_shape=shapes,
        grid_spec=pltpu.PrefetchScalarGridSpec(
            num_scalar_prefetch=1, grid=(tiles,), in_specs=in_specs, out_specs=specs, scratch_shapes=weight_scratch(width)),
        input_output_aliases=aliases,
        compiler_params=params(),
        cost_estimate=pl.CostEstimate(flops=rows * 25_000_000, transcendentals=0, bytes_accessed=24 << 20),
    )(*operands)
    count = 5 if phased else 4
    return outs[:count], outs[count:count + 2], outs[count + 2:]


def join(meta, pieces):
    rows, block = pieces[0].shape[0], 2 * TILE
    return pl.pallas_call(
        join_kernel,
        name="join",
        out_shape=jax.ShapeDtypeStruct((rows, 4 * LANES), BF16),
        grid_spec=pltpu.PrefetchScalarGridSpec(
            num_scalar_prefetch=1,
            grid=(rows // block,),
            in_specs=[pl.BlockSpec((block, p.shape[1]), lambda i, *_: (i, 0)) for p in pieces],
            out_specs=pl.BlockSpec((block, 4 * LANES), lambda i, *_: (i, 0)),
        ),
        cost_estimate=pl.CostEstimate(flops=0, transcendentals=0, bytes_accessed=rows * 16 * LANES),
    )(meta, *pieces)


def swap(value, axis, by):
    return lax.ppermute(value, axis, [(k, k ^ by) for k in range(lax.axis_size(axis))])


def gather_pieces(shard):
    half = shard.shape[1] // 2
    from_x, from_y = swap(shard, "mp", 1), swap(shard, "mp", 2)
    return shard, from_x, from_y, swap(from_x[:, :half], "mp", 2), swap(from_y[:, half:], "mp", 1)


def after(values, *others):
    if not others:
        return values
    return lax.optimization_barrier((values, others))[0]


def direct_sends(parts):
    return parts[0], [swap(part, "mp", r) for r, part in enumerate(parts) if r > 0]


def scatter_sum(parts, extra, meanwhile=()):
    sx, sy, k0, ka, kb = parts
    half = ka.shape[1]
    in_x, in_y = after((swap(sx, "mp", 1), swap(sy, "mp", 2)), *meanwhile)
    if extra is not None:
        extra = mp_total(after(extra, in_x, in_y))
    last_y = swap((ka + in_x[1].astype(F32)).astype(BF16), "mp", 2)
    last_x = swap((kb + in_y[1].astype(F32)).astype(BF16), "mp", 1)
    return jnp.concatenate(
        [k0[:, :half] + in_x[0].astype(F32) + last_y.astype(F32), k0[:, half:] + in_y[0].astype(F32) + last_x.astype(F32)],
        axis=1), extra


def mp_total(values):
    return values + swap(values, "mp", 1) + swap(values, "mp", 2) + swap(values, "mp", 3)


def ring_scatter(block_of, axis):
    count = lax.axis_size(axis)
    rank = lax.axis_index(axis)
    pairs = [(k, (k + 1) % count) for k in range(count)]
    total = block_of((rank + count - 1) % count)
    for step in range(2, count + 1):
        arrived = lax.ppermute(total, axis, pairs)
        total = (arrived.astype(F32) + block_of((rank + count - step) % count).astype(F32)).astype(BF16)
    return total


def dp_total(values):
    count = lax.axis_size("dp")
    if count > 8:
        return lax.psum(values, "dp")
    sent = [lax.ppermute(values, "dp", [(i, (i + k) % count) for i in range(count)]) for k in range(1, count)]
    return sum(sent, values)


def block_sends(block_of, axis):
    count = lax.axis_size(axis)
    rank = lax.axis_index(axis)
    if count > 8:
        return [ring_scatter(block_of, axis)]
    return [block_of(rank)] + [
        lax.ppermute(block_of((rank + k) % count), axis, [(i, (i + k) % count) for i in range(count)]) for k in range(1, count)]


def sum_blocks(blocks):
    total = blocks[0].astype(F32)
    for block in blocks[1:]:
        total = total + block.astype(F32)
    return total.astype(BF16)


def weight_gradient(left, right, half_of, section):
    def product(which):
        a, b = half_of(left, right, which)
        return lax.dot_general(a, b, (((0,), (0,)), ((), ())), preferred_element_type=F32).astype(BF16)

    arrived = swap(product(1 - section), "section", 1)
    return lax.optimization_barrier(product(section)), arrived


def dct_table(order):
    row_index = jnp.arange(order, dtype=F32)[:, None]
    col_index = jnp.arange(order, dtype=F32)[None, :]
    cosines = jnp.sqrt(2.0 / order) * jnp.cos(math.pi * (row_index + 0.5) * col_index / order)
    return cosines * jnp.where(col_index == 0, math.sqrt(0.5), 1.0)


def rotary_tables(length):
    column = jnp.arange(LANES // 2, dtype=jnp.int32) % HEAD
    half = ROT // 2
    index = (column % half).astype(F32)
    angles = jnp.arange(length, dtype=F32)[:, None] * (10000.0 ** (-index * 2.0 / ROT))[None, :]
    turned = (column < ROT)[None, :]
    sign = jnp.where(column < half, -1.0, 1.0)[None, :]
    return jnp.where(turned, jnp.cos(angles), 1.0), jnp.where(turned, sign * jnp.sin(angles), 0.0)


def shards(block_input, cotangent, lengths, ln_gain, ln_bias, w_qkv, w_out, w_up, w_down, freq_table, feat_weight):
    section = lax.axis_index("section")
    place = lax.axis_index("mp")
    group = lax.axis_index("dp")
    groups = lax.axis_size("dp")
    local_slots, length, shard_width = block_input.shape
    width = ln_gain.shape[1]
    heads = freq_table.shape[1]
    is_first = section == 0
    lens = lax.dynamic_slice_in_dim(lengths, section, 1, 0)
    metas = [jnp.stack([place, (section == l).astype(jnp.int32)]).astype(jnp.int32) for l in range(2)]

    def own(values):
        return lax.dynamic_index_in_dim(values, section, 0, keepdims=False)

    shard0 = own(block_input)
    pieces0 = gather_pieces(shard0)

    small = jnp.concatenate([ln_gain[0], ln_bias[0], feat_weight.reshape(-1), freq_table.astype(F32).reshape(-1)])
    small_other = swap(small, "section", 1)
    mine = (w_qkv, w_up, w_out, w_down)
    other = tuple(swap(w, "section", 1) for w in mine)

    def both(mine, other):
        return jnp.where(is_first, mine, other), jnp.where(is_first, other, mine)

    layers_small = both(small, small_other)
    table = dct_table(HEAD)
    eye = jnp.eye(heads, dtype=F32)

    def layer_weights(l):
        vec = layers_small[l]
        gain, bias = vec[:width].reshape(1, width), vec[width:2 * width].reshape(1, width)
        feat = vec[2 * width:2 * width + LANES].reshape(1, LANES)
        freq = vec[2 * width + LANES:].reshape(heads, HEAD, HEAD)
        mixed = jnp.einsum("nk,hkm->hnm", table, freq, precision=lax.Precision.HIGHEST)
        mixed = (eye[:, None, :, None] * mixed[:, :, None, :]).reshape(LANES, LANES)
        high = lax.reduce_precision(mixed, 8, 7)
        return (gain, bias, high.astype(BF16), (mixed - high).astype(BF16), feat), mine, other

    weights0, weights1 = layer_weights(0), layer_weights(1)
    tables = rotary_tables(length)

    cot = after(own(cotangent), pieces0[3], pieces0[4])
    cot_x, cot_y = swap(cot, "mp", 1), swap(cot, "mp", 2)
    part0, all0, _ = forward_layer(metas[0], lens, pieces0, weights0, tables, length, 0, True)
    part0 = after(part0, cot_x, cot_y)
    hidden = (shard0.astype(F32) + scatter_sum(part0, None)[0]).astype(BF16)
    pieces1 = gather_pieces(hidden)
    cot_x, cot_y = after((cot_x, cot_y), pieces1[3], pieces1[4])
    half = shard_width // 2
    pieces_g = cot, cot_x, cot_y, swap(cot_x[:, :half], "mp", 2), swap(cot_y[:, half:], "mp", 1)
    part1, all1, _ = forward_layer(metas[1], lens, pieces1, weights1, tables, length, 0, False)
    out_kept, out_sent = direct_sends(part1)

    def saved_of(arrays):
        return (arrays[0],) + tuple(arrays[3:])

    def in_half(left, right, which):
        n = right.shape[1] // 2
        return left, lax.dynamic_slice_in_dim(right, which * n, n, 1)

    def out_half(left, right, which):
        n = left.shape[1] // 2
        return lax.dynamic_slice_in_dim(left, which * n, n, 1), right

    def in_block(mine, arrived):
        n = mine.shape[0] // groups
        cut = lambda v, i: lax.dynamic_slice_in_dim(v, i * n, n, 0)
        return lambda i: (cut(mine, i).astype(F32) + cut(arrived, i).astype(F32)).astype(BF16)

    def out_block(mine, arrived):
        n = mine.shape[1] // groups
        cut = lambda v, i: lax.dynamic_slice_in_dim(v, i * n, n, 1)
        return lambda i: (cut(mine, i).astype(F32) + cut(arrived, i).astype(F32)).astype(BF16)

    def run_backward(meta, grad, saved, weights, phased):
        parts, (stats, dcat), (_, _, dmix, fsum) = backward_layer(meta, grad, saved, weights, tables, length, 0, phased)
        return parts, stats, dcat, dmix, fsum

    def norm_backward(grad_shard, d_normed, sums, norm, gain_all):
        xhat, rstd = norm
        gain = lax.dynamic_slice_in_dim(gain_all, place * shard_width, shard_width, 1)
        mean_d = (sums[0] * (1.0 / width))[:, None]
        mean_dx = (sums[1] * (1.0 / width))[:, None]
        return grad_shard.astype(F32) + rstd[:, :1] * (d_normed * gain - mean_d - xhat * mean_dx)

    def small_gradients(d_normed, norm, dmix, fsum):
        gain_part = jnp.sum(d_normed * norm[0], axis=0)
        bias_part = jnp.sum(d_normed, axis=0)
        diagonal = jnp.stack([dmix[h * HEAD:(h + 1) * HEAD, h * HEAD:(h + 1) * HEAD] for h in range(heads)])
        return jnp.concatenate([gain_part, bias_part, fsum[0], diagonal.reshape(-1)])

    saved1, saved0 = saved_of(all1), saved_of(all0)
    grad1 = join(metas[1], pieces_g)
    out_blocks1 = block_sends(out_block(*weight_gradient(saved1[6], grad1, out_half, section)), "dp")
    grad1_b = after(grad1, out_blocks1[0])
    parts, stats, dcat1, dmix1, fsum1 = run_backward(metas[1], grad1_b, saved1, weights1, True)
    parts, dcat1 = after((parts, dcat1), *out_blocks1, *out_sent)
    in_blocks1 = block_sends(in_block(*weight_gradient(saved1[0], dcat1, in_half, section)), "dp")
    d_normed, sums = scatter_sum(parts, stats, in_blocks1[:1])
    g0 = norm_backward(cot, d_normed, sums, all1[1:3], weights1[0][0]).astype(BF16)
    small1 = small_gradients(d_normed, all1[1:3], dmix1, fsum1)
    pieces_g0 = gather_pieces(after(g0, *in_blocks1[1:2]))
    pieces_g0 = after(pieces_g0, *in_blocks1)
    out = hidden.astype(F32) + out_kept + out_sent[0].astype(F32) + out_sent[1].astype(F32) + out_sent[2].astype(F32)

    grad0 = join(metas[0], pieces_g0)
    out_blocks0 = block_sends(out_block(*weight_gradient(saved0[6], grad0, out_half, section)), "dp")
    grad0_b = after(grad0, out_blocks0[0])
    parts, stats, dcat0, dmix0, fsum0 = run_backward(metas[0], grad0_b, saved0, weights0, False)
    parts, dcat0 = after((parts, dcat0), *out_blocks0)
    out_blocks1, in_blocks1 = after((out_blocks1, in_blocks1), dcat0)
    kept, sent = direct_sends(parts)
    sums = mp_total(stats)
    mine0, arrived0 = weight_gradient(saved0[0], dcat0, in_half, section)
    red_in0 = sum_blocks(block_sends(in_block(mine0, arrived0), "dp"))
    red_out1, red_in1, red_out0 = sum_blocks(out_blocks1), sum_blocks(in_blocks1), sum_blocks(out_blocks0)
    d_normed = kept + sent[0].astype(F32) + sent[1].astype(F32) + sent[2].astype(F32)
    d_input = norm_backward(g0, d_normed, sums, all0[1:3], weights0[0][0])
    small0 = small_gradients(d_normed, all0[1:3], dmix0, fsum0)

    def to_owner(first, second, axis):
        mine, other = both(first, second)
        arrived = swap(other, "section", 1)
        return jnp.where(is_first, jnp.concatenate([mine, arrived], axis), jnp.concatenate([arrived, mine], axis)).astype(F32)

    grads_in = to_owner(red_in0, red_in1, 1)
    grads_out = to_owner(red_out0, red_out1, 0)
    small_mine, small_send = both(small0, small1)
    small_sum = dp_total(small_mine + swap(small_send, "section", 1))
    feat_grad = small_sum[2 * shard_width:2 * shard_width + LANES].reshape(heads, HEAD) / feat_weight[0]
    freq_grad = jnp.einsum("nk,hnm->hkm", table, small_sum[2 * shard_width + LANES:].reshape(heads, HEAD, HEAD),
                           precision=lax.Precision.HIGHEST)
    keep, send = both(d_input, out)
    arrived = swap(send, "section", 1)
    boundary = jnp.where(is_first, jnp.stack([keep, arrived]), jnp.stack([arrived, keep]))
    qkv_grad = jnp.stack([grads_in[:, t * shard_width:(t + 1) * shard_width] for t in range(3)])
    return (
        boundary[None],
        small_sum[None, :shard_width],
        small_sum[None, shard_width:2 * shard_width],
        qkv_grad[None],
        grads_out[None, :shard_width],
        grads_in[None, :, 3 * shard_width:],
        grads_out[None, shard_width:],
        freq_grad[None],
        feat_grad[None],
    )


def solution(mesh):
    placed = (
        P("dp", None, "mp"), P("dp", None, "mp"), P("dp"), P("section", None), P("section", None),
        P("section", None, None, "mp"), P("section", "mp", None), P("section", None, "mp"), P("section", "mp", None),
        P("section", "mp", None, None), P("section", "mp", None),
    )
    return jax.shard_map(
        shards,
        mesh=mesh,
        in_specs=placed,
        out_specs=(
            P("section", "dp", None, "mp"), P("section", "mp"), P("section", "mp"), P("section", None, "dp", "mp"),
            P("section", "mp", "dp"), P("section", "dp", "mp"), P("section", "mp", "dp"), P("section", "mp", None, None),
            P("section", "mp", None),
        ),
        check_vma=False,
    )
```

```python
import functools
import math

import jax
import jax.numpy as jnp
from jax import lax
from jax.experimental import pallas as pl
from jax.experimental.pallas import tpu as pltpu
from jax.sharding import PartitionSpec as P

ROT = 16
TILE = 256
HEAD = 64
LANES = 256
EPS = 1e-05
F32 = jnp.float32
BF16 = jnp.bfloat16
RSQRT2 = math.sqrt(0.5)
RSQRT2PI = 1.0 / math.sqrt(2.0 * math.pi)
SAVED = 14


def dot_nn(a, b):
    return lax.dot_general(a, b, (((1,), (0,)), ((), ())), preferred_element_type=F32)


def dot_nt(a, b):
    return lax.dot_general(a, b, (((1,), (1,)), ((), ())), preferred_element_type=F32)


def dot_tn(a, b):
    return lax.dot_general(a, b, (((0,), (0,)), ((), ())), preferred_element_type=F32)


def split(values):
    high = values.astype(BF16)
    return high, (values - high.astype(F32)).astype(BF16)


def iota(shape, dim):
    return lax.broadcasted_iota(jnp.int32, shape, dim)


def partner(values):
    later = pltpu.roll(values, LANES - ROT // 2, 1)
    earlier = pltpu.roll(values, ROT // 2, 1)
    lower = iota(values.shape, 1) % HEAD < ROT // 2
    return jnp.where(lower, later, earlier)


def twice(table):
    return jnp.concatenate([table, table], axis=1)


def head_of(shape, dim):
    return iota(shape, dim) // HEAD


def weight_copies(refs, w_in, w_out, sems, which):
    qkv, up, out, down = refs
    ends = [(qkv.at[0, t], w_in.at[:, t * LANES:(t + 1) * LANES]) for t in range(3)] + [
        (up.at[0], w_in.at[:, 3 * LANES:]), (out.at[0], w_out.at[0:LANES, :]), (down.at[0], w_out.at[LANES:, :])]
    return [pltpu.make_async_copy(*ends[i], sems.at[i]) for i in which]


def start_weights(meta, mine, other, w_in, w_out, sems, order):
    def start(refs):
        for copy in weight_copies(refs, w_in, w_out, sems, order):
            copy.start()

    @pl.when(meta[1] == 1)
    def _():
        start(mine)

    @pl.when(meta[1] != 1)
    def _():
        start(other)


def wait_weights(step, refs, w_in, w_out, sems, which):
    @pl.when(step == 0)
    def _():
        for copy in weight_copies(refs, w_in, w_out, sems, which):
            copy.wait()


def forward_kernel(carried, phased, *refs):
    refs = list(refs)
    take = lambda n: [refs.pop(0) for _ in range(n)]
    meta, lens = take(2)
    p0, p1, p2, p3a, p3b, gain, bias, mix_hi, mix_lo, feat_w, cos_t, sin_t = take(12)
    mine, other = take(4), take(4)
    if carried:
        state_in, ksum_in = take(2)
        take(SAVED)
    parts = take(5 if phased else 4)
    normed, xhat, rstd, rq_o, rk_o, qf_o, kf_o, v_o, hcat, dgelu, invz, att_o, prior_s, prior_k = take(SAVED)
    state, ksum, w_in, w_out, sems = take(5)
    tile = pl.program_id(0)
    rank = meta[0]
    half = LANES // 2

    @pl.when(tile == 0)
    def _():
        start_weights(meta, mine, other, w_in, w_out, sems, (0, 1, 2, 3, 4, 5))
        if carried:
            state[...] = state_in[...]
            ksum[...] = ksum_in[...]
        else:
            state[...] = jnp.zeros_like(state)
            ksum[...] = jnp.zeros_like(ksum)

    pieces = [p0[...].astype(F32), p1[...].astype(F32), p2[...].astype(F32),
              jnp.concatenate([p3a[...], p3b[...]], axis=1).astype(F32)]
    width = 4 * LANES
    mean = jnp.sum(pieces[0] + pieces[1] + pieces[2] + pieces[3], axis=1, keepdims=True) * (1.0 / width)
    pieces = [piece - mean for piece in pieces]
    squares = sum(piece * piece for piece in pieces)
    factor = lax.rsqrt(jnp.sum(squares, axis=1, keepdims=True) * (1.0 / width) + EPS)
    for r in range(4):
        at = pl.ds(pl.multiple_of((rank ^ r) * LANES, LANES), LANES)
        hat = pieces[r] * factor
        if r == 0:
            xhat[...] = hat
        normed[:, at] = (hat * gain[:, at] + bias[:, at]).astype(BF16)
    rstd[...] = jnp.broadcast_to(factor, (TILE, half))
    tokens = normed[...]

    wait_weights(tile, mine, w_in, w_out, sems, (0, 1, 2))
    cosine, sine = twice(cos_t[...]), twice(sin_t[...])
    query = dot_nn(tokens, w_in[:, 0:LANES])
    key = dot_nn(tokens, w_in[:, LANES:2 * LANES])
    value = dot_nn(tokens, w_in[:, 2 * LANES:3 * LANES]).astype(BF16)
    rq = query * cosine + partner(query) * sine
    rk = key * cosine + partner(key) * sine
    weight = feat_w[...]

    def logits(rows):
        high, low = split(rows)
        return dot_nn(high, mix_hi[...]) + dot_nn(low, mix_hi[...]) + dot_nn(high, mix_lo[...])

    positions = lens[1] + tile * TILE + iota((TILE, LANES), 0)
    real = (positions < lens[0]).astype(F32)
    qf = (weight * jnp.exp(logits(rq))).astype(BF16)
    kf = (weight * jnp.exp(logits(rk)) * real).astype(BF16)
    rq_o[...] = rq.astype(BF16)
    rk_o[...] = rk.astype(BF16)
    qf_o[...] = qf
    kf_o[...] = kf
    v_o[...] = value

    square = (TILE, TILE)
    lower = iota(square, 0) >= iota(square, 1)
    same = head_of(square, 0) == head_of(square, 1)
    cumulative = dot_nn(lower.astype(BF16), kf) + ksum[0:1, :]
    high, low = split(qf.astype(F32) * cumulative)
    ones = same.astype(BF16)
    inverse = 1.0 / (dot_nn(high, ones) + dot_nn(low, ones))
    prior = jnp.where(same, state[...], 0.0)
    prior_hi, prior_lo = split(prior)
    numer = dot_nn(qf, prior_hi) + dot_nn(qf, prior_lo)
    lane_head = head_of((TILE, LANES), 1)
    zero = jnp.zeros((TILE, LANES), BF16)
    for h in range(LANES // HEAD):
        here = lane_head == h
        scores = dot_nt(qf, jnp.where(here, kf, zero))
        scores = jnp.where(lower, scores, 0.0).astype(BF16)
        numer = numer + dot_nn(scores, jnp.where(here, value, zero))
    prior_s[0] = prior
    prior_k[0] = ksum[...]
    state[...] = state[...] + dot_tn(kf, value)
    ksum[...] = jnp.broadcast_to(cumulative[TILE - 1:TILE, :], ksum.shape)
    invz[...] = inverse
    attended = numer * inverse
    att_o[...] = attended
    hcat[:, 0:LANES] = attended.astype(BF16)

    wait_weights(tile, mine, w_in, w_out, sems, (3,))
    for c in range(4):
        cols = slice(c * LANES, (c + 1) * LANES)
        up = dot_nn(tokens, w_in[:, (3 + c) * LANES:(4 + c) * LANES])
        cdf = 0.5 * (1.0 + lax.erf(up * RSQRT2))
        hcat[:, (1 + c) * LANES:(2 + c) * LANES] = (up * cdf).astype(BF16)
        dgelu[:, cols] = (cdf + up * (RSQRT2PI * jnp.exp(-0.5 * up * up))).astype(BF16)

    wait_weights(tile, mine, w_in, w_out, sems, (4, 5))
    hidden = hcat[...]
    emit(rank, lambda at: dot_nn(hidden, w_out[:, at]), parts)


def emit(rank, product, parts):
    half = LANES // 2
    for r in range(4):
        at = pl.ds(pl.multiple_of((rank ^ r) * LANES, LANES), LANES)
        part = product(at)
        if len(parts) == 4:
            parts[r][...] = part.astype(parts[r].dtype)
            continue
        sx, sy, k0, ka, kb = parts
        if r == 0:
            k0[...] = part
        elif r == 1:
            sx[0] = part[:, :half].astype(BF16)
            kb[...] = part[:, half:]
        elif r == 2:
            ka[...] = part[:, :half]
            sy[0] = part[:, half:].astype(BF16)
        else:
            sx[1] = part[:, :half].astype(BF16)
            sy[1] = part[:, half:].astype(BF16)


def backward_kernel(carried, phased, *refs):
    refs = list(refs)
    take = lambda n: [refs.pop(0) for _ in range(n)]
    meta, = take(1)
    grad, normed, rq, rk, qf_i, kf_i, v_i, att_i, dgelu, invz, prior_s, prior_k, gain, bias, mix_hi, cos_t, sin_t = take(17)
    mine, other = take(4), take(4)
    if carried:
        state_in, gsum_in, dmix_in, fsum_in = take(4)
        take(2)
    parts = take(5 if phased else 4)
    stats, dcat, state, gsum, dmix, fsum = take(6)
    w_in, w_out, sems = take(3)
    step = pl.program_id(0)
    rank = meta[0]

    @pl.when(step == 0)
    def _():
        start_weights(meta, mine, other, w_in, w_out, sems, (4, 5, 0, 1, 2, 3))
        if carried:
            state[...] = state_in[...]
            gsum[...] = gsum_in[...]
            dmix[...] = dmix_in[...]
            fsum[...] = fsum_in[...]
        else:
            state[...] = jnp.zeros_like(state)
            gsum[...] = jnp.zeros_like(gsum)
            dmix[...] = jnp.zeros_like(dmix)
            fsum[...] = jnp.zeros_like(fsum)

    wait_weights(step, mine, w_in, w_out, sems, (4, 5))
    g = grad[...]
    d_att = dot_nt(g, w_out[0:LANES, :]).astype(BF16).astype(F32)
    square = (TILE, TILE)
    same = head_of(square, 0) == head_of(square, 1)
    ones = same.astype(BF16)
    inverse = invz[...]
    dn = (d_att * inverse).astype(BF16)
    dn32 = dn.astype(F32)
    high, low = split(dn32 * att_i[...])
    dden = -(dot_nn(high, ones) + dot_nn(low, ones))
    den_hi = dden.astype(BF16).astype(F32)
    roll_hi = pltpu.roll(den_hi, HEAD, 1)
    roll_lo = pltpu.roll(dden - den_hi, HEAD, 1)
    qf, kf, value = qf_i[...], kf_i[...], v_i[...]
    zero = jnp.zeros((TILE, LANES), BF16)
    one = jnp.ones((TILE, LANES), BF16)
    lane = iota((TILE, LANES), 1)
    lane_head = lane // HEAD
    below = iota(square, 0) >= iota(square, 1)
    above = iota(square, 0) <= iota(square, 1)
    prior_hi, prior_lo = split(prior_s[0])
    later_hi, later_lo = split(jnp.where(same, state[...], 0.0))
    d_qf = dot_nt(dn, prior_hi) + dot_nt(dn, prior_lo) + prior_k[0, 0:1, :] * dden
    d_kf = dot_nt(value, later_hi) + dot_nt(value, later_lo) + gsum[0:1, :]
    d_v = dot_nn(kf, later_hi)
    heads = LANES // HEAD
    for h in range(heads):
        here = lane_head == h
        spare = HEAD * ((h + 1) % heads)
        left = jnp.where(lane == spare, roll_hi, jnp.where(lane == spare + 1, roll_lo, dn32)).astype(BF16)
        right = jnp.where(here, value, jnp.where((lane == spare) | (lane == spare + 1), one, zero))
        k_here = jnp.where(here, kf, zero)
        q_here = jnp.where(here, qf, zero)
        d_here = jnp.where(here, dn, zero)
        scores_t = jnp.where(above, dot_nt(k_here, qf), 0.0).astype(BF16)
        ds = jnp.where(below, dot_nt(left, right), 0.0).astype(BF16)
        ds_t = jnp.where(above, dot_nt(right, left), 0.0).astype(BF16)
        d_qf = d_qf + dot_nn(ds, k_here)
        d_kf = d_kf + dot_nn(ds_t, q_here)
        d_v = d_v + dot_nn(scores_t, d_here)
    state[...] = state[...] + dot_tn(qf, dn)
    gsum[...] = gsum[...] + jnp.sum(qf.astype(F32) * dden, axis=0, keepdims=True)
    dlq = d_qf * qf.astype(F32)
    dlk = d_kf * kf.astype(F32)
    fsum[...] = fsum[...] + jnp.sum(dlq + dlk, axis=0, keepdims=True)
    dlq, dlk = dlq.astype(BF16), dlk.astype(BF16)
    dmix[...] = dmix[...] + dot_tn(rq[...], dlq) + dot_tn(rk[...], dlk)
    cosine, sine = twice(cos_t[...]), twice(sin_t[...])
    for c, dl in ((0, dlq), (1, dlk)):
        dr = dot_nt(dl, mix_hi[...])
        dcat[:, c * LANES:(c + 1) * LANES] = (dr * cosine - partner(dr) * sine).astype(BF16)
    dcat[:, 2 * LANES:3 * LANES] = d_v.astype(BF16)
    for c in range(4):
        cols = slice(c * LANES, (c + 1) * LANES)
        d_act = dot_nt(g, w_out[(1 + c) * LANES:(2 + c) * LANES, :])
        dcat[:, (3 + c) * LANES:(4 + c) * LANES] = (d_act * dgelu[:, cols].astype(F32)).astype(BF16)
    wait_weights(step, mine, w_in, w_out, sems, (0, 1, 2, 3))
    wide = dcat[...]
    row = iota((8, LANES), 0)
    first, second = (row == 0).astype(BF16), (row == 1).astype(BF16)
    totals = []

    def product(at):
        part = dot_nt(wide, w_in[at, :])
        one_side = (part * gain[:, at]).astype(BF16)
        other = (part * (normed[:, at].astype(F32) - bias[:, at])).astype(BF16)
        totals.append(dot_nt(first, one_side) + dot_nt(second, other))
        return part

    emit(rank, product, parts)
    stats[...] = totals[0] + totals[1] + totals[2] + totals[3]


def join_kernel(meta, p0, p1, p2, p3a, p3b, whole):
    half = LANES // 2
    for r, piece in enumerate((p0, p1, p2)):
        whole[:, pl.ds(pl.multiple_of((meta[0] ^ r) * LANES, LANES), LANES)] = piece[...]
    at = pl.multiple_of((meta[0] ^ 3) * LANES, LANES)
    whole[:, pl.ds(at, half)] = p3a[...]
    whole[:, pl.ds(pl.multiple_of(at + half, half), half)] = p3b[...]


def partial_outs(rows, phased, row_of):
    half = LANES // 2
    if not phased:
        shapes = [jax.ShapeDtypeStruct((rows, LANES), F32)] + [jax.ShapeDtypeStruct((rows, LANES), BF16)] * 3
        return shapes, [pl.BlockSpec((TILE, LANES), lambda *i: (row_of(*i), 0))] * 4
    shapes = [jax.ShapeDtypeStruct((2, rows, half), BF16)] * 2 + [
        jax.ShapeDtypeStruct((rows, LANES), F32), jax.ShapeDtypeStruct((rows, half), F32),
        jax.ShapeDtypeStruct((rows, half), F32)]
    specs = [pl.BlockSpec((2, TILE, half), lambda *i: (0, row_of(*i), 0))] * 2 + [
        pl.BlockSpec((TILE, width), lambda *i: (row_of(*i), 0)) for width in (LANES, half, half)]
    return shapes, specs


def fixed(shape):
    return pl.BlockSpec(shape, lambda *i: (0,) * len(shape))


def outside(count):
    return [pl.BlockSpec(memory_space=pl.ANY)] * count


def params(axes=1):
    return pltpu.CompilerParams(dimension_semantics=("arbitrary",) * axes, vmem_limit_bytes=56 << 20)


def weight_scratch(width):
    return [pltpu.VMEM((width, 3 * LANES + width), BF16), pltpu.VMEM((LANES + width, width), BF16),
            pltpu.SemaphoreType.DMA((6,))]


def forward_layer(meta, lens, pieces, weights, tables, length, first_row, phased, carry=None):
    rows = pieces[0].shape[0]
    tiles, before = rows // TILE, first_row // TILE
    half, width = LANES // 2, 4 * LANES
    local = lambda t, *_: t
    there = lambda t, *_: before + t
    by_row = lambda n, row_of: pl.BlockSpec((TILE, n), lambda *i: (row_of(*i), 0))
    (gain, bias, mix_hi, mix_lo, feat_w), mine, other = weights
    small = (gain, bias, mix_hi, mix_lo, feat_w)
    shapes, specs = partial_outs(rows, phased, local)
    extra = [(width, BF16), (LANES, F32), (half, F32)] + [(LANES, BF16)] * 5 + [
        (LANES + width, BF16), (width, BF16), (LANES, F32), (LANES, F32)]
    shapes += [jax.ShapeDtypeStruct((length, n), d) for n, d in extra]
    specs += [by_row(n, there) for n, _ in extra]
    shapes += [jax.ShapeDtypeStruct((length // TILE, LANES, LANES), F32), jax.ShapeDtypeStruct((length // TILE, 8, LANES), F32)]
    specs += [pl.BlockSpec((1, n, LANES), lambda *i: (there(*i), 0, 0)) for n in (LANES, 8)]
    states = [(LANES, LANES), (8, LANES)]
    shapes += [jax.ShapeDtypeStruct(s, F32) for s in states]
    specs += [fixed(s) for s in states]
    operands = [meta, jnp.stack([lens[0], jnp.int32(first_row)]), *pieces, *small, *tables, *mine, *other]
    in_specs = [by_row(p.shape[1], local) for p in pieces] + [fixed(w.shape) for w in small] + [by_row(half, there)] * 2 + outside(8)
    aliases = {}
    if carry is not None:
        state, saved = carry
        operands += [*state, *saved]
        in_specs += [fixed(s) for s in states] + outside(SAVED)
        aliases = {len(operands) - SAVED + i: len(shapes) - 2 - SAVED + i for i in range(SAVED)}
    outs = pl.pallas_call(
        functools.partial(forward_kernel, carry is not None, phased),
        name="layer_forward",
        out_shape=shapes,
        grid_spec=pltpu.PrefetchScalarGridSpec(
            num_scalar_prefetch=2, grid=(tiles,), in_specs=in_specs, out_specs=specs, scratch_shapes=weight_scratch(width)),
        input_output_aliases=aliases,
        compiler_params=params(),
        cost_estimate=pl.CostEstimate(flops=rows * 20_000_000, transcendentals=rows * 5000, bytes_accessed=24 << 20),
    )(*operands)
    count = 5 if phased else 4
    return outs[:count], outs[count:count + SAVED], outs[count + SAVED:]


def backward_layer(meta, grad, saved, weights, tables, length, first_row, phased, carry=None):
    rows = grad.shape[0]
    tiles, before = rows // TILE, first_row // TILE
    half, width = LANES // 2, 4 * LANES
    local = lambda t, *_: tiles - 1 - t
    there = lambda t, *_: before + tiles - 1 - t
    by_row = lambda n, row_of=there: pl.BlockSpec((TILE, n), lambda *i: (row_of(*i), 0))
    normed, rq, rk, qf, kf, value, hcat, dgelu, invz, attended, prior_s, prior_k = saved
    (gain, bias, mix_hi, mix_lo, feat_w), mine, other = weights
    shapes, specs = partial_outs(rows, phased, local)
    shapes += [jax.ShapeDtypeStruct((8, length), F32), jax.ShapeDtypeStruct((length, 3 * LANES + width), BF16)]
    specs += [pl.BlockSpec((8, TILE), lambda *i: (0, there(*i))), by_row(3 * LANES + width)]
    states = [(LANES, LANES), (8, LANES)] * 2
    shapes += [jax.ShapeDtypeStruct(s, F32) for s in states]
    specs += [fixed(s) for s in states]
    operands = [meta, grad, normed, rq, rk, qf, kf, value, attended, dgelu, invz, prior_s, prior_k, gain, bias, mix_hi, *tables,
                *mine, *other]
    in_specs = [by_row(width, local), by_row(width)] + [by_row(LANES)] * 6 + [by_row(width), by_row(LANES)] + [
        pl.BlockSpec((1, n, LANES), lambda *i: (there(*i), 0, 0)) for n in (LANES, 8)] + [
        fixed(w.shape) for w in (gain, bias, mix_hi)] + [by_row(half)] * 2 + outside(8)
    aliases = {}
    if carry is not None:
        state, arrays = carry
        operands += [*state, *arrays]
        in_specs += [fixed(s) for s in states] + outside(2)
        aliases = {len(operands) - 2 + i: len(shapes) - 6 + i for i in range(2)}
    outs = pl.pallas_call(
        functools.partial(backward_kernel, carry is not None, phased),
        name="layer_backward",
        out_shape=shapes,
        grid_spec=pltpu.PrefetchScalarGridSpec(
            num_scalar_prefetch=1, grid=(tiles,), in_specs=in_specs, out_specs=specs, scratch_shapes=weight_scratch(width)),
        input_output_aliases=aliases,
        compiler_params=params(),
        cost_estimate=pl.CostEstimate(flops=rows * 25_000_000, transcendentals=0, bytes_accessed=24 << 20),
    )(*operands)
    count = 5 if phased else 4
    return outs[:count], outs[count:count + 2], outs[count + 2:]


def join(meta, pieces):
    rows, block = pieces[0].shape[0], 2 * TILE
    return pl.pallas_call(
        join_kernel,
        name="join",
        out_shape=jax.ShapeDtypeStruct((rows, 4 * LANES), BF16),
        grid_spec=pltpu.PrefetchScalarGridSpec(
            num_scalar_prefetch=1,
            grid=(rows // block,),
            in_specs=[pl.BlockSpec((block, p.shape[1]), lambda i, *_: (i, 0)) for p in pieces],
            out_specs=pl.BlockSpec((block, 4 * LANES), lambda i, *_: (i, 0)),
        ),
        cost_estimate=pl.CostEstimate(flops=0, transcendentals=0, bytes_accessed=rows * 16 * LANES),
    )(meta, *pieces)


def swap(value, axis, by):
    return lax.ppermute(value, axis, [(k, k ^ by) for k in range(lax.axis_size(axis))])


def gather_pieces(shard, meanwhile=()):
    half = shard.shape[1] // 2
    from_x, from_y = after((swap(shard, "mp", 1), swap(shard, "mp", 2)), *meanwhile)
    return shard, from_x, from_y, swap(from_x[:, :half], "mp", 2), swap(from_y[:, half:], "mp", 1)


def after(values, *others):
    if not others:
        return values
    return lax.optimization_barrier((values, others))[0]


def direct_sends(parts):
    return parts[0], [swap(part, "mp", r) for r, part in enumerate(parts) if r > 0]


def scatter_sum(parts, extra, meanwhile=()):
    sx, sy, k0, ka, kb = parts
    half = ka.shape[1]
    in_x, in_y = after((swap(sx, "mp", 1), swap(sy, "mp", 2)), *meanwhile)
    if extra is not None:
        extra = mp_total(after(extra, in_x, in_y))
    last_y = swap((ka + in_x[1].astype(F32)).astype(BF16), "mp", 2)
    last_x = swap((kb + in_y[1].astype(F32)).astype(BF16), "mp", 1)
    return jnp.concatenate(
        [k0[:, :half] + in_x[0].astype(F32) + last_y.astype(F32), k0[:, half:] + in_y[0].astype(F32) + last_x.astype(F32)],
        axis=1), extra


def mp_total(values):
    return values + swap(values, "mp", 1) + swap(values, "mp", 2) + swap(values, "mp", 3)


def ring_scatter(block_of, axis):
    count = lax.axis_size(axis)
    rank = lax.axis_index(axis)
    pairs = [(k, (k + 1) % count) for k in range(count)]
    total = block_of((rank + count - 1) % count)
    for step in range(2, count + 1):
        arrived = lax.ppermute(total, axis, pairs)
        total = (arrived.astype(F32) + block_of((rank + count - step) % count).astype(F32)).astype(BF16)
    return total


def dp_total(values):
    count = lax.axis_size("dp")
    if count > 8:
        return lax.psum(values, "dp")
    sent = [lax.ppermute(values, "dp", [(i, (i + k) % count) for i in range(count)]) for k in range(1, count)]
    return sum(sent, values)


def block_sends(block_of, axis):
    count = lax.axis_size(axis)
    rank = lax.axis_index(axis)
    if count > 8:
        return [ring_scatter(block_of, axis)]
    return [block_of(rank)] + [
        lax.ppermute(block_of((rank + k) % count), axis, [(i, (i + k) % count) for i in range(count)]) for k in range(1, count)]


def sum_blocks(blocks):
    total = blocks[0].astype(F32)
    for block in blocks[1:]:
        total = total + block.astype(F32)
    return total.astype(BF16)


def weight_gradient(left, right, half_of, section):
    def product(which):
        a, b = half_of(left, right, which)
        return lax.dot_general(a, b, (((0,), (0,)), ((), ())), preferred_element_type=F32).astype(BF16)

    arrived = swap(product(1 - section), "section", 1)
    return lax.optimization_barrier(product(section)), arrived


def dct_table(order):
    row_index = jnp.arange(order, dtype=F32)[:, None]
    col_index = jnp.arange(order, dtype=F32)[None, :]
    cosines = jnp.sqrt(2.0 / order) * jnp.cos(math.pi * (row_index + 0.5) * col_index / order)
    return cosines * jnp.where(col_index == 0, math.sqrt(0.5), 1.0)


def rotary_tables(length):
    column = jnp.arange(LANES // 2, dtype=jnp.int32) % HEAD
    half = ROT // 2
    index = (column % half).astype(F32)
    angles = jnp.arange(length, dtype=F32)[:, None] * (10000.0 ** (-index * 2.0 / ROT))[None, :]
    turned = (column < ROT)[None, :]
    sign = jnp.where(column < half, -1.0, 1.0)[None, :]
    return jnp.where(turned, jnp.cos(angles), 1.0), jnp.where(turned, sign * jnp.sin(angles), 0.0)


def shards(block_input, cotangent, lengths, ln_gain, ln_bias, w_qkv, w_out, w_up, w_down, freq_table, feat_weight):
    section = lax.axis_index("section")
    place = lax.axis_index("mp")
    group = lax.axis_index("dp")
    groups = lax.axis_size("dp")
    local_slots, length, shard_width = block_input.shape
    width = ln_gain.shape[1]
    heads = freq_table.shape[1]
    is_first = section == 0
    lens = lax.dynamic_slice_in_dim(lengths, section, 1, 0)
    metas = [jnp.stack([place, (section == l).astype(jnp.int32)]).astype(jnp.int32) for l in range(2)]

    def own(values):
        return lax.dynamic_index_in_dim(values, section, 0, keepdims=False)

    shard0 = own(block_input)
    pieces0 = gather_pieces(shard0)

    small = jnp.concatenate([ln_gain[0], ln_bias[0], feat_weight.reshape(-1), freq_table.astype(F32).reshape(-1)])
    small_other = swap(small, "section", 1)
    mine = (w_qkv, w_up, w_out, w_down)
    other = tuple(swap(w, "section", 1) for w in mine)

    def both(mine, other):
        return jnp.where(is_first, mine, other), jnp.where(is_first, other, mine)

    layers_small = both(small, small_other)
    table = dct_table(HEAD)
    eye = jnp.eye(heads, dtype=F32)

    def layer_weights(l):
        vec = layers_small[l]
        gain, bias = vec[:width].reshape(1, width), vec[width:2 * width].reshape(1, width)
        feat = vec[2 * width:2 * width + LANES].reshape(1, LANES)
        freq = vec[2 * width + LANES:].reshape(heads, HEAD, HEAD)
        mixed = jnp.einsum("nk,hkm->hnm", table, freq, precision=lax.Precision.HIGHEST)
        mixed = (eye[:, None, :, None] * mixed[:, :, None, :]).reshape(LANES, LANES)
        high = lax.reduce_precision(mixed, 8, 7)
        return (gain, bias, high.astype(BF16), (mixed - high).astype(BF16), feat), mine, other

    weights0, weights1 = layer_weights(0), layer_weights(1)
    tables = rotary_tables(length)

    cot = after(own(cotangent), pieces0[3], pieces0[4])
    cot_x, cot_y = swap(cot, "mp", 1), swap(cot, "mp", 2)
    part0, all0, _ = forward_layer(metas[0], lens, pieces0, weights0, tables, length, 0, True)
    part0 = after(part0, cot_x, cot_y)
    hidden = (shard0.astype(F32) + scatter_sum(part0, None)[0]).astype(BF16)
    pieces1 = gather_pieces(hidden)
    cot_x, cot_y = after((cot_x, cot_y), pieces1[3], pieces1[4])
    half = shard_width // 2
    pieces_g = cot, cot_x, cot_y, swap(cot_x[:, :half], "mp", 2), swap(cot_y[:, half:], "mp", 1)
    part1, all1, _ = forward_layer(metas[1], lens, pieces1, weights1, tables, length, 0, False)
    out_kept, out_sent = direct_sends(part1)

    def saved_of(arrays):
        return (arrays[0],) + tuple(arrays[3:])

    def in_half(left, right, which):
        n = right.shape[1] // 2
        return left, lax.dynamic_slice_in_dim(right, which * n, n, 1)

    def out_half(left, right, which):
        n = left.shape[1] // 2
        return lax.dynamic_slice_in_dim(left, which * n, n, 1), right

    def in_block(mine, arrived):
        n = mine.shape[0] // groups
        cut = lambda v, i: lax.dynamic_slice_in_dim(v, i * n, n, 0)
        return lambda i: (cut(mine, i).astype(F32) + cut(arrived, i).astype(F32)).astype(BF16)

    def out_block(mine, arrived):
        n = mine.shape[1] // groups
        cut = lambda v, i: lax.dynamic_slice_in_dim(v, i * n, n, 1)
        return lambda i: (cut(mine, i).astype(F32) + cut(arrived, i).astype(F32)).astype(BF16)

    def run_backward(meta, grad, saved, weights, phased):
        parts, (stats, dcat), (_, _, dmix, fsum) = backward_layer(meta, grad, saved, weights, tables, length, 0, phased)
        return parts, stats, dcat, dmix, fsum

    def norm_backward(grad_shard, d_normed, sums, norm, gain_all):
        xhat, rstd = norm
        gain = lax.dynamic_slice_in_dim(gain_all, place * shard_width, shard_width, 1)
        mean_d = (sums[0] * (1.0 / width))[:, None]
        mean_dx = (sums[1] * (1.0 / width))[:, None]
        return grad_shard.astype(F32) + rstd[:, :1] * (d_normed * gain - mean_d - xhat * mean_dx)

    def small_gradients(d_normed, norm, dmix, fsum):
        gain_part = jnp.sum(d_normed * norm[0], axis=0)
        bias_part = jnp.sum(d_normed, axis=0)
        diagonal = jnp.stack([dmix[h * HEAD:(h + 1) * HEAD, h * HEAD:(h + 1) * HEAD] for h in range(heads)])
        return jnp.concatenate([gain_part, bias_part, fsum[0], diagonal.reshape(-1)])

    saved1, saved0 = saved_of(all1), saved_of(all0)
    grad1 = join(metas[1], pieces_g)
    out_blocks1 = block_sends(out_block(*weight_gradient(saved1[6], grad1, out_half, section)), "dp")
    grad1_b = after(grad1, out_blocks1[0])
    parts, stats, dcat1, dmix1, fsum1 = run_backward(metas[1], grad1_b, saved1, weights1, True)
    parts, stats, dcat1, dmix1, fsum1 = after((parts, stats, dcat1, dmix1, fsum1), *out_blocks1, *out_sent)
    in_blocks1 = block_sends(in_block(*weight_gradient(saved1[0], dcat1, in_half, section)), "dp")
    d_normed, sums = scatter_sum(parts, stats, in_blocks1[:1])
    g0 = norm_backward(cot, d_normed, sums, all1[1:3], weights1[0][0]).astype(BF16)
    small1 = small_gradients(d_normed, all1[1:3], dmix1, fsum1)
    pieces_g0 = after(gather_pieces(g0, in_blocks1[1:2]), *in_blocks1[:3])
    out = hidden.astype(F32) + out_kept + out_sent[0].astype(F32) + out_sent[1].astype(F32) + out_sent[2].astype(F32)

    grad0 = join(metas[0], pieces_g0)
    mine0, arrived0 = after(weight_gradient(saved0[6], grad0, out_half, section), *in_blocks1)
    out_blocks0 = block_sends(out_block(mine0, arrived0), "dp")
    grad0_b = after(grad0, out_blocks0[0])
    parts, stats, dcat0, dmix0, fsum0 = run_backward(metas[0], grad0_b, saved0, weights0, False)
    parts, stats, dcat0, dmix0, fsum0 = after((parts, stats, dcat0, dmix0, fsum0), *out_blocks0)
    out_blocks1, in_blocks1 = after((out_blocks1, in_blocks1), dcat0)
    kept, sent = direct_sends(parts)
    sums = mp_total(stats)
    mine0, arrived0 = weight_gradient(saved0[0], dcat0, in_half, section)
    in_blocks0 = block_sends(in_block(mine0, arrived0), "dp")
    red_in0 = sum_blocks(in_blocks0)
    red_out1, red_in1, red_out0 = sum_blocks(out_blocks1), sum_blocks(in_blocks1), sum_blocks(out_blocks0)
    sent, dmix0 = after((sent, dmix0), *in_blocks0[1::2])
    d_normed = kept + sent[0].astype(F32) + sent[1].astype(F32) + sent[2].astype(F32)
    d_input = norm_backward(g0, d_normed, sums, all0[1:3], weights0[0][0])
    small0 = small_gradients(d_normed, all0[1:3], dmix0, fsum0)

    def to_owner(first, second, axis):
        mine, other = both(first, second)
        arrived = swap(other, "section", 1)
        return jnp.where(is_first, jnp.concatenate([mine, arrived], axis), jnp.concatenate([arrived, mine], axis)).astype(F32)

    grads_in = to_owner(red_in0, red_in1, 1)
    grads_out = to_owner(red_out0, red_out1, 0)
    small_mine, small_send = both(small0, small1)
    small_sum = dp_total(small_mine + swap(small_send, "section", 1))
    feat_grad = small_sum[2 * shard_width:2 * shard_width + LANES].reshape(heads, HEAD) / feat_weight[0]
    freq_grad = jnp.einsum("nk,hnm->hkm", table, small_sum[2 * shard_width + LANES:].reshape(heads, HEAD, HEAD),
                           precision=lax.Precision.HIGHEST)
    keep, send = both(d_input, out)
    arrived = swap(send, "section", 1)
    boundary = jnp.where(is_first, jnp.stack([keep, arrived]), jnp.stack([arrived, keep]))
    qkv_grad = jnp.stack([grads_in[:, t * shard_width:(t + 1) * shard_width] for t in range(3)])
    return (
        boundary[None],
        small_sum[None, :shard_width],
        small_sum[None, shard_width:2 * shard_width],
        qkv_grad[None],
        grads_out[None, :shard_width],
        grads_in[None, :, 3 * shard_width:],
        grads_out[None, shard_width:],
        freq_grad[None],
        feat_grad[None],
    )


def solution(mesh):
    placed = (
        P("dp", None, "mp"), P("dp", None, "mp"), P("dp"), P("section", None), P("section", None),
        P("section", None, None, "mp"), P("section", "mp", None), P("section", None, "mp"), P("section", "mp", None),
        P("section", "mp", None, None), P("section", "mp", None),
    )
    return jax.shard_map(
        shards,
        mesh=mesh,
        in_specs=placed,
        out_specs=(
            P("section", "dp", None, "mp"), P("section", "mp"), P("section", "mp"), P("section", None, "dp", "mp"),
            P("section", "mp", "dp"), P("section", "dp", "mp"), P("section", "mp", "dp"), P("section", "mp", None, None),
            P("section", "mp", None),
        ),
        check_vma=False,
    )
```

```python
import functools
import math

import jax
import jax.numpy as jnp
from jax import lax
from jax.experimental import pallas as pl
from jax.experimental.pallas import tpu as pltpu
from jax.sharding import PartitionSpec as P

ROT = 16
TILE = 256
HEAD = 64
LANES = 256
EPS = 1e-05
F32 = jnp.float32
BF16 = jnp.bfloat16
RSQRT2 = math.sqrt(0.5)
RSQRT2PI = 1.0 / math.sqrt(2.0 * math.pi)
SAVED = 14


def dot_nn(a, b):
    return lax.dot_general(a, b, (((1,), (0,)), ((), ())), preferred_element_type=F32)


def dot_nt(a, b):
    return lax.dot_general(a, b, (((1,), (1,)), ((), ())), preferred_element_type=F32)


def dot_tn(a, b):
    return lax.dot_general(a, b, (((0,), (0,)), ((), ())), preferred_element_type=F32)


def split(values):
    high = values.astype(BF16)
    return high, (values - high.astype(F32)).astype(BF16)


def iota(shape, dim):
    return lax.broadcasted_iota(jnp.int32, shape, dim)


def partner(values):
    later = pltpu.roll(values, LANES - ROT // 2, 1)
    earlier = pltpu.roll(values, ROT // 2, 1)
    lower = iota(values.shape, 1) % HEAD < ROT // 2
    return jnp.where(lower, later, earlier)


def twice(table):
    return jnp.concatenate([table, table], axis=1)


def head_of(shape, dim):
    return iota(shape, dim) // HEAD


def weight_copies(refs, w_in, w_out, sems, which):
    qkv, up, out, down = refs
    ends = [(qkv.at[0, t], w_in.at[:, t * LANES:(t + 1) * LANES]) for t in range(3)] + [
        (up.at[0], w_in.at[:, 3 * LANES:]), (out.at[0], w_out.at[0:LANES, :]), (down.at[0], w_out.at[LANES:, :])]
    return [pltpu.make_async_copy(*ends[i], sems.at[i]) for i in which]


def start_weights(meta, mine, other, w_in, w_out, sems, order):
    def start(refs):
        for copy in weight_copies(refs, w_in, w_out, sems, order):
            copy.start()

    @pl.when(meta[1] == 1)
    def _():
        start(mine)

    @pl.when(meta[1] != 1)
    def _():
        start(other)


def wait_weights(step, refs, w_in, w_out, sems, which):
    @pl.when(step == 0)
    def _():
        for copy in weight_copies(refs, w_in, w_out, sems, which):
            copy.wait()


def forward_kernel(carried, phased, *refs):
    refs = list(refs)
    take = lambda n: [refs.pop(0) for _ in range(n)]
    meta, lens = take(2)
    p0, p1, p2, p3a, p3b, gain, bias, mix_hi, mix_lo, feat_w, cos_t, sin_t = take(12)
    mine, other = take(4), take(4)
    if carried:
        state_in, ksum_in = take(2)
        take(SAVED)
    parts = take(5 if phased else 4)
    normed, xhat, rstd, rq_o, rk_o, qf_o, kf_o, v_o, hcat, dgelu, invz, att_o, prior_s, prior_k = take(SAVED)
    state, ksum, w_in, w_out, sems = take(5)
    tile = pl.program_id(0)
    rank = meta[0]
    half = LANES // 2

    @pl.when(tile == 0)
    def _():
        start_weights(meta, mine, other, w_in, w_out, sems, (0, 1, 2, 3, 4, 5))
        if carried:
            state[...] = state_in[...]
            ksum[...] = ksum_in[...]
        else:
            state[...] = jnp.zeros_like(state)
            ksum[...] = jnp.zeros_like(ksum)

    pieces = [p0[...].astype(F32), p1[...].astype(F32), p2[...].astype(F32),
              jnp.concatenate([p3a[...], p3b[...]], axis=1).astype(F32)]
    width = 4 * LANES
    mean = jnp.sum(pieces[0] + pieces[1] + pieces[2] + pieces[3], axis=1, keepdims=True) * (1.0 / width)
    pieces = [piece - mean for piece in pieces]
    squares = sum(piece * piece for piece in pieces)
    factor = lax.rsqrt(jnp.sum(squares, axis=1, keepdims=True) * (1.0 / width) + EPS)
    for r in range(4):
        at = pl.ds(pl.multiple_of((rank ^ r) * LANES, LANES), LANES)
        hat = pieces[r] * factor
        if r == 0:
            xhat[...] = hat
        normed[:, at] = (hat * gain[:, at] + bias[:, at]).astype(BF16)
    rstd[...] = jnp.broadcast_to(factor, (TILE, half))
    tokens = normed[...]

    wait_weights(tile, mine, w_in, w_out, sems, (0, 1, 2))
    cosine, sine = twice(cos_t[...]), twice(sin_t[...])
    query = dot_nn(tokens, w_in[:, 0:LANES])
    key = dot_nn(tokens, w_in[:, LANES:2 * LANES])
    value = dot_nn(tokens, w_in[:, 2 * LANES:3 * LANES]).astype(BF16)
    rq = query * cosine + partner(query) * sine
    rk = key * cosine + partner(key) * sine
    weight = feat_w[...]

    def logits(rows):
        high, low = split(rows)
        return dot_nn(high, mix_hi[...]) + dot_nn(low, mix_hi[...]) + dot_nn(high, mix_lo[...])

    positions = lens[1] + tile * TILE + iota((TILE, LANES), 0)
    real = (positions < lens[0]).astype(F32)
    qf = (weight * jnp.exp(logits(rq))).astype(BF16)
    kf = (weight * jnp.exp(logits(rk)) * real).astype(BF16)
    rq_o[...] = rq.astype(BF16)
    rk_o[...] = rk.astype(BF16)
    qf_o[...] = qf
    kf_o[...] = kf
    v_o[...] = value

    square = (TILE, TILE)
    lower = iota(square, 0) >= iota(square, 1)
    same = head_of(square, 0) == head_of(square, 1)
    cumulative = dot_nn(lower.astype(BF16), kf) + ksum[0:1, :]
    high, low = split(qf.astype(F32) * cumulative)
    ones = same.astype(BF16)
    inverse = 1.0 / (dot_nn(high, ones) + dot_nn(low, ones))
    prior = jnp.where(same, state[...], 0.0)
    prior_hi, prior_lo = split(prior)
    numer = dot_nn(qf, prior_hi) + dot_nn(qf, prior_lo)
    lane_head = head_of((TILE, LANES), 1)
    zero = jnp.zeros((TILE, LANES), BF16)
    for h in range(LANES // HEAD):
        here = lane_head == h
        scores = dot_nt(qf, jnp.where(here, kf, zero))
        scores = jnp.where(lower, scores, 0.0).astype(BF16)
        numer = numer + dot_nn(scores, jnp.where(here, value, zero))
    prior_s[0] = prior
    prior_k[0] = ksum[...]
    state[...] = state[...] + dot_tn(kf, value)
    ksum[...] = jnp.broadcast_to(cumulative[TILE - 1:TILE, :], ksum.shape)
    invz[...] = inverse
    attended = numer * inverse
    att_o[...] = attended
    hcat[:, 0:LANES] = attended.astype(BF16)

    wait_weights(tile, mine, w_in, w_out, sems, (3,))
    for c in range(4):
        cols = slice(c * LANES, (c + 1) * LANES)
        up = dot_nn(tokens, w_in[:, (3 + c) * LANES:(4 + c) * LANES])
        cdf = 0.5 * (1.0 + lax.erf(up * RSQRT2))
        hcat[:, (1 + c) * LANES:(2 + c) * LANES] = (up * cdf).astype(BF16)
        dgelu[:, cols] = (cdf + up * (RSQRT2PI * jnp.exp(-0.5 * up * up))).astype(BF16)

    wait_weights(tile, mine, w_in, w_out, sems, (4, 5))
    hidden = hcat[...]
    emit(rank, lambda at: dot_nn(hidden, w_out[:, at]), parts)


def emit(rank, product, parts):
    half = LANES // 2
    for r in range(4):
        at = pl.ds(pl.multiple_of((rank ^ r) * LANES, LANES), LANES)
        part = product(at)
        if len(parts) == 4:
            parts[r][...] = part.astype(parts[r].dtype)
            continue
        sx, sy, k0, ka, kb = parts
        if r == 0:
            k0[...] = part
        elif r == 1:
            sx[0] = part[:, :half].astype(BF16)
            kb[...] = part[:, half:]
        elif r == 2:
            ka[...] = part[:, :half]
            sy[0] = part[:, half:].astype(BF16)
        else:
            sx[1] = part[:, :half].astype(BF16)
            sy[1] = part[:, half:].astype(BF16)


def backward_kernel(carried, phased, *refs):
    refs = list(refs)
    take = lambda n: [refs.pop(0) for _ in range(n)]
    meta, = take(1)
    grad, normed, rq, rk, qf_i, kf_i, v_i, att_i, dgelu, invz, prior_s, prior_k, gain, bias, mix_hi, cos_t, sin_t = take(17)
    mine, other = take(4), take(4)
    if carried:
        state_in, gsum_in, dmix_in, fsum_in = take(4)
        take(2)
    parts = take(5 if phased else 4)
    stats, dcat, state, gsum, dmix, fsum = take(6)
    w_in, w_out, sems = take(3)
    step = pl.program_id(0)
    rank = meta[0]

    @pl.when(step == 0)
    def _():
        start_weights(meta, mine, other, w_in, w_out, sems, (4, 5, 0, 1, 2, 3))
        if carried:
            state[...] = state_in[...]
            gsum[...] = gsum_in[...]
            dmix[...] = dmix_in[...]
            fsum[...] = fsum_in[...]
        else:
            state[...] = jnp.zeros_like(state)
            gsum[...] = jnp.zeros_like(gsum)
            dmix[...] = jnp.zeros_like(dmix)
            fsum[...] = jnp.zeros_like(fsum)

    wait_weights(step, mine, w_in, w_out, sems, (4, 5))
    g = grad[...]
    d_att = dot_nt(g, w_out[0:LANES, :]).astype(BF16).astype(F32)
    square = (TILE, TILE)
    same = head_of(square, 0) == head_of(square, 1)
    ones = same.astype(BF16)
    inverse = invz[...]
    dn = (d_att * inverse).astype(BF16)
    dn32 = dn.astype(F32)
    high, low = split(dn32 * att_i[...])
    dden = -(dot_nn(high, ones) + dot_nn(low, ones))
    den_hi = dden.astype(BF16).astype(F32)
    roll_hi = pltpu.roll(den_hi, HEAD, 1)
    roll_lo = pltpu.roll(dden - den_hi, HEAD, 1)
    qf, kf, value = qf_i[...], kf_i[...], v_i[...]
    zero = jnp.zeros((TILE, LANES), BF16)
    one = jnp.ones((TILE, LANES), BF16)
    lane = iota((TILE, LANES), 1)
    lane_head = lane // HEAD
    below = iota(square, 0) >= iota(square, 1)
    above = iota(square, 0) <= iota(square, 1)
    prior_hi, prior_lo = split(prior_s[0])
    later_hi, later_lo = split(jnp.where(same, state[...], 0.0))
    d_qf = dot_nt(dn, prior_hi) + dot_nt(dn, prior_lo) + prior_k[0, 0:1, :] * dden
    d_kf = dot_nt(value, later_hi) + dot_nt(value, later_lo) + gsum[0:1, :]
    d_v = dot_nn(kf, later_hi)
    heads = LANES // HEAD
    for h in range(heads):
        here = lane_head == h
        spare = HEAD * ((h + 1) % heads)
        left = jnp.where(lane == spare, roll_hi, jnp.where(lane == spare + 1, roll_lo, dn32)).astype(BF16)
        right = jnp.where(here, value, jnp.where((lane == spare) | (lane == spare + 1), one, zero))
        k_here = jnp.where(here, kf, zero)
        q_here = jnp.where(here, qf, zero)
        d_here = jnp.where(here, dn, zero)
        scores_t = jnp.where(above, dot_nt(k_here, qf), 0.0).astype(BF16)
        ds = jnp.where(below, dot_nt(left, right), 0.0).astype(BF16)
        ds_t = jnp.where(above, dot_nt(right, left), 0.0).astype(BF16)
        d_qf = d_qf + dot_nn(ds, k_here)
        d_kf = d_kf + dot_nn(ds_t, q_here)
        d_v = d_v + dot_nn(scores_t, d_here)
    state[...] = state[...] + dot_tn(qf, dn)
    gsum[...] = gsum[...] + jnp.sum(qf.astype(F32) * dden, axis=0, keepdims=True)
    dlq = d_qf * qf.astype(F32)
    dlk = d_kf * kf.astype(F32)
    fsum[...] = fsum[...] + jnp.sum(dlq + dlk, axis=0, keepdims=True)
    dlq, dlk = dlq.astype(BF16), dlk.astype(BF16)
    dmix[...] = dmix[...] + dot_tn(rq[...], dlq) + dot_tn(rk[...], dlk)
    cosine, sine = twice(cos_t[...]), twice(sin_t[...])
    for c, dl in ((0, dlq), (1, dlk)):
        dr = dot_nt(dl, mix_hi[...])
        dcat[:, c * LANES:(c + 1) * LANES] = (dr * cosine - partner(dr) * sine).astype(BF16)
    dcat[:, 2 * LANES:3 * LANES] = d_v.astype(BF16)
    for c in range(4):
        cols = slice(c * LANES, (c + 1) * LANES)
        d_act = dot_nt(g, w_out[(1 + c) * LANES:(2 + c) * LANES, :])
        dcat[:, (3 + c) * LANES:(4 + c) * LANES] = (d_act * dgelu[:, cols].astype(F32)).astype(BF16)
    wait_weights(step, mine, w_in, w_out, sems, (0, 1, 2, 3))
    wide = dcat[...]
    row = iota((8, LANES), 0)
    first, second = (row == 0).astype(BF16), (row == 1).astype(BF16)
    totals = []

    def product(at):
        part = dot_nt(wide, w_in[at, :])
        one_side = (part * gain[:, at]).astype(BF16)
        other = (part * (normed[:, at].astype(F32) - bias[:, at])).astype(BF16)
        totals.append(dot_nt(first, one_side) + dot_nt(second, other))
        return part

    emit(rank, product, parts)
    stats[...] = totals[0] + totals[1] + totals[2] + totals[3]


def join_kernel(meta, p0, p1, p2, p3a, p3b, whole):
    half = LANES // 2
    for r, piece in enumerate((p0, p1, p2)):
        whole[:, pl.ds(pl.multiple_of((meta[0] ^ r) * LANES, LANES), LANES)] = piece[...]
    at = pl.multiple_of((meta[0] ^ 3) * LANES, LANES)
    whole[:, pl.ds(at, half)] = p3a[...]
    whole[:, pl.ds(pl.multiple_of(at + half, half), half)] = p3b[...]


def partial_outs(rows, phased, row_of):
    half = LANES // 2
    if not phased:
        shapes = [jax.ShapeDtypeStruct((rows, LANES), F32)] + [jax.ShapeDtypeStruct((rows, LANES), BF16)] * 3
        return shapes, [pl.BlockSpec((TILE, LANES), lambda *i: (row_of(*i), 0))] * 4
    shapes = [jax.ShapeDtypeStruct((2, rows, half), BF16)] * 2 + [
        jax.ShapeDtypeStruct((rows, LANES), F32), jax.ShapeDtypeStruct((rows, half), F32),
        jax.ShapeDtypeStruct((rows, half), F32)]
    specs = [pl.BlockSpec((2, TILE, half), lambda *i: (0, row_of(*i), 0))] * 2 + [
        pl.BlockSpec((TILE, width), lambda *i: (row_of(*i), 0)) for width in (LANES, half, half)]
    return shapes, specs


def fixed(shape):
    return pl.BlockSpec(shape, lambda *i: (0,) * len(shape))


def outside(count):
    return [pl.BlockSpec(memory_space=pl.ANY)] * count


def params(axes=1):
    return pltpu.CompilerParams(dimension_semantics=("arbitrary",) * axes, vmem_limit_bytes=56 << 20)


def weight_scratch(width):
    return [pltpu.VMEM((width, 3 * LANES + width), BF16), pltpu.VMEM((LANES + width, width), BF16),
            pltpu.SemaphoreType.DMA((6,))]


def forward_layer(meta, lens, pieces, weights, tables, length, first_row, phased, carry=None):
    rows = pieces[0].shape[0]
    tiles, before = rows // TILE, first_row // TILE
    half, width = LANES // 2, 4 * LANES
    local = lambda t, *_: t
    there = lambda t, *_: before + t
    by_row = lambda n, row_of: pl.BlockSpec((TILE, n), lambda *i: (row_of(*i), 0))
    (gain, bias, mix_hi, mix_lo, feat_w), mine, other = weights
    small = (gain, bias, mix_hi, mix_lo, feat_w)
    shapes, specs = partial_outs(rows, phased, local)
    extra = [(width, BF16), (LANES, F32), (half, F32)] + [(LANES, BF16)] * 5 + [
        (LANES + width, BF16), (width, BF16), (LANES, F32), (LANES, F32)]
    shapes += [jax.ShapeDtypeStruct((length, n), d) for n, d in extra]
    specs += [by_row(n, there) for n, _ in extra]
    shapes += [jax.ShapeDtypeStruct((length // TILE, LANES, LANES), F32), jax.ShapeDtypeStruct((length // TILE, 8, LANES), F32)]
    specs += [pl.BlockSpec((1, n, LANES), lambda *i: (there(*i), 0, 0)) for n in (LANES, 8)]
    states = [(LANES, LANES), (8, LANES)]
    shapes += [jax.ShapeDtypeStruct(s, F32) for s in states]
    specs += [fixed(s) for s in states]
    operands = [meta, jnp.stack([lens[0], jnp.int32(first_row)]), *pieces, *small, *tables, *mine, *other]
    in_specs = [by_row(p.shape[1], local) for p in pieces] + [fixed(w.shape) for w in small] + [by_row(half, there)] * 2 + outside(8)
    aliases = {}
    if carry is not None:
        state, saved = carry
        operands += [*state, *saved]
        in_specs += [fixed(s) for s in states] + outside(SAVED)
        aliases = {len(operands) - SAVED + i: len(shapes) - 2 - SAVED + i for i in range(SAVED)}
    outs = pl.pallas_call(
        functools.partial(forward_kernel, carry is not None, phased),
        name="layer_forward",
        out_shape=shapes,
        grid_spec=pltpu.PrefetchScalarGridSpec(
            num_scalar_prefetch=2, grid=(tiles,), in_specs=in_specs, out_specs=specs, scratch_shapes=weight_scratch(width)),
        input_output_aliases=aliases,
        compiler_params=params(),
        cost_estimate=pl.CostEstimate(flops=rows * 20_000_000, transcendentals=rows * 5000, bytes_accessed=24 << 20),
    )(*operands)
    count = 5 if phased else 4
    return outs[:count], outs[count:count + SAVED], outs[count + SAVED:]


def backward_layer(meta, grad, saved, weights, tables, length, first_row, phased, carry=None):
    rows = grad.shape[0]
    tiles, before = rows // TILE, first_row // TILE
    half, width = LANES // 2, 4 * LANES
    local = lambda t, *_: tiles - 1 - t
    there = lambda t, *_: before + tiles - 1 - t
    by_row = lambda n, row_of=there: pl.BlockSpec((TILE, n), lambda *i: (row_of(*i), 0))
    normed, rq, rk, qf, kf, value, hcat, dgelu, invz, attended, prior_s, prior_k = saved
    (gain, bias, mix_hi, mix_lo, feat_w), mine, other = weights
    shapes, specs = partial_outs(rows, phased, local)
    shapes += [jax.ShapeDtypeStruct((8, length), F32), jax.ShapeDtypeStruct((length, 3 * LANES + width), BF16)]
    specs += [pl.BlockSpec((8, TILE), lambda *i: (0, there(*i))), by_row(3 * LANES + width)]
    states = [(LANES, LANES), (8, LANES)] * 2
    shapes += [jax.ShapeDtypeStruct(s, F32) for s in states]
    specs += [fixed(s) for s in states]
    operands = [meta, grad, normed, rq, rk, qf, kf, value, attended, dgelu, invz, prior_s, prior_k, gain, bias, mix_hi, *tables,
                *mine, *other]
    in_specs = [by_row(width, local), by_row(width)] + [by_row(LANES)] * 6 + [by_row(width), by_row(LANES)] + [
        pl.BlockSpec((1, n, LANES), lambda *i: (there(*i), 0, 0)) for n in (LANES, 8)] + [
        fixed(w.shape) for w in (gain, bias, mix_hi)] + [by_row(half)] * 2 + outside(8)
    aliases = {}
    if carry is not None:
        state, arrays = carry
        operands += [*state, *arrays]
        in_specs += [fixed(s) for s in states] + outside(2)
        aliases = {len(operands) - 2 + i: len(shapes) - 6 + i for i in range(2)}
    outs = pl.pallas_call(
        functools.partial(backward_kernel, carry is not None, phased),
        name="layer_backward",
        out_shape=shapes,
        grid_spec=pltpu.PrefetchScalarGridSpec(
            num_scalar_prefetch=1, grid=(tiles,), in_specs=in_specs, out_specs=specs, scratch_shapes=weight_scratch(width)),
        input_output_aliases=aliases,
        compiler_params=params(),
        cost_estimate=pl.CostEstimate(flops=rows * 25_000_000, transcendentals=0, bytes_accessed=24 << 20),
    )(*operands)
    count = 5 if phased else 4
    return outs[:count], outs[count:count + 2], outs[count + 2:]


def join(meta, pieces):
    rows, block = pieces[0].shape[0], 2 * TILE
    return pl.pallas_call(
        join_kernel,
        name="join",
        out_shape=jax.ShapeDtypeStruct((rows, 4 * LANES), BF16),
        grid_spec=pltpu.PrefetchScalarGridSpec(
            num_scalar_prefetch=1,
            grid=(rows // block,),
            in_specs=[pl.BlockSpec((block, p.shape[1]), lambda i, *_: (i, 0)) for p in pieces],
            out_specs=pl.BlockSpec((block, 4 * LANES), lambda i, *_: (i, 0)),
        ),
        cost_estimate=pl.CostEstimate(flops=0, transcendentals=0, bytes_accessed=rows * 16 * LANES),
    )(meta, *pieces)


def swap(value, axis, by):
    return lax.ppermute(value, axis, [(k, k ^ by) for k in range(lax.axis_size(axis))])


def gather_pieces(shard, meanwhile=()):
    half = shard.shape[1] // 2
    from_x, from_y = after((swap(shard, "mp", 1), swap(shard, "mp", 2)), *meanwhile)
    return shard, from_x, from_y, swap(from_x[:, :half], "mp", 2), swap(from_y[:, half:], "mp", 1)


def after(values, *others):
    if not others:
        return values
    return lax.optimization_barrier((values, others))[0]


def direct_sends(parts):
    return parts[0], [swap(part, "mp", r) for r, part in enumerate(parts) if r > 0]


def scatter_start(parts):
    return swap(parts[0], "mp", 1), swap(parts[1], "mp", 2)


def scatter_turn(parts, arrived):
    _, _, _, ka, kb = parts
    in_x, in_y = arrived
    return (ka + in_x[1].astype(F32)).astype(BF16), (kb + in_y[1].astype(F32)).astype(BF16)


def scatter_end(parts, arrived, to_y, to_x):
    _, _, k0, ka, _ = parts
    in_x, in_y = arrived
    half = ka.shape[1]
    last_y, last_x = swap(to_y, "mp", 2), swap(to_x, "mp", 1)
    return jnp.concatenate(
        [k0[:, :half] + in_x[0].astype(F32) + last_y.astype(F32), k0[:, half:] + in_y[0].astype(F32) + last_x.astype(F32)],
        axis=1)


def scatter_sum(parts):
    arrived = scatter_start(parts)
    return scatter_end(parts, arrived, *scatter_turn(parts, arrived))


def mp_total(values):
    return values + swap(values, "mp", 1) + swap(values, "mp", 2) + swap(values, "mp", 3)


def ring_scatter(block_of, axis):
    count = lax.axis_size(axis)
    rank = lax.axis_index(axis)
    pairs = [(k, (k + 1) % count) for k in range(count)]
    total = block_of((rank + count - 1) % count)
    for step in range(2, count + 1):
        arrived = lax.ppermute(total, axis, pairs)
        total = (arrived.astype(F32) + block_of((rank + count - step) % count).astype(F32)).astype(BF16)
    return total


def dp_total(values):
    count = lax.axis_size("dp")
    if count > 8:
        return lax.psum(values, "dp")
    sent = [lax.ppermute(values, "dp", [(i, (i + k) % count) for i in range(count)]) for k in range(1, count)]
    return sum(sent, values)


def block_sends(block_of, axis):
    count = lax.axis_size(axis)
    rank = lax.axis_index(axis)
    if count > 8:
        return [ring_scatter(block_of, axis)]
    return [block_of(rank)] + [
        lax.ppermute(block_of((rank + k) % count), axis, [(i, (i + k) % count) for i in range(count)]) for k in range(1, count)]


def sum_blocks(blocks):
    total = blocks[0].astype(F32)
    for block in blocks[1:]:
        total = total + block.astype(F32)
    return total.astype(BF16)


def weight_gradient(left, right, half_of, section, *before_own):
    def product(which, *before):
        a, b = half_of(left, after(right, *before), which)
        return lax.dot_general(a, b, (((0,), (0,)), ((), ())), preferred_element_type=F32).astype(BF16)

    arrived = swap(product(1 - section), "section", 1)
    return lax.optimization_barrier(product(section, *before_own)), arrived


def dct_table(order):
    row_index = jnp.arange(order, dtype=F32)[:, None]
    col_index = jnp.arange(order, dtype=F32)[None, :]
    cosines = jnp.sqrt(2.0 / order) * jnp.cos(math.pi * (row_index + 0.5) * col_index / order)
    return cosines * jnp.where(col_index == 0, math.sqrt(0.5), 1.0)


def rotary_tables(length):
    column = jnp.arange(LANES // 2, dtype=jnp.int32) % HEAD
    half = ROT // 2
    index = (column % half).astype(F32)
    angles = jnp.arange(length, dtype=F32)[:, None] * (10000.0 ** (-index * 2.0 / ROT))[None, :]
    turned = (column < ROT)[None, :]
    sign = jnp.where(column < half, -1.0, 1.0)[None, :]
    return jnp.where(turned, jnp.cos(angles), 1.0), jnp.where(turned, sign * jnp.sin(angles), 0.0)


def shards(block_input, cotangent, lengths, ln_gain, ln_bias, w_qkv, w_out, w_up, w_down, freq_table, feat_weight):
    section = lax.axis_index("section")
    place = lax.axis_index("mp")
    group = lax.axis_index("dp")
    groups = lax.axis_size("dp")
    local_slots, length, shard_width = block_input.shape
    width = ln_gain.shape[1]
    heads = freq_table.shape[1]
    is_first = section == 0
    lens = lax.dynamic_slice_in_dim(lengths, section, 1, 0)
    metas = [jnp.stack([place, (section == l).astype(jnp.int32)]).astype(jnp.int32) for l in range(2)]

    def own(values):
        return lax.dynamic_index_in_dim(values, section, 0, keepdims=False)

    shard0 = own(block_input)
    pieces0 = gather_pieces(shard0)

    small = jnp.concatenate([ln_gain[0], ln_bias[0], feat_weight.reshape(-1), freq_table.astype(F32).reshape(-1)])
    small_other = swap(small, "section", 1)
    mine = (w_qkv, w_up, w_out, w_down)
    other = tuple(swap(w, "section", 1) for w in mine)

    def both(mine, other):
        return jnp.where(is_first, mine, other), jnp.where(is_first, other, mine)

    layers_small = both(small, small_other)
    table = dct_table(HEAD)
    eye = jnp.eye(heads, dtype=F32)

    def layer_weights(l):
        vec = layers_small[l]
        gain, bias = vec[:width].reshape(1, width), vec[width:2 * width].reshape(1, width)
        feat = vec[2 * width:2 * width + LANES].reshape(1, LANES)
        freq = vec[2 * width + LANES:].reshape(heads, HEAD, HEAD)
        mixed = jnp.einsum("nk,hkm->hnm", table, freq, precision=lax.Precision.HIGHEST)
        mixed = (eye[:, None, :, None] * mixed[:, :, None, :]).reshape(LANES, LANES)
        high = lax.reduce_precision(mixed, 8, 7)
        return (gain, bias, high.astype(BF16), (mixed - high).astype(BF16), feat), mine, other

    weights0, weights1 = layer_weights(0), layer_weights(1)
    tables = rotary_tables(length)

    cot = after(own(cotangent), pieces0[3], pieces0[4])
    cot_x, cot_y = swap(cot, "mp", 1), swap(cot, "mp", 2)
    part0, all0, _ = forward_layer(metas[0], lens, pieces0, weights0, tables, length, 0, True)
    part0 = after(part0, cot_x, cot_y)
    hidden = (shard0.astype(F32) + scatter_sum(part0)).astype(BF16)
    pieces1 = gather_pieces(hidden)
    cot_x, cot_y = after((cot_x, cot_y), pieces1[3], pieces1[4])
    half = shard_width // 2
    pieces_g = cot, cot_x, cot_y, swap(cot_x[:, :half], "mp", 2), swap(cot_y[:, half:], "mp", 1)
    part1, all1, _ = forward_layer(metas[1], lens, pieces1, weights1, tables, length, 0, False)
    out_kept, out_sent = direct_sends(part1)

    def saved_of(arrays):
        return (arrays[0],) + tuple(arrays[3:])

    def in_half(left, right, which):
        n = right.shape[1] // 2
        return left, lax.dynamic_slice_in_dim(right, which * n, n, 1)

    def out_half(left, right, which):
        n = left.shape[1] // 2
        return lax.dynamic_slice_in_dim(left, which * n, n, 1), right

    def in_block(mine, arrived):
        n = mine.shape[0] // groups
        cut = lambda v, i: lax.dynamic_slice_in_dim(v, i * n, n, 0)
        return lambda i: (cut(mine, i).astype(F32) + cut(arrived, i).astype(F32)).astype(BF16)

    def out_block(mine, arrived):
        n = mine.shape[1] // groups
        cut = lambda v, i: lax.dynamic_slice_in_dim(v, i * n, n, 1)
        return lambda i: (cut(mine, i).astype(F32) + cut(arrived, i).astype(F32)).astype(BF16)

    def run_backward(meta, grad, saved, weights, phased):
        parts, (stats, dcat), (_, _, dmix, fsum) = backward_layer(meta, grad, saved, weights, tables, length, 0, phased)
        return parts, stats, dcat, dmix, fsum

    def norm_backward(grad_shard, d_normed, sums, norm, gain_all):
        xhat, rstd = norm
        gain = lax.dynamic_slice_in_dim(gain_all, place * shard_width, shard_width, 1)
        mean_d = (sums[0] * (1.0 / width))[:, None]
        mean_dx = (sums[1] * (1.0 / width))[:, None]
        return grad_shard.astype(F32) + rstd[:, :1] * (d_normed * gain - mean_d - xhat * mean_dx)

    def small_gradients(d_normed, norm, dmix, fsum):
        gain_part = jnp.sum(d_normed * norm[0], axis=0)
        bias_part = jnp.sum(d_normed, axis=0)
        diagonal = jnp.stack([dmix[h * HEAD:(h + 1) * HEAD, h * HEAD:(h + 1) * HEAD] for h in range(heads)])
        return jnp.concatenate([gain_part, bias_part, fsum[0], diagonal.reshape(-1)])

    saved1, saved0 = saved_of(all1), saved_of(all0)
    grad1 = join(metas[1], pieces_g)
    out_blocks1 = block_sends(out_block(*weight_gradient(saved1[6], grad1, out_half, section)), "dp")
    grad1_b = after(grad1, out_blocks1[0])
    parts, stats, dcat1, dmix1, fsum1 = run_backward(metas[1], grad1_b, saved1, weights1, True)
    parts, stats, dcat1, dmix1, fsum1 = after((parts, stats, dcat1, dmix1, fsum1), *out_blocks1, *out_sent)
    arrived = scatter_start(parts)
    turn = scatter_turn(parts, arrived)
    sums = mp_total(after(stats, *turn))
    dcat1 = after(dcat1, *turn)
    in_blocks1 = block_sends(in_block(*weight_gradient(saved1[0], dcat1, in_half, section)), "dp")
    d_normed = scatter_end(parts, arrived, *turn)
    g0 = norm_backward(cot, d_normed, sums, all1[1:3], weights1[0][0]).astype(BF16)
    small1 = small_gradients(d_normed, all1[1:3], dmix1, fsum1)
    pieces_g0 = after(gather_pieces(after(g0, *in_blocks1[:2])), *in_blocks1[:3])
    out = hidden.astype(F32) + out_kept + out_sent[0].astype(F32) + out_sent[1].astype(F32) + out_sent[2].astype(F32)

    grad0 = join(metas[0], pieces_g0)
    mine0, arrived0 = after(weight_gradient(saved0[6], grad0, out_half, section), *in_blocks1)
    out_blocks0 = block_sends(out_block(mine0, arrived0), "dp")
    grad0_b = after(grad0, out_blocks0[0])
    parts, stats, dcat0, dmix0, fsum0 = run_backward(metas[0], grad0_b, saved0, weights0, False)
    parts, stats, dcat0, dmix0, fsum0 = after((parts, stats, dcat0, dmix0, fsum0), *out_blocks0)
    out_blocks1, in_blocks1 = after((out_blocks1, in_blocks1), dcat0)
    kept, sent = direct_sends(parts)
    sums = mp_total(stats)
    mine0, arrived0 = weight_gradient(saved0[0], dcat0, in_half, section)
    in_blocks0 = block_sends(in_block(mine0, arrived0), "dp")
    sent, dmix0, out_blocks0, out_blocks1, in_blocks1 = after((sent, dmix0, out_blocks0, out_blocks1, in_blocks1), *in_blocks0[:2])
    d_normed = kept + sent[0].astype(F32) + sent[1].astype(F32) + sent[2].astype(F32)
    d_input = norm_backward(g0, d_normed, sums, all0[1:3], weights0[0][0])
    small0 = small_gradients(d_normed, all0[1:3], dmix0, fsum0)

    def to_owner(first, second, axis):
        mine, other = both(first, second)
        arrived = swap(other, "section", 1)
        return jnp.where(is_first, jnp.concatenate([mine, arrived], axis), jnp.concatenate([arrived, mine], axis)).astype(F32)

    grads_out = to_owner(sum_blocks(out_blocks0), sum_blocks(out_blocks1), 0)
    red_in1 = sum_blocks(in_blocks1)
    small_mine, small_send = both(small0, small1)
    small_sum = dp_total(small_mine + swap(small_send, "section", 1))
    feat_grad = small_sum[2 * shard_width:2 * shard_width + LANES].reshape(heads, HEAD) / feat_weight[0]
    freq_grad = jnp.einsum("nk,hnm->hkm", table, small_sum[2 * shard_width + LANES:].reshape(heads, HEAD, HEAD),
                           precision=lax.Precision.HIGHEST)
    keep, send = both(d_input, out)
    arrived = swap(send, "section", 1)
    boundary = jnp.where(is_first, jnp.stack([keep, arrived]), jnp.stack([arrived, keep]))
    in_blocks0 = after(in_blocks0, grads_out, small_sum, boundary, red_in1)
    grads_in = to_owner(sum_blocks(in_blocks0), red_in1, 1)
    qkv_grad = jnp.stack([grads_in[:, t * shard_width:(t + 1) * shard_width] for t in range(3)])
    return (
        boundary[None],
        small_sum[None, :shard_width],
        small_sum[None, shard_width:2 * shard_width],
        qkv_grad[None],
        grads_out[None, :shard_width],
        grads_in[None, :, 3 * shard_width:],
        grads_out[None, shard_width:],
        freq_grad[None],
        feat_grad[None],
    )


def solution(mesh):
    placed = (
        P("dp", None, "mp"), P("dp", None, "mp"), P("dp"), P("section", None), P("section", None),
        P("section", None, None, "mp"), P("section", "mp", None), P("section", None, "mp"), P("section", "mp", None),
        P("section", "mp", None, None), P("section", "mp", None),
    )
    return jax.shard_map(
        shards,
        mesh=mesh,
        in_specs=placed,
        out_specs=(
            P("section", "dp", None, "mp"), P("section", "mp"), P("section", "mp"), P("section", None, "dp", "mp"),
            P("section", "mp", "dp"), P("section", "dp", "mp"), P("section", "mp", "dp"), P("section", "mp", None, None),
            P("section", "mp", None),
        ),
        check_vma=False,
    )
```

```python
import functools
import math

import jax
import jax.numpy as jnp
from jax import lax
from jax.experimental import pallas as pl
from jax.experimental.pallas import tpu as pltpu
from jax.sharding import PartitionSpec as P

ROT = 16
TILE = 256
HEAD = 64
LANES = 256
EPS = 1e-05
F32 = jnp.float32
BF16 = jnp.bfloat16
RSQRT2 = math.sqrt(0.5)
RSQRT2PI = 1.0 / math.sqrt(2.0 * math.pi)
SAVED = 14


def dot_nn(a, b):
    return lax.dot_general(a, b, (((1,), (0,)), ((), ())), preferred_element_type=F32)


def dot_nt(a, b):
    return lax.dot_general(a, b, (((1,), (1,)), ((), ())), preferred_element_type=F32)


def dot_tn(a, b):
    return lax.dot_general(a, b, (((0,), (0,)), ((), ())), preferred_element_type=F32)


def split(values):
    high = values.astype(BF16)
    return high, (values - high.astype(F32)).astype(BF16)


def iota(shape, dim):
    return lax.broadcasted_iota(jnp.int32, shape, dim)


def partner(values):
    later = pltpu.roll(values, LANES - ROT // 2, 1)
    earlier = pltpu.roll(values, ROT // 2, 1)
    lower = iota(values.shape, 1) % HEAD < ROT // 2
    return jnp.where(lower, later, earlier)


def twice(table):
    return jnp.concatenate([table, table], axis=1)


def head_of(shape, dim):
    return iota(shape, dim) // HEAD


def weight_copies(refs, w_in, w_out, sems, which):
    qkv, up, out, down = refs
    ends = [(qkv.at[0, t], w_in.at[:, t * LANES:(t + 1) * LANES]) for t in range(3)] + [
        (up.at[0], w_in.at[:, 3 * LANES:]), (out.at[0], w_out.at[0:LANES, :]), (down.at[0], w_out.at[LANES:, :])]
    return [pltpu.make_async_copy(*ends[i], sems.at[i]) for i in which]


def start_weights(meta, mine, other, w_in, w_out, sems, order):
    def start(refs):
        for copy in weight_copies(refs, w_in, w_out, sems, order):
            copy.start()

    @pl.when(meta[1] == 1)
    def _():
        start(mine)

    @pl.when(meta[1] != 1)
    def _():
        start(other)


def wait_weights(step, refs, w_in, w_out, sems, which):
    @pl.when(step == 0)
    def _():
        for copy in weight_copies(refs, w_in, w_out, sems, which):
            copy.wait()


def forward_kernel(carried, phased, *refs):
    refs = list(refs)
    take = lambda n: [refs.pop(0) for _ in range(n)]
    meta, lens = take(2)
    p0, p1, p2, p3a, p3b, gain, bias, mix_hi, mix_lo, feat_w, cos_t, sin_t = take(12)
    mine, other = take(4), take(4)
    if carried:
        state_in, ksum_in = take(2)
        take(SAVED)
    parts = take(5 if phased else 4)
    normed, xhat, rstd, rq_o, rk_o, qf_o, kf_o, v_o, hcat, dgelu, invz, att_o, prior_s, prior_k = take(SAVED)
    state, ksum, w_in, w_out, sems = take(5)
    tile = pl.program_id(0)
    rank = meta[0]
    half = LANES // 2

    @pl.when(tile == 0)
    def _():
        start_weights(meta, mine, other, w_in, w_out, sems, (0, 1, 2, 3, 4, 5))
        if carried:
            state[...] = state_in[...]
            ksum[...] = ksum_in[...]
        else:
            state[...] = jnp.zeros_like(state)
            ksum[...] = jnp.zeros_like(ksum)

    pieces = [p0[...].astype(F32), p1[...].astype(F32), p2[...].astype(F32),
              jnp.concatenate([p3a[...], p3b[...]], axis=1).astype(F32)]
    width = 4 * LANES
    mean = jnp.sum(pieces[0] + pieces[1] + pieces[2] + pieces[3], axis=1, keepdims=True) * (1.0 / width)
    pieces = [piece - mean for piece in pieces]
    squares = sum(piece * piece for piece in pieces)
    factor = lax.rsqrt(jnp.sum(squares, axis=1, keepdims=True) * (1.0 / width) + EPS)
    for r in range(4):
        at = pl.ds(pl.multiple_of((rank ^ r) * LANES, LANES), LANES)
        hat = pieces[r] * factor
        if r == 0:
            xhat[...] = hat
        normed[:, at] = (hat * gain[:, at] + bias[:, at]).astype(BF16)
    rstd[...] = jnp.broadcast_to(factor, (TILE, half))
    tokens = normed[...]

    wait_weights(tile, mine, w_in, w_out, sems, (0, 1, 2))
    cosine, sine = twice(cos_t[...]), twice(sin_t[...])
    query = dot_nn(tokens, w_in[:, 0:LANES])
    key = dot_nn(tokens, w_in[:, LANES:2 * LANES])
    value = dot_nn(tokens, w_in[:, 2 * LANES:3 * LANES]).astype(BF16)
    rq = query * cosine + partner(query) * sine
    rk = key * cosine + partner(key) * sine
    weight = feat_w[...]

    def logits(rows):
        high, low = split(rows)
        return dot_nn(high, mix_hi[...]) + dot_nn(low, mix_hi[...]) + dot_nn(high, mix_lo[...])

    positions = lens[1] + tile * TILE + iota((TILE, LANES), 0)
    real = (positions < lens[0]).astype(F32)
    qf = (weight * jnp.exp(logits(rq))).astype(BF16)
    kf = (weight * jnp.exp(logits(rk)) * real).astype(BF16)
    rq_o[...] = rq.astype(BF16)
    rk_o[...] = rk.astype(BF16)
    qf_o[...] = qf
    kf_o[...] = kf
    v_o[...] = value

    square = (TILE, TILE)
    lower = iota(square, 0) >= iota(square, 1)
    same = head_of(square, 0) == head_of(square, 1)
    cumulative = dot_nn(lower.astype(BF16), kf) + ksum[0:1, :]
    high, low = split(qf.astype(F32) * cumulative)
    ones = same.astype(BF16)
    inverse = 1.0 / (dot_nn(high, ones) + dot_nn(low, ones))
    prior = jnp.where(same, state[...], 0.0)
    prior_hi, prior_lo = split(prior)
    numer = dot_nn(qf, prior_hi) + dot_nn(qf, prior_lo)
    lane_head = head_of((TILE, LANES), 1)
    zero = jnp.zeros((TILE, LANES), BF16)
    for h in range(LANES // HEAD):
        here = lane_head == h
        scores = dot_nt(qf, jnp.where(here, kf, zero))
        scores = jnp.where(lower, scores, 0.0).astype(BF16)
        numer = numer + dot_nn(scores, jnp.where(here, value, zero))
    prior_s[0] = prior
    prior_k[0] = ksum[...]
    state[...] = state[...] + dot_tn(kf, value)
    ksum[...] = jnp.broadcast_to(cumulative[TILE - 1:TILE, :], ksum.shape)
    invz[...] = inverse
    attended = numer * inverse
    att_o[...] = attended
    hcat[:, 0:LANES] = attended.astype(BF16)

    wait_weights(tile, mine, w_in, w_out, sems, (3,))
    for c in range(4):
        cols = slice(c * LANES, (c + 1) * LANES)
        up = dot_nn(tokens, w_in[:, (3 + c) * LANES:(4 + c) * LANES])
        cdf = 0.5 * (1.0 + lax.erf(up * RSQRT2))
        hcat[:, (1 + c) * LANES:(2 + c) * LANES] = (up * cdf).astype(BF16)
        dgelu[:, cols] = (cdf + up * (RSQRT2PI * jnp.exp(-0.5 * up * up))).astype(BF16)

    wait_weights(tile, mine, w_in, w_out, sems, (4, 5))
    hidden = hcat[...]
    emit(rank, lambda at: dot_nn(hidden, w_out[:, at]), parts)


def emit(rank, product, parts):
    half = LANES // 2
    for r in range(4):
        at = pl.ds(pl.multiple_of((rank ^ r) * LANES, LANES), LANES)
        part = product(at)
        if len(parts) == 4:
            parts[r][...] = part.astype(parts[r].dtype)
            continue
        sx, sy, k0, ka, kb = parts
        if r == 0:
            k0[...] = part
        elif r == 1:
            sx[0] = part[:, :half].astype(BF16)
            kb[...] = part[:, half:]
        elif r == 2:
            ka[...] = part[:, :half]
            sy[0] = part[:, half:].astype(BF16)
        else:
            sx[1] = part[:, :half].astype(BF16)
            sy[1] = part[:, half:].astype(BF16)


def backward_kernel(carried, phased, *refs):
    refs = list(refs)
    take = lambda n: [refs.pop(0) for _ in range(n)]
    meta, = take(1)
    grad, normed, rq, rk, qf_i, kf_i, v_i, att_i, dgelu, invz, prior_s, prior_k, gain, bias, mix_hi, cos_t, sin_t = take(17)
    mine, other = take(4), take(4)
    if carried:
        state_in, gsum_in, dmix_in, fsum_in = take(4)
        take(2)
    parts = take(5 if phased else 4)
    stats, dcat, state, gsum, dmix, fsum = take(6)
    w_in, w_out, sems = take(3)
    step = pl.program_id(0)
    rank = meta[0]

    @pl.when(step == 0)
    def _():
        start_weights(meta, mine, other, w_in, w_out, sems, (4, 5, 0, 1, 2, 3))
        if carried:
            state[...] = state_in[...]
            gsum[...] = gsum_in[...]
            dmix[...] = dmix_in[...]
            fsum[...] = fsum_in[...]
        else:
            state[...] = jnp.zeros_like(state)
            gsum[...] = jnp.zeros_like(gsum)
            dmix[...] = jnp.zeros_like(dmix)
            fsum[...] = jnp.zeros_like(fsum)

    wait_weights(step, mine, w_in, w_out, sems, (4, 5))
    g = grad[...]
    d_att = dot_nt(g, w_out[0:LANES, :]).astype(BF16).astype(F32)
    square = (TILE, TILE)
    same = head_of(square, 0) == head_of(square, 1)
    ones = same.astype(BF16)
    inverse = invz[...]
    dn = (d_att * inverse).astype(BF16)
    dn32 = dn.astype(F32)
    high, low = split(dn32 * att_i[...])
    dden = -(dot_nn(high, ones) + dot_nn(low, ones))
    den_hi = dden.astype(BF16).astype(F32)
    roll_hi = pltpu.roll(den_hi, HEAD, 1)
    roll_lo = pltpu.roll(dden - den_hi, HEAD, 1)
    qf, kf, value = qf_i[...], kf_i[...], v_i[...]
    zero = jnp.zeros((TILE, LANES), BF16)
    one = jnp.ones((TILE, LANES), BF16)
    lane = iota((TILE, LANES), 1)
    lane_head = lane // HEAD
    below = iota(square, 0) >= iota(square, 1)
    above = iota(square, 0) <= iota(square, 1)
    prior_hi, prior_lo = split(prior_s[0])
    later_hi, later_lo = split(jnp.where(same, state[...], 0.0))
    d_qf = dot_nt(dn, prior_hi) + dot_nt(dn, prior_lo) + prior_k[0, 0:1, :] * dden
    d_kf = dot_nt(value, later_hi) + dot_nt(value, later_lo) + gsum[0:1, :]
    d_v = dot_nn(kf, later_hi)
    heads = LANES // HEAD
    for h in range(heads):
        here = lane_head == h
        spare = HEAD * ((h + 1) % heads)
        left = jnp.where(lane == spare, roll_hi, jnp.where(lane == spare + 1, roll_lo, dn32)).astype(BF16)
        right = jnp.where(here, value, jnp.where((lane == spare) | (lane == spare + 1), one, zero))
        k_here = jnp.where(here, kf, zero)
        q_here = jnp.where(here, qf, zero)
        d_here = jnp.where(here, dn, zero)
        scores_t = jnp.where(above, dot_nt(k_here, qf), 0.0).astype(BF16)
        ds = jnp.where(below, dot_nt(left, right), 0.0).astype(BF16)
        ds_t = jnp.where(above, dot_nt(right, left), 0.0).astype(BF16)
        d_qf = d_qf + dot_nn(ds, k_here)
        d_kf = d_kf + dot_nn(ds_t, q_here)
        d_v = d_v + dot_nn(scores_t, d_here)
    state[...] = state[...] + dot_tn(qf, dn)
    gsum[...] = gsum[...] + jnp.sum(qf.astype(F32) * dden, axis=0, keepdims=True)
    dlq = d_qf * qf.astype(F32)
    dlk = d_kf * kf.astype(F32)
    fsum[...] = fsum[...] + jnp.sum(dlq + dlk, axis=0, keepdims=True)
    dlq, dlk = dlq.astype(BF16), dlk.astype(BF16)
    dmix[...] = dmix[...] + dot_tn(rq[...], dlq) + dot_tn(rk[...], dlk)
    cosine, sine = twice(cos_t[...]), twice(sin_t[...])
    for c, dl in ((0, dlq), (1, dlk)):
        dr = dot_nt(dl, mix_hi[...])
        dcat[:, c * LANES:(c + 1) * LANES] = (dr * cosine - partner(dr) * sine).astype(BF16)
    dcat[:, 2 * LANES:3 * LANES] = d_v.astype(BF16)
    for c in range(4):
        cols = slice(c * LANES, (c + 1) * LANES)
        d_act = dot_nt(g, w_out[(1 + c) * LANES:(2 + c) * LANES, :])
        dcat[:, (3 + c) * LANES:(4 + c) * LANES] = (d_act * dgelu[:, cols].astype(F32)).astype(BF16)
    wait_weights(step, mine, w_in, w_out, sems, (0, 1, 2, 3))
    wide = dcat[...]
    row = iota((8, LANES), 0)
    first, second = (row == 0).astype(BF16), (row == 1).astype(BF16)
    totals = []

    def product(at):
        part = dot_nt(wide, w_in[at, :])
        one_side = (part * gain[:, at]).astype(BF16)
        other = (part * (normed[:, at].astype(F32) - bias[:, at])).astype(BF16)
        totals.append(dot_nt(first, one_side) + dot_nt(second, other))
        return part

    emit(rank, product, parts)
    stats[...] = totals[0] + totals[1] + totals[2] + totals[3]


def product_kernel(which, left, right, out):
    out[...] = dot_tn(left[...], right[...]).astype(BF16)


def join_kernel(meta, p0, p1, p2, p3a, p3b, whole):
    half = LANES // 2
    for r, piece in enumerate((p0, p1, p2)):
        whole[:, pl.ds(pl.multiple_of((meta[0] ^ r) * LANES, LANES), LANES)] = piece[...]
    at = pl.multiple_of((meta[0] ^ 3) * LANES, LANES)
    whole[:, pl.ds(at, half)] = p3a[...]
    whole[:, pl.ds(pl.multiple_of(at + half, half), half)] = p3b[...]


def partial_outs(rows, phased, row_of):
    half = LANES // 2
    if not phased:
        shapes = [jax.ShapeDtypeStruct((rows, LANES), F32)] + [jax.ShapeDtypeStruct((rows, LANES), BF16)] * 3
        return shapes, [pl.BlockSpec((TILE, LANES), lambda *i: (row_of(*i), 0))] * 4
    shapes = [jax.ShapeDtypeStruct((2, rows, half), BF16)] * 2 + [
        jax.ShapeDtypeStruct((rows, LANES), F32), jax.ShapeDtypeStruct((rows, half), F32),
        jax.ShapeDtypeStruct((rows, half), F32)]
    specs = [pl.BlockSpec((2, TILE, half), lambda *i: (0, row_of(*i), 0))] * 2 + [
        pl.BlockSpec((TILE, width), lambda *i: (row_of(*i), 0)) for width in (LANES, half, half)]
    return shapes, specs


def fixed(shape):
    return pl.BlockSpec(shape, lambda *i: (0,) * len(shape))


def outside(count):
    return [pl.BlockSpec(memory_space=pl.ANY)] * count


def params(size):
    return pltpu.CompilerParams(dimension_semantics=("arbitrary",), vmem_limit_bytes=size << 20)


def weight_scratch(width):
    return [pltpu.VMEM((width, 3 * LANES + width), BF16), pltpu.VMEM((LANES + width, width), BF16),
            pltpu.SemaphoreType.DMA((6,))]


def forward_layer(meta, lens, pieces, weights, tables, length, first_row, phased, carry=None):
    rows = pieces[0].shape[0]
    tiles, before = rows // TILE, first_row // TILE
    half, width = LANES // 2, 4 * LANES
    local = lambda t, *_: t
    there = lambda t, *_: before + t
    by_row = lambda n, row_of: pl.BlockSpec((TILE, n), lambda *i: (row_of(*i), 0))
    (gain, bias, mix_hi, mix_lo, feat_w), mine, other = weights
    small = (gain, bias, mix_hi, mix_lo, feat_w)
    shapes, specs = partial_outs(rows, phased, local)
    extra = [(width, BF16), (LANES, F32), (half, F32)] + [(LANES, BF16)] * 5 + [
        (LANES + width, BF16), (width, BF16), (LANES, F32), (LANES, F32)]
    shapes += [jax.ShapeDtypeStruct((length, n), d) for n, d in extra]
    specs += [by_row(n, there) for n, _ in extra]
    shapes += [jax.ShapeDtypeStruct((length // TILE, LANES, LANES), F32), jax.ShapeDtypeStruct((length // TILE, 8, LANES), F32)]
    specs += [pl.BlockSpec((1, n, LANES), lambda *i: (there(*i), 0, 0)) for n in (LANES, 8)]
    states = [(LANES, LANES), (8, LANES)]
    shapes += [jax.ShapeDtypeStruct(s, F32) for s in states]
    specs += [fixed(s) for s in states]
    operands = [meta, jnp.stack([lens[0], jnp.int32(first_row)]), *pieces, *small, *tables, *mine, *other]
    in_specs = [by_row(p.shape[1], local) for p in pieces] + [fixed(w.shape) for w in small] + [by_row(half, there)] * 2 + outside(8)
    aliases = {}
    if carry is not None:
        state, saved = carry
        operands += [*state, *saved]
        in_specs += [fixed(s) for s in states] + outside(SAVED)
        aliases = {len(operands) - SAVED + i: len(shapes) - 2 - SAVED + i for i in range(SAVED)}
    outs = pl.pallas_call(
        functools.partial(forward_kernel, carry is not None, phased),
        name="layer_forward",
        out_shape=shapes,
        grid_spec=pltpu.PrefetchScalarGridSpec(
            num_scalar_prefetch=2, grid=(tiles,), in_specs=in_specs, out_specs=specs, scratch_shapes=weight_scratch(width)),
        input_output_aliases=aliases,
        compiler_params=params(32),
        cost_estimate=pl.CostEstimate(flops=rows * 20_000_000, transcendentals=rows * 5000, bytes_accessed=24 << 20),
    )(*operands)
    count = 5 if phased else 4
    return outs[:count], outs[count:count + SAVED], outs[count + SAVED:]


def backward_layer(meta, grad, saved, weights, tables, length, first_row, phased, carry=None):
    rows = grad.shape[0]
    tiles, before = rows // TILE, first_row // TILE
    half, width = LANES // 2, 4 * LANES
    local = lambda t, *_: tiles - 1 - t
    there = lambda t, *_: before + tiles - 1 - t
    by_row = lambda n, row_of=there: pl.BlockSpec((TILE, n), lambda *i: (row_of(*i), 0))
    normed, rq, rk, qf, kf, value, hcat, dgelu, invz, attended, prior_s, prior_k = saved
    (gain, bias, mix_hi, mix_lo, feat_w), mine, other = weights
    shapes, specs = partial_outs(rows, phased, local)
    shapes += [jax.ShapeDtypeStruct((8, length), F32), jax.ShapeDtypeStruct((length, 3 * LANES + width), BF16)]
    specs += [pl.BlockSpec((8, TILE), lambda *i: (0, there(*i))), by_row(3 * LANES + width)]
    states = [(LANES, LANES), (8, LANES)] * 2
    shapes += [jax.ShapeDtypeStruct(s, F32) for s in states]
    specs += [fixed(s) for s in states]
    operands = [meta, grad, normed, rq, rk, qf, kf, value, attended, dgelu, invz, prior_s, prior_k, gain, bias, mix_hi, *tables,
                *mine, *other]
    in_specs = [by_row(width, local), by_row(width)] + [by_row(LANES)] * 6 + [by_row(width), by_row(LANES)] + [
        pl.BlockSpec((1, n, LANES), lambda *i: (there(*i), 0, 0)) for n in (LANES, 8)] + [
        fixed(w.shape) for w in (gain, bias, mix_hi)] + [by_row(half)] * 2 + outside(8)
    aliases = {}
    if carry is not None:
        state, arrays = carry
        operands += [*state, *arrays]
        in_specs += [fixed(s) for s in states] + outside(2)
        aliases = {len(operands) - 2 + i: len(shapes) - 6 + i for i in range(2)}
    outs = pl.pallas_call(
        functools.partial(backward_kernel, carry is not None, phased),
        name="layer_backward",
        out_shape=shapes,
        grid_spec=pltpu.PrefetchScalarGridSpec(
            num_scalar_prefetch=1, grid=(tiles,), in_specs=in_specs, out_specs=specs, scratch_shapes=weight_scratch(width)),
        input_output_aliases=aliases,
        compiler_params=params(32),
        cost_estimate=pl.CostEstimate(flops=rows * 25_000_000, transcendentals=0, bytes_accessed=24 << 20),
    )(*operands)
    count = 5 if phased else 4
    return outs[:count], outs[count:count + 2], outs[count + 2:]


def join(meta, pieces):
    rows, block = pieces[0].shape[0], 2 * TILE
    return pl.pallas_call(
        join_kernel,
        name="join",
        out_shape=jax.ShapeDtypeStruct((rows, 4 * LANES), BF16),
        grid_spec=pltpu.PrefetchScalarGridSpec(
            num_scalar_prefetch=1,
            grid=(rows // block,),
            in_specs=[pl.BlockSpec((block, p.shape[1]), lambda i, *_: (i, 0)) for p in pieces],
            out_specs=pl.BlockSpec((block, 4 * LANES), lambda i, *_: (i, 0)),
        ),
        compiler_params=params(8),
        cost_estimate=pl.CostEstimate(flops=0, transcendentals=0, bytes_accessed=rows * 16 * LANES),
    )(meta, *pieces)


def swap(value, axis, by):
    return lax.ppermute(value, axis, [(k, k ^ by) for k in range(lax.axis_size(axis))])


def gather_pieces(shard, meanwhile=()):
    half = shard.shape[1] // 2
    from_x, from_y = after((swap(shard, "mp", 1), swap(shard, "mp", 2)), *meanwhile)
    return shard, from_x, from_y, swap(from_x[:, :half], "mp", 2), swap(from_y[:, half:], "mp", 1)


def after(values, *others):
    if not others:
        return values
    return lax.optimization_barrier((values, others))[0]


def direct_sends(parts):
    return parts[0], [swap(part, "mp", r) for r, part in enumerate(parts) if r > 0]


def scatter_start(parts):
    return swap(parts[0], "mp", 1), swap(parts[1], "mp", 2)


def scatter_turn(parts, arrived):
    _, _, _, ka, kb = parts
    in_x, in_y = arrived
    return (ka + in_x[1].astype(F32)).astype(BF16), (kb + in_y[1].astype(F32)).astype(BF16)


def scatter_end(parts, arrived, to_y, to_x):
    _, _, k0, ka, _ = parts
    in_x, in_y = arrived
    half = ka.shape[1]
    last_y, last_x = swap(to_y, "mp", 2), swap(to_x, "mp", 1)
    return jnp.concatenate(
        [k0[:, :half] + in_x[0].astype(F32) + last_y.astype(F32), k0[:, half:] + in_y[0].astype(F32) + last_x.astype(F32)],
        axis=1)


def scatter_sum(parts):
    arrived = scatter_start(parts)
    return scatter_end(parts, arrived, *scatter_turn(parts, arrived))


def mp_total(values):
    return values + swap(values, "mp", 1) + swap(values, "mp", 2) + swap(values, "mp", 3)


def ring_scatter(block_of, axis):
    count = lax.axis_size(axis)
    rank = lax.axis_index(axis)
    pairs = [(k, (k + 1) % count) for k in range(count)]
    total = block_of((rank + count - 1) % count)
    for step in range(2, count + 1):
        arrived = lax.ppermute(total, axis, pairs)
        total = (arrived.astype(F32) + block_of((rank + count - step) % count).astype(F32)).astype(BF16)
        yield arrived, total


def dp_total(values):
    count = lax.axis_size("dp")
    if count > 8:
        return lax.psum(values, "dp")
    sent = [lax.ppermute(values, "dp", [(i, (i + k) % count) for i in range(count)]) for k in range(1, count)]
    return sum(sent, values)


def block_sends(block_of, axis):
    count = lax.axis_size(axis)
    rank = lax.axis_index(axis)
    if count > 8:
        return [list(ring_scatter(block_of, axis))[-1][1]]
    return [block_of(rank)] + [
        lax.ppermute(block_of((rank + k) % count), axis, [(i, (i + k) % count) for i in range(count)]) for k in range(1, count)]


def sum_blocks(blocks):
    total = blocks[0].astype(F32)
    for block in blocks[1:]:
        total = total + block.astype(F32)
    return total.astype(BF16)


def weight_gradient(left, right, cut_left, section):
    rows = left.shape[0]
    m, n = left.shape[1] // (2 if cut_left else 1), right.shape[1] // (1 if cut_left else 2)
    block = 128 if cut_left else 256
    steps = m // block
    left_at = (lambda i, which: (0, which[0] * steps + i)) if cut_left else (lambda i, which: (0, i))
    right_at = (lambda i, which: (0, 0)) if cut_left else (lambda i, which: (0, which[0]))

    def product(which):
        return pl.pallas_call(
            product_kernel,
            name="weight_gradient",
            out_shape=jax.ShapeDtypeStruct((m, n), BF16),
            grid_spec=pltpu.PrefetchScalarGridSpec(
                num_scalar_prefetch=1, grid=(steps,),
                in_specs=[pl.BlockSpec((rows, block), left_at), pl.BlockSpec((rows, n), right_at)],
                out_specs=pl.BlockSpec((block, n), lambda i, which: (i, 0))),
            compiler_params=params(20),
            cost_estimate=pl.CostEstimate(flops=2 * rows * m * n, transcendentals=0, bytes_accessed=2 * (rows * (m + n) + m * n)),
        )(which.reshape(1).astype(jnp.int32), left, right)

    arrived = swap(product(1 - section), "section", 1)
    return product(section), arrived


def dct_table(order):
    row_index = jnp.arange(order, dtype=F32)[:, None]
    col_index = jnp.arange(order, dtype=F32)[None, :]
    cosines = jnp.sqrt(2.0 / order) * jnp.cos(math.pi * (row_index + 0.5) * col_index / order)
    return cosines * jnp.where(col_index == 0, math.sqrt(0.5), 1.0)


def rotary_tables(length):
    column = jnp.arange(LANES // 2, dtype=jnp.int32) % HEAD
    half = ROT // 2
    index = (column % half).astype(F32)
    angles = jnp.arange(length, dtype=F32)[:, None] * (10000.0 ** (-index * 2.0 / ROT))[None, :]
    turned = (column < ROT)[None, :]
    sign = jnp.where(column < half, -1.0, 1.0)[None, :]
    return jnp.where(turned, jnp.cos(angles), 1.0), jnp.where(turned, sign * jnp.sin(angles), 0.0)


def shards(block_input, cotangent, lengths, ln_gain, ln_bias, w_qkv, w_out, w_up, w_down, freq_table, feat_weight):
    section = lax.axis_index("section")
    place = lax.axis_index("mp")
    group = lax.axis_index("dp")
    groups = lax.axis_size("dp")
    local_slots, length, shard_width = block_input.shape
    width = ln_gain.shape[1]
    heads = freq_table.shape[1]
    is_first = section == 0
    lens = lax.dynamic_slice_in_dim(lengths, section, 1, 0)
    metas = [jnp.stack([place, (section == l).astype(jnp.int32)]).astype(jnp.int32) for l in range(2)]

    def own(values):
        return lax.dynamic_index_in_dim(values, section, 0, keepdims=False)

    shard0 = own(block_input)
    pieces0 = gather_pieces(shard0)

    small = jnp.concatenate([ln_gain[0], ln_bias[0], feat_weight.reshape(-1), freq_table.astype(F32).reshape(-1)])
    small_other = swap(small, "section", 1)
    mine = (w_qkv, w_up, w_out, w_down)
    other = tuple(swap(w, "section", 1) for w in mine)

    def both(mine, other):
        return jnp.where(is_first, mine, other), jnp.where(is_first, other, mine)

    layers_small = both(small, small_other)
    table = dct_table(HEAD)
    eye = jnp.eye(heads, dtype=F32)

    def layer_weights(l):
        vec = layers_small[l]
        gain, bias = vec[:width].reshape(1, width), vec[width:2 * width].reshape(1, width)
        feat = vec[2 * width:2 * width + LANES].reshape(1, LANES)
        freq = vec[2 * width + LANES:].reshape(heads, HEAD, HEAD)
        mixed = jnp.einsum("nk,hkm->hnm", table, freq, precision=lax.Precision.HIGHEST)
        mixed = (eye[:, None, :, None] * mixed[:, :, None, :]).reshape(LANES, LANES)
        high = lax.reduce_precision(mixed, 8, 7)
        return (gain, bias, high.astype(BF16), (mixed - high).astype(BF16), feat), mine, other

    weights0, weights1 = layer_weights(0), layer_weights(1)
    tables = rotary_tables(length)

    cot = after(own(cotangent), pieces0[3], pieces0[4])
    cot_x, cot_y = swap(cot, "mp", 1), swap(cot, "mp", 2)
    part0, all0, _ = forward_layer(metas[0], lens, pieces0, weights0, tables, length, 0, True)
    part0 = after(part0, cot_x, cot_y)
    hidden = (shard0.astype(F32) + scatter_sum(part0)).astype(BF16)
    pieces1 = gather_pieces(hidden)
    cot_x, cot_y = after((cot_x, cot_y), pieces1[3], pieces1[4])
    half = shard_width // 2
    pieces_g = cot, cot_x, cot_y, swap(cot_x[:, :half], "mp", 2), swap(cot_y[:, half:], "mp", 1)
    part1, all1, _ = forward_layer(metas[1], lens, pieces1, weights1, tables, length, 0, False)
    out_kept, out_sent = direct_sends(part1)

    def saved_of(arrays):
        return (arrays[0],) + tuple(arrays[3:])

    def in_block(mine, arrived):
        n = mine.shape[0] // groups
        cut = lambda v, i: lax.dynamic_slice_in_dim(v, i * n, n, 0)
        return lambda i: (cut(mine, i).astype(F32) + cut(arrived, i).astype(F32)).astype(BF16)

    def out_block(mine, arrived):
        n = mine.shape[1] // groups
        cut = lambda v, i: lax.dynamic_slice_in_dim(v, i * n, n, 1)
        return lambda i: (cut(mine, i).astype(F32) + cut(arrived, i).astype(F32)).astype(BF16)

    def run_backward(meta, grad, saved, weights, phased):
        parts, (stats, dcat), (_, _, dmix, fsum) = backward_layer(meta, grad, saved, weights, tables, length, 0, phased)
        return parts, stats, dcat, dmix, fsum

    def norm_backward(grad_shard, d_normed, sums, norm, gain_all):
        xhat, rstd = norm
        gain = lax.dynamic_slice_in_dim(gain_all, place * shard_width, shard_width, 1)
        mean_d = (sums[0] * (1.0 / width))[:, None]
        mean_dx = (sums[1] * (1.0 / width))[:, None]
        return grad_shard.astype(F32) + rstd[:, :1] * (d_normed * gain - mean_d - xhat * mean_dx)

    def small_gradients(d_normed, norm, dmix, fsum):
        gain_part = jnp.sum(d_normed * norm[0], axis=0)
        bias_part = jnp.sum(d_normed, axis=0)
        diagonal = jnp.stack([dmix[h * HEAD:(h + 1) * HEAD, h * HEAD:(h + 1) * HEAD] for h in range(heads)])
        return jnp.concatenate([gain_part, bias_part, fsum[0], diagonal.reshape(-1)])

    saved1, saved0 = saved_of(all1), saved_of(all0)
    grad1 = join(metas[1], pieces_g)
    out_blocks1 = block_sends(out_block(*weight_gradient(saved1[6], grad1, True, section)), "dp")
    grad1_b = after(grad1, out_blocks1[0])
    parts, stats, dcat1, dmix1, fsum1 = run_backward(metas[1], grad1_b, saved1, weights1, True)
    parts, stats, dcat1, dmix1, fsum1 = after((parts, stats, dcat1, dmix1, fsum1), *out_blocks1, *out_sent)
    arrived = scatter_start(parts)
    turn = scatter_turn(parts, arrived)
    sums = mp_total(after(stats, *turn))
    steps1 = list(ring_scatter(in_block(*weight_gradient(saved1[0], dcat1, False, section)), "dp"))
    arrivals1, red_in1 = [arrival for arrival, _ in steps1], steps1[-1][1]
    d_normed = scatter_end(parts, arrived, *turn)
    g0 = norm_backward(cot, d_normed, sums, all1[1:3], weights1[0][0]).astype(BF16)
    small1 = small_gradients(d_normed, all1[1:3], dmix1, fsum1)
    pieces_g0 = gather_pieces(after(g0, arrivals1[0]), arrivals1[1:2])
    pieces_g0 = after(pieces_g0, *arrivals1[2:3])
    out = hidden.astype(F32) + out_kept + out_sent[0].astype(F32) + out_sent[1].astype(F32) + out_sent[2].astype(F32)

    grad0 = join(metas[0], pieces_g0)
    out_blocks0 = block_sends(out_block(*weight_gradient(saved0[6], grad0, True, section)), "dp")
    grad0_b = after(grad0, out_blocks0[0])
    parts, stats, dcat0, dmix0, fsum0 = run_backward(metas[0], grad0_b, saved0, weights0, False)
    parts, stats, dcat0, dmix0, fsum0 = after((parts, stats, dcat0, dmix0, fsum0), *out_blocks0)
    out_blocks1 = after(out_blocks1, dcat0)
    kept, sent = direct_sends(parts)
    sums = mp_total(stats)
    mine0, arrived0 = weight_gradient(saved0[0], dcat0, False, section)
    block0 = in_block(mine0, arrived0)
    steps0 = list(ring_scatter(block0, "dp"))
    sent, dmix0, out_blocks0, out_blocks1 = after((sent, dmix0, out_blocks0, out_blocks1), steps0[0][0])
    d_normed = kept + sent[0].astype(F32) + sent[1].astype(F32) + sent[2].astype(F32)
    d_input = norm_backward(g0, d_normed, sums, all0[1:3], weights0[0][0])
    small0 = small_gradients(d_normed, all0[1:3], dmix0, fsum0)

    def to_owner(first, second, axis):
        mine, other = both(first, second)
        arrived = swap(other, "section", 1)
        return jnp.where(is_first, jnp.concatenate([mine, arrived], axis), jnp.concatenate([arrived, mine], axis)).astype(F32)

    grads_out = to_owner(sum_blocks(out_blocks0), sum_blocks(out_blocks1), 0)
    small_mine, small_send = both(small0, small1)
    small_sum = dp_total(small_mine + swap(small_send, "section", 1))
    feat_grad = small_sum[2 * shard_width:2 * shard_width + LANES].reshape(heads, HEAD) / feat_weight[0]
    freq_grad = jnp.einsum("nk,hnm->hkm", table, small_sum[2 * shard_width + LANES:].reshape(heads, HEAD, HEAD),
                           precision=lax.Precision.HIGHEST)
    keep, send = both(d_input, out)
    arrived = swap(send, "section", 1)
    boundary = jnp.where(is_first, jnp.stack([keep, arrived]), jnp.stack([arrived, keep]))
    grads_in = to_owner(steps0[-1][1], red_in1, 1)
    qkv_grad = jnp.stack([grads_in[:, t * shard_width:(t + 1) * shard_width] for t in range(3)])
    return (
        boundary[None],
        small_sum[None, :shard_width],
        small_sum[None, shard_width:2 * shard_width],
        qkv_grad[None],
        grads_out[None, :shard_width],
        grads_in[None, :, 3 * shard_width:],
        grads_out[None, shard_width:],
        freq_grad[None],
        feat_grad[None],
    )


def solution(mesh):
    placed = (
        P("dp", None, "mp"), P("dp", None, "mp"), P("dp"), P("section", None), P("section", None),
        P("section", None, None, "mp"), P("section", "mp", None), P("section", None, "mp"), P("section", "mp", None),
        P("section", "mp", None, None), P("section", "mp", None),
    )
    return jax.shard_map(
        shards,
        mesh=mesh,
        in_specs=placed,
        out_specs=(
            P("section", "dp", None, "mp"), P("section", "mp"), P("section", "mp"), P("section", None, "dp", "mp"),
            P("section", "mp", "dp"), P("section", "dp", "mp"), P("section", "mp", "dp"), P("section", "mp", None, None),
            P("section", "mp", None),
        ),
        check_vma=False,
    )
```

```python
import functools
import math

import jax
import jax.numpy as jnp
from jax import lax
from jax.experimental import pallas as pl
from jax.experimental.pallas import tpu as pltpu
from jax.sharding import PartitionSpec as P

ROT = 16
TILE = 256
HEAD = 64
LANES = 256
EPS = 1e-05
F32 = jnp.float32
BF16 = jnp.bfloat16
RSQRT2 = math.sqrt(0.5)
RSQRT2PI = 1.0 / math.sqrt(2.0 * math.pi)
SAVED = 14


def dot_nn(a, b):
    return lax.dot_general(a, b, (((1,), (0,)), ((), ())), preferred_element_type=F32)


def dot_nt(a, b):
    return lax.dot_general(a, b, (((1,), (1,)), ((), ())), preferred_element_type=F32)


def dot_tn(a, b):
    return lax.dot_general(a, b, (((0,), (0,)), ((), ())), preferred_element_type=F32)


def split(values):
    high = values.astype(BF16)
    return high, (values - high.astype(F32)).astype(BF16)


def iota(shape, dim):
    return lax.broadcasted_iota(jnp.int32, shape, dim)


def partner(values):
    later = pltpu.roll(values, LANES - ROT // 2, 1)
    earlier = pltpu.roll(values, ROT // 2, 1)
    lower = iota(values.shape, 1) % HEAD < ROT // 2
    return jnp.where(lower, later, earlier)


def twice(table):
    return jnp.concatenate([table, table], axis=1)


def head_of(shape, dim):
    return iota(shape, dim) // HEAD


def weight_copies(refs, w_in, w_out, sems, which):
    qkv, up, out, down = refs
    ends = [(qkv.at[0, t], w_in.at[:, t * LANES:(t + 1) * LANES]) for t in range(3)] + [
        (up.at[0], w_in.at[:, 3 * LANES:]), (out.at[0], w_out.at[0:LANES, :]), (down.at[0], w_out.at[LANES:, :])]
    return [pltpu.make_async_copy(*ends[i], sems.at[i]) for i in which]


def start_weights(meta, mine, other, w_in, w_out, sems, order):
    def start(refs):
        for copy in weight_copies(refs, w_in, w_out, sems, order):
            copy.start()

    @pl.when(meta[1] == 1)
    def _():
        start(mine)

    @pl.when(meta[1] != 1)
    def _():
        start(other)


def wait_weights(step, refs, w_in, w_out, sems, which):
    @pl.when(step == 0)
    def _():
        for copy in weight_copies(refs, w_in, w_out, sems, which):
            copy.wait()


def forward_kernel(carried, phased, *refs):
    refs = list(refs)
    take = lambda n: [refs.pop(0) for _ in range(n)]
    meta, lens = take(2)
    p0, p1, p2, p3a, p3b, gain, bias, mix_hi, mix_lo, feat_w, cos_t, sin_t = take(12)
    mine, other = take(4), take(4)
    if carried:
        state_in, ksum_in = take(2)
        take(SAVED)
    parts = take(5 if phased else 4)
    normed, xhat, rstd, rq_o, rk_o, qf_o, kf_o, v_o, hcat, dgelu, invz, att_o, prior_s, prior_k = take(SAVED)
    state, ksum, w_in, w_out, sems = take(5)
    tile = pl.program_id(0)
    rank = meta[0]
    half = LANES // 2

    @pl.when(tile == 0)
    def _():
        start_weights(meta, mine, other, w_in, w_out, sems, (0, 1, 2, 3, 4, 5))
        if carried:
            state[...] = state_in[...]
            ksum[...] = ksum_in[...]
        else:
            state[...] = jnp.zeros_like(state)
            ksum[...] = jnp.zeros_like(ksum)

    pieces = [p0[...].astype(F32), p1[...].astype(F32), p2[...].astype(F32),
              jnp.concatenate([p3a[...], p3b[...]], axis=1).astype(F32)]
    width = 4 * LANES
    mean = jnp.sum(pieces[0] + pieces[1] + pieces[2] + pieces[3], axis=1, keepdims=True) * (1.0 / width)
    pieces = [piece - mean for piece in pieces]
    squares = sum(piece * piece for piece in pieces)
    factor = lax.rsqrt(jnp.sum(squares, axis=1, keepdims=True) * (1.0 / width) + EPS)
    for r in range(4):
        at = pl.ds(pl.multiple_of((rank ^ r) * LANES, LANES), LANES)
        hat = pieces[r] * factor
        if r == 0:
            xhat[...] = hat
        normed[:, at] = (hat * gain[:, at] + bias[:, at]).astype(BF16)
    rstd[...] = jnp.broadcast_to(factor, (TILE, half))
    tokens = normed[...]

    wait_weights(tile, mine, w_in, w_out, sems, (0, 1, 2))
    cosine, sine = twice(cos_t[...]), twice(sin_t[...])
    query = dot_nn(tokens, w_in[:, 0:LANES])
    key = dot_nn(tokens, w_in[:, LANES:2 * LANES])
    value = dot_nn(tokens, w_in[:, 2 * LANES:3 * LANES]).astype(BF16)
    rq = query * cosine + partner(query) * sine
    rk = key * cosine + partner(key) * sine
    weight = feat_w[...]

    def logits(rows):
        high, low = split(rows)
        return dot_nn(high, mix_hi[...]) + dot_nn(low, mix_hi[...]) + dot_nn(high, mix_lo[...])

    positions = lens[1] + tile * TILE + iota((TILE, LANES), 0)
    real = (positions < lens[0]).astype(F32)
    qf = (weight * jnp.exp(logits(rq))).astype(BF16)
    kf = (weight * jnp.exp(logits(rk)) * real).astype(BF16)
    rq_o[...] = rq.astype(BF16)
    rk_o[...] = rk.astype(BF16)
    qf_o[...] = qf
    kf_o[...] = kf
    v_o[...] = value

    square = (TILE, TILE)
    lower = iota(square, 0) >= iota(square, 1)
    same = head_of(square, 0) == head_of(square, 1)
    cumulative = dot_nn(lower.astype(BF16), kf) + ksum[0:1, :]
    high, low = split(qf.astype(F32) * cumulative)
    ones = same.astype(BF16)
    inverse = 1.0 / (dot_nn(high, ones) + dot_nn(low, ones))
    prior = jnp.where(same, state[...], 0.0)
    prior_hi, prior_lo = split(prior)
    numer = dot_nn(qf, prior_hi) + dot_nn(qf, prior_lo)
    lane_head = head_of((TILE, LANES), 1)
    zero = jnp.zeros((TILE, LANES), BF16)
    for h in range(LANES // HEAD):
        here = lane_head == h
        scores = dot_nt(qf, jnp.where(here, kf, zero))
        scores = jnp.where(lower, scores, 0.0).astype(BF16)
        numer = numer + dot_nn(scores, jnp.where(here, value, zero))
    prior_s[0] = prior
    prior_k[0] = ksum[...]
    state[...] = state[...] + dot_tn(kf, value)
    ksum[...] = jnp.broadcast_to(cumulative[TILE - 1:TILE, :], ksum.shape)
    invz[...] = inverse
    attended = numer * inverse
    att_o[...] = attended
    hcat[:, 0:LANES] = attended.astype(BF16)

    wait_weights(tile, mine, w_in, w_out, sems, (3,))
    for c in range(4):
        cols = slice(c * LANES, (c + 1) * LANES)
        up = dot_nn(tokens, w_in[:, (3 + c) * LANES:(4 + c) * LANES])
        cdf = 0.5 * (1.0 + lax.erf(up * RSQRT2))
        hcat[:, (1 + c) * LANES:(2 + c) * LANES] = (up * cdf).astype(BF16)
        dgelu[:, cols] = (cdf + up * (RSQRT2PI * jnp.exp(-0.5 * up * up))).astype(BF16)

    wait_weights(tile, mine, w_in, w_out, sems, (4, 5))
    hidden = hcat[...]
    emit(rank, lambda at: dot_nn(hidden, w_out[:, at]), parts)


def emit(rank, product, parts):
    half = LANES // 2
    for r in range(4):
        at = pl.ds(pl.multiple_of((rank ^ r) * LANES, LANES), LANES)
        part = product(at)
        if len(parts) == 4:
            parts[r][...] = part.astype(parts[r].dtype)
            continue
        sx, sy, k0, ka, kb = parts
        if r == 0:
            k0[...] = part
        elif r == 1:
            sx[0] = part[:, :half].astype(BF16)
            kb[...] = part[:, half:]
        elif r == 2:
            ka[...] = part[:, :half]
            sy[0] = part[:, half:].astype(BF16)
        else:
            sx[1] = part[:, :half].astype(BF16)
            sy[1] = part[:, half:].astype(BF16)


def backward_kernel(carried, phased, *refs):
    refs = list(refs)
    take = lambda n: [refs.pop(0) for _ in range(n)]
    meta, = take(1)
    grad, normed, rq, rk, qf_i, kf_i, v_i, att_i, dgelu, invz, prior_s, prior_k, gain, bias, mix_hi, cos_t, sin_t = take(17)
    mine, other = take(4), take(4)
    if carried:
        state_in, gsum_in, dmix_in, fsum_in = take(4)
        take(2)
    parts = take(5 if phased else 4)
    stats, dcat, state, gsum, dmix, fsum = take(6)
    w_in, w_out, sems = take(3)
    step = pl.program_id(0)
    rank = meta[0]

    @pl.when(step == 0)
    def _():
        start_weights(meta, mine, other, w_in, w_out, sems, (4, 5, 0, 1, 2, 3))
        if carried:
            state[...] = state_in[...]
            gsum[...] = gsum_in[...]
            dmix[...] = dmix_in[...]
            fsum[...] = fsum_in[...]
        else:
            state[...] = jnp.zeros_like(state)
            gsum[...] = jnp.zeros_like(gsum)
            dmix[...] = jnp.zeros_like(dmix)
            fsum[...] = jnp.zeros_like(fsum)

    wait_weights(step, mine, w_in, w_out, sems, (4, 5))
    g = grad[...]
    d_att = dot_nt(g, w_out[0:LANES, :]).astype(BF16).astype(F32)
    square = (TILE, TILE)
    same = head_of(square, 0) == head_of(square, 1)
    ones = same.astype(BF16)
    inverse = invz[...]
    dn = (d_att * inverse).astype(BF16)
    dn32 = dn.astype(F32)
    high, low = split(dn32 * att_i[...])
    dden = -(dot_nn(high, ones) + dot_nn(low, ones))
    den_hi = dden.astype(BF16).astype(F32)
    roll_hi = pltpu.roll(den_hi, HEAD, 1)
    roll_lo = pltpu.roll(dden - den_hi, HEAD, 1)
    qf, kf, value = qf_i[...], kf_i[...], v_i[...]
    zero = jnp.zeros((TILE, LANES), BF16)
    one = jnp.ones((TILE, LANES), BF16)
    lane = iota((TILE, LANES), 1)
    lane_head = lane // HEAD
    below = iota(square, 0) >= iota(square, 1)
    above = iota(square, 0) <= iota(square, 1)
    prior_hi, prior_lo = split(prior_s[0])
    later_hi, later_lo = split(jnp.where(same, state[...], 0.0))
    d_qf = dot_nt(dn, prior_hi) + dot_nt(dn, prior_lo) + prior_k[0, 0:1, :] * dden
    d_kf = dot_nt(value, later_hi) + dot_nt(value, later_lo) + gsum[0:1, :]
    d_v = dot_nn(kf, later_hi)
    heads = LANES // HEAD
    for h in range(heads):
        here = lane_head == h
        spare = HEAD * ((h + 1) % heads)
        left = jnp.where(lane == spare, roll_hi, jnp.where(lane == spare + 1, roll_lo, dn32)).astype(BF16)
        right = jnp.where(here, value, jnp.where((lane == spare) | (lane == spare + 1), one, zero))
        k_here = jnp.where(here, kf, zero)
        q_here = jnp.where(here, qf, zero)
        d_here = jnp.where(here, dn, zero)
        scores_t = jnp.where(above, dot_nt(k_here, qf), 0.0).astype(BF16)
        ds = jnp.where(below, dot_nt(left, right), 0.0).astype(BF16)
        ds_t = jnp.where(above, dot_nt(right, left), 0.0).astype(BF16)
        d_qf = d_qf + dot_nn(ds, k_here)
        d_kf = d_kf + dot_nn(ds_t, q_here)
        d_v = d_v + dot_nn(scores_t, d_here)
    state[...] = state[...] + dot_tn(qf, dn)
    gsum[...] = gsum[...] + jnp.sum(qf.astype(F32) * dden, axis=0, keepdims=True)
    dlq = d_qf * qf.astype(F32)
    dlk = d_kf * kf.astype(F32)
    fsum[...] = fsum[...] + jnp.sum(dlq + dlk, axis=0, keepdims=True)
    dlq, dlk = dlq.astype(BF16), dlk.astype(BF16)
    dmix[...] = dmix[...] + dot_tn(rq[...], dlq) + dot_tn(rk[...], dlk)
    cosine, sine = twice(cos_t[...]), twice(sin_t[...])
    for c, dl in ((0, dlq), (1, dlk)):
        dr = dot_nt(dl, mix_hi[...])
        dcat[:, c * LANES:(c + 1) * LANES] = (dr * cosine - partner(dr) * sine).astype(BF16)
    dcat[:, 2 * LANES:3 * LANES] = d_v.astype(BF16)
    for c in range(4):
        cols = slice(c * LANES, (c + 1) * LANES)
        d_act = dot_nt(g, w_out[(1 + c) * LANES:(2 + c) * LANES, :])
        dcat[:, (3 + c) * LANES:(4 + c) * LANES] = (d_act * dgelu[:, cols].astype(F32)).astype(BF16)
    wait_weights(step, mine, w_in, w_out, sems, (0, 1, 2, 3))
    wide = dcat[...]
    row = iota((8, LANES), 0)
    first, second = (row == 0).astype(BF16), (row == 1).astype(BF16)
    totals = []

    def product(at):
        part = dot_nt(wide, w_in[at, :])
        one_side = (part * gain[:, at]).astype(BF16)
        other = (part * (normed[:, at].astype(F32) - bias[:, at])).astype(BF16)
        totals.append(dot_nt(first, one_side) + dot_nt(second, other))
        return part

    emit(rank, product, parts)
    stats[...] = totals[0] + totals[1] + totals[2] + totals[3]


def product_kernel(which, left, right, out):
    out[...] = dot_tn(left[...], right[...]).astype(BF16)


def join_kernel(meta, p0, p1, p2, p3a, p3b, whole):
    half = LANES // 2
    for r, piece in enumerate((p0, p1, p2)):
        whole[:, pl.ds(pl.multiple_of((meta[0] ^ r) * LANES, LANES), LANES)] = piece[...]
    at = pl.multiple_of((meta[0] ^ 3) * LANES, LANES)
    whole[:, pl.ds(at, half)] = p3a[...]
    whole[:, pl.ds(pl.multiple_of(at + half, half), half)] = p3b[...]


def partial_outs(rows, phased, row_of):
    half = LANES // 2
    if not phased:
        shapes = [jax.ShapeDtypeStruct((rows, LANES), F32)] + [jax.ShapeDtypeStruct((rows, LANES), BF16)] * 3
        return shapes, [pl.BlockSpec((TILE, LANES), lambda *i: (row_of(*i), 0))] * 4
    shapes = [jax.ShapeDtypeStruct((2, rows, half), BF16)] * 2 + [
        jax.ShapeDtypeStruct((rows, LANES), F32), jax.ShapeDtypeStruct((rows, half), F32),
        jax.ShapeDtypeStruct((rows, half), F32)]
    specs = [pl.BlockSpec((2, TILE, half), lambda *i: (0, row_of(*i), 0))] * 2 + [
        pl.BlockSpec((TILE, width), lambda *i: (row_of(*i), 0)) for width in (LANES, half, half)]
    return shapes, specs


def fixed(shape):
    return pl.BlockSpec(shape, lambda *i: (0,) * len(shape))


def outside(count):
    return [pl.BlockSpec(memory_space=pl.ANY)] * count


def params(size):
    return pltpu.CompilerParams(dimension_semantics=("arbitrary",), vmem_limit_bytes=size << 20)


def weight_scratch(width):
    return [pltpu.VMEM((width, 3 * LANES + width), BF16), pltpu.VMEM((LANES + width, width), BF16),
            pltpu.SemaphoreType.DMA((6,))]


def forward_layer(meta, lens, pieces, weights, tables, length, first_row, phased, carry=None):
    rows = pieces[0].shape[0]
    tiles, before = rows // TILE, first_row // TILE
    half, width = LANES // 2, 4 * LANES
    local = lambda t, *_: t
    there = lambda t, *_: before + t
    by_row = lambda n, row_of: pl.BlockSpec((TILE, n), lambda *i: (row_of(*i), 0))
    (gain, bias, mix_hi, mix_lo, feat_w), mine, other = weights
    small = (gain, bias, mix_hi, mix_lo, feat_w)
    shapes, specs = partial_outs(rows, phased, local)
    extra = [(width, BF16), (LANES, F32), (half, F32)] + [(LANES, BF16)] * 5 + [
        (LANES + width, BF16), (width, BF16), (LANES, F32), (LANES, F32)]
    shapes += [jax.ShapeDtypeStruct((length, n), d) for n, d in extra]
    specs += [by_row(n, there) for n, _ in extra]
    shapes += [jax.ShapeDtypeStruct((length // TILE, LANES, LANES), F32), jax.ShapeDtypeStruct((length // TILE, 8, LANES), F32)]
    specs += [pl.BlockSpec((1, n, LANES), lambda *i: (there(*i), 0, 0)) for n in (LANES, 8)]
    states = [(LANES, LANES), (8, LANES)]
    shapes += [jax.ShapeDtypeStruct(s, F32) for s in states]
    specs += [fixed(s) for s in states]
    operands = [meta, jnp.stack([lens[0], jnp.int32(first_row)]), *pieces, *small, *tables, *mine, *other]
    in_specs = [by_row(p.shape[1], local) for p in pieces] + [fixed(w.shape) for w in small] + [by_row(half, there)] * 2 + outside(8)
    aliases = {}
    if carry is not None:
        state, saved = carry
        operands += [*state, *saved]
        in_specs += [fixed(s) for s in states] + outside(SAVED)
        aliases = {len(operands) - SAVED + i: len(shapes) - 2 - SAVED + i for i in range(SAVED)}
    outs = pl.pallas_call(
        functools.partial(forward_kernel, carry is not None, phased),
        name="layer_forward",
        out_shape=shapes,
        grid_spec=pltpu.PrefetchScalarGridSpec(
            num_scalar_prefetch=2, grid=(tiles,), in_specs=in_specs, out_specs=specs, scratch_shapes=weight_scratch(width)),
        input_output_aliases=aliases,
        compiler_params=params(56),
        cost_estimate=pl.CostEstimate(flops=rows * 20_000_000, transcendentals=rows * 5000, bytes_accessed=24 << 20),
    )(*operands)
    count = 5 if phased else 4
    return outs[:count], outs[count:count + SAVED], outs[count + SAVED:]


def backward_layer(meta, grad, saved, weights, tables, length, first_row, phased, carry=None):
    rows = grad.shape[0]
    tiles, before = rows // TILE, first_row // TILE
    half, width = LANES // 2, 4 * LANES
    local = lambda t, *_: tiles - 1 - t
    there = lambda t, *_: before + tiles - 1 - t
    by_row = lambda n, row_of=there: pl.BlockSpec((TILE, n), lambda *i: (row_of(*i), 0))
    normed, rq, rk, qf, kf, value, hcat, dgelu, invz, attended, prior_s, prior_k = saved
    (gain, bias, mix_hi, mix_lo, feat_w), mine, other = weights
    shapes, specs = partial_outs(rows, phased, local)
    shapes += [jax.ShapeDtypeStruct((8, length), F32), jax.ShapeDtypeStruct((length, 3 * LANES + width), BF16)]
    specs += [pl.BlockSpec((8, TILE), lambda *i: (0, there(*i))), by_row(3 * LANES + width)]
    states = [(LANES, LANES), (8, LANES)] * 2
    shapes += [jax.ShapeDtypeStruct(s, F32) for s in states]
    specs += [fixed(s) for s in states]
    operands = [meta, grad, normed, rq, rk, qf, kf, value, attended, dgelu, invz, prior_s, prior_k, gain, bias, mix_hi, *tables,
                *mine, *other]
    in_specs = [by_row(width, local), by_row(width)] + [by_row(LANES)] * 6 + [by_row(width), by_row(LANES)] + [
        pl.BlockSpec((1, n, LANES), lambda *i: (there(*i), 0, 0)) for n in (LANES, 8)] + [
        fixed(w.shape) for w in (gain, bias, mix_hi)] + [by_row(half)] * 2 + outside(8)
    aliases = {}
    if carry is not None:
        state, arrays = carry
        operands += [*state, *arrays]
        in_specs += [fixed(s) for s in states] + outside(2)
        aliases = {len(operands) - 2 + i: len(shapes) - 6 + i for i in range(2)}
    outs = pl.pallas_call(
        functools.partial(backward_kernel, carry is not None, phased),
        name="layer_backward",
        out_shape=shapes,
        grid_spec=pltpu.PrefetchScalarGridSpec(
            num_scalar_prefetch=1, grid=(tiles,), in_specs=in_specs, out_specs=specs, scratch_shapes=weight_scratch(width)),
        input_output_aliases=aliases,
        compiler_params=params(56),
        cost_estimate=pl.CostEstimate(flops=rows * 25_000_000, transcendentals=0, bytes_accessed=24 << 20),
    )(*operands)
    count = 5 if phased else 4
    return outs[:count], outs[count:count + 2], outs[count + 2:]


def join(meta, pieces):
    rows, block = pieces[0].shape[0], 2 * TILE
    return pl.pallas_call(
        join_kernel,
        name="join",
        out_shape=jax.ShapeDtypeStruct((rows, 4 * LANES), BF16),
        grid_spec=pltpu.PrefetchScalarGridSpec(
            num_scalar_prefetch=1,
            grid=(rows // block,),
            in_specs=[pl.BlockSpec((block, p.shape[1]), lambda i, *_: (i, 0)) for p in pieces],
            out_specs=pl.BlockSpec((block, 4 * LANES), lambda i, *_: (i, 0)),
        ),
        compiler_params=params(8),
        cost_estimate=pl.CostEstimate(flops=0, transcendentals=0, bytes_accessed=rows * 16 * LANES),
    )(meta, *pieces)


def swap(value, axis, by):
    return lax.ppermute(value, axis, [(k, k ^ by) for k in range(lax.axis_size(axis))])


def gather_pieces(shard, meanwhile=()):
    half = shard.shape[1] // 2
    from_x, from_y = after((swap(shard, "mp", 1), swap(shard, "mp", 2)), *meanwhile)
    return shard, from_x, from_y, swap(from_x[:, :half], "mp", 2), swap(from_y[:, half:], "mp", 1)


def after(values, *others):
    if not others:
        return values
    return lax.optimization_barrier((values, others))[0]


def direct_sends(parts):
    return parts[0], [swap(part, "mp", r) for r, part in enumerate(parts) if r > 0]


def scatter_start(parts):
    return swap(parts[0], "mp", 1), swap(parts[1], "mp", 2)


def scatter_turn(parts, arrived):
    _, _, _, ka, kb = parts
    in_x, in_y = arrived
    return (ka + in_x[1].astype(F32)).astype(BF16), (kb + in_y[1].astype(F32)).astype(BF16)


def scatter_end(parts, arrived, to_y, to_x):
    _, _, k0, ka, _ = parts
    in_x, in_y = arrived
    half = ka.shape[1]
    last_y, last_x = swap(to_y, "mp", 2), swap(to_x, "mp", 1)
    return jnp.concatenate(
        [k0[:, :half] + in_x[0].astype(F32) + last_y.astype(F32), k0[:, half:] + in_y[0].astype(F32) + last_x.astype(F32)],
        axis=1)


def scatter_sum(parts):
    arrived = scatter_start(parts)
    return scatter_end(parts, arrived, *scatter_turn(parts, arrived))


def mp_total(values):
    return values + swap(values, "mp", 1) + swap(values, "mp", 2) + swap(values, "mp", 3)


def ring_scatter(block_of, axis):
    count = lax.axis_size(axis)
    rank = lax.axis_index(axis)
    pairs = [(k, (k + 1) % count) for k in range(count)]
    total = block_of((rank + count - 1) % count)
    for step in range(2, count + 1):
        arrived = lax.ppermute(total, axis, pairs)
        total = (arrived.astype(F32) + block_of((rank + count - step) % count).astype(F32)).astype(BF16)
        yield arrived, total


def dp_total(values):
    count = lax.axis_size("dp")
    if count > 8:
        return lax.psum(values, "dp")
    sent = [lax.ppermute(values, "dp", [(i, (i + k) % count) for i in range(count)]) for k in range(1, count)]
    return sum(sent, values)


def block_sends(block_of, axis):
    count = lax.axis_size(axis)
    rank = lax.axis_index(axis)
    if count > 8:
        return [list(ring_scatter(block_of, axis))[-1][1]]
    return [block_of(rank)] + [
        lax.ppermute(block_of((rank + k) % count), axis, [(i, (i + k) % count) for i in range(count)]) for k in range(1, count)]


def sum_blocks(blocks):
    total = blocks[0].astype(F32)
    for block in blocks[1:]:
        total = total + block.astype(F32)
    return total.astype(BF16)


def weight_gradient(left, right, cut_left, section):
    rows = left.shape[0]
    m, n = left.shape[1] // (2 if cut_left else 1), right.shape[1] // (1 if cut_left else 2)
    block = 128 if cut_left else 256
    steps = m // block
    left_at = (lambda i, which: (0, which[0] * steps + i)) if cut_left else (lambda i, which: (0, i))
    right_at = (lambda i, which: (0, 0)) if cut_left else (lambda i, which: (0, which[0]))

    def product(which):
        return pl.pallas_call(
            product_kernel,
            name="weight_gradient",
            out_shape=jax.ShapeDtypeStruct((m, n), BF16),
            grid_spec=pltpu.PrefetchScalarGridSpec(
                num_scalar_prefetch=1, grid=(steps,),
                in_specs=[pl.BlockSpec((rows, block), left_at), pl.BlockSpec((rows, n), right_at)],
                out_specs=pl.BlockSpec((block, n), lambda i, which: (i, 0))),
            compiler_params=params(20),
            cost_estimate=pl.CostEstimate(flops=2 * rows * m * n, transcendentals=0, bytes_accessed=2 * (rows * (m + n) + m * n)),
        )(which.reshape(1).astype(jnp.int32), left, right)

    arrived = swap(product(1 - section), "section", 1)
    return product(section), arrived


def dct_table(order):
    row_index = jnp.arange(order, dtype=F32)[:, None]
    col_index = jnp.arange(order, dtype=F32)[None, :]
    cosines = jnp.sqrt(2.0 / order) * jnp.cos(math.pi * (row_index + 0.5) * col_index / order)
    return cosines * jnp.where(col_index == 0, math.sqrt(0.5), 1.0)


def rotary_tables(length):
    column = jnp.arange(LANES // 2, dtype=jnp.int32) % HEAD
    half = ROT // 2
    index = (column % half).astype(F32)
    angles = jnp.arange(length, dtype=F32)[:, None] * (10000.0 ** (-index * 2.0 / ROT))[None, :]
    turned = (column < ROT)[None, :]
    sign = jnp.where(column < half, -1.0, 1.0)[None, :]
    return jnp.where(turned, jnp.cos(angles), 1.0), jnp.where(turned, sign * jnp.sin(angles), 0.0)


def shards(block_input, cotangent, lengths, ln_gain, ln_bias, w_qkv, w_out, w_up, w_down, freq_table, feat_weight):
    section = lax.axis_index("section")
    place = lax.axis_index("mp")
    group = lax.axis_index("dp")
    groups = lax.axis_size("dp")
    local_slots, length, shard_width = block_input.shape
    width = ln_gain.shape[1]
    heads = freq_table.shape[1]
    is_first = section == 0
    lens = lax.dynamic_slice_in_dim(lengths, section, 1, 0)
    metas = [jnp.stack([place, (section == l).astype(jnp.int32)]).astype(jnp.int32) for l in range(2)]

    def own(values):
        return lax.dynamic_index_in_dim(values, section, 0, keepdims=False)

    shard0 = own(block_input)
    pieces0 = gather_pieces(shard0)

    small = jnp.concatenate([ln_gain[0], ln_bias[0], feat_weight.reshape(-1), freq_table.astype(F32).reshape(-1)])
    small_other = swap(small, "section", 1)
    mine = (w_qkv, w_up, w_out, w_down)
    other = tuple(swap(w, "section", 1) for w in mine)

    def both(mine, other):
        return jnp.where(is_first, mine, other), jnp.where(is_first, other, mine)

    layers_small = both(small, small_other)
    table = dct_table(HEAD)
    eye = jnp.eye(heads, dtype=F32)

    def layer_weights(l):
        vec = layers_small[l]
        gain, bias = vec[:width].reshape(1, width), vec[width:2 * width].reshape(1, width)
        feat = vec[2 * width:2 * width + LANES].reshape(1, LANES)
        freq = vec[2 * width + LANES:].reshape(heads, HEAD, HEAD)
        mixed = jnp.einsum("nk,hkm->hnm", table, freq, precision=lax.Precision.HIGHEST)
        mixed = (eye[:, None, :, None] * mixed[:, :, None, :]).reshape(LANES, LANES)
        high = lax.reduce_precision(mixed, 8, 7)
        return (gain, bias, high.astype(BF16), (mixed - high).astype(BF16), feat), mine, other

    weights0, weights1 = layer_weights(0), layer_weights(1)
    tables = rotary_tables(length)

    cot = after(own(cotangent), pieces0[3], pieces0[4])
    cot_x, cot_y = swap(cot, "mp", 1), swap(cot, "mp", 2)
    part0, all0, _ = forward_layer(metas[0], lens, pieces0, weights0, tables, length, 0, True)
    part0 = after(part0, cot_x, cot_y)
    hidden = (shard0.astype(F32) + scatter_sum(part0)).astype(BF16)
    pieces1 = gather_pieces(hidden)
    cot_x, cot_y = after((cot_x, cot_y), pieces1[3], pieces1[4])
    half = shard_width // 2
    pieces_g = cot, cot_x, cot_y, swap(cot_x[:, :half], "mp", 2), swap(cot_y[:, half:], "mp", 1)
    part1, all1, _ = forward_layer(metas[1], lens, pieces1, weights1, tables, length, 0, False)
    out_kept, out_sent = direct_sends(part1)

    def saved_of(arrays):
        return (arrays[0],) + tuple(arrays[3:])

    def in_block(mine, arrived):
        n = mine.shape[0] // groups
        cut = lambda v, i: lax.dynamic_slice_in_dim(v, i * n, n, 0)
        return lambda i: (cut(mine, i).astype(F32) + cut(arrived, i).astype(F32)).astype(BF16)

    def out_block(mine, arrived):
        n = mine.shape[1] // groups
        cut = lambda v, i: lax.dynamic_slice_in_dim(v, i * n, n, 1)
        return lambda i: (cut(mine, i).astype(F32) + cut(arrived, i).astype(F32)).astype(BF16)

    def run_backward(meta, grad, saved, weights, phased):
        parts, (stats, dcat), (_, _, dmix, fsum) = backward_layer(meta, grad, saved, weights, tables, length, 0, phased)
        return parts, stats, dcat, dmix, fsum

    def norm_backward(grad_shard, d_normed, sums, norm, gain_all):
        xhat, rstd = norm
        gain = lax.dynamic_slice_in_dim(gain_all, place * shard_width, shard_width, 1)
        mean_d = (sums[0] * (1.0 / width))[:, None]
        mean_dx = (sums[1] * (1.0 / width))[:, None]
        return grad_shard.astype(F32) + rstd[:, :1] * (d_normed * gain - mean_d - xhat * mean_dx)

    def small_gradients(d_normed, norm, dmix, fsum):
        gain_part = jnp.sum(d_normed * norm[0], axis=0)
        bias_part = jnp.sum(d_normed, axis=0)
        diagonal = jnp.stack([dmix[h * HEAD:(h + 1) * HEAD, h * HEAD:(h + 1) * HEAD] for h in range(heads)])
        return jnp.concatenate([gain_part, bias_part, fsum[0], diagonal.reshape(-1)])

    saved1, saved0 = saved_of(all1), saved_of(all0)
    grad1 = join(metas[1], pieces_g)
    out_blocks1 = block_sends(out_block(*weight_gradient(saved1[6], grad1, True, section)), "dp")
    grad1_b = after(grad1, out_blocks1[0])
    parts, stats, dcat1, dmix1, fsum1 = run_backward(metas[1], grad1_b, saved1, weights1, True)
    parts, stats, dcat1, dmix1, fsum1 = after((parts, stats, dcat1, dmix1, fsum1), *out_blocks1, *out_sent)
    arrived = scatter_start(parts)
    turn = scatter_turn(parts, arrived)
    sums = mp_total(after(stats, *turn))
    steps1 = list(ring_scatter(in_block(*weight_gradient(saved1[0], dcat1, False, section)), "dp"))
    arrivals1, red_in1 = [arrival for arrival, _ in steps1], steps1[-1][1]
    d_normed = scatter_end(parts, arrived, *turn)
    g0 = norm_backward(cot, d_normed, sums, all1[1:3], weights1[0][0]).astype(BF16)
    small1 = small_gradients(d_normed, all1[1:3], dmix1, fsum1)
    pieces_g0 = gather_pieces(after(g0, arrivals1[0]), arrivals1[1:2])
    pieces_g0 = after(pieces_g0, *arrivals1[2:3])
    out = hidden.astype(F32) + out_kept + out_sent[0].astype(F32) + out_sent[1].astype(F32) + out_sent[2].astype(F32)

    grad0 = join(metas[0], pieces_g0)
    out_blocks0 = block_sends(out_block(*weight_gradient(saved0[6], grad0, True, section)), "dp")
    grad0_b = after(grad0, out_blocks0[0])
    parts, stats, dcat0, dmix0, fsum0 = run_backward(metas[0], grad0_b, saved0, weights0, False)
    parts, stats, dcat0, dmix0, fsum0 = after((parts, stats, dcat0, dmix0, fsum0), *out_blocks0)
    out_blocks1 = after(out_blocks1, dcat0)
    kept, sent = direct_sends(parts)
    sums = mp_total(stats)
    mine0, arrived0 = weight_gradient(saved0[0], dcat0, False, section)
    block0 = in_block(mine0, arrived0)
    steps0 = list(ring_scatter(block0, "dp"))
    sent, dmix0, out_blocks0, out_blocks1 = after((sent, dmix0, out_blocks0, out_blocks1), steps0[min(1, len(steps0) - 1)][0])
    d_normed = kept + sent[0].astype(F32) + sent[1].astype(F32) + sent[2].astype(F32)
    d_input = norm_backward(g0, d_normed, sums, all0[1:3], weights0[0][0])
    small0 = small_gradients(d_normed, all0[1:3], dmix0, fsum0)

    def to_owner(first, second, axis):
        mine, other = both(first, second)
        arrived = swap(other, "section", 1)
        return jnp.where(is_first, jnp.concatenate([mine, arrived], axis), jnp.concatenate([arrived, mine], axis)).astype(F32)

    grads_out = to_owner(sum_blocks(out_blocks0), sum_blocks(out_blocks1), 0)
    small_mine, small_send = both(small0, small1)
    small_sum = dp_total(small_mine + swap(small_send, "section", 1))
    feat_grad = small_sum[2 * shard_width:2 * shard_width + LANES].reshape(heads, HEAD) / feat_weight[0]
    freq_grad = jnp.einsum("nk,hnm->hkm", table, small_sum[2 * shard_width + LANES:].reshape(heads, HEAD, HEAD),
                           precision=lax.Precision.HIGHEST)
    keep, send = both(d_input, out)
    arrived = swap(send, "section", 1)
    boundary = jnp.where(is_first, jnp.stack([keep, arrived]), jnp.stack([arrived, keep]))
    grads_in = to_owner(steps0[-1][1], red_in1, 1)
    qkv_grad = jnp.stack([grads_in[:, t * shard_width:(t + 1) * shard_width] for t in range(3)])
    return (
        boundary[None],
        small_sum[None, :shard_width],
        small_sum[None, shard_width:2 * shard_width],
        qkv_grad[None],
        grads_out[None, :shard_width],
        grads_in[None, :, 3 * shard_width:],
        grads_out[None, shard_width:],
        freq_grad[None],
        feat_grad[None],
    )


def solution(mesh):
    placed = (
        P("dp", None, "mp"), P("dp", None, "mp"), P("dp"), P("section", None), P("section", None),
        P("section", None, None, "mp"), P("section", "mp", None), P("section", None, "mp"), P("section", "mp", None),
        P("section", "mp", None, None), P("section", "mp", None),
    )
    return jax.shard_map(
        shards,
        mesh=mesh,
        in_specs=placed,
        out_specs=(
            P("section", "dp", None, "mp"), P("section", "mp"), P("section", "mp"), P("section", None, "dp", "mp"),
            P("section", "mp", "dp"), P("section", "dp", "mp"), P("section", "mp", "dp"), P("section", "mp", None, None),
            P("section", "mp", None),
        ),
        check_vma=False,
    )
```

```python
import functools
import math

import jax
import jax.numpy as jnp
from jax import lax
from jax.experimental import pallas as pl
from jax.experimental.pallas import tpu as pltpu
from jax.sharding import PartitionSpec as P

ROT = 16
TILE = 256
HEAD = 64
LANES = 256
EPS = 1e-05
F32 = jnp.float32
BF16 = jnp.bfloat16
RSQRT2 = math.sqrt(0.5)
RSQRT2PI = 1.0 / math.sqrt(2.0 * math.pi)
SAVED = 14


def dot_nn(a, b):
    return lax.dot_general(a, b, (((1,), (0,)), ((), ())), preferred_element_type=F32)


def dot_nt(a, b):
    return lax.dot_general(a, b, (((1,), (1,)), ((), ())), preferred_element_type=F32)


def dot_tn(a, b):
    return lax.dot_general(a, b, (((0,), (0,)), ((), ())), preferred_element_type=F32)


def split(values):
    high = values.astype(BF16)
    return high, (values - high.astype(F32)).astype(BF16)


def iota(shape, dim):
    return lax.broadcasted_iota(jnp.int32, shape, dim)


def partner(values):
    later = pltpu.roll(values, LANES - ROT // 2, 1)
    earlier = pltpu.roll(values, ROT // 2, 1)
    lower = iota(values.shape, 1) % HEAD < ROT // 2
    return jnp.where(lower, later, earlier)


def twice(table):
    return jnp.concatenate([table, table], axis=1)


def head_of(shape, dim):
    return iota(shape, dim) // HEAD


def weight_copies(refs, w_in, w_out, sems, which):
    qkv, up, out, down = refs
    ends = [(qkv.at[0, t], w_in.at[:, t * LANES:(t + 1) * LANES]) for t in range(3)] + [
        (up.at[0], w_in.at[:, 3 * LANES:]), (out.at[0], w_out.at[0:LANES, :]), (down.at[0], w_out.at[LANES:, :])]
    return [pltpu.make_async_copy(*ends[i], sems.at[i]) for i in which]


def start_weights(meta, mine, other, w_in, w_out, sems, order):
    def start(refs):
        for copy in weight_copies(refs, w_in, w_out, sems, order):
            copy.start()

    @pl.when(meta[1] == 1)
    def _():
        start(mine)

    @pl.when(meta[1] != 1)
    def _():
        start(other)


def wait_weights(step, refs, w_in, w_out, sems, which):
    @pl.when(step == 0)
    def _():
        for copy in weight_copies(refs, w_in, w_out, sems, which):
            copy.wait()


def forward_kernel(carried, phased, *refs):
    refs = list(refs)
    take = lambda n: [refs.pop(0) for _ in range(n)]
    meta, lens = take(2)
    p0, p1, p2, p3a, p3b, gain, bias, mix_hi, mix_lo, feat_w, cos_t, sin_t = take(12)
    mine, other = take(4), take(4)
    if carried:
        state_in, ksum_in = take(2)
        take(SAVED)
    parts = take(5 if phased else 4)
    normed, xhat, rstd, rq_o, rk_o, qf_o, kf_o, v_o, hcat, dgelu, invz, att_o, prior_s, prior_k = take(SAVED)
    state, ksum, w_in, w_out, sems = take(5)
    tile = pl.program_id(0)
    rank = meta[0]
    half = LANES // 2

    @pl.when(tile == 0)
    def _():
        start_weights(meta, mine, other, w_in, w_out, sems, (0, 1, 2, 3, 4, 5))
        if carried:
            state[...] = state_in[...]
            ksum[...] = ksum_in[...]
        else:
            state[...] = jnp.zeros_like(state)
            ksum[...] = jnp.zeros_like(ksum)

    pieces = [p0[...].astype(F32), p1[...].astype(F32), p2[...].astype(F32),
              jnp.concatenate([p3a[...], p3b[...]], axis=1).astype(F32)]
    width = 4 * LANES
    mean = jnp.sum(pieces[0] + pieces[1] + pieces[2] + pieces[3], axis=1, keepdims=True) * (1.0 / width)
    pieces = [piece - mean for piece in pieces]
    squares = sum(piece * piece for piece in pieces)
    factor = lax.rsqrt(jnp.sum(squares, axis=1, keepdims=True) * (1.0 / width) + EPS)
    for r in range(4):
        at = pl.ds(pl.multiple_of((rank ^ r) * LANES, LANES), LANES)
        hat = pieces[r] * factor
        if r == 0:
            xhat[...] = hat
        normed[:, at] = (hat * gain[:, at] + bias[:, at]).astype(BF16)
    rstd[...] = jnp.broadcast_to(factor, (TILE, half))
    tokens = normed[...]

    wait_weights(tile, mine, w_in, w_out, sems, (0, 1, 2))
    cosine, sine = twice(cos_t[...]), twice(sin_t[...])
    query = dot_nn(tokens, w_in[:, 0:LANES])
    key = dot_nn(tokens, w_in[:, LANES:2 * LANES])
    value = dot_nn(tokens, w_in[:, 2 * LANES:3 * LANES]).astype(BF16)
    rq = query * cosine + partner(query) * sine
    rk = key * cosine + partner(key) * sine
    weight = feat_w[...]

    def logits(rows):
        high, low = split(rows)
        return dot_nn(high, mix_hi[...]) + dot_nn(low, mix_hi[...]) + dot_nn(high, mix_lo[...])

    positions = lens[1] + tile * TILE + iota((TILE, LANES), 0)
    real = (positions < lens[0]).astype(F32)
    qf = (weight * jnp.exp(logits(rq))).astype(BF16)
    kf = (weight * jnp.exp(logits(rk)) * real).astype(BF16)
    rq_o[...] = rq.astype(BF16)
    rk_o[...] = rk.astype(BF16)
    qf_o[...] = qf
    kf_o[...] = kf
    v_o[...] = value

    square = (TILE, TILE)
    lower = iota(square, 0) >= iota(square, 1)
    same = head_of(square, 0) == head_of(square, 1)
    cumulative = dot_nn(lower.astype(BF16), kf) + ksum[0:1, :]
    high, low = split(qf.astype(F32) * cumulative)
    ones = same.astype(BF16)
    inverse = 1.0 / (dot_nn(high, ones) + dot_nn(low, ones))
    prior = jnp.where(same, state[...], 0.0)
    prior_hi, prior_lo = split(prior)
    numer = dot_nn(qf, prior_hi) + dot_nn(qf, prior_lo)
    lane_head = head_of((TILE, LANES), 1)
    zero = jnp.zeros((TILE, LANES), BF16)
    for h in range(LANES // HEAD):
        here = lane_head == h
        scores = dot_nt(qf, jnp.where(here, kf, zero))
        scores = jnp.where(lower, scores, 0.0).astype(BF16)
        numer = numer + dot_nn(scores, jnp.where(here, value, zero))
    prior_s[0] = prior
    prior_k[0] = ksum[...]
    state[...] = state[...] + dot_tn(kf, value)
    ksum[...] = jnp.broadcast_to(cumulative[TILE - 1:TILE, :], ksum.shape)
    invz[...] = inverse
    attended = numer * inverse
    att_o[...] = attended
    hcat[:, 0:LANES] = attended.astype(BF16)

    wait_weights(tile, mine, w_in, w_out, sems, (3,))
    for c in range(4):
        cols = slice(c * LANES, (c + 1) * LANES)
        up = dot_nn(tokens, w_in[:, (3 + c) * LANES:(4 + c) * LANES])
        cdf = 0.5 * (1.0 + lax.erf(up * RSQRT2))
        hcat[:, (1 + c) * LANES:(2 + c) * LANES] = (up * cdf).astype(BF16)
        dgelu[:, cols] = (cdf + up * (RSQRT2PI * jnp.exp(-0.5 * up * up))).astype(BF16)

    wait_weights(tile, mine, w_in, w_out, sems, (4, 5))
    hidden = hcat[...]
    emit(rank, lambda at: dot_nn(hidden, w_out[:, at]), parts)


def emit(rank, product, parts):
    half = LANES // 2
    for r in range(4):
        at = pl.ds(pl.multiple_of((rank ^ r) * LANES, LANES), LANES)
        part = product(at)
        if len(parts) == 4:
            parts[r][...] = part.astype(parts[r].dtype)
            continue
        sx, sy, k0, ka, kb = parts
        if r == 0:
            k0[...] = part
        elif r == 1:
            sx[0] = part[:, :half].astype(BF16)
            kb[...] = part[:, half:]
        elif r == 2:
            ka[...] = part[:, :half]
            sy[0] = part[:, half:].astype(BF16)
        else:
            sx[1] = part[:, :half].astype(BF16)
            sy[1] = part[:, half:].astype(BF16)


def backward_kernel(carried, phased, *refs):
    refs = list(refs)
    take = lambda n: [refs.pop(0) for _ in range(n)]
    meta, = take(1)
    grad, normed, rq, rk, qf_i, kf_i, v_i, att_i, dgelu, invz, prior_s, prior_k, gain, bias, mix_hi, cos_t, sin_t = take(17)
    mine, other = take(4), take(4)
    if carried:
        state_in, gsum_in, dmix_in, fsum_in = take(4)
        take(2)
    parts = take(5 if phased else 4)
    stats, dcat, state, gsum, dmix, fsum = take(6)
    w_in, w_out, sems = take(3)
    step = pl.program_id(0)
    rank = meta[0]

    @pl.when(step == 0)
    def _():
        start_weights(meta, mine, other, w_in, w_out, sems, (4, 5, 0, 1, 2, 3))
        if carried:
            state[...] = state_in[...]
            gsum[...] = gsum_in[...]
            dmix[...] = dmix_in[...]
            fsum[...] = fsum_in[...]
        else:
            state[...] = jnp.zeros_like(state)
            gsum[...] = jnp.zeros_like(gsum)
            dmix[...] = jnp.zeros_like(dmix)
            fsum[...] = jnp.zeros_like(fsum)

    wait_weights(step, mine, w_in, w_out, sems, (4, 5))
    g = grad[...]
    d_att = dot_nt(g, w_out[0:LANES, :]).astype(BF16).astype(F32)
    square = (TILE, TILE)
    same = head_of(square, 0) == head_of(square, 1)
    ones = same.astype(BF16)
    inverse = invz[...]
    dn = (d_att * inverse).astype(BF16)
    dn32 = dn.astype(F32)
    high, low = split(dn32 * att_i[...])
    dden = -(dot_nn(high, ones) + dot_nn(low, ones))
    den_hi = dden.astype(BF16).astype(F32)
    roll_hi = pltpu.roll(den_hi, HEAD, 1)
    roll_lo = pltpu.roll(dden - den_hi, HEAD, 1)
    qf, kf, value = qf_i[...], kf_i[...], v_i[...]
    zero = jnp.zeros((TILE, LANES), BF16)
    one = jnp.ones((TILE, LANES), BF16)
    lane = iota((TILE, LANES), 1)
    lane_head = lane // HEAD
    below = iota(square, 0) >= iota(square, 1)
    above = iota(square, 0) <= iota(square, 1)
    prior_hi, prior_lo = split(prior_s[0])
    later_hi, later_lo = split(jnp.where(same, state[...], 0.0))
    d_qf = dot_nt(dn, prior_hi) + dot_nt(dn, prior_lo) + prior_k[0, 0:1, :] * dden
    d_kf = dot_nt(value, later_hi) + dot_nt(value, later_lo) + gsum[0:1, :]
    d_v = dot_nn(kf, later_hi)
    heads = LANES // HEAD
    for h in range(heads):
        here = lane_head == h
        spare = HEAD * ((h + 1) % heads)
        left = jnp.where(lane == spare, roll_hi, jnp.where(lane == spare + 1, roll_lo, dn32)).astype(BF16)
        right = jnp.where(here, value, jnp.where((lane == spare) | (lane == spare + 1), one, zero))
        k_here = jnp.where(here, kf, zero)
        q_here = jnp.where(here, qf, zero)
        d_here = jnp.where(here, dn, zero)
        scores_t = jnp.where(above, dot_nt(k_here, qf), 0.0).astype(BF16)
        ds = jnp.where(below, dot_nt(left, right), 0.0).astype(BF16)
        ds_t = jnp.where(above, dot_nt(right, left), 0.0).astype(BF16)
        d_qf = d_qf + dot_nn(ds, k_here)
        d_kf = d_kf + dot_nn(ds_t, q_here)
        d_v = d_v + dot_nn(scores_t, d_here)
    state[...] = state[...] + dot_tn(qf, dn)
    gsum[...] = gsum[...] + jnp.sum(qf.astype(F32) * dden, axis=0, keepdims=True)
    dlq = d_qf * qf.astype(F32)
    dlk = d_kf * kf.astype(F32)
    fsum[...] = fsum[...] + jnp.sum(dlq + dlk, axis=0, keepdims=True)
    dlq, dlk = dlq.astype(BF16), dlk.astype(BF16)
    dmix[...] = dmix[...] + dot_tn(rq[...], dlq) + dot_tn(rk[...], dlk)
    cosine, sine = twice(cos_t[...]), twice(sin_t[...])
    for c, dl in ((0, dlq), (1, dlk)):
        dr = dot_nt(dl, mix_hi[...])
        dcat[:, c * LANES:(c + 1) * LANES] = (dr * cosine - partner(dr) * sine).astype(BF16)
    dcat[:, 2 * LANES:3 * LANES] = d_v.astype(BF16)
    for c in range(4):
        cols = slice(c * LANES, (c + 1) * LANES)
        d_act = dot_nt(g, w_out[(1 + c) * LANES:(2 + c) * LANES, :])
        dcat[:, (3 + c) * LANES:(4 + c) * LANES] = (d_act * dgelu[:, cols].astype(F32)).astype(BF16)
    wait_weights(step, mine, w_in, w_out, sems, (0, 1, 2, 3))
    wide = dcat[...]
    row = iota((8, LANES), 0)
    first, second = (row == 0).astype(BF16), (row == 1).astype(BF16)
    totals = []

    def product(at):
        part = dot_nt(wide, w_in[at, :])
        one_side = (part * gain[:, at]).astype(BF16)
        other = (part * (normed[:, at].astype(F32) - bias[:, at])).astype(BF16)
        totals.append(dot_nt(first, one_side) + dot_nt(second, other))
        return part

    emit(rank, product, parts)
    stats[...] = totals[0] + totals[1] + totals[2] + totals[3]


def product_kernel(which, left, right, out):
    out[...] = dot_tn(left[...], right[...]).astype(BF16)


def join_kernel(meta, p0, p1, p2, p3a, p3b, whole):
    half = LANES // 2
    for r, piece in enumerate((p0, p1, p2)):
        whole[:, pl.ds(pl.multiple_of((meta[0] ^ r) * LANES, LANES), LANES)] = piece[...]
    at = pl.multiple_of((meta[0] ^ 3) * LANES, LANES)
    whole[:, pl.ds(at, half)] = p3a[...]
    whole[:, pl.ds(pl.multiple_of(at + half, half), half)] = p3b[...]


def partial_outs(rows, phased, row_of):
    half = LANES // 2
    if not phased:
        shapes = [jax.ShapeDtypeStruct((rows, LANES), F32)] + [jax.ShapeDtypeStruct((rows, LANES), BF16)] * 3
        return shapes, [pl.BlockSpec((TILE, LANES), lambda *i: (row_of(*i), 0))] * 4
    shapes = [jax.ShapeDtypeStruct((2, rows, half), BF16)] * 2 + [
        jax.ShapeDtypeStruct((rows, LANES), F32), jax.ShapeDtypeStruct((rows, half), F32),
        jax.ShapeDtypeStruct((rows, half), F32)]
    specs = [pl.BlockSpec((2, TILE, half), lambda *i: (0, row_of(*i), 0))] * 2 + [
        pl.BlockSpec((TILE, width), lambda *i: (row_of(*i), 0)) for width in (LANES, half, half)]
    return shapes, specs


def fixed(shape):
    return pl.BlockSpec(shape, lambda *i: (0,) * len(shape))


def outside(count):
    return [pl.BlockSpec(memory_space=pl.ANY)] * count


def params(size):
    return pltpu.CompilerParams(dimension_semantics=("arbitrary",), vmem_limit_bytes=size << 20)


def weight_scratch(width):
    return [pltpu.VMEM((width, 3 * LANES + width), BF16), pltpu.VMEM((LANES + width, width), BF16),
            pltpu.SemaphoreType.DMA((6,))]


def forward_layer(meta, lens, pieces, weights, tables, length, first_row, phased, carry=None):
    rows = pieces[0].shape[0]
    tiles, before = rows // TILE, first_row // TILE
    half, width = LANES // 2, 4 * LANES
    local = lambda t, *_: t
    there = lambda t, *_: before + t
    by_row = lambda n, row_of: pl.BlockSpec((TILE, n), lambda *i: (row_of(*i), 0))
    (gain, bias, mix_hi, mix_lo, feat_w), mine, other = weights
    small = (gain, bias, mix_hi, mix_lo, feat_w)
    shapes, specs = partial_outs(rows, phased, local)
    extra = [(width, BF16), (LANES, F32), (half, F32)] + [(LANES, BF16)] * 5 + [
        (LANES + width, BF16), (width, BF16), (LANES, F32), (LANES, F32)]
    shapes += [jax.ShapeDtypeStruct((length, n), d) for n, d in extra]
    specs += [by_row(n, there) for n, _ in extra]
    shapes += [jax.ShapeDtypeStruct((length // TILE, LANES, LANES), F32), jax.ShapeDtypeStruct((length // TILE, 8, LANES), F32)]
    specs += [pl.BlockSpec((1, n, LANES), lambda *i: (there(*i), 0, 0)) for n in (LANES, 8)]
    states = [(LANES, LANES), (8, LANES)]
    shapes += [jax.ShapeDtypeStruct(s, F32) for s in states]
    specs += [fixed(s) for s in states]
    operands = [meta, jnp.stack([lens[0], jnp.int32(first_row)]), *pieces, *small, *tables, *mine, *other]
    in_specs = [by_row(p.shape[1], local) for p in pieces] + [fixed(w.shape) for w in small] + [by_row(half, there)] * 2 + outside(8)
    aliases = {}
    if carry is not None:
        state, saved = carry
        operands += [*state, *saved]
        in_specs += [fixed(s) for s in states] + outside(SAVED)
        aliases = {len(operands) - SAVED + i: len(shapes) - 2 - SAVED + i for i in range(SAVED)}
    outs = pl.pallas_call(
        functools.partial(forward_kernel, carry is not None, phased),
        name="layer_forward",
        out_shape=shapes,
        grid_spec=pltpu.PrefetchScalarGridSpec(
            num_scalar_prefetch=2, grid=(tiles,), in_specs=in_specs, out_specs=specs, scratch_shapes=weight_scratch(width)),
        input_output_aliases=aliases,
        compiler_params=params(56),
        cost_estimate=pl.CostEstimate(flops=rows * 20_000_000, transcendentals=rows * 5000, bytes_accessed=24 << 20),
    )(*operands)
    count = 5 if phased else 4
    return outs[:count], outs[count:count + SAVED], outs[count + SAVED:]


def backward_layer(meta, grad, saved, weights, tables, length, first_row, phased, carry=None):
    rows = grad.shape[0]
    tiles, before = rows // TILE, first_row // TILE
    half, width = LANES // 2, 4 * LANES
    local = lambda t, *_: tiles - 1 - t
    there = lambda t, *_: before + tiles - 1 - t
    by_row = lambda n, row_of=there: pl.BlockSpec((TILE, n), lambda *i: (row_of(*i), 0))
    normed, rq, rk, qf, kf, value, hcat, dgelu, invz, attended, prior_s, prior_k = saved
    (gain, bias, mix_hi, mix_lo, feat_w), mine, other = weights
    shapes, specs = partial_outs(rows, phased, local)
    shapes += [jax.ShapeDtypeStruct((8, length), F32), jax.ShapeDtypeStruct((length, 3 * LANES + width), BF16)]
    specs += [pl.BlockSpec((8, TILE), lambda *i: (0, there(*i))), by_row(3 * LANES + width)]
    states = [(LANES, LANES), (8, LANES)] * 2
    shapes += [jax.ShapeDtypeStruct(s, F32) for s in states]
    specs += [fixed(s) for s in states]
    operands = [meta, grad, normed, rq, rk, qf, kf, value, attended, dgelu, invz, prior_s, prior_k, gain, bias, mix_hi, *tables,
                *mine, *other]
    in_specs = [by_row(width, local), by_row(width)] + [by_row(LANES)] * 6 + [by_row(width), by_row(LANES)] + [
        pl.BlockSpec((1, n, LANES), lambda *i: (there(*i), 0, 0)) for n in (LANES, 8)] + [
        fixed(w.shape) for w in (gain, bias, mix_hi)] + [by_row(half)] * 2 + outside(8)
    aliases = {}
    if carry is not None:
        state, arrays = carry
        operands += [*state, *arrays]
        in_specs += [fixed(s) for s in states] + outside(2)
        aliases = {len(operands) - 2 + i: len(shapes) - 6 + i for i in range(2)}
    outs = pl.pallas_call(
        functools.partial(backward_kernel, carry is not None, phased),
        name="layer_backward",
        out_shape=shapes,
        grid_spec=pltpu.PrefetchScalarGridSpec(
            num_scalar_prefetch=1, grid=(tiles,), in_specs=in_specs, out_specs=specs, scratch_shapes=weight_scratch(width)),
        input_output_aliases=aliases,
        compiler_params=params(56),
        cost_estimate=pl.CostEstimate(flops=rows * 25_000_000, transcendentals=0, bytes_accessed=24 << 20),
    )(*operands)
    count = 5 if phased else 4
    return outs[:count], outs[count:count + 2], outs[count + 2:]


def join(meta, pieces):
    rows, block = pieces[0].shape[0], 2 * TILE
    return pl.pallas_call(
        join_kernel,
        name="join",
        out_shape=jax.ShapeDtypeStruct((rows, 4 * LANES), BF16),
        grid_spec=pltpu.PrefetchScalarGridSpec(
            num_scalar_prefetch=1,
            grid=(rows // block,),
            in_specs=[pl.BlockSpec((block, p.shape[1]), lambda i, *_: (i, 0)) for p in pieces],
            out_specs=pl.BlockSpec((block, 4 * LANES), lambda i, *_: (i, 0)),
        ),
        compiler_params=params(8),
        cost_estimate=pl.CostEstimate(flops=0, transcendentals=0, bytes_accessed=rows * 16 * LANES),
    )(meta, *pieces)


def swap(value, axis, by):
    return lax.ppermute(value, axis, [(k, k ^ by) for k in range(lax.axis_size(axis))])


def gather_pieces(shard, meanwhile=()):
    half = shard.shape[1] // 2
    from_x, from_y = after((swap(shard, "mp", 1), swap(shard, "mp", 2)), *meanwhile)
    return shard, from_x, from_y, swap(from_x[:, :half], "mp", 2), swap(from_y[:, half:], "mp", 1)


def after(values, *others):
    if not others:
        return values
    return lax.optimization_barrier((values, others))[0]


def direct_sends(parts):
    return parts[0], [swap(part, "mp", r) for r, part in enumerate(parts) if r > 0]


def scatter_start(parts):
    return swap(parts[0], "mp", 1), swap(parts[1], "mp", 2)


def scatter_turn(parts, arrived):
    _, _, _, ka, kb = parts
    in_x, in_y = arrived
    return (ka + in_x[1].astype(F32)).astype(BF16), (kb + in_y[1].astype(F32)).astype(BF16)


def scatter_end(parts, arrived, to_y, to_x):
    _, _, k0, ka, _ = parts
    in_x, in_y = arrived
    half = ka.shape[1]
    last_y, last_x = swap(to_y, "mp", 2), swap(to_x, "mp", 1)
    return jnp.concatenate(
        [k0[:, :half] + in_x[0].astype(F32) + last_y.astype(F32), k0[:, half:] + in_y[0].astype(F32) + last_x.astype(F32)],
        axis=1)


def scatter_sum(parts):
    arrived = scatter_start(parts)
    return scatter_end(parts, arrived, *scatter_turn(parts, arrived))


def mp_total(values):
    return values + swap(values, "mp", 1) + swap(values, "mp", 2) + swap(values, "mp", 3)


def ring_scatter(block_of, axis, meanwhile=()):
    count = lax.axis_size(axis)
    rank = lax.axis_index(axis)
    pairs = [(k, (k + 1) % count) for k in range(count)]
    total = block_of((rank + count - 1) % count)
    for step in range(2, count + 1):
        arrived = after(lax.ppermute(total, axis, pairs), *meanwhile)
        total = (arrived.astype(F32) + block_of((rank + count - step) % count).astype(F32)).astype(BF16)
        yield arrived, total


def dp_total(values):
    count = lax.axis_size("dp")
    if count > 8:
        return lax.psum(values, "dp")
    sent = [lax.ppermute(values, "dp", [(i, (i + k) % count) for i in range(count)]) for k in range(1, count)]
    return sum(sent, values)


def block_sends(block_of, axis):
    count = lax.axis_size(axis)
    rank = lax.axis_index(axis)
    if count > 8:
        return [list(ring_scatter(block_of, axis))[-1][1]]
    return [block_of(rank)] + [
        lax.ppermute(block_of((rank + k) % count), axis, [(i, (i + k) % count) for i in range(count)]) for k in range(1, count)]


def sum_blocks(blocks):
    total = blocks[0].astype(F32)
    for block in blocks[1:]:
        total = total + block.astype(F32)
    return total.astype(BF16)


def weight_gradient(left, right, cut_left, section):
    rows = left.shape[0]
    m, n = left.shape[1] // (2 if cut_left else 1), right.shape[1] // (1 if cut_left else 2)
    block = 128 if cut_left else 256
    steps = m // block
    left_at = (lambda i, which: (0, which[0] * steps + i)) if cut_left else (lambda i, which: (0, i))
    right_at = (lambda i, which: (0, 0)) if cut_left else (lambda i, which: (0, which[0]))

    def product(which):
        return pl.pallas_call(
            product_kernel,
            name="weight_gradient",
            out_shape=jax.ShapeDtypeStruct((m, n), BF16),
            grid_spec=pltpu.PrefetchScalarGridSpec(
                num_scalar_prefetch=1, grid=(steps,),
                in_specs=[pl.BlockSpec((rows, block), left_at), pl.BlockSpec((rows, n), right_at)],
                out_specs=pl.BlockSpec((block, n), lambda i, which: (i, 0))),
            compiler_params=params(58),
            cost_estimate=pl.CostEstimate(flops=2 * rows * m * n, transcendentals=0, bytes_accessed=2 * (rows * (m + n) + m * n)),
        )(which.reshape(1).astype(jnp.int32), left, right)

    arrived = swap(product(1 - section), "section", 1)
    return product(section), arrived


def dct_table(order):
    row_index = jnp.arange(order, dtype=F32)[:, None]
    col_index = jnp.arange(order, dtype=F32)[None, :]
    cosines = jnp.sqrt(2.0 / order) * jnp.cos(math.pi * (row_index + 0.5) * col_index / order)
    return cosines * jnp.where(col_index == 0, math.sqrt(0.5), 1.0)


def rotary_tables(length):
    column = jnp.arange(LANES // 2, dtype=jnp.int32) % HEAD
    half = ROT // 2
    index = (column % half).astype(F32)
    angles = jnp.arange(length, dtype=F32)[:, None] * (10000.0 ** (-index * 2.0 / ROT))[None, :]
    turned = (column < ROT)[None, :]
    sign = jnp.where(column < half, -1.0, 1.0)[None, :]
    return jnp.where(turned, jnp.cos(angles), 1.0), jnp.where(turned, sign * jnp.sin(angles), 0.0)


def shards(block_input, cotangent, lengths, ln_gain, ln_bias, w_qkv, w_out, w_up, w_down, freq_table, feat_weight):
    section = lax.axis_index("section")
    place = lax.axis_index("mp")
    group = lax.axis_index("dp")
    groups = lax.axis_size("dp")
    local_slots, length, shard_width = block_input.shape
    width = ln_gain.shape[1]
    heads = freq_table.shape[1]
    is_first = section == 0
    lens = lax.dynamic_slice_in_dim(lengths, section, 1, 0)
    metas = [jnp.stack([place, (section == l).astype(jnp.int32)]).astype(jnp.int32) for l in range(2)]

    def own(values):
        return lax.dynamic_index_in_dim(values, section, 0, keepdims=False)

    shard0 = own(block_input)
    pieces0 = gather_pieces(shard0)

    small = jnp.concatenate([ln_gain[0], ln_bias[0], feat_weight.reshape(-1), freq_table.astype(F32).reshape(-1)])
    small_other = swap(small, "section", 1)
    mine = (w_qkv, w_up, w_out, w_down)
    other = tuple(swap(w, "section", 1) for w in mine)

    def both(mine, other):
        return jnp.where(is_first, mine, other), jnp.where(is_first, other, mine)

    layers_small = both(small, small_other)
    table = dct_table(HEAD)
    eye = jnp.eye(heads, dtype=F32)

    def layer_weights(l):
        vec = layers_small[l]
        gain, bias = vec[:width].reshape(1, width), vec[width:2 * width].reshape(1, width)
        feat = vec[2 * width:2 * width + LANES].reshape(1, LANES)
        freq = vec[2 * width + LANES:].reshape(heads, HEAD, HEAD)
        mixed = jnp.einsum("nk,hkm->hnm", table, freq, precision=lax.Precision.HIGHEST)
        mixed = (eye[:, None, :, None] * mixed[:, :, None, :]).reshape(LANES, LANES)
        high = lax.reduce_precision(mixed, 8, 7)
        return (gain, bias, high.astype(BF16), (mixed - high).astype(BF16), feat), mine, other

    weights0, weights1 = layer_weights(0), layer_weights(1)
    tables = rotary_tables(length)

    cot = after(own(cotangent), pieces0[3], pieces0[4])
    cot_x, cot_y = swap(cot, "mp", 1), swap(cot, "mp", 2)
    part0, all0, _ = forward_layer(metas[0], lens, pieces0, weights0, tables, length, 0, True)
    part0 = after(part0, cot_x, cot_y)
    hidden = (shard0.astype(F32) + scatter_sum(part0)).astype(BF16)
    pieces1 = gather_pieces(hidden)
    cot_x, cot_y = after((cot_x, cot_y), pieces1[3], pieces1[4])
    half = shard_width // 2
    pieces_g = cot, cot_x, cot_y, swap(cot_x[:, :half], "mp", 2), swap(cot_y[:, half:], "mp", 1)
    part1, all1, _ = forward_layer(metas[1], lens, pieces1, weights1, tables, length, 0, False)
    out_kept, out_sent = direct_sends(part1)

    def saved_of(arrays):
        return (arrays[0],) + tuple(arrays[3:])

    def in_block(mine, arrived):
        n = mine.shape[0] // groups
        cut = lambda v, i: lax.dynamic_slice_in_dim(v, i * n, n, 0)
        return lambda i: (cut(mine, i).astype(F32) + cut(arrived, i).astype(F32)).astype(BF16)

    def out_block(mine, arrived):
        n = mine.shape[1] // groups
        cut = lambda v, i: lax.dynamic_slice_in_dim(v, i * n, n, 1)
        return lambda i: (cut(mine, i).astype(F32) + cut(arrived, i).astype(F32)).astype(BF16)

    def run_backward(meta, grad, saved, weights, phased):
        parts, (stats, dcat), (_, _, dmix, fsum) = backward_layer(meta, grad, saved, weights, tables, length, 0, phased)
        return parts, stats, dcat, dmix, fsum

    def norm_backward(grad_shard, d_normed, sums, norm, gain_all):
        xhat, rstd = norm
        gain = lax.dynamic_slice_in_dim(gain_all, place * shard_width, shard_width, 1)
        mean_d = (sums[0] * (1.0 / width))[:, None]
        mean_dx = (sums[1] * (1.0 / width))[:, None]
        return grad_shard.astype(F32) + rstd[:, :1] * (d_normed * gain - mean_d - xhat * mean_dx)

    def small_gradients(d_normed, norm, dmix, fsum):
        gain_part = jnp.sum(d_normed * norm[0], axis=0)
        bias_part = jnp.sum(d_normed, axis=0)
        diagonal = jnp.stack([dmix[h * HEAD:(h + 1) * HEAD, h * HEAD:(h + 1) * HEAD] for h in range(heads)])
        return jnp.concatenate([gain_part, bias_part, fsum[0], diagonal.reshape(-1)])

    saved1, saved0 = saved_of(all1), saved_of(all0)
    grad1 = join(metas[1], pieces_g)
    out_blocks1 = block_sends(out_block(*weight_gradient(saved1[6], grad1, True, section)), "dp")
    grad1_b = after(grad1, out_blocks1[0])
    parts, stats, dcat1, dmix1, fsum1 = run_backward(metas[1], grad1_b, saved1, weights1, True)
    parts, stats, dcat1, dmix1, fsum1 = after((parts, stats, dcat1, dmix1, fsum1), *out_blocks1, *out_sent)
    arrived = scatter_start(parts)
    turn = scatter_turn(parts, arrived)
    steps1 = list(ring_scatter(in_block(*weight_gradient(saved1[0], dcat1, False, section)), "dp"))
    arrivals1, red_in1 = [arrival for arrival, _ in steps1], steps1[-1][1]
    d_normed = scatter_end(parts, arrived, *turn)
    sums = mp_total(after(stats, *turn))
    g0 = norm_backward(cot, d_normed, sums, all1[1:3], weights1[0][0]).astype(BF16)
    small1 = small_gradients(d_normed, all1[1:3], dmix1, fsum1)
    pieces_g0 = gather_pieces(after(g0, arrivals1[0]), arrivals1[1:2])
    pieces_g0 = after(pieces_g0, *arrivals1[2:3])
    out = hidden.astype(F32) + out_kept + out_sent[0].astype(F32) + out_sent[1].astype(F32) + out_sent[2].astype(F32)

    grad0 = join(metas[0], pieces_g0)
    out_blocks0 = block_sends(out_block(*weight_gradient(saved0[6], grad0, True, section)), "dp")
    grad0_b = after(grad0, out_blocks0[0])
    parts, stats, dcat0, dmix0, fsum0 = run_backward(metas[0], grad0_b, saved0, weights0, False)
    parts, stats, dcat0, dmix0, fsum0 = after((parts, stats, dcat0, dmix0, fsum0), *out_blocks0)
    out_blocks1 = after(out_blocks1, dcat0)
    kept, sent = direct_sends(parts)
    mine0, arrived0 = weight_gradient(saved0[0], dcat0, False, section)
    block0 = in_block(mine0, arrived0)
    steps0 = list(ring_scatter(block0, "dp", sent))
    sums = mp_total(after(stats, steps0[0][0]))
    sent, dmix0, out_blocks0, out_blocks1 = after((sent, dmix0, out_blocks0, out_blocks1), steps0[0][0])
    d_normed = kept + sent[0].astype(F32) + sent[1].astype(F32) + sent[2].astype(F32)
    d_input = norm_backward(g0, d_normed, sums, all0[1:3], weights0[0][0])
    small0 = small_gradients(d_normed, all0[1:3], dmix0, fsum0)

    def to_owner(first, second, axis):
        mine, other = both(first, second)
        arrived = swap(other, "section", 1)
        return jnp.where(is_first, jnp.concatenate([mine, arrived], axis), jnp.concatenate([arrived, mine], axis)).astype(F32)

    grads_out = to_owner(sum_blocks(out_blocks0), sum_blocks(out_blocks1), 0)
    small_mine, small_send = both(small0, small1)
    small_sum = dp_total(small_mine + swap(small_send, "section", 1))
    feat_grad = small_sum[2 * shard_width:2 * shard_width + LANES].reshape(heads, HEAD) / feat_weight[0]
    freq_grad = jnp.einsum("nk,hnm->hkm", table, small_sum[2 * shard_width + LANES:].reshape(heads, HEAD, HEAD),
                           precision=lax.Precision.HIGHEST)
    keep, send = both(d_input, out)
    arrived = swap(send, "section", 1)
    boundary = jnp.where(is_first, jnp.stack([keep, arrived]), jnp.stack([arrived, keep]))
    grads_in = to_owner(steps0[-1][1], red_in1, 1)
    qkv_grad = jnp.stack([grads_in[:, t * shard_width:(t + 1) * shard_width] for t in range(3)])
    return (
        boundary[None],
        small_sum[None, :shard_width],
        small_sum[None, shard_width:2 * shard_width],
        qkv_grad[None],
        grads_out[None, :shard_width],
        grads_in[None, :, 3 * shard_width:],
        grads_out[None, shard_width:],
        freq_grad[None],
        feat_grad[None],
    )


def solution(mesh):
    placed = (
        P("dp", None, "mp"), P("dp", None, "mp"), P("dp"), P("section", None), P("section", None),
        P("section", None, None, "mp"), P("section", "mp", None), P("section", None, "mp"), P("section", "mp", None),
        P("section", "mp", None, None), P("section", "mp", None),
    )
    return jax.shard_map(
        shards,
        mesh=mesh,
        in_specs=placed,
        out_specs=(
            P("section", "dp", None, "mp"), P("section", "mp"), P("section", "mp"), P("section", None, "dp", "mp"),
            P("section", "mp", "dp"), P("section", "dp", "mp"), P("section", "mp", "dp"), P("section", "mp", None, None),
            P("section", "mp", None),
        ),
        check_vma=False,
    )
```

```python
import functools
import math

import jax
import jax.numpy as jnp
from jax import lax
from jax.experimental import pallas as pl
from jax.experimental.pallas import tpu as pltpu
from jax.sharding import PartitionSpec as P

ROT = 16
TILE = 256
HEAD = 64
LANES = 256
EPS = 1e-05
F32 = jnp.float32
BF16 = jnp.bfloat16
RSQRT2 = math.sqrt(0.5)
RSQRT2PI = 1.0 / math.sqrt(2.0 * math.pi)
SAVED = 14


def dot_nn(a, b):
    return lax.dot_general(a, b, (((1,), (0,)), ((), ())), preferred_element_type=F32)


def dot_nt(a, b):
    return lax.dot_general(a, b, (((1,), (1,)), ((), ())), preferred_element_type=F32)


def dot_tn(a, b):
    return lax.dot_general(a, b, (((0,), (0,)), ((), ())), preferred_element_type=F32)


def split(values):
    high = values.astype(BF16)
    return high, (values - high.astype(F32)).astype(BF16)


def iota(shape, dim):
    return lax.broadcasted_iota(jnp.int32, shape, dim)


def partner(values):
    later = pltpu.roll(values, LANES - ROT // 2, 1)
    earlier = pltpu.roll(values, ROT // 2, 1)
    lower = iota(values.shape, 1) % HEAD < ROT // 2
    return jnp.where(lower, later, earlier)


def twice(table):
    return jnp.concatenate([table, table], axis=1)


def head_of(shape, dim):
    return iota(shape, dim) // HEAD


def weight_copies(refs, w_in, w_out, sems, which):
    qkv, up, out, down = refs
    ends = [(qkv.at[0, t], w_in.at[:, t * LANES:(t + 1) * LANES]) for t in range(3)] + [
        (up.at[0], w_in.at[:, 3 * LANES:]), (out.at[0], w_out.at[0:LANES, :]), (down.at[0], w_out.at[LANES:, :])]
    return [pltpu.make_async_copy(*ends[i], sems.at[i]) for i in which]


def start_weights(meta, mine, other, w_in, w_out, sems, order):
    def start(refs):
        for copy in weight_copies(refs, w_in, w_out, sems, order):
            copy.start()

    @pl.when(meta[1] == 1)
    def _():
        start(mine)

    @pl.when(meta[1] != 1)
    def _():
        start(other)


def wait_weights(step, refs, w_in, w_out, sems, which):
    @pl.when(step == 0)
    def _():
        for copy in weight_copies(refs, w_in, w_out, sems, which):
            copy.wait()


def forward_kernel(carried, phased, *refs):
    refs = list(refs)
    take = lambda n: [refs.pop(0) for _ in range(n)]
    meta, lens = take(2)
    p0, p1, p2, p3a, p3b, gain, bias, mix_hi, mix_lo, feat_w, cos_t, sin_t = take(12)
    mine, other = take(4), take(4)
    if carried:
        state_in, ksum_in = take(2)
        take(SAVED)
    parts = take(5 if phased else 4)
    normed, xhat, rstd, rq_o, rk_o, qf_o, kf_o, v_o, hcat, dgelu, invz, att_o, prior_s, prior_k = take(SAVED)
    state, ksum, w_in, w_out, sems = take(5)
    tile = pl.program_id(0)
    rank = meta[0]
    half = LANES // 2

    @pl.when(tile == 0)
    def _():
        start_weights(meta, mine, other, w_in, w_out, sems, (0, 1, 2, 3, 4, 5))
        if carried:
            state[...] = state_in[...]
            ksum[...] = ksum_in[...]
        else:
            state[...] = jnp.zeros_like(state)
            ksum[...] = jnp.zeros_like(ksum)

    pieces = [p0[...].astype(F32), p1[...].astype(F32), p2[...].astype(F32),
              jnp.concatenate([p3a[...], p3b[...]], axis=1).astype(F32)]
    width = 4 * LANES
    mean = jnp.sum(pieces[0] + pieces[1] + pieces[2] + pieces[3], axis=1, keepdims=True) * (1.0 / width)
    pieces = [piece - mean for piece in pieces]
    squares = sum(piece * piece for piece in pieces)
    factor = lax.rsqrt(jnp.sum(squares, axis=1, keepdims=True) * (1.0 / width) + EPS)
    for r in range(4):
        at = pl.ds(pl.multiple_of((rank ^ r) * LANES, LANES), LANES)
        hat = pieces[r] * factor
        if r == 0:
            xhat[...] = hat
        normed[:, at] = (hat * gain[:, at] + bias[:, at]).astype(BF16)
    rstd[...] = jnp.broadcast_to(factor, (TILE, half))
    tokens = normed[...]

    wait_weights(tile, mine, w_in, w_out, sems, (0, 1, 2))
    cosine, sine = twice(cos_t[...]), twice(sin_t[...])
    query = dot_nn(tokens, w_in[:, 0:LANES])
    key = dot_nn(tokens, w_in[:, LANES:2 * LANES])
    value = dot_nn(tokens, w_in[:, 2 * LANES:3 * LANES]).astype(BF16)
    rq = query * cosine + partner(query) * sine
    rk = key * cosine + partner(key) * sine
    weight = feat_w[...]

    def logits(rows):
        high, low = split(rows)
        return dot_nn(high, mix_hi[...]) + dot_nn(low, mix_hi[...]) + dot_nn(high, mix_lo[...])

    positions = lens[1] + tile * TILE + iota((TILE, LANES), 0)
    real = (positions < lens[0]).astype(F32)
    qf = (weight * jnp.exp(logits(rq))).astype(BF16)
    kf = (weight * jnp.exp(logits(rk)) * real).astype(BF16)
    rq_o[...] = rq.astype(BF16)
    rk_o[...] = rk.astype(BF16)
    qf_o[...] = qf
    kf_o[...] = kf
    v_o[...] = value

    square = (TILE, TILE)
    lower = iota(square, 0) >= iota(square, 1)
    same = head_of(square, 0) == head_of(square, 1)
    cumulative = dot_nn(lower.astype(BF16), kf) + ksum[0:1, :]
    high, low = split(qf.astype(F32) * cumulative)
    ones = same.astype(BF16)
    inverse = 1.0 / (dot_nn(high, ones) + dot_nn(low, ones))
    prior = jnp.where(same, state[...], 0.0)
    prior_hi, prior_lo = split(prior)
    numer = dot_nn(qf, prior_hi) + dot_nn(qf, prior_lo)
    lane_head = head_of((TILE, LANES), 1)
    zero = jnp.zeros((TILE, LANES), BF16)
    for h in range(LANES // HEAD):
        here = lane_head == h
        scores = dot_nt(qf, jnp.where(here, kf, zero))
        scores = jnp.where(lower, scores, 0.0).astype(BF16)
        numer = numer + dot_nn(scores, jnp.where(here, value, zero))
    prior_s[0] = prior
    prior_k[0] = ksum[...]
    state[...] = state[...] + dot_tn(kf, value)
    ksum[...] = jnp.broadcast_to(cumulative[TILE - 1:TILE, :], ksum.shape)
    invz[...] = inverse
    attended = numer * inverse
    att_o[...] = attended
    hcat[:, 0:LANES] = attended.astype(BF16)

    wait_weights(tile, mine, w_in, w_out, sems, (3,))
    for c in range(4):
        cols = slice(c * LANES, (c + 1) * LANES)
        up = dot_nn(tokens, w_in[:, (3 + c) * LANES:(4 + c) * LANES])
        cdf = 0.5 * (1.0 + lax.erf(up * RSQRT2))
        hcat[:, (1 + c) * LANES:(2 + c) * LANES] = (up * cdf).astype(BF16)
        dgelu[:, cols] = (cdf + up * (RSQRT2PI * jnp.exp(-0.5 * up * up))).astype(BF16)

    wait_weights(tile, mine, w_in, w_out, sems, (4, 5))
    hidden = hcat[...]
    emit(rank, lambda at: dot_nn(hidden, w_out[:, at]), parts)


def emit(rank, product, parts):
    half = LANES // 2
    for r in range(4):
        at = pl.ds(pl.multiple_of((rank ^ r) * LANES, LANES), LANES)
        part = product(at)
        if len(parts) == 4:
            parts[r][...] = part.astype(parts[r].dtype)
            continue
        sx, sy, k0, ka, kb = parts
        if r == 0:
            k0[...] = part
        elif r == 1:
            sx[0] = part[:, :half].astype(BF16)
            kb[...] = part[:, half:]
        elif r == 2:
            ka[...] = part[:, :half]
            sy[0] = part[:, half:].astype(BF16)
        else:
            sx[1] = part[:, :half].astype(BF16)
            sy[1] = part[:, half:].astype(BF16)


def backward_kernel(carried, phased, *refs):
    refs = list(refs)
    take = lambda n: [refs.pop(0) for _ in range(n)]
    meta, = take(1)
    grad, normed, rq, rk, qf_i, kf_i, v_i, att_i, dgelu, invz, prior_s, prior_k, gain, bias, mix_hi, cos_t, sin_t = take(17)
    mine, other = take(4), take(4)
    if carried:
        state_in, gsum_in, dmix_in, fsum_in = take(4)
        take(2)
    parts = take(5 if phased else 4)
    stats, dcat, state, gsum, dmix, fsum = take(6)
    w_in, w_out, sems = take(3)
    step = pl.program_id(0)
    rank = meta[0]

    @pl.when(step == 0)
    def _():
        start_weights(meta, mine, other, w_in, w_out, sems, (4, 5, 0, 1, 2, 3))
        if carried:
            state[...] = state_in[...]
            gsum[...] = gsum_in[...]
            dmix[...] = dmix_in[...]
            fsum[...] = fsum_in[...]
        else:
            state[...] = jnp.zeros_like(state)
            gsum[...] = jnp.zeros_like(gsum)
            dmix[...] = jnp.zeros_like(dmix)
            fsum[...] = jnp.zeros_like(fsum)

    wait_weights(step, mine, w_in, w_out, sems, (4, 5))
    g = grad[...]
    d_att = dot_nt(g, w_out[0:LANES, :]).astype(BF16).astype(F32)
    square = (TILE, TILE)
    same = head_of(square, 0) == head_of(square, 1)
    ones = same.astype(BF16)
    inverse = invz[...]
    dn = (d_att * inverse).astype(BF16)
    dn32 = dn.astype(F32)
    high, low = split(dn32 * att_i[...])
    dden = -(dot_nn(high, ones) + dot_nn(low, ones))
    den_hi = dden.astype(BF16).astype(F32)
    roll_hi = pltpu.roll(den_hi, HEAD, 1)
    roll_lo = pltpu.roll(dden - den_hi, HEAD, 1)
    qf, kf, value = qf_i[...], kf_i[...], v_i[...]
    zero = jnp.zeros((TILE, LANES), BF16)
    one = jnp.ones((TILE, LANES), BF16)
    lane = iota((TILE, LANES), 1)
    lane_head = lane // HEAD
    below = iota(square, 0) >= iota(square, 1)
    above = iota(square, 0) <= iota(square, 1)
    prior_hi, prior_lo = split(prior_s[0])
    later_hi, later_lo = split(jnp.where(same, state[...], 0.0))
    d_qf = dot_nt(dn, prior_hi) + dot_nt(dn, prior_lo) + prior_k[0, 0:1, :] * dden
    d_kf = dot_nt(value, later_hi) + dot_nt(value, later_lo) + gsum[0:1, :]
    d_v = dot_nn(kf, later_hi)
    heads = LANES // HEAD
    for h in range(heads):
        here = lane_head == h
        spare = HEAD * ((h + 1) % heads)
        left = jnp.where(lane == spare, roll_hi, jnp.where(lane == spare + 1, roll_lo, dn32)).astype(BF16)
        right = jnp.where(here, value, jnp.where((lane == spare) | (lane == spare + 1), one, zero))
        k_here = jnp.where(here, kf, zero)
        q_here = jnp.where(here, qf, zero)
        d_here = jnp.where(here, dn, zero)
        scores_t = jnp.where(above, dot_nt(k_here, qf), 0.0).astype(BF16)
        ds = jnp.where(below, dot_nt(left, right), 0.0).astype(BF16)
        ds_t = jnp.where(above, dot_nt(right, left), 0.0).astype(BF16)
        d_qf = d_qf + dot_nn(ds, k_here)
        d_kf = d_kf + dot_nn(ds_t, q_here)
        d_v = d_v + dot_nn(scores_t, d_here)
    state[...] = state[...] + dot_tn(qf, dn)
    gsum[...] = gsum[...] + jnp.sum(qf.astype(F32) * dden, axis=0, keepdims=True)
    dlq = d_qf * qf.astype(F32)
    dlk = d_kf * kf.astype(F32)
    fsum[...] = fsum[...] + jnp.sum(dlq + dlk, axis=0, keepdims=True)
    dlq, dlk = dlq.astype(BF16), dlk.astype(BF16)
    dmix[...] = dmix[...] + dot_tn(rq[...], dlq) + dot_tn(rk[...], dlk)
    cosine, sine = twice(cos_t[...]), twice(sin_t[...])
    for c, dl in ((0, dlq), (1, dlk)):
        dr = dot_nt(dl, mix_hi[...])
        dcat[:, c * LANES:(c + 1) * LANES] = (dr * cosine - partner(dr) * sine).astype(BF16)
    dcat[:, 2 * LANES:3 * LANES] = d_v.astype(BF16)
    for c in range(4):
        cols = slice(c * LANES, (c + 1) * LANES)
        d_act = dot_nt(g, w_out[(1 + c) * LANES:(2 + c) * LANES, :])
        dcat[:, (3 + c) * LANES:(4 + c) * LANES] = (d_act * dgelu[:, cols].astype(F32)).astype(BF16)
    wait_weights(step, mine, w_in, w_out, sems, (0, 1, 2, 3))
    wide = dcat[...]
    row = iota((8, LANES), 0)
    first, second = (row == 0).astype(BF16), (row == 1).astype(BF16)
    totals = []

    def product(at):
        part = dot_nt(wide, w_in[at, :])
        one_side = (part * gain[:, at]).astype(BF16)
        other = (part * (normed[:, at].astype(F32) - bias[:, at])).astype(BF16)
        totals.append(dot_nt(first, one_side) + dot_nt(second, other))
        return part

    emit(rank, product, parts)
    stats[...] = totals[0] + totals[1] + totals[2] + totals[3]


def product_kernel(which, left, right, out):
    out[...] = dot_tn(left[...], right[...]).astype(BF16)


def join_kernel(meta, p0, p1, p2, p3a, p3b, whole):
    half = LANES // 2
    for r, piece in enumerate((p0, p1, p2)):
        whole[:, pl.ds(pl.multiple_of((meta[0] ^ r) * LANES, LANES), LANES)] = piece[...]
    at = pl.multiple_of((meta[0] ^ 3) * LANES, LANES)
    whole[:, pl.ds(at, half)] = p3a[...]
    whole[:, pl.ds(pl.multiple_of(at + half, half), half)] = p3b[...]


def partial_outs(rows, phased, row_of):
    half = LANES // 2
    if not phased:
        shapes = [jax.ShapeDtypeStruct((rows, LANES), F32)] + [jax.ShapeDtypeStruct((rows, LANES), BF16)] * 3
        return shapes, [pl.BlockSpec((TILE, LANES), lambda *i: (row_of(*i), 0))] * 4
    shapes = [jax.ShapeDtypeStruct((2, rows, half), BF16)] * 2 + [
        jax.ShapeDtypeStruct((rows, LANES), F32), jax.ShapeDtypeStruct((rows, half), F32),
        jax.ShapeDtypeStruct((rows, half), F32)]
    specs = [pl.BlockSpec((2, TILE, half), lambda *i: (0, row_of(*i), 0))] * 2 + [
        pl.BlockSpec((TILE, width), lambda *i: (row_of(*i), 0)) for width in (LANES, half, half)]
    return shapes, specs


def fixed(shape):
    return pl.BlockSpec(shape, lambda *i: (0,) * len(shape))


def outside(count):
    return [pl.BlockSpec(memory_space=pl.ANY)] * count


def params(size):
    return pltpu.CompilerParams(dimension_semantics=("arbitrary",), vmem_limit_bytes=size << 20)


def weight_scratch(width):
    return [pltpu.VMEM((width, 3 * LANES + width), BF16), pltpu.VMEM((LANES + width, width), BF16),
            pltpu.SemaphoreType.DMA((6,))]


def forward_layer(meta, lens, pieces, weights, tables, length, first_row, phased, carry=None):
    rows = pieces[0].shape[0]
    tiles, before = rows // TILE, first_row // TILE
    half, width = LANES // 2, 4 * LANES
    local = lambda t, *_: t
    there = lambda t, *_: before + t
    by_row = lambda n, row_of: pl.BlockSpec((TILE, n), lambda *i: (row_of(*i), 0))
    (gain, bias, mix_hi, mix_lo, feat_w), mine, other = weights
    small = (gain, bias, mix_hi, mix_lo, feat_w)
    shapes, specs = partial_outs(rows, phased, local)
    extra = [(width, BF16), (LANES, F32), (half, F32)] + [(LANES, BF16)] * 5 + [
        (LANES + width, BF16), (width, BF16), (LANES, F32), (LANES, F32)]
    shapes += [jax.ShapeDtypeStruct((length, n), d) for n, d in extra]
    specs += [by_row(n, there) for n, _ in extra]
    shapes += [jax.ShapeDtypeStruct((length // TILE, LANES, LANES), F32), jax.ShapeDtypeStruct((length // TILE, 8, LANES), F32)]
    specs += [pl.BlockSpec((1, n, LANES), lambda *i: (there(*i), 0, 0)) for n in (LANES, 8)]
    states = [(LANES, LANES), (8, LANES)]
    shapes += [jax.ShapeDtypeStruct(s, F32) for s in states]
    specs += [fixed(s) for s in states]
    operands = [meta, jnp.stack([lens[0], jnp.int32(first_row)]), *pieces, *small, *tables, *mine, *other]
    in_specs = [by_row(p.shape[1], local) for p in pieces] + [fixed(w.shape) for w in small] + [by_row(half, there)] * 2 + outside(8)
    aliases = {}
    if carry is not None:
        state, saved = carry
        operands += [*state, *saved]
        in_specs += [fixed(s) for s in states] + outside(SAVED)
        aliases = {len(operands) - SAVED + i: len(shapes) - 2 - SAVED + i for i in range(SAVED)}
    outs = pl.pallas_call(
        functools.partial(forward_kernel, carry is not None, phased),
        name="layer_forward",
        out_shape=shapes,
        grid_spec=pltpu.PrefetchScalarGridSpec(
            num_scalar_prefetch=2, grid=(tiles,), in_specs=in_specs, out_specs=specs, scratch_shapes=weight_scratch(width)),
        input_output_aliases=aliases,
        compiler_params=params(56),
        cost_estimate=pl.CostEstimate(flops=rows * 20_000_000, transcendentals=rows * 5000, bytes_accessed=24 << 20),
    )(*operands)
    count = 5 if phased else 4
    return outs[:count], outs[count:count + SAVED], outs[count + SAVED:]


def backward_layer(meta, grad, saved, weights, tables, length, first_row, phased, carry=None):
    rows = grad.shape[0]
    tiles, before = rows // TILE, first_row // TILE
    half, width = LANES // 2, 4 * LANES
    local = lambda t, *_: tiles - 1 - t
    there = lambda t, *_: before + tiles - 1 - t
    by_row = lambda n, row_of=there: pl.BlockSpec((TILE, n), lambda *i: (row_of(*i), 0))
    normed, rq, rk, qf, kf, value, hcat, dgelu, invz, attended, prior_s, prior_k = saved
    (gain, bias, mix_hi, mix_lo, feat_w), mine, other = weights
    shapes, specs = partial_outs(rows, phased, local)
    shapes += [jax.ShapeDtypeStruct((8, length), F32), jax.ShapeDtypeStruct((length, 3 * LANES + width), BF16)]
    specs += [pl.BlockSpec((8, TILE), lambda *i: (0, there(*i))), by_row(3 * LANES + width)]
    states = [(LANES, LANES), (8, LANES)] * 2
    shapes += [jax.ShapeDtypeStruct(s, F32) for s in states]
    specs += [fixed(s) for s in states]
    operands = [meta, grad, normed, rq, rk, qf, kf, value, attended, dgelu, invz, prior_s, prior_k, gain, bias, mix_hi, *tables,
                *mine, *other]
    in_specs = [by_row(width, local), by_row(width)] + [by_row(LANES)] * 6 + [by_row(width), by_row(LANES)] + [
        pl.BlockSpec((1, n, LANES), lambda *i: (there(*i), 0, 0)) for n in (LANES, 8)] + [
        fixed(w.shape) for w in (gain, bias, mix_hi)] + [by_row(half)] * 2 + outside(8)
    aliases = {}
    if carry is not None:
        state, arrays = carry
        operands += [*state, *arrays]
        in_specs += [fixed(s) for s in states] + outside(2)
        aliases = {len(operands) - 2 + i: len(shapes) - 6 + i for i in range(2)}
    outs = pl.pallas_call(
        functools.partial(backward_kernel, carry is not None, phased),
        name="layer_backward",
        out_shape=shapes,
        grid_spec=pltpu.PrefetchScalarGridSpec(
            num_scalar_prefetch=1, grid=(tiles,), in_specs=in_specs, out_specs=specs, scratch_shapes=weight_scratch(width)),
        input_output_aliases=aliases,
        compiler_params=params(56),
        cost_estimate=pl.CostEstimate(flops=rows * 25_000_000, transcendentals=0, bytes_accessed=24 << 20),
    )(*operands)
    count = 5 if phased else 4
    return outs[:count], outs[count:count + 2], outs[count + 2:]


def join(meta, pieces):
    rows, block = pieces[0].shape[0], 2 * TILE
    return pl.pallas_call(
        join_kernel,
        name="join",
        out_shape=jax.ShapeDtypeStruct((rows, 4 * LANES), BF16),
        grid_spec=pltpu.PrefetchScalarGridSpec(
            num_scalar_prefetch=1,
            grid=(rows // block,),
            in_specs=[pl.BlockSpec((block, p.shape[1]), lambda i, *_: (i, 0)) for p in pieces],
            out_specs=pl.BlockSpec((block, 4 * LANES), lambda i, *_: (i, 0)),
        ),
        compiler_params=params(8),
        cost_estimate=pl.CostEstimate(flops=0, transcendentals=0, bytes_accessed=rows * 16 * LANES),
    )(meta, *pieces)


def swap(value, axis, by):
    return lax.ppermute(value, axis, [(k, k ^ by) for k in range(lax.axis_size(axis))])


def gather_pieces(shard, meanwhile=()):
    from_x, from_y = after((swap(shard, "mp", 1), swap(shard, "mp", 2)), *meanwhile)
    return (shard, from_x, from_y) + last_pieces(from_x, from_y)


def last_pieces(from_x, from_y):
    half = from_x.shape[1] // 2
    return tuple(lax.optimization_barrier((swap(from_x[:, :half], "mp", 2), swap(from_y[:, half:], "mp", 1))))


def after(values, *others):
    if not others:
        return values
    return lax.optimization_barrier((values, others))[0]


def direct_sends(parts):
    return parts[0], [swap(part, "mp", r) for r, part in enumerate(parts) if r > 0]


def scatter_start(parts):
    return swap(parts[0], "mp", 1), swap(parts[1], "mp", 2)


def scatter_turn(parts, arrived):
    _, _, _, ka, kb = parts
    in_x, in_y = arrived
    return (ka + in_x[1].astype(F32)).astype(BF16), (kb + in_y[1].astype(F32)).astype(BF16)


def scatter_end(parts, arrived, to_y, to_x):
    _, _, k0, ka, _ = parts
    in_x, in_y = arrived
    half = ka.shape[1]
    last_y, last_x = swap(to_y, "mp", 2), swap(to_x, "mp", 1)
    return jnp.concatenate(
        [k0[:, :half] + in_x[0].astype(F32) + last_y.astype(F32), k0[:, half:] + in_y[0].astype(F32) + last_x.astype(F32)],
        axis=1)


def scatter_sum(parts):
    arrived = scatter_start(parts)
    return scatter_end(parts, arrived, *scatter_turn(parts, arrived))


def mp_total(values):
    return values + swap(values, "mp", 1) + swap(values, "mp", 2) + swap(values, "mp", 3)


def ring_scatter(block_of, axis, meanwhile=()):
    count = lax.axis_size(axis)
    rank = lax.axis_index(axis)
    pairs = [(k, (k + 1) % count) for k in range(count)]
    total = block_of((rank + count - 1) % count)
    for step in range(2, count + 1):
        arrived = lax.ppermute(total, axis, pairs)
        if step in (2, count):
            arrived = after(arrived, *meanwhile)
        total = (arrived.astype(F32) + block_of((rank + count - step) % count).astype(F32)).astype(BF16)
        yield arrived, total


def dp_sends(values):
    count = lax.axis_size("dp")
    if count > 8:
        return [lax.psum(values, "dp")]
    return [values] + [lax.ppermute(values, "dp", [(i, (i + k) % count) for i in range(count)]) for k in range(1, count)]


def block_sends(block_of, axis):
    count = lax.axis_size(axis)
    rank = lax.axis_index(axis)
    if count > 8:
        return [list(ring_scatter(block_of, axis))[-1][1]]
    return [block_of(rank)] + [
        lax.ppermute(block_of((rank + k) % count), axis, [(i, (i + k) % count) for i in range(count)]) for k in range(1, count)]


def sum_blocks(blocks):
    total = blocks[0].astype(F32)
    for block in blocks[1:]:
        total = total + block.astype(F32)
    return total.astype(BF16)


def weight_gradient(left, right, cut_left, section):
    rows = left.shape[0]
    m, n = left.shape[1] // (2 if cut_left else 1), right.shape[1] // (1 if cut_left else 2)
    block = 128 if cut_left else 256
    steps = m // block
    left_at = (lambda i, which: (0, which[0] * steps + i)) if cut_left else (lambda i, which: (0, i))
    right_at = (lambda i, which: (0, 0)) if cut_left else (lambda i, which: (0, which[0]))

    def product(which):
        return pl.pallas_call(
            product_kernel,
            name="weight_gradient",
            out_shape=jax.ShapeDtypeStruct((m, n), BF16),
            grid_spec=pltpu.PrefetchScalarGridSpec(
                num_scalar_prefetch=1, grid=(steps,),
                in_specs=[pl.BlockSpec((rows, block), left_at), pl.BlockSpec((rows, n), right_at)],
                out_specs=pl.BlockSpec((block, n), lambda i, which: (i, 0))),
            compiler_params=params(20),
            cost_estimate=pl.CostEstimate(flops=2 * rows * m * n, transcendentals=0, bytes_accessed=2 * (rows * (m + n) + m * n)),
        )(which.reshape(1).astype(jnp.int32), left, right)

    arrived = swap(product(1 - section), "section", 1)
    return product(section), arrived


def dct_table(order):
    row_index = jnp.arange(order, dtype=F32)[:, None]
    col_index = jnp.arange(order, dtype=F32)[None, :]
    cosines = jnp.sqrt(2.0 / order) * jnp.cos(math.pi * (row_index + 0.5) * col_index / order)
    return cosines * jnp.where(col_index == 0, math.sqrt(0.5), 1.0)


def rotary_tables(length):
    column = jnp.arange(LANES // 2, dtype=jnp.int32) % HEAD
    half = ROT // 2
    index = (column % half).astype(F32)
    angles = jnp.arange(length, dtype=F32)[:, None] * (10000.0 ** (-index * 2.0 / ROT))[None, :]
    turned = (column < ROT)[None, :]
    sign = jnp.where(column < half, -1.0, 1.0)[None, :]
    return jnp.where(turned, jnp.cos(angles), 1.0), jnp.where(turned, sign * jnp.sin(angles), 0.0)


def shards(block_input, cotangent, lengths, ln_gain, ln_bias, w_qkv, w_out, w_up, w_down, freq_table, feat_weight):
    section = lax.axis_index("section")
    place = lax.axis_index("mp")
    group = lax.axis_index("dp")
    groups = lax.axis_size("dp")
    local_slots, length, shard_width = block_input.shape
    width = ln_gain.shape[1]
    heads = freq_table.shape[1]
    is_first = section == 0
    lens = lax.dynamic_slice_in_dim(lengths, section, 1, 0)
    metas = [jnp.stack([place, (section == l).astype(jnp.int32)]).astype(jnp.int32) for l in range(2)]

    def own(values):
        return lax.dynamic_index_in_dim(values, section, 0, keepdims=False)

    shard0 = own(block_input)
    pieces0 = gather_pieces(shard0)

    small = jnp.concatenate([ln_gain[0], ln_bias[0], feat_weight.reshape(-1), freq_table.astype(F32).reshape(-1)])
    small_other = swap(small, "section", 1)
    mine = (w_qkv, w_up, w_out, w_down)
    other = tuple(swap(w, "section", 1) for w in mine)

    def both(mine, other):
        return jnp.where(is_first, mine, other), jnp.where(is_first, other, mine)

    layers_small = both(small, small_other)
    table = dct_table(HEAD)
    eye = jnp.eye(heads, dtype=F32)

    def layer_weights(l):
        vec = layers_small[l]
        gain, bias = vec[:width].reshape(1, width), vec[width:2 * width].reshape(1, width)
        feat = vec[2 * width:2 * width + LANES].reshape(1, LANES)
        freq = vec[2 * width + LANES:].reshape(heads, HEAD, HEAD)
        mixed = jnp.einsum("nk,hkm->hnm", table, freq, precision=lax.Precision.HIGHEST)
        mixed = (eye[:, None, :, None] * mixed[:, :, None, :]).reshape(LANES, LANES)
        high = lax.reduce_precision(mixed, 8, 7)
        return (gain, bias, high.astype(BF16), (mixed - high).astype(BF16), feat), mine, other

    weights0, weights1 = layer_weights(0), layer_weights(1)
    tables = rotary_tables(length)

    cot = after(own(cotangent), pieces0[3], pieces0[4])
    cot_x, cot_y = swap(cot, "mp", 1), swap(cot, "mp", 2)
    part0, all0, _ = forward_layer(metas[0], lens, pieces0, weights0, tables, length, 0, True)
    part0 = after(part0, cot_x, cot_y)
    hidden = (shard0.astype(F32) + scatter_sum(part0)).astype(BF16)
    pieces1 = gather_pieces(hidden)
    cot_x, cot_y = after((cot_x, cot_y), pieces1[3], pieces1[4])
    pieces_g = (cot, cot_x, cot_y) + last_pieces(cot_x, cot_y)
    part1, all1, _ = forward_layer(metas[1], lens, pieces1, weights1, tables, length, 0, False)
    out_kept, out_sent = direct_sends(part1)

    def saved_of(arrays):
        return (arrays[0],) + tuple(arrays[3:])

    def in_block(mine, arrived):
        n = mine.shape[0] // groups
        cut = lambda v, i: lax.dynamic_slice_in_dim(v, i * n, n, 0)
        return lambda i: (cut(mine, i).astype(F32) + cut(arrived, i).astype(F32)).astype(BF16)

    def out_block(mine, arrived):
        n = mine.shape[1] // groups
        cut = lambda v, i: lax.dynamic_slice_in_dim(v, i * n, n, 1)
        return lambda i: (cut(mine, i).astype(F32) + cut(arrived, i).astype(F32)).astype(BF16)

    def run_backward(meta, grad, saved, weights, phased):
        parts, (stats, dcat), (_, _, dmix, fsum) = backward_layer(meta, grad, saved, weights, tables, length, 0, phased)
        return parts, stats, dcat, dmix, fsum

    def norm_backward(grad_shard, d_normed, sums, norm, gain_all):
        xhat, rstd = norm
        gain = lax.dynamic_slice_in_dim(gain_all, place * shard_width, shard_width, 1)
        mean_d = (sums[0] * (1.0 / width))[:, None]
        mean_dx = (sums[1] * (1.0 / width))[:, None]
        return grad_shard.astype(F32) + rstd[:, :1] * (d_normed * gain - mean_d - xhat * mean_dx)

    def small_gradients(d_normed, norm, dmix, fsum):
        gain_part = jnp.sum(d_normed * norm[0], axis=0)
        bias_part = jnp.sum(d_normed, axis=0)
        diagonal = jnp.stack([dmix[h * HEAD:(h + 1) * HEAD, h * HEAD:(h + 1) * HEAD] for h in range(heads)])
        return jnp.concatenate([gain_part, bias_part, fsum[0], diagonal.reshape(-1)])

    saved1, saved0 = saved_of(all1), saved_of(all0)
    grad1 = join(metas[1], pieces_g)
    out_blocks1 = block_sends(out_block(*weight_gradient(saved1[6], grad1, True, section)), "dp")
    grad1_b = after(grad1, out_blocks1[0])
    parts, stats, dcat1, dmix1, fsum1 = run_backward(metas[1], grad1_b, saved1, weights1, True)
    parts, stats, dcat1, dmix1, fsum1 = after((parts, stats, dcat1, dmix1, fsum1), *out_blocks1, *out_sent)
    arrived = scatter_start(parts)
    turn = scatter_turn(parts, arrived)
    steps1 = list(ring_scatter(in_block(*weight_gradient(saved1[0], dcat1, False, section)), "dp"))
    arrivals1, red_in1 = [arrival for arrival, _ in steps1], steps1[-1][1]
    d_normed = scatter_end(parts, arrived, *turn)
    sums = mp_total(after(stats, *turn))
    g0 = norm_backward(cot, d_normed, sums, all1[1:3], weights1[0][0]).astype(BF16)
    small1 = small_gradients(d_normed, all1[1:3], dmix1, fsum1)
    pieces_g0 = gather_pieces(after(g0, arrivals1[0]), arrivals1[1:2])
    pieces_g0 = after(pieces_g0, *arrivals1[2:3])
    out = hidden.astype(F32) + out_kept + out_sent[0].astype(F32) + out_sent[1].astype(F32) + out_sent[2].astype(F32)

    grad0 = join(metas[0], pieces_g0)
    out_blocks0 = block_sends(out_block(*weight_gradient(saved0[6], grad0, True, section)), "dp")
    grad0_b = after(grad0, out_blocks0[0])
    parts, stats, dcat0, dmix0, fsum0 = run_backward(metas[0], grad0_b, saved0, weights0, False)
    parts, stats, dcat0, dmix0, fsum0 = after((parts, stats, dcat0, dmix0, fsum0), *out_blocks0)
    out_blocks1 = after(out_blocks1, dcat0)
    kept, sent = direct_sends(parts)
    mine0, arrived0 = weight_gradient(saved0[0], dcat0, False, section)
    block0 = in_block(mine0, arrived0)
    meanwhile = list(sent)
    ring0 = ring_scatter(block0, "dp", meanwhile)
    steps0 = [next(ring0)]
    meanwhile.clear()
    sums = mp_total(after(stats, steps0[0][1]))
    sent, dmix0, out_blocks0, out_blocks1 = after((sent, dmix0, out_blocks0, out_blocks1), steps0[0][1])
    d_normed = kept + sent[0].astype(F32) + sent[1].astype(F32) + sent[2].astype(F32)
    d_input = norm_backward(g0, d_normed, sums, all0[1:3], weights0[0][0])
    small0 = small_gradients(d_normed, all0[1:3], dmix0, fsum0)

    def to_owner(first, second, axis):
        mine, other = both(first, second)
        arrived = swap(other, "section", 1)
        return jnp.where(is_first, jnp.concatenate([mine, arrived], axis), jnp.concatenate([arrived, mine], axis)).astype(F32)

    grads_out = to_owner(sum_blocks(out_blocks0), sum_blocks(out_blocks1), 0)
    small_mine, small_send = both(small0, small1)
    small_sum = small_mine + swap(small_send, "section", 1)
    small_parts = dp_sends(small_sum)
    keep, send = both(d_input, out)
    arrived = swap(send, "section", 1)
    boundary = jnp.where(is_first, jnp.stack([keep, arrived]), jnp.stack([arrived, keep]))
    meanwhile.append(arrived)
    steps0 += list(ring0)
    grads_in = to_owner(steps0[-1][1], red_in1, 1)
    small_sum = sum(after(small_parts, steps0[-1][0]))
    feat_grad = small_sum[2 * shard_width:2 * shard_width + LANES].reshape(heads, HEAD) / feat_weight[0]
    freq_grad = jnp.einsum("nk,hnm->hkm", table, small_sum[2 * shard_width + LANES:].reshape(heads, HEAD, HEAD),
                           precision=lax.Precision.HIGHEST)
    qkv_grad = jnp.stack([grads_in[:, t * shard_width:(t + 1) * shard_width] for t in range(3)])
    return (
        boundary[None],
        small_sum[None, :shard_width],
        small_sum[None, shard_width:2 * shard_width],
        qkv_grad[None],
        grads_out[None, :shard_width],
        grads_in[None, :, 3 * shard_width:],
        grads_out[None, shard_width:],
        freq_grad[None],
        feat_grad[None],
    )


def solution(mesh):
    placed = (
        P("dp", None, "mp"), P("dp", None, "mp"), P("dp"), P("section", None), P("section", None),
        P("section", None, None, "mp"), P("section", "mp", None), P("section", None, "mp"), P("section", "mp", None),
        P("section", "mp", None, None), P("section", "mp", None),
    )
    return jax.shard_map(
        shards,
        mesh=mesh,
        in_specs=placed,
        out_specs=(
            P("section", "dp", None, "mp"), P("section", "mp"), P("section", "mp"), P("section", None, "dp", "mp"),
            P("section", "mp", "dp"), P("section", "dp", "mp"), P("section", "mp", "dp"), P("section", "mp", None, None),
            P("section", "mp", None),
        ),
        check_vma=False,
    )
```

```python
import functools
import math

import jax
import jax.numpy as jnp
from jax import lax
from jax.experimental import pallas as pl
from jax.experimental.pallas import tpu as pltpu
from jax.sharding import PartitionSpec as P

ROT = 16
TILE = 256
HEAD = 64
LANES = 256
EPS = 1e-05
F32 = jnp.float32
BF16 = jnp.bfloat16
RSQRT2 = math.sqrt(0.5)
RSQRT2PI = 1.0 / math.sqrt(2.0 * math.pi)
SAVED = 14


def dot_nn(a, b):
    return lax.dot_general(a, b, (((1,), (0,)), ((), ())), preferred_element_type=F32)


def dot_nt(a, b):
    return lax.dot_general(a, b, (((1,), (1,)), ((), ())), preferred_element_type=F32)


def dot_tn(a, b):
    return lax.dot_general(a, b, (((0,), (0,)), ((), ())), preferred_element_type=F32)


def split(values):
    high = values.astype(BF16)
    return high, (values - high.astype(F32)).astype(BF16)


def iota(shape, dim):
    return lax.broadcasted_iota(jnp.int32, shape, dim)


def partner(values):
    later = pltpu.roll(values, LANES - ROT // 2, 1)
    earlier = pltpu.roll(values, ROT // 2, 1)
    lower = iota(values.shape, 1) % HEAD < ROT // 2
    return jnp.where(lower, later, earlier)


def twice(table):
    return jnp.concatenate([table, table], axis=1)


def head_of(shape, dim):
    return iota(shape, dim) // HEAD


def weight_copies(refs, w_in, w_out, sems, which):
    qkv, up, out, down = refs
    ends = [(qkv.at[0, t], w_in.at[:, t * LANES:(t + 1) * LANES]) for t in range(3)] + [
        (up.at[0], w_in.at[:, 3 * LANES:]), (out.at[0], w_out.at[0:LANES, :]), (down.at[0], w_out.at[LANES:, :])]
    return [pltpu.make_async_copy(*ends[i], sems.at[i]) for i in which]


def start_weights(meta, mine, other, w_in, w_out, sems, order):
    def start(refs):
        for copy in weight_copies(refs, w_in, w_out, sems, order):
            copy.start()

    @pl.when(meta[1] == 1)
    def _():
        start(mine)

    @pl.when(meta[1] != 1)
    def _():
        start(other)


def wait_weights(step, refs, w_in, w_out, sems, which):
    @pl.when(step == 0)
    def _():
        for copy in weight_copies(refs, w_in, w_out, sems, which):
            copy.wait()


def forward_kernel(carried, phased, *refs):
    refs = list(refs)
    take = lambda n: [refs.pop(0) for _ in range(n)]
    meta, lens = take(2)
    p0, p1, p2, p3a, p3b, gain, bias, mix_hi, mix_lo, feat_w, cos_t, sin_t = take(12)
    mine, other = take(4), take(4)
    if carried:
        state_in, ksum_in = take(2)
        take(SAVED)
    parts = take(5 if phased else 4)
    normed, xhat, rstd, rq_o, rk_o, qf_o, kf_o, v_o, hcat, dgelu, invz, att_o, prior_s, prior_k = take(SAVED)
    state, ksum, w_in, w_out, sems = take(5)
    tile = pl.program_id(0)
    rank = meta[0]
    half = LANES // 2

    @pl.when(tile == 0)
    def _():
        start_weights(meta, mine, other, w_in, w_out, sems, (0, 1, 2, 3, 4, 5))
        if carried:
            state[...] = state_in[...]
            ksum[...] = ksum_in[...]
        else:
            state[...] = jnp.zeros_like(state)
            ksum[...] = jnp.zeros_like(ksum)

    pieces = [p0[...].astype(F32), p1[...].astype(F32), p2[...].astype(F32),
              jnp.concatenate([p3a[...], p3b[...]], axis=1).astype(F32)]
    width = 4 * LANES
    mean = jnp.sum(pieces[0] + pieces[1] + pieces[2] + pieces[3], axis=1, keepdims=True) * (1.0 / width)
    pieces = [piece - mean for piece in pieces]
    squares = sum(piece * piece for piece in pieces)
    factor = lax.rsqrt(jnp.sum(squares, axis=1, keepdims=True) * (1.0 / width) + EPS)
    for r in range(4):
        at = pl.ds(pl.multiple_of((rank ^ r) * LANES, LANES), LANES)
        hat = pieces[r] * factor
        if r == 0:
            xhat[...] = hat
        normed[:, at] = (hat * gain[:, at] + bias[:, at]).astype(BF16)
    rstd[...] = jnp.broadcast_to(factor, (TILE, half))
    tokens = normed[...]

    wait_weights(tile, mine, w_in, w_out, sems, (0, 1, 2))
    cosine, sine = twice(cos_t[...]), twice(sin_t[...])
    query = dot_nn(tokens, w_in[:, 0:LANES])
    key = dot_nn(tokens, w_in[:, LANES:2 * LANES])
    value = dot_nn(tokens, w_in[:, 2 * LANES:3 * LANES]).astype(BF16)
    rq = query * cosine + partner(query) * sine
    rk = key * cosine + partner(key) * sine
    weight = feat_w[...]

    def logits(rows):
        high, low = split(rows)
        return dot_nn(high, mix_hi[...]) + dot_nn(low, mix_hi[...]) + dot_nn(high, mix_lo[...])

    positions = lens[1] + tile * TILE + iota((TILE, LANES), 0)
    real = (positions < lens[0]).astype(F32)
    qf = (weight * jnp.exp(logits(rq))).astype(BF16)
    kf = (weight * jnp.exp(logits(rk)) * real).astype(BF16)
    rq_o[...] = rq.astype(BF16)
    rk_o[...] = rk.astype(BF16)
    qf_o[...] = qf
    kf_o[...] = kf
    v_o[...] = value

    square = (TILE, TILE)
    lower = iota(square, 0) >= iota(square, 1)
    same = head_of(square, 0) == head_of(square, 1)
    cumulative = dot_nn(lower.astype(BF16), kf) + ksum[0:1, :]
    high, low = split(qf.astype(F32) * cumulative)
    ones = same.astype(BF16)
    inverse = 1.0 / (dot_nn(high, ones) + dot_nn(low, ones))
    prior = jnp.where(same, state[...], 0.0)
    prior_hi, prior_lo = split(prior)
    numer = dot_nn(qf, prior_hi) + dot_nn(qf, prior_lo)
    lane_head = head_of((TILE, LANES), 1)
    zero = jnp.zeros((TILE, LANES), BF16)
    for h in range(LANES // HEAD):
        here = lane_head == h
        scores = dot_nt(qf, jnp.where(here, kf, zero))
        scores = jnp.where(lower, scores, 0.0).astype(BF16)
        numer = numer + dot_nn(scores, jnp.where(here, value, zero))
    prior_s[0] = prior
    prior_k[0] = ksum[...]
    state[...] = state[...] + dot_tn(kf, value)
    ksum[...] = jnp.broadcast_to(cumulative[TILE - 1:TILE, :], ksum.shape)
    invz[...] = inverse
    attended = numer * inverse
    att_o[...] = attended
    hcat[:, 0:LANES] = attended.astype(BF16)

    wait_weights(tile, mine, w_in, w_out, sems, (3,))

    def hidden_units(c, _):
        at = lambda k: pl.ds(pl.multiple_of((2 * c + k) * LANES, LANES), 2 * LANES)
        up = dot_nn(tokens, w_in[:, at(3)])
        cdf = 0.5 * (1.0 + lax.erf(up * RSQRT2))
        hcat[:, at(1)] = (up * cdf).astype(BF16)
        dgelu[:, at(0)] = (cdf + up * (RSQRT2PI * jnp.exp(-0.5 * up * up))).astype(BF16)
        return _

    lax.fori_loop(0, 2, hidden_units, 0)

    wait_weights(tile, mine, w_in, w_out, sems, (4, 5))
    hidden = hcat[...]
    emit(rank, lambda at: dot_nn(hidden, w_out[:, at]), parts)


def emit(rank, product, parts):
    half = LANES // 2
    for r in range(4):
        at = pl.ds(pl.multiple_of((rank ^ r) * LANES, LANES), LANES)
        part = product(at)
        if len(parts) == 4:
            parts[r][...] = part.astype(parts[r].dtype)
            continue
        sx, sy, k0, ka, kb = parts
        if r == 0:
            k0[...] = part
        elif r == 1:
            sx[0] = part[:, :half].astype(BF16)
            kb[...] = part[:, half:]
        elif r == 2:
            ka[...] = part[:, :half]
            sy[0] = part[:, half:].astype(BF16)
        else:
            sx[1] = part[:, :half].astype(BF16)
            sy[1] = part[:, half:].astype(BF16)


def backward_kernel(carried, phased, *refs):
    refs = list(refs)
    take = lambda n: [refs.pop(0) for _ in range(n)]
    meta, = take(1)
    pieces = take(5)
    normed, rq, rk, qf_i, kf_i, v_i, att_i, dgelu, invz, prior_s, prior_k, gain, bias, mix_hi, cos_t, sin_t = take(16)
    mine, other = take(4), take(4)
    if carried:
        state_in, gsum_in, dmix_in, fsum_in = take(4)
        take(2)
    parts = take(5 if phased else 4)
    stats, dcat, state, gsum, dmix, fsum = take(6)
    w_in, w_out, sems, grad = take(4)
    step = pl.program_id(0)
    rank = meta[0]

    @pl.when(step == 0)
    def _():
        start_weights(meta, mine, other, w_in, w_out, sems, (4, 5, 0, 1, 2, 3))
        if carried:
            state[...] = state_in[...]
            gsum[...] = gsum_in[...]
            dmix[...] = dmix_in[...]
            fsum[...] = fsum_in[...]
        else:
            state[...] = jnp.zeros_like(state)
            gsum[...] = jnp.zeros_like(gsum)
            dmix[...] = jnp.zeros_like(dmix)
            fsum[...] = jnp.zeros_like(fsum)

    wait_weights(step, mine, w_in, w_out, sems, (4, 5))
    assemble(rank, pieces, grad)
    g = grad[...]
    d_att = dot_nt(g, w_out[0:LANES, :]).astype(BF16).astype(F32)
    square = (TILE, TILE)
    same = head_of(square, 0) == head_of(square, 1)
    ones = same.astype(BF16)
    inverse = invz[...]
    dn = (d_att * inverse).astype(BF16)
    dn32 = dn.astype(F32)
    high, low = split(dn32 * att_i[...])
    dden = -(dot_nn(high, ones) + dot_nn(low, ones))
    den_hi = dden.astype(BF16).astype(F32)
    roll_hi = pltpu.roll(den_hi, HEAD, 1)
    roll_lo = pltpu.roll(dden - den_hi, HEAD, 1)
    qf, kf, value = qf_i[...], kf_i[...], v_i[...]
    zero = jnp.zeros((TILE, LANES), BF16)
    one = jnp.ones((TILE, LANES), BF16)
    lane = iota((TILE, LANES), 1)
    lane_head = lane // HEAD
    below = iota(square, 0) >= iota(square, 1)
    above = iota(square, 0) <= iota(square, 1)
    prior_hi, prior_lo = split(prior_s[0])
    later_hi, later_lo = split(jnp.where(same, state[...], 0.0))
    d_qf = dot_nt(dn, prior_hi) + dot_nt(dn, prior_lo) + prior_k[0, 0:1, :] * dden
    d_kf = dot_nt(value, later_hi) + dot_nt(value, later_lo) + gsum[0:1, :]
    d_v = dot_nn(kf, later_hi)
    heads = LANES // HEAD
    for h in range(heads):
        here = lane_head == h
        spare = HEAD * ((h + 1) % heads)
        left = jnp.where(lane == spare, roll_hi, jnp.where(lane == spare + 1, roll_lo, dn32)).astype(BF16)
        right = jnp.where(here, value, jnp.where((lane == spare) | (lane == spare + 1), one, zero))
        k_here = jnp.where(here, kf, zero)
        q_here = jnp.where(here, qf, zero)
        d_here = jnp.where(here, dn, zero)
        scores_t = jnp.where(above, dot_nt(k_here, qf), 0.0).astype(BF16)
        ds = jnp.where(below, dot_nt(left, right), 0.0).astype(BF16)
        ds_t = jnp.where(above, dot_nt(right, left), 0.0).astype(BF16)
        d_qf = d_qf + dot_nn(ds, k_here)
        d_kf = d_kf + dot_nn(ds_t, q_here)
        d_v = d_v + dot_nn(scores_t, d_here)
    state[...] = state[...] + dot_tn(qf, dn)
    gsum[...] = gsum[...] + jnp.sum(qf.astype(F32) * dden, axis=0, keepdims=True)
    dlq = d_qf * qf.astype(F32)
    dlk = d_kf * kf.astype(F32)
    fsum[...] = fsum[...] + jnp.sum(dlq + dlk, axis=0, keepdims=True)
    dlq, dlk = dlq.astype(BF16), dlk.astype(BF16)
    dmix[...] = dmix[...] + dot_tn(rq[...], dlq) + dot_tn(rk[...], dlk)
    cosine, sine = twice(cos_t[...]), twice(sin_t[...])
    for c, dl in ((0, dlq), (1, dlk)):
        dr = dot_nt(dl, mix_hi[...])
        dcat[:, c * LANES:(c + 1) * LANES] = (dr * cosine - partner(dr) * sine).astype(BF16)
    dcat[:, 2 * LANES:3 * LANES] = d_v.astype(BF16)

    def hidden_units(c, _):
        at = lambda k: pl.ds(pl.multiple_of((c + k) * LANES, LANES), LANES)
        d_act = dot_nt(g, w_out[at(1), :])
        dcat[:, at(3)] = (d_act * dgelu[:, at(0)].astype(F32)).astype(BF16)
        return _

    lax.fori_loop(0, 4, hidden_units, 0)
    wait_weights(step, mine, w_in, w_out, sems, (0, 1, 2, 3))
    wide = dcat[...]
    row = iota((8, LANES), 0)
    first, second = (row == 0).astype(BF16), (row == 1).astype(BF16)
    totals = []

    def product(at):
        part = dot_nt(wide, w_in[at, :])
        one_side = (part * gain[:, at]).astype(BF16)
        other = (part * (normed[:, at].astype(F32) - bias[:, at])).astype(BF16)
        totals.append(dot_nt(first, one_side) + dot_nt(second, other))
        return part

    emit(rank, product, parts)
    stats[...] = totals[0] + totals[1] + totals[2] + totals[3]


def assemble(rank, pieces, whole):
    half = LANES // 2
    for r in range(3):
        whole[:, pl.ds(pl.multiple_of((rank ^ r) * LANES, LANES), LANES)] = pieces[r][...]
    at = pl.multiple_of((rank ^ 3) * LANES, LANES)
    whole[:, pl.ds(at, half)] = pieces[3][...]
    whole[:, pl.ds(pl.multiple_of(at + half, half), half)] = pieces[4][...]


def product_kernel(which, left, right, out):
    out[...] = dot_tn(left[...], right[...]).astype(BF16)


def product_pieces_kernel(which, left, p0, p1, p2, p3a, p3b, out, right):
    @pl.when(pl.program_id(0) == 0)
    def _():
        assemble(which[1], (p0, p1, p2, p3a, p3b), right)

    out[...] = dot_tn(left[...], right[...]).astype(BF16)


def partial_outs(rows, phased, row_of):
    half = LANES // 2
    if not phased:
        shapes = [jax.ShapeDtypeStruct((rows, LANES), F32)] + [jax.ShapeDtypeStruct((rows, LANES), BF16)] * 3
        return shapes, [pl.BlockSpec((TILE, LANES), lambda *i: (row_of(*i), 0))] * 4
    shapes = [jax.ShapeDtypeStruct((2, rows, half), BF16)] * 2 + [
        jax.ShapeDtypeStruct((rows, LANES), F32), jax.ShapeDtypeStruct((rows, half), F32),
        jax.ShapeDtypeStruct((rows, half), F32)]
    specs = [pl.BlockSpec((2, TILE, half), lambda *i: (0, row_of(*i), 0))] * 2 + [
        pl.BlockSpec((TILE, width), lambda *i: (row_of(*i), 0)) for width in (LANES, half, half)]
    return shapes, specs


def fixed(shape):
    return pl.BlockSpec(shape, lambda *i: (0,) * len(shape))


def outside(count):
    return [pl.BlockSpec(memory_space=pl.ANY)] * count


def params(size):
    return pltpu.CompilerParams(dimension_semantics=("arbitrary",), vmem_limit_bytes=size << 20)


def weight_scratch(width):
    return [pltpu.VMEM((width, 3 * LANES + width), BF16), pltpu.VMEM((LANES + width, width), BF16),
            pltpu.SemaphoreType.DMA((6,))]


def forward_layer(meta, lens, pieces, weights, tables, length, first_row, phased, carry=None):
    rows = pieces[0].shape[0]
    tiles, before = rows // TILE, first_row // TILE
    half, width = LANES // 2, 4 * LANES
    local = lambda t, *_: t
    there = lambda t, *_: before + t
    by_row = lambda n, row_of: pl.BlockSpec((TILE, n), lambda *i: (row_of(*i), 0))
    (gain, bias, mix_hi, mix_lo, feat_w), mine, other = weights
    small = (gain, bias, mix_hi, mix_lo, feat_w)
    shapes, specs = partial_outs(rows, phased, local)
    extra = [(width, BF16), (LANES, F32), (half, F32)] + [(LANES, BF16)] * 5 + [
        (LANES + width, BF16), (width, BF16), (LANES, F32), (LANES, F32)]
    shapes += [jax.ShapeDtypeStruct((length, n), d) for n, d in extra]
    specs += [by_row(n, there) for n, _ in extra]
    shapes += [jax.ShapeDtypeStruct((length // TILE, LANES, LANES), F32), jax.ShapeDtypeStruct((length // TILE, 8, LANES), F32)]
    specs += [pl.BlockSpec((1, n, LANES), lambda *i: (there(*i), 0, 0)) for n in (LANES, 8)]
    states = [(LANES, LANES), (8, LANES)]
    shapes += [jax.ShapeDtypeStruct(s, F32) for s in states]
    specs += [fixed(s) for s in states]
    operands = [meta, jnp.stack([lens[0], jnp.int32(first_row)]), *pieces, *small, *tables, *mine, *other]
    in_specs = [by_row(p.shape[1], local) for p in pieces] + [fixed(w.shape) for w in small] + [by_row(half, there)] * 2 + outside(8)
    aliases = {}
    if carry is not None:
        state, saved = carry
        operands += [*state, *saved]
        in_specs += [fixed(s) for s in states] + outside(SAVED)
        aliases = {len(operands) - SAVED + i: len(shapes) - 2 - SAVED + i for i in range(SAVED)}
    outs = pl.pallas_call(
        functools.partial(forward_kernel, carry is not None, phased),
        name="layer_forward",
        out_shape=shapes,
        grid_spec=pltpu.PrefetchScalarGridSpec(
            num_scalar_prefetch=2, grid=(tiles,), in_specs=in_specs, out_specs=specs, scratch_shapes=weight_scratch(width)),
        input_output_aliases=aliases,
        compiler_params=params(56),
        cost_estimate=pl.CostEstimate(flops=rows * 20_000_000, transcendentals=rows * 5000, bytes_accessed=24 << 20),
    )(*operands)
    count = 5 if phased else 4
    return outs[:count], outs[count:count + SAVED], outs[count + SAVED:]


def backward_layer(meta, pieces, saved, weights, tables, length, first_row, phased, carry=None):
    rows = pieces[0].shape[0]
    tiles, before = rows // TILE, first_row // TILE
    half, width = LANES // 2, 4 * LANES
    local = lambda t, *_: tiles - 1 - t
    there = lambda t, *_: before + tiles - 1 - t
    by_row = lambda n, row_of=there: pl.BlockSpec((TILE, n), lambda *i: (row_of(*i), 0))
    normed, rq, rk, qf, kf, value, hcat, dgelu, invz, attended, prior_s, prior_k = saved
    (gain, bias, mix_hi, mix_lo, feat_w), mine, other = weights
    shapes, specs = partial_outs(rows, phased, local)
    shapes += [jax.ShapeDtypeStruct((8, length), F32), jax.ShapeDtypeStruct((length, 3 * LANES + width), BF16)]
    specs += [pl.BlockSpec((8, TILE), lambda *i: (0, there(*i))), by_row(3 * LANES + width)]
    states = [(LANES, LANES), (8, LANES)] * 2
    shapes += [jax.ShapeDtypeStruct(s, F32) for s in states]
    specs += [fixed(s) for s in states]
    operands = [meta, *pieces, normed, rq, rk, qf, kf, value, attended, dgelu, invz, prior_s, prior_k, gain, bias, mix_hi, *tables,
                *mine, *other]
    in_specs = [by_row(p.shape[1], local) for p in pieces] + [by_row(width)] + [by_row(LANES)] * 6 + [by_row(width), by_row(LANES)] + [
        pl.BlockSpec((1, n, LANES), lambda *i: (there(*i), 0, 0)) for n in (LANES, 8)] + [
        fixed(w.shape) for w in (gain, bias, mix_hi)] + [by_row(half)] * 2 + outside(8)
    aliases = {}
    if carry is not None:
        state, arrays = carry
        operands += [*state, *arrays]
        in_specs += [fixed(s) for s in states] + outside(2)
        aliases = {len(operands) - 2 + i: len(shapes) - 6 + i for i in range(2)}
    outs = pl.pallas_call(
        functools.partial(backward_kernel, carry is not None, phased),
        name="layer_backward",
        out_shape=shapes,
        grid_spec=pltpu.PrefetchScalarGridSpec(
            num_scalar_prefetch=1, grid=(tiles,), in_specs=in_specs, out_specs=specs,
            scratch_shapes=weight_scratch(width) + [pltpu.VMEM((TILE, width), BF16)]),
        input_output_aliases=aliases,
        compiler_params=params(56),
        cost_estimate=pl.CostEstimate(flops=rows * 25_000_000, transcendentals=0, bytes_accessed=24 << 20),
    )(*operands)
    count = 5 if phased else 4
    return outs[:count], outs[count:count + 2], outs[count + 2:]


def swap(value, axis, by):
    return lax.ppermute(value, axis, [(k, k ^ by) for k in range(lax.axis_size(axis))])


def gather_pieces(shard, meanwhile=()):
    from_x, from_y = after((swap(shard, "mp", 1), swap(shard, "mp", 2)), *meanwhile)
    return (shard, from_x, from_y) + last_pieces(from_x, from_y)


def last_pieces(from_x, from_y):
    half = from_x.shape[1] // 2
    return tuple(lax.optimization_barrier((swap(from_x[:, :half], "mp", 2), swap(from_y[:, half:], "mp", 1))))


def after(values, *others):
    if not others:
        return values
    return lax.optimization_barrier((values, others))[0]


def direct_sends(parts):
    return parts[0], [swap(part, "mp", r) for r, part in enumerate(parts) if r > 0]


def scatter_start(parts):
    return swap(parts[0], "mp", 1), swap(parts[1], "mp", 2)


def scatter_turn(parts, arrived):
    _, _, _, ka, kb = parts
    in_x, in_y = arrived
    return (ka + in_x[1].astype(F32)).astype(BF16), (kb + in_y[1].astype(F32)).astype(BF16)


def scatter_end(parts, arrived, to_y, to_x):
    _, _, k0, ka, _ = parts
    in_x, in_y = arrived
    half = ka.shape[1]
    last_y, last_x = swap(to_y, "mp", 2), swap(to_x, "mp", 1)
    return jnp.concatenate(
        [k0[:, :half] + in_x[0].astype(F32) + last_y.astype(F32), k0[:, half:] + in_y[0].astype(F32) + last_x.astype(F32)],
        axis=1)


def scatter_sum(parts):
    arrived = scatter_start(parts)
    return scatter_end(parts, arrived, *scatter_turn(parts, arrived))


def mp_total(values):
    return values + swap(values, "mp", 1) + swap(values, "mp", 2) + swap(values, "mp", 3)


def ring_scatter(block_of, axis, meanwhile=()):
    count = lax.axis_size(axis)
    rank = lax.axis_index(axis)
    pairs = [(k, (k + 1) % count) for k in range(count)]
    total = block_of((rank + count - 1) % count)
    for step in range(2, count + 1):
        arrived = lax.ppermute(total, axis, pairs)
        if step in (2, count):
            arrived = after(arrived, *meanwhile)
        total = (arrived.astype(F32) + block_of((rank + count - step) % count).astype(F32)).astype(BF16)
        yield arrived, total


def dp_sends(values):
    count = lax.axis_size("dp")
    if count > 8:
        return [lax.psum(values, "dp")]
    return [values] + [lax.ppermute(values, "dp", [(i, (i + k) % count) for i in range(count)]) for k in range(1, count)]


def block_sends(block_of, axis):
    count = lax.axis_size(axis)
    rank = lax.axis_index(axis)
    if count > 8:
        return [list(ring_scatter(block_of, axis))[-1][1]]
    return [block_of(rank)] + [
        lax.ppermute(block_of((rank + k) % count), axis, [(i, (i + k) % count) for i in range(count)]) for k in range(1, count)]


def sum_blocks(blocks):
    total = blocks[0].astype(F32)
    for block in blocks[1:]:
        total = total + block.astype(F32)
    return total.astype(BF16)


def weight_gradient(left, rights, section, place):
    rows, block = left.shape[0], 128
    whole = len(rights) == 1
    m = left.shape[1] // (1 if whole else 2)
    n = rights[0].shape[1] // 2 if whole else 4 * LANES
    steps = m // block
    if whole:
        left_at = lambda i, which: (0, i)
        right_specs = [pl.BlockSpec((rows, n), lambda i, which: (0, which[0]))]
    else:
        left_at = lambda i, which: (0, which[0] * steps + i)
        right_specs = [fixed(p.shape) for p in rights]

    def product(which):
        return pl.pallas_call(
            product_kernel if whole else product_pieces_kernel,
            name="weight_gradient",
            out_shape=jax.ShapeDtypeStruct((m, n), BF16),
            grid_spec=pltpu.PrefetchScalarGridSpec(
                num_scalar_prefetch=1, grid=(steps,),
                in_specs=[pl.BlockSpec((rows, block), left_at)] + right_specs,
                out_specs=pl.BlockSpec((block, n), lambda i, which: (i, 0)),
                scratch_shapes=[] if whole else [pltpu.VMEM((rows, n), BF16)]),
            compiler_params=params(20),
            cost_estimate=pl.CostEstimate(flops=2 * rows * m * n, transcendentals=0, bytes_accessed=2 * (rows * (m + n) + m * n)),
        )(jnp.stack([which, place]).astype(jnp.int32), left, *rights)

    arrived = swap(product(1 - section), "section", 1)
    return product(section), arrived


def dct_table(order):
    row_index = jnp.arange(order, dtype=F32)[:, None]
    col_index = jnp.arange(order, dtype=F32)[None, :]
    cosines = jnp.sqrt(2.0 / order) * jnp.cos(math.pi * (row_index + 0.5) * col_index / order)
    return cosines * jnp.where(col_index == 0, math.sqrt(0.5), 1.0)


def rotary_tables(length):
    column = jnp.arange(LANES // 2, dtype=jnp.int32) % HEAD
    half = ROT // 2
    index = (column % half).astype(F32)
    angles = jnp.arange(length, dtype=F32)[:, None] * (10000.0 ** (-index * 2.0 / ROT))[None, :]
    turned = (column < ROT)[None, :]
    sign = jnp.where(column < half, -1.0, 1.0)[None, :]
    return jnp.where(turned, jnp.cos(angles), 1.0), jnp.where(turned, sign * jnp.sin(angles), 0.0)


def shards(block_input, cotangent, lengths, ln_gain, ln_bias, w_qkv, w_out, w_up, w_down, freq_table, feat_weight):
    section = lax.axis_index("section")
    place = lax.axis_index("mp")
    group = lax.axis_index("dp")
    groups = lax.axis_size("dp")
    local_slots, length, shard_width = block_input.shape
    width = ln_gain.shape[1]
    heads = freq_table.shape[1]
    is_first = section == 0
    lens = lax.dynamic_slice_in_dim(lengths, section, 1, 0)
    metas = [jnp.stack([place, (section == l).astype(jnp.int32)]).astype(jnp.int32) for l in range(2)]

    def own(values):
        return lax.dynamic_index_in_dim(values, section, 0, keepdims=False)

    shard0 = own(block_input)
    pieces0 = gather_pieces(shard0)

    small = jnp.concatenate([ln_gain[0], ln_bias[0], feat_weight.reshape(-1), freq_table.astype(F32).reshape(-1)])
    small_other = swap(small, "section", 1)
    mine = (w_qkv, w_up, w_out, w_down)
    other = tuple(swap(w, "section", 1) for w in mine)

    def both(mine, other):
        return jnp.where(is_first, mine, other), jnp.where(is_first, other, mine)

    layers_small = both(small, small_other)
    table = dct_table(HEAD)
    eye = jnp.eye(heads, dtype=F32)

    def layer_weights(l):
        vec = layers_small[l]
        gain, bias = vec[:width].reshape(1, width), vec[width:2 * width].reshape(1, width)
        feat = vec[2 * width:2 * width + LANES].reshape(1, LANES)
        freq = vec[2 * width + LANES:].reshape(heads, HEAD, HEAD)
        mixed = jnp.einsum("nk,hkm->hnm", table, freq, precision=lax.Precision.HIGHEST)
        mixed = (eye[:, None, :, None] * mixed[:, :, None, :]).reshape(LANES, LANES)
        high = lax.reduce_precision(mixed, 8, 7)
        return (gain, bias, high.astype(BF16), (mixed - high).astype(BF16), feat), mine, other

    weights0, weights1 = layer_weights(0), layer_weights(1)
    tables = rotary_tables(length)

    cot = after(own(cotangent), pieces0[3], pieces0[4])
    cot_x, cot_y = swap(cot, "mp", 1), swap(cot, "mp", 2)
    part0, all0, _ = forward_layer(metas[0], lens, pieces0, weights0, tables, length, 0, True)
    part0 = after(part0, cot_x, cot_y)
    hidden = (shard0.astype(F32) + scatter_sum(part0)).astype(BF16)
    pieces1 = gather_pieces(hidden)
    cot_x, cot_y = after((cot_x, cot_y), pieces1[3], pieces1[4])
    pieces_g = (cot, cot_x, cot_y) + last_pieces(cot_x, cot_y)
    part1, all1, _ = forward_layer(metas[1], lens, pieces1, weights1, tables, length, 0, False)
    out_kept, out_sent = direct_sends(part1)

    def saved_of(arrays):
        return (arrays[0],) + tuple(arrays[3:])

    def in_block(mine, arrived):
        n = mine.shape[0] // groups
        cut = lambda v, i: lax.dynamic_slice_in_dim(v, i * n, n, 0)
        return lambda i: (cut(mine, i).astype(F32) + cut(arrived, i).astype(F32)).astype(BF16)

    def out_block(mine, arrived):
        n = mine.shape[1] // groups
        cut = lambda v, i: lax.dynamic_slice_in_dim(v, i * n, n, 1)
        return lambda i: (cut(mine, i).astype(F32) + cut(arrived, i).astype(F32)).astype(BF16)

    def run_backward(meta, grad, saved, weights, phased):
        parts, (stats, dcat), (_, _, dmix, fsum) = backward_layer(meta, grad, saved, weights, tables, length, 0, phased)
        return parts, stats, dcat, dmix, fsum

    def norm_backward(grad_shard, d_normed, sums, norm, gain_all):
        xhat, rstd = norm
        gain = lax.dynamic_slice_in_dim(gain_all, place * shard_width, shard_width, 1)
        mean_d = (sums[0] * (1.0 / width))[:, None]
        mean_dx = (sums[1] * (1.0 / width))[:, None]
        return grad_shard.astype(F32) + rstd[:, :1] * (d_normed * gain - mean_d - xhat * mean_dx)

    def small_gradients(d_normed, norm, dmix, fsum):
        gain_part = jnp.sum(d_normed * norm[0], axis=0)
        bias_part = jnp.sum(d_normed, axis=0)
        diagonal = jnp.stack([dmix[h * HEAD:(h + 1) * HEAD, h * HEAD:(h + 1) * HEAD] for h in range(heads)])
        return jnp.concatenate([gain_part, bias_part, fsum[0], diagonal.reshape(-1)])

    saved1, saved0 = saved_of(all1), saved_of(all0)
    out_blocks1 = block_sends(out_block(*weight_gradient(saved1[6], pieces_g, section, place)), "dp")
    grad1_b = after(pieces_g, out_blocks1[0])
    parts, stats, dcat1, dmix1, fsum1 = run_backward(metas[1], grad1_b, saved1, weights1, True)
    parts, stats, dcat1, dmix1, fsum1 = after((parts, stats, dcat1, dmix1, fsum1), *out_blocks1, *out_sent)
    arrived = scatter_start(parts)
    turn = scatter_turn(parts, arrived)
    steps1 = list(ring_scatter(in_block(*weight_gradient(saved1[0], (dcat1,), section, place)), "dp"))
    arrivals1, red_in1 = [arrival for arrival, _ in steps1], steps1[-1][1]
    d_normed = scatter_end(parts, arrived, *turn)
    sums = mp_total(after(stats, *turn))
    g0 = norm_backward(cot, d_normed, sums, all1[1:3], weights1[0][0]).astype(BF16)
    small1 = small_gradients(d_normed, all1[1:3], dmix1, fsum1)
    pieces_g0 = gather_pieces(after(g0, arrivals1[0]), arrivals1[1:2])
    pieces_g0 = after(pieces_g0, *arrivals1[2:3])
    out = hidden.astype(F32) + out_kept + out_sent[0].astype(F32) + out_sent[1].astype(F32) + out_sent[2].astype(F32)

    out_blocks0 = block_sends(out_block(*weight_gradient(saved0[6], pieces_g0, section, place)), "dp")
    grad0_b = after(pieces_g0, out_blocks0[0])
    parts, stats, dcat0, dmix0, fsum0 = run_backward(metas[0], grad0_b, saved0, weights0, False)
    parts, stats, dcat0, dmix0, fsum0 = after((parts, stats, dcat0, dmix0, fsum0), *out_blocks0)
    out_blocks1 = after(out_blocks1, dcat0)
    kept, sent = direct_sends(parts)
    mine0, arrived0 = weight_gradient(saved0[0], (dcat0,), section, place)
    block0 = in_block(mine0, arrived0)
    meanwhile = list(sent)
    ring0 = ring_scatter(block0, "dp", meanwhile)
    steps0 = [next(ring0)]
    meanwhile.clear()
    sums = mp_total(after(stats, steps0[0][1]))
    sent, dmix0, out_blocks0, out_blocks1 = after((sent, dmix0, out_blocks0, out_blocks1), steps0[0][1])
    d_normed = kept + sent[0].astype(F32) + sent[1].astype(F32) + sent[2].astype(F32)
    d_input = norm_backward(g0, d_normed, sums, all0[1:3], weights0[0][0])
    small0 = small_gradients(d_normed, all0[1:3], dmix0, fsum0)

    def to_owner(first, second, axis):
        mine, other = both(first, second)
        arrived = swap(other, "section", 1)
        return jnp.where(is_first, jnp.concatenate([mine, arrived], axis), jnp.concatenate([arrived, mine], axis)).astype(F32)

    grads_out = to_owner(sum_blocks(out_blocks0), sum_blocks(out_blocks1), 0)
    small_mine, small_send = both(small0, small1)
    small_sum = small_mine + swap(small_send, "section", 1)
    small_parts = dp_sends(small_sum)
    keep, send = both(d_input, out)
    arrived = swap(send, "section", 1)
    boundary = jnp.where(is_first, jnp.stack([keep, arrived]), jnp.stack([arrived, keep]))
    meanwhile.append(arrived)
    steps0 += list(ring0)
    grads_in = to_owner(steps0[-1][1], red_in1, 1)
    small_sum = sum(after(small_parts, steps0[-1][0]))
    feat_grad = small_sum[2 * shard_width:2 * shard_width + LANES].reshape(heads, HEAD) / feat_weight[0]
    freq_grad = jnp.einsum("nk,hnm->hkm", table, small_sum[2 * shard_width + LANES:].reshape(heads, HEAD, HEAD),
                           precision=lax.Precision.HIGHEST)
    qkv_grad = jnp.stack([grads_in[:, t * shard_width:(t + 1) * shard_width] for t in range(3)])
    return (
        boundary[None],
        small_sum[None, :shard_width],
        small_sum[None, shard_width:2 * shard_width],
        qkv_grad[None],
        grads_out[None, :shard_width],
        grads_in[None, :, 3 * shard_width:],
        grads_out[None, shard_width:],
        freq_grad[None],
        feat_grad[None],
    )


def solution(mesh):
    placed = (
        P("dp", None, "mp"), P("dp", None, "mp"), P("dp"), P("section", None), P("section", None),
        P("section", None, None, "mp"), P("section", "mp", None), P("section", None, "mp"), P("section", "mp", None),
        P("section", "mp", None, None), P("section", "mp", None),
    )
    return jax.shard_map(
        shards,
        mesh=mesh,
        in_specs=placed,
        out_specs=(
            P("section", "dp", None, "mp"), P("section", "mp"), P("section", "mp"), P("section", None, "dp", "mp"),
            P("section", "mp", "dp"), P("section", "dp", "mp"), P("section", "mp", "dp"), P("section", "mp", None, None),
            P("section", "mp", None),
        ),
        check_vma=False,
    )
```

```python
import functools
import math

import jax
import jax.numpy as jnp
from jax import lax
from jax.experimental import pallas as pl
from jax.experimental.pallas import tpu as pltpu
from jax.sharding import PartitionSpec as P

ROT = 16
TILE = 256
HEAD = 64
LANES = 256
EPS = 1e-05
F32 = jnp.float32
BF16 = jnp.bfloat16
RSQRT2 = math.sqrt(0.5)
RSQRT2PI = 1.0 / math.sqrt(2.0 * math.pi)
SAVED = 14


def dot_nn(a, b):
    return lax.dot_general(a, b, (((1,), (0,)), ((), ())), preferred_element_type=F32)


def dot_nt(a, b):
    return lax.dot_general(a, b, (((1,), (1,)), ((), ())), preferred_element_type=F32)


def dot_tn(a, b):
    return lax.dot_general(a, b, (((0,), (0,)), ((), ())), preferred_element_type=F32)


def split(values):
    high = values.astype(BF16)
    return high, (values - high.astype(F32)).astype(BF16)


def iota(shape, dim):
    return lax.broadcasted_iota(jnp.int32, shape, dim)


def partner(values):
    later = pltpu.roll(values, LANES - ROT // 2, 1)
    earlier = pltpu.roll(values, ROT // 2, 1)
    lower = iota(values.shape, 1) % HEAD < ROT // 2
    return jnp.where(lower, later, earlier)


def twice(table):
    return jnp.concatenate([table, table], axis=1)


def head_of(shape, dim):
    return iota(shape, dim) // HEAD


def weight_copies(refs, w_in, w_out, sems, which):
    qkv, up, out, down = refs
    ends = [(qkv.at[0, t], w_in.at[:, t * LANES:(t + 1) * LANES]) for t in range(3)] + [
        (up.at[0], w_in.at[:, 3 * LANES:]), (out.at[0], w_out.at[0:LANES, :]), (down.at[0], w_out.at[LANES:, :])]
    return [pltpu.make_async_copy(*ends[i], sems.at[i]) for i in which]


def start_weights(meta, mine, other, w_in, w_out, sems, order):
    def start(refs):
        for copy in weight_copies(refs, w_in, w_out, sems, order):
            copy.start()

    @pl.when(meta[1] == 1)
    def _():
        start(mine)

    @pl.when(meta[1] != 1)
    def _():
        start(other)


def wait_weights(step, refs, w_in, w_out, sems, which):
    @pl.when(step == 0)
    def _():
        for copy in weight_copies(refs, w_in, w_out, sems, which):
            copy.wait()


def forward_kernel(carried, phased, *refs):
    refs = list(refs)
    take = lambda n: [refs.pop(0) for _ in range(n)]
    meta, lens = take(2)
    p0, p1, p2, p3a, p3b, gain, bias, mix_hi, mix_lo, feat_w, cos_t, sin_t = take(12)
    mine, other = take(4), take(4)
    if carried:
        state_in, ksum_in = take(2)
        take(SAVED)
    parts = take(5 if phased else 4)
    normed, xhat, rstd, rq_o, rk_o, qf_o, kf_o, v_o, hcat, dgelu, invz, att_o, prior_s, prior_k = take(SAVED)
    state, ksum, w_in, w_out, sems = take(5)
    tile = pl.program_id(0)
    rank = meta[0]
    half = LANES // 2

    @pl.when(tile == 0)
    def _():
        start_weights(meta, mine, other, w_in, w_out, sems, (0, 1, 2, 3, 4, 5))
        if carried:
            state[...] = state_in[...]
            ksum[...] = ksum_in[...]
        else:
            state[...] = jnp.zeros_like(state)
            ksum[...] = jnp.zeros_like(ksum)

    pieces = [p0[...].astype(F32), p1[...].astype(F32), p2[...].astype(F32),
              jnp.concatenate([p3a[...], p3b[...]], axis=1).astype(F32)]
    width = 4 * LANES
    mean = jnp.sum(pieces[0] + pieces[1] + pieces[2] + pieces[3], axis=1, keepdims=True) * (1.0 / width)
    pieces = [piece - mean for piece in pieces]
    squares = sum(piece * piece for piece in pieces)
    factor = lax.rsqrt(jnp.sum(squares, axis=1, keepdims=True) * (1.0 / width) + EPS)
    for r in range(4):
        at = pl.ds(pl.multiple_of((rank ^ r) * LANES, LANES), LANES)
        hat = pieces[r] * factor
        if r == 0:
            xhat[...] = hat
        normed[:, at] = (hat * gain[:, at] + bias[:, at]).astype(BF16)
    rstd[...] = jnp.broadcast_to(factor, (TILE, half))
    tokens = normed[...]

    wait_weights(tile, mine, w_in, w_out, sems, (0, 1, 2))
    cosine, sine = twice(cos_t[...]), twice(sin_t[...])
    query = dot_nn(tokens, w_in[:, 0:LANES])
    key = dot_nn(tokens, w_in[:, LANES:2 * LANES])
    value = dot_nn(tokens, w_in[:, 2 * LANES:3 * LANES]).astype(BF16)
    rq = query * cosine + partner(query) * sine
    rk = key * cosine + partner(key) * sine
    weight = feat_w[...]

    def logits(rows):
        high, low = split(rows)
        return dot_nn(high, mix_hi[...]) + dot_nn(low, mix_hi[...]) + dot_nn(high, mix_lo[...])

    positions = lens[1] + tile * TILE + iota((TILE, LANES), 0)
    real = (positions < lens[0]).astype(F32)
    qf = (weight * jnp.exp(logits(rq))).astype(BF16)
    kf = (weight * jnp.exp(logits(rk)) * real).astype(BF16)
    rq_o[...] = rq.astype(BF16)
    rk_o[...] = rk.astype(BF16)
    qf_o[...] = qf
    kf_o[...] = kf
    v_o[...] = value

    square = (TILE, TILE)
    lower = iota(square, 0) >= iota(square, 1)
    same = head_of(square, 0) == head_of(square, 1)
    cumulative = dot_nn(lower.astype(BF16), kf) + ksum[0:1, :]
    high, low = split(qf.astype(F32) * cumulative)
    ones = same.astype(BF16)
    inverse = 1.0 / (dot_nn(high, ones) + dot_nn(low, ones))
    prior = jnp.where(same, state[...], 0.0)
    prior_hi, prior_lo = split(prior)
    numer = dot_nn(qf, prior_hi) + dot_nn(qf, prior_lo)
    lane_head = head_of((TILE, LANES), 1)
    zero = jnp.zeros((TILE, LANES), BF16)
    for h in range(LANES // HEAD):
        here = lane_head == h
        scores = dot_nt(qf, jnp.where(here, kf, zero))
        scores = jnp.where(lower, scores, 0.0).astype(BF16)
        numer = numer + dot_nn(scores, jnp.where(here, value, zero))
    prior_s[0] = prior
    prior_k[0] = ksum[...]
    state[...] = state[...] + dot_tn(kf, value)
    ksum[...] = jnp.broadcast_to(cumulative[TILE - 1:TILE, :], ksum.shape)
    invz[...] = inverse
    attended = numer * inverse
    att_o[...] = attended
    hcat[:, 0:LANES] = attended.astype(BF16)

    wait_weights(tile, mine, w_in, w_out, sems, (3,))
    for c in range(4):
        cols = slice(c * LANES, (c + 1) * LANES)
        up = dot_nn(tokens, w_in[:, (3 + c) * LANES:(4 + c) * LANES])
        cdf = 0.5 * (1.0 + lax.erf(up * RSQRT2))
        hcat[:, (1 + c) * LANES:(2 + c) * LANES] = (up * cdf).astype(BF16)
        dgelu[:, cols] = (cdf + up * (RSQRT2PI * jnp.exp(-0.5 * up * up))).astype(BF16)

    wait_weights(tile, mine, w_in, w_out, sems, (4, 5))
    hidden = hcat[...]
    emit(rank, lambda at: dot_nn(hidden, w_out[:, at]), parts)


def emit(rank, product, parts):
    half = LANES // 2
    for r in range(4):
        at = pl.ds(pl.multiple_of((rank ^ r) * LANES, LANES), LANES)
        part = product(at)
        if len(parts) == 4:
            parts[r][...] = part.astype(parts[r].dtype)
            continue
        sx, sy, k0, ka, kb = parts
        if r == 0:
            k0[...] = part
        elif r == 1:
            sx[0] = part[:, :half].astype(BF16)
            kb[...] = part[:, half:]
        elif r == 2:
            ka[...] = part[:, :half]
            sy[0] = part[:, half:].astype(BF16)
        else:
            sx[1] = part[:, :half].astype(BF16)
            sy[1] = part[:, half:].astype(BF16)


def backward_kernel(carried, phased, *refs):
    refs = list(refs)
    take = lambda n: [refs.pop(0) for _ in range(n)]
    meta, = take(1)
    pieces = take(5)
    normed, rq, rk, qf_i, kf_i, v_i, att_i, dgelu, invz, prior_s, prior_k, gain, bias, mix_hi, cos_t, sin_t = take(16)
    mine, other = take(4), take(4)
    if carried:
        state_in, gsum_in, dmix_in, fsum_in = take(4)
        take(2)
    parts = take(5 if phased else 4)
    stats, dcat, state, gsum, dmix, fsum = take(6)
    w_in, w_out, sems, grad = take(4)
    step = pl.program_id(0)
    rank = meta[0]

    @pl.when(step == 0)
    def _():
        start_weights(meta, mine, other, w_in, w_out, sems, (4, 5, 0, 1, 2, 3))
        if carried:
            state[...] = state_in[...]
            gsum[...] = gsum_in[...]
            dmix[...] = dmix_in[...]
            fsum[...] = fsum_in[...]
        else:
            state[...] = jnp.zeros_like(state)
            gsum[...] = jnp.zeros_like(gsum)
            dmix[...] = jnp.zeros_like(dmix)
            fsum[...] = jnp.zeros_like(fsum)

    wait_weights(step, mine, w_in, w_out, sems, (4, 5))
    assemble(rank, pieces, grad)
    g = grad[...]
    d_att = dot_nt(g, w_out[0:LANES, :]).astype(BF16).astype(F32)
    square = (TILE, TILE)
    same = head_of(square, 0) == head_of(square, 1)
    ones = same.astype(BF16)
    inverse = invz[...]
    dn = (d_att * inverse).astype(BF16)
    dn32 = dn.astype(F32)
    high, low = split(dn32 * att_i[...])
    dden = -(dot_nn(high, ones) + dot_nn(low, ones))
    den_hi = dden.astype(BF16).astype(F32)
    roll_hi = pltpu.roll(den_hi, HEAD, 1)
    roll_lo = pltpu.roll(dden - den_hi, HEAD, 1)
    qf, kf, value = qf_i[...], kf_i[...], v_i[...]
    zero = jnp.zeros((TILE, LANES), BF16)
    one = jnp.ones((TILE, LANES), BF16)
    lane = iota((TILE, LANES), 1)
    lane_head = lane // HEAD
    below = iota(square, 0) >= iota(square, 1)
    above = iota(square, 0) <= iota(square, 1)
    prior_hi, prior_lo = split(prior_s[0])
    later_hi, later_lo = split(jnp.where(same, state[...], 0.0))
    d_qf = dot_nt(dn, prior_hi) + dot_nt(dn, prior_lo) + prior_k[0, 0:1, :] * dden
    d_kf = dot_nt(value, later_hi) + dot_nt(value, later_lo) + gsum[0:1, :]
    d_v = dot_nn(kf, later_hi)
    heads = LANES // HEAD
    for h in range(heads):
        here = lane_head == h
        spare = HEAD * ((h + 1) % heads)
        left = jnp.where(lane == spare, roll_hi, jnp.where(lane == spare + 1, roll_lo, dn32)).astype(BF16)
        right = jnp.where(here, value, jnp.where((lane == spare) | (lane == spare + 1), one, zero))
        k_here = jnp.where(here, kf, zero)
        q_here = jnp.where(here, qf, zero)
        d_here = jnp.where(here, dn, zero)
        scores_t = jnp.where(above, dot_nt(k_here, qf), 0.0).astype(BF16)
        ds = jnp.where(below, dot_nt(left, right), 0.0).astype(BF16)
        ds_t = jnp.where(above, dot_nt(right, left), 0.0).astype(BF16)
        d_qf = d_qf + dot_nn(ds, k_here)
        d_kf = d_kf + dot_nn(ds_t, q_here)
        d_v = d_v + dot_nn(scores_t, d_here)
    state[...] = state[...] + dot_tn(qf, dn)
    gsum[...] = gsum[...] + jnp.sum(qf.astype(F32) * dden, axis=0, keepdims=True)
    dlq = d_qf * qf.astype(F32)
    dlk = d_kf * kf.astype(F32)
    fsum[...] = fsum[...] + jnp.sum(dlq + dlk, axis=0, keepdims=True)
    dlq, dlk = dlq.astype(BF16), dlk.astype(BF16)
    dmix[...] = dmix[...] + dot_tn(rq[...], dlq) + dot_tn(rk[...], dlk)
    cosine, sine = twice(cos_t[...]), twice(sin_t[...])
    for c, dl in ((0, dlq), (1, dlk)):
        dr = dot_nt(dl, mix_hi[...])
        dcat[:, c * LANES:(c + 1) * LANES] = (dr * cosine - partner(dr) * sine).astype(BF16)
    dcat[:, 2 * LANES:3 * LANES] = d_v.astype(BF16)
    for c in range(4):
        cols = slice(c * LANES, (c + 1) * LANES)
        d_act = dot_nt(g, w_out[(1 + c) * LANES:(2 + c) * LANES, :])
        dcat[:, (3 + c) * LANES:(4 + c) * LANES] = (d_act * dgelu[:, cols].astype(F32)).astype(BF16)
    wait_weights(step, mine, w_in, w_out, sems, (0, 1, 2, 3))
    wide = dcat[...]
    row = iota((8, LANES), 0)
    first, second = (row == 0).astype(BF16), (row == 1).astype(BF16)
    totals = []

    def product(at):
        part = dot_nt(wide, w_in[at, :])
        one_side = (part * gain[:, at]).astype(BF16)
        other = (part * (normed[:, at].astype(F32) - bias[:, at])).astype(BF16)
        totals.append(dot_nt(first, one_side) + dot_nt(second, other))
        return part

    emit(rank, product, parts)
    stats[...] = totals[0] + totals[1] + totals[2] + totals[3]


def assemble(rank, pieces, whole):
    half = LANES // 2
    for r in range(3):
        whole[:, pl.ds(pl.multiple_of((rank ^ r) * LANES, LANES), LANES)] = pieces[r][...]
    at = pl.multiple_of((rank ^ 3) * LANES, LANES)
    whole[:, pl.ds(at, half)] = pieces[3][...]
    whole[:, pl.ds(pl.multiple_of(at + half, half), half)] = pieces[4][...]


def product_kernel(steps, meta, left, *refs):
    *rights, out_other, out_own = refs[:-1] if len(refs) > 3 else refs
    step = pl.program_id(0)
    if len(rights) == 1:
        right = rights[0]
    else:
        right = refs[-1]

        @pl.when(step == 0)
        def _():
            assemble(meta[1], rights, right)

    product = dot_tn(left[...], right[...]).astype(BF16)

    @pl.when(step < steps)
    def _():
        out_other[...] = product

    @pl.when(step >= steps)
    def _():
        out_own[...] = product


def partial_outs(rows, phased, row_of):
    half = LANES // 2
    if not phased:
        shapes = [jax.ShapeDtypeStruct((rows, LANES), F32)] + [jax.ShapeDtypeStruct((rows, LANES), BF16)] * 3
        return shapes, [pl.BlockSpec((TILE, LANES), lambda *i: (row_of(*i), 0))] * 4
    shapes = [jax.ShapeDtypeStruct((2, rows, half), BF16)] * 2 + [
        jax.ShapeDtypeStruct((rows, LANES), F32), jax.ShapeDtypeStruct((rows, half), F32),
        jax.ShapeDtypeStruct((rows, half), F32)]
    specs = [pl.BlockSpec((2, TILE, half), lambda *i: (0, row_of(*i), 0))] * 2 + [
        pl.BlockSpec((TILE, width), lambda *i: (row_of(*i), 0)) for width in (LANES, half, half)]
    return shapes, specs


def fixed(shape):
    return pl.BlockSpec(shape, lambda *i: (0,) * len(shape))


def outside(count):
    return [pl.BlockSpec(memory_space=pl.ANY)] * count


def params(size):
    return pltpu.CompilerParams(dimension_semantics=("arbitrary",), vmem_limit_bytes=size << 20)


def weight_scratch(width):
    return [pltpu.VMEM((width, 3 * LANES + width), BF16), pltpu.VMEM((LANES + width, width), BF16),
            pltpu.SemaphoreType.DMA((6,))]


def forward_layer(meta, lens, pieces, weights, tables, length, first_row, phased, carry=None):
    rows = pieces[0].shape[0]
    tiles, before = rows // TILE, first_row // TILE
    half, width = LANES // 2, 4 * LANES
    local = lambda t, *_: t
    there = lambda t, *_: before + t
    by_row = lambda n, row_of: pl.BlockSpec((TILE, n), lambda *i: (row_of(*i), 0))
    (gain, bias, mix_hi, mix_lo, feat_w), mine, other = weights
    small = (gain, bias, mix_hi, mix_lo, feat_w)
    shapes, specs = partial_outs(rows, phased, local)
    extra = [(width, BF16), (LANES, F32), (half, F32)] + [(LANES, BF16)] * 5 + [
        (LANES + width, BF16), (width, BF16), (LANES, F32), (LANES, F32)]
    shapes += [jax.ShapeDtypeStruct((length, n), d) for n, d in extra]
    specs += [by_row(n, there) for n, _ in extra]
    shapes += [jax.ShapeDtypeStruct((length // TILE, LANES, LANES), F32), jax.ShapeDtypeStruct((length // TILE, 8, LANES), F32)]
    specs += [pl.BlockSpec((1, n, LANES), lambda *i: (there(*i), 0, 0)) for n in (LANES, 8)]
    states = [(LANES, LANES), (8, LANES)]
    shapes += [jax.ShapeDtypeStruct(s, F32) for s in states]
    specs += [fixed(s) for s in states]
    operands = [meta, jnp.stack([lens[0], jnp.int32(first_row)]), *pieces, *small, *tables, *mine, *other]
    in_specs = [by_row(p.shape[1], local) for p in pieces] + [fixed(w.shape) for w in small] + [by_row(half, there)] * 2 + outside(8)
    aliases = {}
    if carry is not None:
        state, saved = carry
        operands += [*state, *saved]
        in_specs += [fixed(s) for s in states] + outside(SAVED)
        aliases = {len(operands) - SAVED + i: len(shapes) - 2 - SAVED + i for i in range(SAVED)}
    outs = pl.pallas_call(
        functools.partial(forward_kernel, carry is not None, phased),
        name="layer_forward",
        out_shape=shapes,
        grid_spec=pltpu.PrefetchScalarGridSpec(
            num_scalar_prefetch=2, grid=(tiles,), in_specs=in_specs, out_specs=specs, scratch_shapes=weight_scratch(width)),
        input_output_aliases=aliases,
        compiler_params=params(56),
        cost_estimate=pl.CostEstimate(flops=rows * 20_000_000, transcendentals=rows * 5000, bytes_accessed=24 << 20),
    )(*operands)
    count = 5 if phased else 4
    return outs[:count], outs[count:count + SAVED], outs[count + SAVED:]


def backward_layer(meta, pieces, saved, weights, tables, length, first_row, phased, carry=None):
    rows = pieces[0].shape[0]
    tiles, before = rows // TILE, first_row // TILE
    half, width = LANES // 2, 4 * LANES
    local = lambda t, *_: tiles - 1 - t
    there = lambda t, *_: before + tiles - 1 - t
    by_row = lambda n, row_of=there: pl.BlockSpec((TILE, n), lambda *i: (row_of(*i), 0))
    normed, rq, rk, qf, kf, value, hcat, dgelu, invz, attended, prior_s, prior_k = saved
    (gain, bias, mix_hi, mix_lo, feat_w), mine, other = weights
    shapes, specs = partial_outs(rows, phased, local)
    shapes += [jax.ShapeDtypeStruct((8, length), F32), jax.ShapeDtypeStruct((length, 3 * LANES + width), BF16)]
    specs += [pl.BlockSpec((8, TILE), lambda *i: (0, there(*i))), by_row(3 * LANES + width)]
    states = [(LANES, LANES), (8, LANES)] * 2
    shapes += [jax.ShapeDtypeStruct(s, F32) for s in states]
    specs += [fixed(s) for s in states]
    operands = [meta, *pieces, normed, rq, rk, qf, kf, value, attended, dgelu, invz, prior_s, prior_k, gain, bias, mix_hi, *tables,
                *mine, *other]
    in_specs = [by_row(p.shape[1], local) for p in pieces] + [by_row(width)] + [by_row(LANES)] * 6 + [by_row(width), by_row(LANES)] + [
        pl.BlockSpec((1, n, LANES), lambda *i: (there(*i), 0, 0)) for n in (LANES, 8)] + [
        fixed(w.shape) for w in (gain, bias, mix_hi)] + [by_row(half)] * 2 + outside(8)
    aliases = {}
    if carry is not None:
        state, arrays = carry
        operands += [*state, *arrays]
        in_specs += [fixed(s) for s in states] + outside(2)
        aliases = {len(operands) - 2 + i: len(shapes) - 6 + i for i in range(2)}
    outs = pl.pallas_call(
        functools.partial(backward_kernel, carry is not None, phased),
        name="layer_backward",
        out_shape=shapes,
        grid_spec=pltpu.PrefetchScalarGridSpec(
            num_scalar_prefetch=1, grid=(tiles,), in_specs=in_specs, out_specs=specs,
            scratch_shapes=weight_scratch(width) + [pltpu.VMEM((TILE, width), BF16)]),
        input_output_aliases=aliases,
        compiler_params=params(56),
        cost_estimate=pl.CostEstimate(flops=rows * 25_000_000, transcendentals=0, bytes_accessed=24 << 20),
    )(*operands)
    count = 5 if phased else 4
    return outs[:count], outs[count:count + 2], outs[count + 2:]


def swap(value, axis, by):
    return lax.ppermute(value, axis, [(k, k ^ by) for k in range(lax.axis_size(axis))])


def gather_pieces(shard, meanwhile=()):
    from_x, from_y = after((swap(shard, "mp", 1), swap(shard, "mp", 2)), *meanwhile)
    return (shard, from_x, from_y) + last_pieces(from_x, from_y)


def last_pieces(from_x, from_y):
    half = from_x.shape[1] // 2
    return tuple(lax.optimization_barrier((swap(from_x[:, :half], "mp", 2), swap(from_y[:, half:], "mp", 1))))


def after(values, *others):
    if not others:
        return values
    return lax.optimization_barrier((values, others))[0]


def direct_sends(parts):
    return parts[0], [swap(part, "mp", r) for r, part in enumerate(parts) if r > 0]


def scatter_start(parts):
    return swap(parts[0], "mp", 1), swap(parts[1], "mp", 2)


def scatter_turn(parts, arrived):
    _, _, _, ka, kb = parts
    in_x, in_y = arrived
    return (ka + in_x[1].astype(F32)).astype(BF16), (kb + in_y[1].astype(F32)).astype(BF16)


def scatter_end(parts, arrived, to_y, to_x):
    _, _, k0, ka, _ = parts
    in_x, in_y = arrived
    half = ka.shape[1]
    last_y, last_x = swap(to_y, "mp", 2), swap(to_x, "mp", 1)
    return jnp.concatenate(
        [k0[:, :half] + in_x[0].astype(F32) + last_y.astype(F32), k0[:, half:] + in_y[0].astype(F32) + last_x.astype(F32)],
        axis=1)


def scatter_sum(parts):
    arrived = scatter_start(parts)
    return scatter_end(parts, arrived, *scatter_turn(parts, arrived))


def mp_total(values):
    return values + swap(values, "mp", 1) + swap(values, "mp", 2) + swap(values, "mp", 3)


def ring_scatter(block_of, axis, meanwhile=()):
    count = lax.axis_size(axis)
    rank = lax.axis_index(axis)
    pairs = [(k, (k + 1) % count) for k in range(count)]
    total = block_of((rank + count - 1) % count)
    for step in range(2, count + 1):
        arrived = lax.ppermute(total, axis, pairs)
        if step in (2, count):
            arrived = after(arrived, *meanwhile)
        total = (arrived.astype(F32) + block_of((rank + count - step) % count).astype(F32)).astype(BF16)
        yield arrived, total


def dp_sends(values):
    count = lax.axis_size("dp")
    if count > 8:
        return [lax.psum(values, "dp")]
    return [values] + [lax.ppermute(values, "dp", [(i, (i + k) % count) for i in range(count)]) for k in range(1, count)]


def block_sends(block_of, axis):
    count = lax.axis_size(axis)
    rank = lax.axis_index(axis)
    if count > 8:
        return [list(ring_scatter(block_of, axis))[-1][1]]
    return [block_of(rank)] + [
        lax.ppermute(block_of((rank + k) % count), axis, [(i, (i + k) % count) for i in range(count)]) for k in range(1, count)]


def sum_blocks(blocks):
    total = blocks[0].astype(F32)
    for block in blocks[1:]:
        total = total + block.astype(F32)
    return total.astype(BF16)


def weight_gradient(left, rights, section, place):
    rows = left.shape[0]
    whole = len(rights) == 1
    block = 256 if whole else 128
    m = left.shape[1] // (1 if whole else 2)
    n = rights[0].shape[1] // 2 if whole else 4 * LANES
    steps = m // block
    half_at = lambda i, meta: jnp.where(i < steps, 1 - meta[0], meta[0])
    if whole:
        left_at = lambda i, meta: (0, i % steps)
        right_specs = [pl.BlockSpec((rows, n), lambda i, meta: (0, half_at(i, meta)))]
    else:
        left_at = lambda i, meta: (0, half_at(i, meta) * steps + i % steps)
        right_specs = [fixed(p.shape) for p in rights]
    other, own = pl.pallas_call(
        functools.partial(product_kernel, steps),
        name="weight_gradient",
        out_shape=[jax.ShapeDtypeStruct((m, n), BF16)] * 2,
        grid_spec=pltpu.PrefetchScalarGridSpec(
            num_scalar_prefetch=1, grid=(2 * steps,),
            in_specs=[pl.BlockSpec((rows, block), left_at)] + right_specs,
            out_specs=[pl.BlockSpec((block, n), lambda i, meta: (jnp.minimum(i, steps - 1), 0)),
                       pl.BlockSpec((block, n), lambda i, meta: (jnp.maximum(i - steps, 0), 0))],
            scratch_shapes=[] if whole else [pltpu.VMEM((rows, n), BF16)]),
        compiler_params=params(20),
        cost_estimate=pl.CostEstimate(flops=4 * rows * m * n, transcendentals=0, bytes_accessed=4 * (rows * (m + n) + m * n)),
    )(jnp.stack([section, place]).astype(jnp.int32), left, *rights)
    return own, swap(other, "section", 1)


def dct_table(order):
    row_index = jnp.arange(order, dtype=F32)[:, None]
    col_index = jnp.arange(order, dtype=F32)[None, :]
    cosines = jnp.sqrt(2.0 / order) * jnp.cos(math.pi * (row_index + 0.5) * col_index / order)
    return cosines * jnp.where(col_index == 0, math.sqrt(0.5), 1.0)


def rotary_tables(length):
    column = jnp.arange(LANES // 2, dtype=jnp.int32) % HEAD
    half = ROT // 2
    index = (column % half).astype(F32)
    angles = jnp.arange(length, dtype=F32)[:, None] * (10000.0 ** (-index * 2.0 / ROT))[None, :]
    turned = (column < ROT)[None, :]
    sign = jnp.where(column < half, -1.0, 1.0)[None, :]
    return jnp.where(turned, jnp.cos(angles), 1.0), jnp.where(turned, sign * jnp.sin(angles), 0.0)


def shards(block_input, cotangent, lengths, ln_gain, ln_bias, w_qkv, w_out, w_up, w_down, freq_table, feat_weight):
    section = lax.axis_index("section")
    place = lax.axis_index("mp")
    group = lax.axis_index("dp")
    groups = lax.axis_size("dp")
    local_slots, length, shard_width = block_input.shape
    width = ln_gain.shape[1]
    heads = freq_table.shape[1]
    is_first = section == 0
    lens = lax.dynamic_slice_in_dim(lengths, section, 1, 0)
    metas = [jnp.stack([place, (section == l).astype(jnp.int32)]).astype(jnp.int32) for l in range(2)]

    def own(values):
        return lax.dynamic_index_in_dim(values, section, 0, keepdims=False)

    shard0 = own(block_input)
    pieces0 = gather_pieces(shard0)

    small = jnp.concatenate([ln_gain[0], ln_bias[0], feat_weight.reshape(-1), freq_table.astype(F32).reshape(-1)])
    small_other = swap(small, "section", 1)
    mine = (w_qkv, w_up, w_out, w_down)
    other = tuple(swap(w, "section", 1) for w in mine)

    def both(mine, other):
        return jnp.where(is_first, mine, other), jnp.where(is_first, other, mine)

    layers_small = both(small, small_other)
    table = dct_table(HEAD)
    eye = jnp.eye(heads, dtype=F32)

    def layer_weights(l):
        vec = layers_small[l]
        gain, bias = vec[:width].reshape(1, width), vec[width:2 * width].reshape(1, width)
        feat = vec[2 * width:2 * width + LANES].reshape(1, LANES)
        freq = vec[2 * width + LANES:].reshape(heads, HEAD, HEAD)
        mixed = jnp.einsum("nk,hkm->hnm", table, freq, precision=lax.Precision.HIGHEST)
        mixed = (eye[:, None, :, None] * mixed[:, :, None, :]).reshape(LANES, LANES)
        high = lax.reduce_precision(mixed, 8, 7)
        return (gain, bias, high.astype(BF16), (mixed - high).astype(BF16), feat), mine, other

    weights0, weights1 = layer_weights(0), layer_weights(1)
    tables = rotary_tables(length)

    cot = after(own(cotangent), pieces0[3], pieces0[4])
    cot_x, cot_y = swap(cot, "mp", 1), swap(cot, "mp", 2)
    part0, all0, _ = forward_layer(metas[0], lens, pieces0, weights0, tables, length, 0, True)
    part0 = after(part0, cot_x, cot_y)
    hidden = (shard0.astype(F32) + scatter_sum(part0)).astype(BF16)
    pieces1 = gather_pieces(hidden)
    cot_x, cot_y = after((cot_x, cot_y), pieces1[3], pieces1[4])
    pieces_g = (cot, cot_x, cot_y) + last_pieces(cot_x, cot_y)
    part1, all1, _ = forward_layer(metas[1], lens, pieces1, weights1, tables, length, 0, False)
    out_kept, out_sent = direct_sends(part1)

    def saved_of(arrays):
        return (arrays[0],) + tuple(arrays[3:])

    def in_block(mine, arrived):
        n = mine.shape[0] // groups
        cut = lambda v, i: lax.dynamic_slice_in_dim(v, i * n, n, 0)
        return lambda i: (cut(mine, i).astype(F32) + cut(arrived, i).astype(F32)).astype(BF16)

    def out_block(mine, arrived):
        n = mine.shape[1] // groups
        cut = lambda v, i: lax.dynamic_slice_in_dim(v, i * n, n, 1)
        return lambda i: (cut(mine, i).astype(F32) + cut(arrived, i).astype(F32)).astype(BF16)

    def run_backward(meta, grad, saved, weights, phased):
        parts, (stats, dcat), (_, _, dmix, fsum) = backward_layer(meta, grad, saved, weights, tables, length, 0, phased)
        return parts, stats, dcat, dmix, fsum

    def norm_backward(grad_shard, d_normed, sums, norm, gain_all):
        xhat, rstd = norm
        gain = lax.dynamic_slice_in_dim(gain_all, place * shard_width, shard_width, 1)
        mean_d = (sums[0] * (1.0 / width))[:, None]
        mean_dx = (sums[1] * (1.0 / width))[:, None]
        return grad_shard.astype(F32) + rstd[:, :1] * (d_normed * gain - mean_d - xhat * mean_dx)

    def small_gradients(d_normed, norm, dmix, fsum):
        gain_part = jnp.sum(d_normed * norm[0], axis=0)
        bias_part = jnp.sum(d_normed, axis=0)
        diagonal = jnp.stack([dmix[h * HEAD:(h + 1) * HEAD, h * HEAD:(h + 1) * HEAD] for h in range(heads)])
        return jnp.concatenate([gain_part, bias_part, fsum[0], diagonal.reshape(-1)])

    saved1, saved0 = saved_of(all1), saved_of(all0)
    out_blocks1 = block_sends(out_block(*weight_gradient(saved1[6], pieces_g, section, place)), "dp")
    grad1_b = after(pieces_g, out_blocks1[0])
    parts, stats, dcat1, dmix1, fsum1 = run_backward(metas[1], grad1_b, saved1, weights1, True)
    parts, stats, dcat1, dmix1, fsum1 = after((parts, stats, dcat1, dmix1, fsum1), *out_blocks1, *out_sent)
    sums = mp_total(stats)
    arrived = after(scatter_start(parts), sums)
    turn = scatter_turn(parts, arrived)
    steps1 = list(ring_scatter(in_block(*weight_gradient(saved1[0], (dcat1,), section, place)), "dp"))
    arrivals1, red_in1 = [arrival for arrival, _ in steps1], steps1[-1][1]
    d_normed = scatter_end(parts, arrived, *turn)
    g0 = norm_backward(cot, d_normed, sums, all1[1:3], weights1[0][0]).astype(BF16)
    small1 = small_gradients(d_normed, all1[1:3], dmix1, fsum1)
    pieces_g0 = gather_pieces(after(g0, arrivals1[0]), arrivals1[1:2])
    pieces_g0 = after(pieces_g0, *arrivals1[2:3])
    out = hidden.astype(F32) + out_kept + out_sent[0].astype(F32) + out_sent[1].astype(F32) + out_sent[2].astype(F32)

    out_blocks0 = block_sends(out_block(*weight_gradient(saved0[6], pieces_g0, section, place)), "dp")
    grad0_b = after(pieces_g0, out_blocks0[0])
    parts, stats, dcat0, dmix0, fsum0 = run_backward(metas[0], grad0_b, saved0, weights0, False)
    parts, stats, dcat0, dmix0, fsum0 = after((parts, stats, dcat0, dmix0, fsum0), *out_blocks0)
    out_blocks1 = after(out_blocks1, dcat0)
    kept, sent = direct_sends(parts)
    mine0, arrived0 = weight_gradient(saved0[0], (dcat0,), section, place)
    block0 = in_block(mine0, arrived0)
    sums = mp_total(after(stats, arrived0))
    meanwhile = list(sent) + [sums]
    ring0 = ring_scatter(block0, "dp", meanwhile)
    steps0 = [next(ring0)]
    meanwhile.clear()
    sent, dmix0, out_blocks0, out_blocks1 = after((sent, dmix0, out_blocks0, out_blocks1), steps0[0][1])
    d_normed = kept + sent[0].astype(F32) + sent[1].astype(F32) + sent[2].astype(F32)
    d_input = norm_backward(g0, d_normed, sums, all0[1:3], weights0[0][0])
    small0 = small_gradients(d_normed, all0[1:3], dmix0, fsum0)

    def to_owner(first, second, axis):
        mine, other = both(first, second)
        arrived = swap(other, "section", 1)
        return jnp.where(is_first, jnp.concatenate([mine, arrived], axis), jnp.concatenate([arrived, mine], axis)).astype(F32)

    grads_out = to_owner(sum_blocks(out_blocks0), sum_blocks(out_blocks1), 0)
    small_mine, small_send = both(small0, small1)
    small_sum = small_mine + swap(small_send, "section", 1)
    small_parts = dp_sends(small_sum)
    keep, send = both(d_input, out)
    arrived = swap(send, "section", 1)
    boundary = jnp.where(is_first, jnp.stack([keep, arrived]), jnp.stack([arrived, keep]))
    meanwhile.append(arrived)
    steps0 += list(ring0)
    grads_in = to_owner(steps0[-1][1], red_in1, 1)
    small_sum = sum(after(small_parts, steps0[-1][0]))
    feat_grad = small_sum[2 * shard_width:2 * shard_width + LANES].reshape(heads, HEAD) / feat_weight[0]
    freq_grad = jnp.einsum("nk,hnm->hkm", table, small_sum[2 * shard_width + LANES:].reshape(heads, HEAD, HEAD),
                           precision=lax.Precision.HIGHEST)
    qkv_grad = jnp.stack([grads_in[:, t * shard_width:(t + 1) * shard_width] for t in range(3)])
    return (
        boundary[None],
        small_sum[None, :shard_width],
        small_sum[None, shard_width:2 * shard_width],
        qkv_grad[None],
        grads_out[None, :shard_width],
        grads_in[None, :, 3 * shard_width:],
        grads_out[None, shard_width:],
        freq_grad[None],
        feat_grad[None],
    )


def solution(mesh):
    placed = (
        P("dp", None, "mp"), P("dp", None, "mp"), P("dp"), P("section", None), P("section", None),
        P("section", None, None, "mp"), P("section", "mp", None), P("section", None, "mp"), P("section", "mp", None),
        P("section", "mp", None, None), P("section", "mp", None),
    )
    return jax.shard_map(
        shards,
        mesh=mesh,
        in_specs=placed,
        out_specs=(
            P("section", "dp", None, "mp"), P("section", "mp"), P("section", "mp"), P("section", None, "dp", "mp"),
            P("section", "mp", "dp"), P("section", "dp", "mp"), P("section", "mp", "dp"), P("section", "mp", None, None),
            P("section", "mp", None),
        ),
        check_vma=False,
    )
```

```python
import functools
import math

import jax
import jax.numpy as jnp
from jax import lax
from jax.experimental import pallas as pl
from jax.experimental.pallas import tpu as pltpu
from jax.sharding import PartitionSpec as P

ROT = 16
TILE = 256
HEAD = 64
LANES = 256
EPS = 1e-05
F32 = jnp.float32
BF16 = jnp.bfloat16
RSQRT2 = math.sqrt(0.5)
RSQRT2PI = 1.0 / math.sqrt(2.0 * math.pi)
SAVED = 14


def dot_nn(a, b):
    return lax.dot_general(a, b, (((1,), (0,)), ((), ())), preferred_element_type=F32)


def dot_nt(a, b):
    return lax.dot_general(a, b, (((1,), (1,)), ((), ())), preferred_element_type=F32)


def dot_tn(a, b):
    return lax.dot_general(a, b, (((0,), (0,)), ((), ())), preferred_element_type=F32)


def split(values):
    high = values.astype(BF16)
    return high, (values - high.astype(F32)).astype(BF16)


def iota(shape, dim):
    return lax.broadcasted_iota(jnp.int32, shape, dim)


def partner(values):
    later = pltpu.roll(values, LANES - ROT // 2, 1)
    earlier = pltpu.roll(values, ROT // 2, 1)
    lower = iota(values.shape, 1) % HEAD < ROT // 2
    return jnp.where(lower, later, earlier)


def twice(table):
    return jnp.concatenate([table, table], axis=1)


def head_of(shape, dim):
    return iota(shape, dim) // HEAD


def weight_copies(refs, w_in, w_out, sems, which):
    qkv, up, out, down = refs
    ends = [(qkv.at[0, t], w_in.at[:, t * LANES:(t + 1) * LANES]) for t in range(3)] + [
        (up.at[0], w_in.at[:, 3 * LANES:]), (out.at[0], w_out.at[0:LANES, :]), (down.at[0], w_out.at[LANES:, :])]
    return [pltpu.make_async_copy(*ends[i], sems.at[i]) for i in which]


def start_weights(meta, mine, other, w_in, w_out, sems, order):
    def start(refs):
        for copy in weight_copies(refs, w_in, w_out, sems, order):
            copy.start()

    @pl.when(meta[1] == 1)
    def _():
        start(mine)

    @pl.when(meta[1] != 1)
    def _():
        start(other)


def wait_weights(step, refs, w_in, w_out, sems, which):
    @pl.when(step == 0)
    def _():
        for copy in weight_copies(refs, w_in, w_out, sems, which):
            copy.wait()


def forward_kernel(carried, phased, *refs):
    refs = list(refs)
    take = lambda n: [refs.pop(0) for _ in range(n)]
    meta, lens = take(2)
    p0, p1, p2, p3a, p3b, gain, bias, mix_hi, mix_lo, feat_w, cos_t, sin_t = take(12)
    mine, other = take(4), take(4)
    if carried:
        state_in, ksum_in = take(2)
        take(SAVED)
    parts = take(5 if phased else 4)
    normed, xhat, rstd, rq_o, rk_o, qf_o, kf_o, v_o, hcat, dgelu, invz, att_o, prior_s, prior_k = take(SAVED)
    state, ksum, w_in, w_out, sems = take(5)
    tile = pl.program_id(0)
    rank = meta[0]
    half = LANES // 2

    @pl.when(tile == 0)
    def _():
        start_weights(meta, mine, other, w_in, w_out, sems, (0, 1, 2, 3, 4, 5))
        if carried:
            state[...] = state_in[...]
            ksum[...] = ksum_in[...]
        else:
            state[...] = jnp.zeros_like(state)
            ksum[...] = jnp.zeros_like(ksum)

    pieces = [p0[...].astype(F32), p1[...].astype(F32), p2[...].astype(F32),
              jnp.concatenate([p3a[...], p3b[...]], axis=1).astype(F32)]
    width = 4 * LANES
    mean = jnp.sum(pieces[0] + pieces[1] + pieces[2] + pieces[3], axis=1, keepdims=True) * (1.0 / width)
    pieces = [piece - mean for piece in pieces]
    squares = sum(piece * piece for piece in pieces)
    factor = lax.rsqrt(jnp.sum(squares, axis=1, keepdims=True) * (1.0 / width) + EPS)
    for r in range(4):
        at = pl.ds(pl.multiple_of((rank ^ r) * LANES, LANES), LANES)
        hat = pieces[r] * factor
        if r == 0:
            xhat[...] = hat
        normed[:, at] = (hat * gain[:, at] + bias[:, at]).astype(BF16)
    rstd[...] = jnp.broadcast_to(factor, (TILE, half))
    tokens = normed[...]

    wait_weights(tile, mine, w_in, w_out, sems, (0, 1, 2))
    cosine, sine = twice(cos_t[...]), twice(sin_t[...])
    query = dot_nn(tokens, w_in[:, 0:LANES])
    key = dot_nn(tokens, w_in[:, LANES:2 * LANES])
    value = dot_nn(tokens, w_in[:, 2 * LANES:3 * LANES]).astype(BF16)
    rq = query * cosine + partner(query) * sine
    rk = key * cosine + partner(key) * sine
    weight = feat_w[...]

    def logits(rows):
        high, low = split(rows)
        return dot_nn(high, mix_hi[...]) + dot_nn(low, mix_hi[...]) + dot_nn(high, mix_lo[...])

    positions = lens[1] + tile * TILE + iota((TILE, LANES), 0)
    real = (positions < lens[0]).astype(F32)
    qf = (weight * jnp.exp(logits(rq))).astype(BF16)
    kf = (weight * jnp.exp(logits(rk)) * real).astype(BF16)
    rq_o[...] = rq.astype(BF16)
    rk_o[...] = rk.astype(BF16)
    qf_o[...] = qf
    kf_o[...] = kf
    v_o[...] = value

    square = (TILE, TILE)
    lower = iota(square, 0) >= iota(square, 1)
    same = head_of(square, 0) == head_of(square, 1)
    cumulative = dot_nn(lower.astype(BF16), kf) + ksum[0:1, :]
    high, low = split(qf.astype(F32) * cumulative)
    ones = same.astype(BF16)
    inverse = 1.0 / (dot_nn(high, ones) + dot_nn(low, ones))
    prior = jnp.where(same, state[...], 0.0)
    prior_hi, prior_lo = split(prior)
    numer = dot_nn(qf, prior_hi) + dot_nn(qf, prior_lo)
    lane_head = head_of((TILE, LANES), 1)
    zero = jnp.zeros((TILE, LANES), BF16)
    for h in range(LANES // HEAD):
        here = lane_head == h
        scores = dot_nt(qf, jnp.where(here, kf, zero))
        scores = jnp.where(lower, scores, 0.0).astype(BF16)
        numer = numer + dot_nn(scores, jnp.where(here, value, zero))
    prior_s[0] = prior
    prior_k[0] = ksum[...]
    state[...] = state[...] + dot_tn(kf, value)
    ksum[...] = jnp.broadcast_to(cumulative[TILE - 1:TILE, :], ksum.shape)
    invz[...] = inverse
    attended = numer * inverse
    att_o[...] = attended
    hcat[:, 0:LANES] = attended.astype(BF16)

    wait_weights(tile, mine, w_in, w_out, sems, (3,))
    for c in range(4):
        cols = slice(c * LANES, (c + 1) * LANES)
        up = dot_nn(tokens, w_in[:, (3 + c) * LANES:(4 + c) * LANES])
        cdf = 0.5 * (1.0 + lax.erf(up * RSQRT2))
        hcat[:, (1 + c) * LANES:(2 + c) * LANES] = (up * cdf).astype(BF16)
        dgelu[:, cols] = (cdf + up * (RSQRT2PI * jnp.exp(-0.5 * up * up))).astype(BF16)

    wait_weights(tile, mine, w_in, w_out, sems, (4, 5))
    hidden = hcat[...]
    emit(rank, lambda at: dot_nn(hidden, w_out[:, at]), parts)


def emit(rank, product, parts):
    half = LANES // 2
    for r in range(4):
        at = pl.ds(pl.multiple_of((rank ^ r) * LANES, LANES), LANES)
        part = product(at)
        if len(parts) == 4:
            parts[r][...] = part.astype(parts[r].dtype)
            continue
        sx, sy, k0, ka, kb = parts
        if r == 0:
            k0[...] = part
        elif r == 1:
            sx[0] = part[:, :half].astype(BF16)
            kb[...] = part[:, half:]
        elif r == 2:
            ka[...] = part[:, :half]
            sy[0] = part[:, half:].astype(BF16)
        else:
            sx[1] = part[:, :half].astype(BF16)
            sy[1] = part[:, half:].astype(BF16)


def backward_kernel(carried, phased, *refs):
    refs = list(refs)
    take = lambda n: [refs.pop(0) for _ in range(n)]
    meta, = take(1)
    pieces = take(5)
    normed, rq, rk, qf_i, kf_i, v_i, att_i, dgelu, invz, prior_s, prior_k, gain, bias, mix_hi, cos_t, sin_t = take(16)
    mine, other = take(4), take(4)
    if carried:
        state_in, gsum_in, dmix_in, fsum_in = take(4)
        take(2)
    parts = take(5 if phased else 4)
    stats, dcat, state, gsum, dmix, fsum = take(6)
    w_in, w_out, sems, grad = take(4)
    step = pl.program_id(0)
    rank = meta[0]

    @pl.when(step == 0)
    def _():
        start_weights(meta, mine, other, w_in, w_out, sems, (4, 5, 0, 1, 2, 3))
        if carried:
            state[...] = state_in[...]
            gsum[...] = gsum_in[...]
            dmix[...] = dmix_in[...]
            fsum[...] = fsum_in[...]
        else:
            state[...] = jnp.zeros_like(state)
            gsum[...] = jnp.zeros_like(gsum)
            dmix[...] = jnp.zeros_like(dmix)
            fsum[...] = jnp.zeros_like(fsum)

    wait_weights(step, mine, w_in, w_out, sems, (4, 5))
    assemble(rank, pieces, grad)
    g = grad[...]
    d_att = dot_nt(g, w_out[0:LANES, :]).astype(BF16).astype(F32)
    square = (TILE, TILE)
    same = head_of(square, 0) == head_of(square, 1)
    ones = same.astype(BF16)
    inverse = invz[...]
    dn = (d_att * inverse).astype(BF16)
    dn32 = dn.astype(F32)
    high, low = split(dn32 * att_i[...])
    dden = -(dot_nn(high, ones) + dot_nn(low, ones))
    den_hi = dden.astype(BF16).astype(F32)
    roll_hi = pltpu.roll(den_hi, HEAD, 1)
    roll_lo = pltpu.roll(dden - den_hi, HEAD, 1)
    qf, kf, value = qf_i[...], kf_i[...], v_i[...]
    zero = jnp.zeros((TILE, LANES), BF16)
    one = jnp.ones((TILE, LANES), BF16)
    lane = iota((TILE, LANES), 1)
    lane_head = lane // HEAD
    below = iota(square, 0) >= iota(square, 1)
    above = iota(square, 0) <= iota(square, 1)
    prior_hi, prior_lo = split(prior_s[0])
    later_hi, later_lo = split(jnp.where(same, state[...], 0.0))
    d_qf = dot_nt(dn, prior_hi) + dot_nt(dn, prior_lo) + prior_k[0, 0:1, :] * dden
    d_kf = dot_nt(value, later_hi) + dot_nt(value, later_lo) + gsum[0:1, :]
    d_v = dot_nn(kf, later_hi)
    heads = LANES // HEAD
    for h in range(heads):
        here = lane_head == h
        spare = HEAD * ((h + 1) % heads)
        left = jnp.where(lane == spare, roll_hi, jnp.where(lane == spare + 1, roll_lo, dn32)).astype(BF16)
        right = jnp.where(here, value, jnp.where((lane == spare) | (lane == spare + 1), one, zero))
        k_here = jnp.where(here, kf, zero)
        q_here = jnp.where(here, qf, zero)
        d_here = jnp.where(here, dn, zero)
        scores_t = jnp.where(above, dot_nt(k_here, qf), 0.0).astype(BF16)
        ds = jnp.where(below, dot_nt(left, right), 0.0).astype(BF16)
        ds_t = jnp.where(above, dot_nt(right, left), 0.0).astype(BF16)
        d_qf = d_qf + dot_nn(ds, k_here)
        d_kf = d_kf + dot_nn(ds_t, q_here)
        d_v = d_v + dot_nn(scores_t, d_here)
    state[...] = state[...] + dot_tn(qf, dn)
    gsum[...] = gsum[...] + jnp.sum(qf.astype(F32) * dden, axis=0, keepdims=True)
    dlq = d_qf * qf.astype(F32)
    dlk = d_kf * kf.astype(F32)
    fsum[...] = fsum[...] + jnp.sum(dlq + dlk, axis=0, keepdims=True)
    dlq, dlk = dlq.astype(BF16), dlk.astype(BF16)
    dmix[...] = dmix[...] + dot_tn(rq[...], dlq) + dot_tn(rk[...], dlk)
    cosine, sine = twice(cos_t[...]), twice(sin_t[...])
    for c, dl in ((0, dlq), (1, dlk)):
        dr = dot_nt(dl, mix_hi[...])
        dcat[:, c * LANES:(c + 1) * LANES] = (dr * cosine - partner(dr) * sine).astype(BF16)
    dcat[:, 2 * LANES:3 * LANES] = d_v.astype(BF16)
    for c in range(4):
        cols = slice(c * LANES, (c + 1) * LANES)
        d_act = dot_nt(g, w_out[(1 + c) * LANES:(2 + c) * LANES, :])
        dcat[:, (3 + c) * LANES:(4 + c) * LANES] = (d_act * dgelu[:, cols].astype(F32)).astype(BF16)
    wait_weights(step, mine, w_in, w_out, sems, (0, 1, 2, 3))
    wide = dcat[...]
    row = iota((8, LANES), 0)
    first, second = (row == 0).astype(BF16), (row == 1).astype(BF16)
    totals = []

    def product(at):
        part = dot_nt(wide, w_in[at, :])
        one_side = (part * gain[:, at]).astype(BF16)
        other = (part * (normed[:, at].astype(F32) - bias[:, at])).astype(BF16)
        totals.append(dot_nt(first, one_side) + dot_nt(second, other))
        return part

    emit(rank, product, parts)
    stats[...] = totals[0] + totals[1] + totals[2] + totals[3]


def assemble(rank, pieces, whole):
    half = LANES // 2
    for r in range(3):
        whole[:, pl.ds(pl.multiple_of((rank ^ r) * LANES, LANES), LANES)] = pieces[r][...]
    at = pl.multiple_of((rank ^ 3) * LANES, LANES)
    whole[:, pl.ds(at, half)] = pieces[3][...]
    whole[:, pl.ds(pl.multiple_of(at + half, half), half)] = pieces[4][...]


def product_kernel(steps, meta, left, *refs):
    *rights, out_other, out_own = refs[:-1] if len(refs) > 3 else refs
    step = pl.program_id(0)
    if len(rights) == 1:
        right = rights[0]
    else:
        right = refs[-1]

        @pl.when(step == 0)
        def _():
            assemble(meta[1], rights, right)

    product = dot_tn(left[...], right[...]).astype(BF16)

    @pl.when(step < steps)
    def _():
        out_other[...] = product

    @pl.when(step >= steps)
    def _():
        out_own[...] = product


def partial_outs(rows, phased, row_of):
    half = LANES // 2
    if not phased:
        shapes = [jax.ShapeDtypeStruct((rows, LANES), F32)] + [jax.ShapeDtypeStruct((rows, LANES), BF16)] * 3
        return shapes, [pl.BlockSpec((TILE, LANES), lambda *i: (row_of(*i), 0))] * 4
    shapes = [jax.ShapeDtypeStruct((2, rows, half), BF16)] * 2 + [
        jax.ShapeDtypeStruct((rows, LANES), F32), jax.ShapeDtypeStruct((rows, half), F32),
        jax.ShapeDtypeStruct((rows, half), F32)]
    specs = [pl.BlockSpec((2, TILE, half), lambda *i: (0, row_of(*i), 0))] * 2 + [
        pl.BlockSpec((TILE, width), lambda *i: (row_of(*i), 0)) for width in (LANES, half, half)]
    return shapes, specs


def fixed(shape):
    return pl.BlockSpec(shape, lambda *i: (0,) * len(shape))


def outside(count):
    return [pl.BlockSpec(memory_space=pl.ANY)] * count


def params(size):
    return pltpu.CompilerParams(dimension_semantics=("arbitrary",), vmem_limit_bytes=size << 20)


def weight_scratch(width):
    return [pltpu.VMEM((width, 3 * LANES + width), BF16), pltpu.VMEM((LANES + width, width), BF16),
            pltpu.SemaphoreType.DMA((6,))]


def forward_layer(meta, lens, pieces, weights, tables, length, first_row, phased, carry=None):
    rows = pieces[0].shape[0]
    tiles, before = rows // TILE, first_row // TILE
    half, width = LANES // 2, 4 * LANES
    local = lambda t, *_: t
    there = lambda t, *_: before + t
    by_row = lambda n, row_of: pl.BlockSpec((TILE, n), lambda *i: (row_of(*i), 0))
    (gain, bias, mix_hi, mix_lo, feat_w), mine, other = weights
    small = (gain, bias, mix_hi, mix_lo, feat_w)
    shapes, specs = partial_outs(rows, phased, local)
    extra = [(width, BF16), (LANES, F32), (half, F32)] + [(LANES, BF16)] * 5 + [
        (LANES + width, BF16), (width, BF16), (LANES, F32), (LANES, F32)]
    shapes += [jax.ShapeDtypeStruct((length, n), d) for n, d in extra]
    specs += [by_row(n, there) for n, _ in extra]
    shapes += [jax.ShapeDtypeStruct((length // TILE, LANES, LANES), F32), jax.ShapeDtypeStruct((length // TILE, 8, LANES), F32)]
    specs += [pl.BlockSpec((1, n, LANES), lambda *i: (there(*i), 0, 0)) for n in (LANES, 8)]
    states = [(LANES, LANES), (8, LANES)]
    shapes += [jax.ShapeDtypeStruct(s, F32) for s in states]
    specs += [fixed(s) for s in states]
    operands = [meta, jnp.stack([lens[0], jnp.int32(first_row)]), *pieces, *small, *tables, *mine, *other]
    in_specs = [by_row(p.shape[1], local) for p in pieces] + [fixed(w.shape) for w in small] + [by_row(half, there)] * 2 + outside(8)
    aliases = {}
    if carry is not None:
        state, saved = carry
        operands += [*state, *saved]
        in_specs += [fixed(s) for s in states] + outside(SAVED)
        aliases = {len(operands) - SAVED + i: len(shapes) - 2 - SAVED + i for i in range(SAVED)}
    outs = pl.pallas_call(
        functools.partial(forward_kernel, carry is not None, phased),
        name="layer_forward",
        out_shape=shapes,
        grid_spec=pltpu.PrefetchScalarGridSpec(
            num_scalar_prefetch=2, grid=(tiles,), in_specs=in_specs, out_specs=specs, scratch_shapes=weight_scratch(width)),
        input_output_aliases=aliases,
        compiler_params=params(56),
        cost_estimate=pl.CostEstimate(flops=rows * 20_000_000, transcendentals=rows * 5000, bytes_accessed=24 << 20),
    )(*operands)
    count = 5 if phased else 4
    return outs[:count], outs[count:count + SAVED], outs[count + SAVED:]


def backward_layer(meta, pieces, saved, weights, tables, length, first_row, phased, carry=None):
    rows = pieces[0].shape[0]
    tiles, before = rows // TILE, first_row // TILE
    half, width = LANES // 2, 4 * LANES
    local = lambda t, *_: tiles - 1 - t
    there = lambda t, *_: before + tiles - 1 - t
    by_row = lambda n, row_of=there: pl.BlockSpec((TILE, n), lambda *i: (row_of(*i), 0))
    normed, rq, rk, qf, kf, value, hcat, dgelu, invz, attended, prior_s, prior_k = saved
    (gain, bias, mix_hi, mix_lo, feat_w), mine, other = weights
    shapes, specs = partial_outs(rows, phased, local)
    shapes += [jax.ShapeDtypeStruct((8, length), F32), jax.ShapeDtypeStruct((length, 3 * LANES + width), BF16)]
    specs += [pl.BlockSpec((8, TILE), lambda *i: (0, there(*i))), by_row(3 * LANES + width)]
    states = [(LANES, LANES), (8, LANES)] * 2
    shapes += [jax.ShapeDtypeStruct(s, F32) for s in states]
    specs += [fixed(s) for s in states]
    operands = [meta, *pieces, normed, rq, rk, qf, kf, value, attended, dgelu, invz, prior_s, prior_k, gain, bias, mix_hi, *tables,
                *mine, *other]
    in_specs = [by_row(p.shape[1], local) for p in pieces] + [by_row(width)] + [by_row(LANES)] * 6 + [by_row(width), by_row(LANES)] + [
        pl.BlockSpec((1, n, LANES), lambda *i: (there(*i), 0, 0)) for n in (LANES, 8)] + [
        fixed(w.shape) for w in (gain, bias, mix_hi)] + [by_row(half)] * 2 + outside(8)
    aliases = {}
    if carry is not None:
        state, arrays = carry
        operands += [*state, *arrays]
        in_specs += [fixed(s) for s in states] + outside(2)
        aliases = {len(operands) - 2 + i: len(shapes) - 6 + i for i in range(2)}
    outs = pl.pallas_call(
        functools.partial(backward_kernel, carry is not None, phased),
        name="layer_backward",
        out_shape=shapes,
        grid_spec=pltpu.PrefetchScalarGridSpec(
            num_scalar_prefetch=1, grid=(tiles,), in_specs=in_specs, out_specs=specs,
            scratch_shapes=weight_scratch(width) + [pltpu.VMEM((TILE, width), BF16)]),
        input_output_aliases=aliases,
        compiler_params=params(56),
        cost_estimate=pl.CostEstimate(flops=rows * 25_000_000, transcendentals=0, bytes_accessed=24 << 20),
    )(*operands)
    count = 5 if phased else 4
    return outs[:count], outs[count:count + 2], outs[count + 2:]


def swap(value, axis, by):
    return lax.ppermute(value, axis, [(k, k ^ by) for k in range(lax.axis_size(axis))])


def gather_pieces(shard, meanwhile=()):
    from_x, from_y = after((swap(shard, "mp", 1), swap(shard, "mp", 2)), *meanwhile)
    return (shard, from_x, from_y) + last_pieces(from_x, from_y)


def last_pieces(from_x, from_y):
    half = from_x.shape[1] // 2
    return tuple(lax.optimization_barrier((swap(from_x[:, :half], "mp", 2), swap(from_y[:, half:], "mp", 1))))


def after(values, *others):
    if not others:
        return values
    return lax.optimization_barrier((values, others))[0]


def direct_sends(parts):
    return parts[0], [swap(part, "mp", r) for r, part in enumerate(parts) if r > 0]


def scatter_start(parts):
    return swap(parts[0], "mp", 1), swap(parts[1], "mp", 2)


def scatter_turn(parts, arrived):
    _, _, _, ka, kb = parts
    in_x, in_y = arrived
    return (ka + in_x[1].astype(F32)).astype(BF16), (kb + in_y[1].astype(F32)).astype(BF16)


def scatter_end(parts, arrived, to_y, to_x):
    _, _, k0, ka, _ = parts
    in_x, in_y = arrived
    half = ka.shape[1]
    last_y, last_x = swap(to_y, "mp", 2), swap(to_x, "mp", 1)
    return jnp.concatenate(
        [k0[:, :half] + in_x[0].astype(F32) + last_y.astype(F32), k0[:, half:] + in_y[0].astype(F32) + last_x.astype(F32)],
        axis=1)


def scatter_sum(parts):
    arrived = scatter_start(parts)
    return scatter_end(parts, arrived, *scatter_turn(parts, arrived))


def mp_total(values):
    return values + swap(values, "mp", 1) + swap(values, "mp", 2) + swap(values, "mp", 3)


def ring_scatter(block_of, axis, meanwhile=()):
    count = lax.axis_size(axis)
    rank = lax.axis_index(axis)
    pairs = [(k, (k + 1) % count) for k in range(count)]
    total = block_of((rank + count - 1) % count)
    for step in range(2, count + 1):
        arrived = lax.ppermute(total, axis, pairs)
        if step in (2, count):
            arrived = after(arrived, *meanwhile)
        total = (arrived.astype(F32) + block_of((rank + count - step) % count).astype(F32)).astype(BF16)
        yield arrived, total


def dp_sends(values):
    count = lax.axis_size("dp")
    if count > 8:
        return [lax.psum(values, "dp")]
    return [values] + [lax.ppermute(values, "dp", [(i, (i + k) % count) for i in range(count)]) for k in range(1, count)]


def block_sends(block_of, axis):
    count = lax.axis_size(axis)
    rank = lax.axis_index(axis)
    if count > 8:
        return [list(ring_scatter(block_of, axis))[-1][1]]
    return [block_of(rank)] + [
        lax.ppermute(block_of((rank + k) % count), axis, [(i, (i + k) % count) for i in range(count)]) for k in range(1, count)]


def sum_blocks(blocks):
    total = blocks[0].astype(F32)
    for block in blocks[1:]:
        total = total + block.astype(F32)
    return total.astype(BF16)


def weight_gradient(left, rights, section, place):
    rows = left.shape[0]
    whole = len(rights) == 1
    block = 256 if whole else 128
    m = left.shape[1] // (1 if whole else 2)
    n = rights[0].shape[1] // 2 if whole else 4 * LANES
    steps = m // block
    half_at = lambda i, meta: jnp.where(i < steps, 1 - meta[0], meta[0])
    if whole:
        left_at = lambda i, meta: (0, i % steps)
        right_specs = [pl.BlockSpec((rows, n), lambda i, meta: (0, half_at(i, meta)))]
    else:
        left_at = lambda i, meta: (0, half_at(i, meta) * steps + i % steps)
        right_specs = [fixed(p.shape) for p in rights]
    other, own = pl.pallas_call(
        functools.partial(product_kernel, steps),
        name="weight_gradient",
        out_shape=[jax.ShapeDtypeStruct((m, n), BF16)] * 2,
        grid_spec=pltpu.PrefetchScalarGridSpec(
            num_scalar_prefetch=1, grid=(2 * steps,),
            in_specs=[pl.BlockSpec((rows, block), left_at)] + right_specs,
            out_specs=[pl.BlockSpec((block, n), lambda i, meta: (jnp.minimum(i, steps - 1), 0)),
                       pl.BlockSpec((block, n), lambda i, meta: (jnp.maximum(i - steps, 0), 0))],
            scratch_shapes=[] if whole else [pltpu.VMEM((rows, n), BF16)]),
        compiler_params=params(20),
        cost_estimate=pl.CostEstimate(flops=4 * rows * m * n, transcendentals=0, bytes_accessed=4 * (rows * (m + n) + m * n)),
    )(jnp.stack([section, place]).astype(jnp.int32), left, *rights)
    return own, swap(other, "section", 1)


def dct_table(order):
    row_index = jnp.arange(order, dtype=F32)[:, None]
    col_index = jnp.arange(order, dtype=F32)[None, :]
    cosines = jnp.sqrt(2.0 / order) * jnp.cos(math.pi * (row_index + 0.5) * col_index / order)
    return cosines * jnp.where(col_index == 0, math.sqrt(0.5), 1.0)


def rotary_tables(length):
    column = jnp.arange(LANES // 2, dtype=jnp.int32) % HEAD
    half = ROT // 2
    index = (column % half).astype(F32)
    angles = jnp.arange(length, dtype=F32)[:, None] * (10000.0 ** (-index * 2.0 / ROT))[None, :]
    turned = (column < ROT)[None, :]
    sign = jnp.where(column < half, -1.0, 1.0)[None, :]
    return jnp.where(turned, jnp.cos(angles), 1.0), jnp.where(turned, sign * jnp.sin(angles), 0.0)


def shards(block_input, cotangent, lengths, ln_gain, ln_bias, w_qkv, w_out, w_up, w_down, freq_table, feat_weight):
    section = lax.axis_index("section")
    place = lax.axis_index("mp")
    group = lax.axis_index("dp")
    groups = lax.axis_size("dp")
    local_slots, length, shard_width = block_input.shape
    width = ln_gain.shape[1]
    heads = freq_table.shape[1]
    is_first = section == 0
    lens = lax.dynamic_slice_in_dim(lengths, section, 1, 0)
    metas = [jnp.stack([place, (section == l).astype(jnp.int32)]).astype(jnp.int32) for l in range(2)]

    def own(values):
        return lax.dynamic_index_in_dim(values, section, 0, keepdims=False)

    shard0 = own(block_input)

    small = jnp.concatenate([ln_gain[0], ln_bias[0], feat_weight.reshape(-1), freq_table.astype(F32).reshape(-1)])
    small_other = swap(small, "section", 1)
    mine = (w_qkv, w_up, w_out, w_down)
    other = tuple(swap(w, "section", 1) for w in mine)
    pieces0 = gather_pieces(shard0, [small_other, other[2]])

    def both(mine, other):
        return jnp.where(is_first, mine, other), jnp.where(is_first, other, mine)

    layers_small = both(small, small_other)
    table = dct_table(HEAD)
    eye = jnp.eye(heads, dtype=F32)

    def layer_weights(l):
        vec = layers_small[l]
        gain, bias = vec[:width].reshape(1, width), vec[width:2 * width].reshape(1, width)
        feat = vec[2 * width:2 * width + LANES].reshape(1, LANES)
        freq = vec[2 * width + LANES:].reshape(heads, HEAD, HEAD)
        mixed = jnp.einsum("nk,hkm->hnm", table, freq, precision=lax.Precision.HIGHEST)
        mixed = (eye[:, None, :, None] * mixed[:, :, None, :]).reshape(LANES, LANES)
        high = lax.reduce_precision(mixed, 8, 7)
        return (gain, bias, high.astype(BF16), (mixed - high).astype(BF16), feat), mine, other

    weights0, weights1 = layer_weights(0), layer_weights(1)
    tables = rotary_tables(length)

    cot = after(own(cotangent), pieces0[3], pieces0[4])
    cot_x, cot_y = swap(cot, "mp", 1), swap(cot, "mp", 2)
    part0, all0, _ = forward_layer(metas[0], lens, pieces0, weights0, tables, length, 0, True)
    part0 = after(part0, cot_x, cot_y)
    hidden = (shard0.astype(F32) + scatter_sum(part0)).astype(BF16)
    pieces1 = gather_pieces(hidden)
    cot_x, cot_y = after((cot_x, cot_y), pieces1[3], pieces1[4])
    pieces_g = (cot, cot_x, cot_y) + last_pieces(cot_x, cot_y)
    part1, all1, _ = forward_layer(metas[1], lens, pieces1, weights1, tables, length, 0, False)
    out_kept, out_sent = direct_sends(part1)

    def saved_of(arrays):
        return (arrays[0],) + tuple(arrays[3:])

    def in_block(mine, arrived):
        n = mine.shape[0] // groups
        cut = lambda v, i: lax.dynamic_slice_in_dim(v, i * n, n, 0)
        return lambda i: (cut(mine, i).astype(F32) + cut(arrived, i).astype(F32)).astype(BF16)

    def out_block(mine, arrived):
        n = mine.shape[1] // groups
        cut = lambda v, i: lax.dynamic_slice_in_dim(v, i * n, n, 1)
        return lambda i: (cut(mine, i).astype(F32) + cut(arrived, i).astype(F32)).astype(BF16)

    def run_backward(meta, grad, saved, weights, phased):
        parts, (stats, dcat), (_, _, dmix, fsum) = backward_layer(meta, grad, saved, weights, tables, length, 0, phased)
        return parts, stats, dcat, dmix, fsum

    def norm_backward(grad_shard, d_normed, sums, norm, gain_all):
        xhat, rstd = norm
        gain = lax.dynamic_slice_in_dim(gain_all, place * shard_width, shard_width, 1)
        mean_d = (sums[0] * (1.0 / width))[:, None]
        mean_dx = (sums[1] * (1.0 / width))[:, None]
        return grad_shard.astype(F32) + rstd[:, :1] * (d_normed * gain - mean_d - xhat * mean_dx)

    def small_gradients(d_normed, norm, dmix, fsum):
        gain_part = jnp.sum(d_normed * norm[0], axis=0)
        bias_part = jnp.sum(d_normed, axis=0)
        diagonal = jnp.stack([dmix[h * HEAD:(h + 1) * HEAD, h * HEAD:(h + 1) * HEAD] for h in range(heads)])
        return jnp.concatenate([gain_part, bias_part, fsum[0], diagonal.reshape(-1)])

    saved1, saved0 = saved_of(all1), saved_of(all0)
    out_blocks1 = block_sends(out_block(*weight_gradient(saved1[6], pieces_g, section, place)), "dp")
    grad1_b = after(pieces_g, out_blocks1[0])
    parts, stats, dcat1, dmix1, fsum1 = run_backward(metas[1], grad1_b, saved1, weights1, True)
    parts, stats, dcat1, dmix1, fsum1 = after((parts, stats, dcat1, dmix1, fsum1), *out_blocks1, *out_sent[:2])
    arrived = scatter_start(parts)
    turn = scatter_turn(parts, arrived)
    steps1 = list(ring_scatter(in_block(*weight_gradient(saved1[0], (dcat1,), section, place)), "dp"))
    arrivals1, red_in1 = [arrival for arrival, _ in steps1], steps1[-1][1]
    d_normed = scatter_end(parts, arrived, *turn)
    sums = mp_total(after(stats, *turn))
    g0 = norm_backward(cot, d_normed, sums, all1[1:3], weights1[0][0]).astype(BF16)
    small1 = small_gradients(d_normed, all1[1:3], dmix1, fsum1)
    pieces_g0 = gather_pieces(after(g0, arrivals1[0]), arrivals1[1:2])
    pieces_g0 = after(pieces_g0, *arrivals1[2:3])
    out = hidden.astype(F32) + out_kept + out_sent[0].astype(F32) + out_sent[1].astype(F32) + out_sent[2].astype(F32)

    out_blocks0 = block_sends(out_block(*weight_gradient(saved0[6], pieces_g0, section, place)), "dp")
    grad0_b = after(pieces_g0, out_blocks0[0])
    parts, stats, dcat0, dmix0, fsum0 = run_backward(metas[0], grad0_b, saved0, weights0, False)
    parts, stats, dcat0, dmix0, fsum0 = after((parts, stats, dcat0, dmix0, fsum0), *out_blocks0, out_sent[2])
    out_blocks1 = after(out_blocks1, dcat0)
    kept, sent = direct_sends(parts)
    mine0, arrived0 = weight_gradient(saved0[0], (dcat0,), section, place)
    block0 = in_block(mine0, arrived0)
    meanwhile = list(sent)
    ring0 = ring_scatter(block0, "dp", meanwhile)
    steps0 = [next(ring0)]
    meanwhile.clear()
    sums = mp_total(after(stats, steps0[0][1]))
    sent, dmix0, out_blocks0, out_blocks1 = after((sent, dmix0, out_blocks0, out_blocks1), steps0[0][1])
    d_normed = kept + sent[0].astype(F32) + sent[1].astype(F32) + sent[2].astype(F32)
    d_input = norm_backward(g0, d_normed, sums, all0[1:3], weights0[0][0])
    small0 = small_gradients(d_normed, all0[1:3], dmix0, fsum0)

    def to_owner(first, second, axis):
        mine, other = both(first, second)
        arrived = swap(other, "section", 1)
        return jnp.where(is_first, jnp.concatenate([mine, arrived], axis), jnp.concatenate([arrived, mine], axis)).astype(F32)

    grads_out = to_owner(sum_blocks(out_blocks0), sum_blocks(out_blocks1), 0)
    small_mine, small_send = both(small0, small1)
    small_sum = small_mine + swap(small_send, "section", 1)
    small_parts = dp_sends(small_sum)
    keep, send = both(d_input, out)
    arrived = swap(send, "section", 1)
    boundary = jnp.where(is_first, jnp.stack([keep, arrived]), jnp.stack([arrived, keep]))
    meanwhile.append(arrived)
    steps0 += list(ring0)
    grads_in = to_owner(steps0[-1][1], red_in1, 1)
    small_sum = sum(after(small_parts, steps0[-1][0]))
    feat_grad = small_sum[2 * shard_width:2 * shard_width + LANES].reshape(heads, HEAD) / feat_weight[0]
    freq_grad = jnp.einsum("nk,hnm->hkm", table, small_sum[2 * shard_width + LANES:].reshape(heads, HEAD, HEAD),
                           precision=lax.Precision.HIGHEST)
    qkv_grad = jnp.stack([grads_in[:, t * shard_width:(t + 1) * shard_width] for t in range(3)])
    return (
        boundary[None],
        small_sum[None, :shard_width],
        small_sum[None, shard_width:2 * shard_width],
        qkv_grad[None],
        grads_out[None, :shard_width],
        grads_in[None, :, 3 * shard_width:],
        grads_out[None, shard_width:],
        freq_grad[None],
        feat_grad[None],
    )


def solution(mesh):
    placed = (
        P("dp", None, "mp"), P("dp", None, "mp"), P("dp"), P("section", None), P("section", None),
        P("section", None, None, "mp"), P("section", "mp", None), P("section", None, "mp"), P("section", "mp", None),
        P("section", "mp", None, None), P("section", "mp", None),
    )
    return jax.shard_map(
        shards,
        mesh=mesh,
        in_specs=placed,
        out_specs=(
            P("section", "dp", None, "mp"), P("section", "mp"), P("section", "mp"), P("section", None, "dp", "mp"),
            P("section", "mp", "dp"), P("section", "dp", "mp"), P("section", "mp", "dp"), P("section", "mp", None, None),
            P("section", "mp", None),
        ),
        check_vma=False,
    )
```

```python
import functools
import math

import jax
import jax.numpy as jnp
from jax import lax
from jax.experimental import pallas as pl
from jax.experimental.pallas import tpu as pltpu
from jax.sharding import PartitionSpec as P

ROT = 16
TILE = 256
HEAD = 64
LANES = 256
EPS = 1e-05
F32 = jnp.float32
BF16 = jnp.bfloat16
RSQRT2 = math.sqrt(0.5)
RSQRT2PI = 1.0 / math.sqrt(2.0 * math.pi)
SAVED = 14


def dot_nn(a, b):
    return lax.dot_general(a, b, (((1,), (0,)), ((), ())), preferred_element_type=F32)


def dot_nt(a, b):
    return lax.dot_general(a, b, (((1,), (1,)), ((), ())), preferred_element_type=F32)


def dot_tn(a, b):
    return lax.dot_general(a, b, (((0,), (0,)), ((), ())), preferred_element_type=F32)


def split(values):
    high = values.astype(BF16)
    return high, (values - high.astype(F32)).astype(BF16)


def iota(shape, dim):
    return lax.broadcasted_iota(jnp.int32, shape, dim)


def partner(values):
    later = pltpu.roll(values, LANES - ROT // 2, 1)
    earlier = pltpu.roll(values, ROT // 2, 1)
    lower = iota(values.shape, 1) % HEAD < ROT // 2
    return jnp.where(lower, later, earlier)


def twice(table):
    return jnp.concatenate([table, table], axis=1)


def head_of(shape, dim):
    return iota(shape, dim) // HEAD


def weight_copies(refs, w_in, w_out, sems, which):
    qkv, up, out, down = refs
    ends = [(qkv.at[0, t], w_in.at[:, t * LANES:(t + 1) * LANES]) for t in range(3)] + [
        (up.at[0], w_in.at[:, 3 * LANES:]), (out.at[0], w_out.at[0:LANES, :]), (down.at[0], w_out.at[LANES:, :])]
    return [pltpu.make_async_copy(*ends[i], sems.at[i]) for i in which]


def start_weights(meta, mine, other, w_in, w_out, sems, order):
    def start(refs):
        for copy in weight_copies(refs, w_in, w_out, sems, order):
            copy.start()

    @pl.when(meta[1] == 1)
    def _():
        start(mine)

    @pl.when(meta[1] != 1)
    def _():
        start(other)


def wait_weights(step, refs, w_in, w_out, sems, which):
    @pl.when(step == 0)
    def _():
        for copy in weight_copies(refs, w_in, w_out, sems, which):
            copy.wait()


def forward_kernel(carried, phased, *refs):
    refs = list(refs)
    take = lambda n: [refs.pop(0) for _ in range(n)]
    meta, lens = take(2)
    p0, p1, p2, p3a, p3b, gain, bias, mix_hi, mix_lo, feat_w, cos_t, sin_t = take(12)
    mine, other = take(4), take(4)
    if carried:
        state_in, ksum_in = take(2)
        take(SAVED)
    parts = take(5 if phased else 4)
    normed, xhat, rstd, rq_o, rk_o, qf_o, kf_o, v_o, hcat, dgelu, invz, att_o, prior_s, prior_k = take(SAVED)
    state, ksum, w_in, w_out, sems = take(5)
    tile = pl.program_id(0)
    rank = meta[0]
    half = LANES // 2

    @pl.when(tile == 0)
    def _():
        start_weights(meta, mine, other, w_in, w_out, sems, (0, 1, 2, 3, 4, 5))
        if carried:
            state[...] = state_in[...]
            ksum[...] = ksum_in[...]
        else:
            state[...] = jnp.zeros_like(state)
            ksum[...] = jnp.zeros_like(ksum)

    pieces = [p0[...].astype(F32), p1[...].astype(F32), p2[...].astype(F32),
              jnp.concatenate([p3a[...], p3b[...]], axis=1).astype(F32)]
    width = 4 * LANES
    mean = jnp.sum(pieces[0] + pieces[1] + pieces[2] + pieces[3], axis=1, keepdims=True) * (1.0 / width)
    pieces = [piece - mean for piece in pieces]
    squares = sum(piece * piece for piece in pieces)
    factor = lax.rsqrt(jnp.sum(squares, axis=1, keepdims=True) * (1.0 / width) + EPS)
    for r in range(4):
        at = pl.ds(pl.multiple_of((rank ^ r) * LANES, LANES), LANES)
        hat = pieces[r] * factor
        if r == 0:
            xhat[...] = hat
        normed[:, at] = (hat * gain[:, at] + bias[:, at]).astype(BF16)
    rstd[...] = jnp.broadcast_to(factor, (TILE, half))
    tokens = normed[...]

    wait_weights(tile, mine, w_in, w_out, sems, (0, 1, 2))
    cosine, sine = twice(cos_t[...]), twice(sin_t[...])
    query = dot_nn(tokens, w_in[:, 0:LANES])
    key = dot_nn(tokens, w_in[:, LANES:2 * LANES])
    value = dot_nn(tokens, w_in[:, 2 * LANES:3 * LANES]).astype(BF16)
    rq = query * cosine + partner(query) * sine
    rk = key * cosine + partner(key) * sine
    weight = feat_w[...]

    def logits(rows):
        high, low = split(rows)
        return dot_nn(high, mix_hi[...]) + dot_nn(low, mix_hi[...]) + dot_nn(high, mix_lo[...])

    positions = lens[1] + tile * TILE + iota((TILE, LANES), 0)
    real = (positions < lens[0]).astype(F32)
    qf = (weight * jnp.exp(logits(rq))).astype(BF16)
    kf = (weight * jnp.exp(logits(rk)) * real).astype(BF16)
    rq_o[...] = rq.astype(BF16)
    rk_o[...] = rk.astype(BF16)
    qf_o[...] = qf
    kf_o[...] = kf
    v_o[...] = value

    square = (TILE, TILE)
    lower = iota(square, 0) >= iota(square, 1)
    same = head_of(square, 0) == head_of(square, 1)
    cumulative = dot_nn(lower.astype(BF16), kf) + ksum[0:1, :]
    high, low = split(qf.astype(F32) * cumulative)
    ones = same.astype(BF16)
    inverse = 1.0 / (dot_nn(high, ones) + dot_nn(low, ones))
    prior = jnp.where(same, state[...], 0.0)
    prior_hi, prior_lo = split(prior)
    numer = dot_nn(qf, prior_hi) + dot_nn(qf, prior_lo)
    lane_head = head_of((TILE, LANES), 1)
    zero = jnp.zeros((TILE, LANES), BF16)
    for h in range(LANES // HEAD):
        here = lane_head == h
        scores = dot_nt(qf, jnp.where(here, kf, zero))
        scores = jnp.where(lower, scores, 0.0).astype(BF16)
        numer = numer + dot_nn(scores, jnp.where(here, value, zero))
    prior_s[0] = prior
    prior_k[0] = ksum[...]
    state[...] = state[...] + dot_tn(kf, value)
    ksum[...] = jnp.broadcast_to(cumulative[TILE - 1:TILE, :], ksum.shape)
    invz[...] = inverse
    attended = numer * inverse
    att_o[...] = attended
    hcat[:, 0:LANES] = attended.astype(BF16)

    wait_weights(tile, mine, w_in, w_out, sems, (3,))
    for c in range(4):
        cols = slice(c * LANES, (c + 1) * LANES)
        up = dot_nn(tokens, w_in[:, (3 + c) * LANES:(4 + c) * LANES])
        cdf = 0.5 * (1.0 + lax.erf(up * RSQRT2))
        hcat[:, (1 + c) * LANES:(2 + c) * LANES] = (up * cdf).astype(BF16)
        dgelu[:, cols] = (cdf + up * (RSQRT2PI * jnp.exp(-0.5 * up * up))).astype(BF16)

    wait_weights(tile, mine, w_in, w_out, sems, (4, 5))
    hidden = hcat[...]
    emit(rank, lambda at: dot_nn(hidden, w_out[:, at]), parts)


def emit(rank, product, parts):
    half = LANES // 2
    for r in range(4):
        at = pl.ds(pl.multiple_of((rank ^ r) * LANES, LANES), LANES)
        part = product(at)
        if len(parts) == 4:
            parts[r][...] = part.astype(parts[r].dtype)
            continue
        sx, sy, k0, ka, kb = parts
        if r == 0:
            k0[...] = part
        elif r == 1:
            sx[0] = part[:, :half].astype(BF16)
            kb[...] = part[:, half:]
        elif r == 2:
            ka[...] = part[:, :half]
            sy[0] = part[:, half:].astype(BF16)
        else:
            sx[1] = part[:, :half].astype(BF16)
            sy[1] = part[:, half:].astype(BF16)


def backward_kernel(carried, phased, *refs):
    refs = list(refs)
    take = lambda n: [refs.pop(0) for _ in range(n)]
    meta, = take(1)
    pieces = take(5)
    normed, rq, rk, qf_i, kf_i, v_i, att_i, dgelu, invz, prior_s, prior_k, gain, bias, mix_hi, cos_t, sin_t = take(16)
    mine, other = take(4), take(4)
    if carried:
        state_in, gsum_in, dmix_in, fsum_in = take(4)
        take(2)
    parts = take(5 if phased else 4)
    stats, dcat, state, gsum, dmix, fsum = take(6)
    w_in, w_out, sems, grad = take(4)
    step = pl.program_id(0)
    rank = meta[0]

    @pl.when(step == 0)
    def _():
        start_weights(meta, mine, other, w_in, w_out, sems, (4, 5, 0, 1, 2, 3))
        if carried:
            state[...] = state_in[...]
            gsum[...] = gsum_in[...]
            dmix[...] = dmix_in[...]
            fsum[...] = fsum_in[...]
        else:
            state[...] = jnp.zeros_like(state)
            gsum[...] = jnp.zeros_like(gsum)
            dmix[...] = jnp.zeros_like(dmix)
            fsum[...] = jnp.zeros_like(fsum)

    wait_weights(step, mine, w_in, w_out, sems, (4, 5))
    assemble(rank, pieces, grad)
    g = grad[...]
    d_att = dot_nt(g, w_out[0:LANES, :]).astype(BF16).astype(F32)
    square = (TILE, TILE)
    same = head_of(square, 0) == head_of(square, 1)
    ones = same.astype(BF16)
    inverse = invz[...]
    dn = (d_att * inverse).astype(BF16)
    dn32 = dn.astype(F32)
    high, low = split(dn32 * att_i[...])
    dden = -(dot_nn(high, ones) + dot_nn(low, ones))
    den_hi = dden.astype(BF16).astype(F32)
    roll_hi = pltpu.roll(den_hi, HEAD, 1)
    roll_lo = pltpu.roll(dden - den_hi, HEAD, 1)
    qf, kf, value = qf_i[...], kf_i[...], v_i[...]
    zero = jnp.zeros((TILE, LANES), BF16)
    one = jnp.ones((TILE, LANES), BF16)
    lane = iota((TILE, LANES), 1)
    lane_head = lane // HEAD
    below = iota(square, 0) >= iota(square, 1)
    above = iota(square, 0) <= iota(square, 1)
    prior_hi, prior_lo = split(prior_s[0])
    later_hi, later_lo = split(jnp.where(same, state[...], 0.0))
    d_qf = dot_nt(dn, prior_hi) + dot_nt(dn, prior_lo) + prior_k[0, 0:1, :] * dden
    d_kf = dot_nt(value, later_hi) + dot_nt(value, later_lo) + gsum[0:1, :]
    d_v = dot_nn(kf, later_hi)
    heads = LANES // HEAD
    for h in range(heads):
        here = lane_head == h
        spare = HEAD * ((h + 1) % heads)
        left = jnp.where(lane == spare, roll_hi, jnp.where(lane == spare + 1, roll_lo, dn32)).astype(BF16)
        right = jnp.where(here, value, jnp.where((lane == spare) | (lane == spare + 1), one, zero))
        k_here = jnp.where(here, kf, zero)
        q_here = jnp.where(here, qf, zero)
        d_here = jnp.where(here, dn, zero)
        scores_t = jnp.where(above, dot_nt(k_here, qf), 0.0).astype(BF16)
        ds = jnp.where(below, dot_nt(left, right), 0.0).astype(BF16)
        ds_t = jnp.where(above, dot_nt(right, left), 0.0).astype(BF16)
        d_qf = d_qf + dot_nn(ds, k_here)
        d_kf = d_kf + dot_nn(ds_t, q_here)
        d_v = d_v + dot_nn(scores_t, d_here)
    state[...] = state[...] + dot_tn(qf, dn)
    gsum[...] = gsum[...] + jnp.sum(qf.astype(F32) * dden, axis=0, keepdims=True)
    dlq = d_qf * qf.astype(F32)
    dlk = d_kf * kf.astype(F32)
    fsum[...] = fsum[...] + jnp.sum(dlq + dlk, axis=0, keepdims=True)
    dlq, dlk = dlq.astype(BF16), dlk.astype(BF16)
    dmix[...] = dmix[...] + dot_tn(rq[...], dlq) + dot_tn(rk[...], dlk)
    cosine, sine = twice(cos_t[...]), twice(sin_t[...])
    for c, dl in ((0, dlq), (1, dlk)):
        dr = dot_nt(dl, mix_hi[...])
        dcat[:, c * LANES:(c + 1) * LANES] = (dr * cosine - partner(dr) * sine).astype(BF16)
    dcat[:, 2 * LANES:3 * LANES] = d_v.astype(BF16)
    for c in range(4):
        cols = slice(c * LANES, (c + 1) * LANES)
        d_act = dot_nt(g, w_out[(1 + c) * LANES:(2 + c) * LANES, :])
        dcat[:, (3 + c) * LANES:(4 + c) * LANES] = (d_act * dgelu[:, cols].astype(F32)).astype(BF16)
    wait_weights(step, mine, w_in, w_out, sems, (0, 1, 2, 3))
    wide = dcat[...]
    row = iota((8, LANES), 0)
    first, second = (row == 0).astype(BF16), (row == 1).astype(BF16)
    totals = []

    def product(at):
        part = dot_nt(wide, w_in[at, :])
        one_side = (part * gain[:, at]).astype(BF16)
        other = (part * (normed[:, at].astype(F32) - bias[:, at])).astype(BF16)
        totals.append(dot_nt(first, one_side) + dot_nt(second, other))
        return part

    emit(rank, product, parts)
    stats[...] = totals[0] + totals[1] + totals[2] + totals[3]


def assemble(rank, pieces, whole):
    half = LANES // 2
    for r in range(3):
        whole[:, pl.ds(pl.multiple_of((rank ^ r) * LANES, LANES), LANES)] = pieces[r][...]
    at = pl.multiple_of((rank ^ 3) * LANES, LANES)
    whole[:, pl.ds(at, half)] = pieces[3][...]
    whole[:, pl.ds(pl.multiple_of(at + half, half), half)] = pieces[4][...]


def product_kernel(steps, meta, left, *refs):
    *rights, out_other, out_own = refs[:-1] if len(refs) > 3 else refs
    step = pl.program_id(0)
    if len(rights) == 1:
        right = rights[0]
    else:
        right = refs[-1]

        @pl.when(step == 0)
        def _():
            assemble(meta[1], rights, right)

    product = dot_tn(left[...], right[...]).astype(BF16)

    @pl.when(step < steps)
    def _():
        out_other[...] = product

    @pl.when(step >= steps)
    def _():
        out_own[...] = product


def partial_outs(rows, phased, row_of):
    half = LANES // 2
    if not phased:
        shapes = [jax.ShapeDtypeStruct((rows, LANES), F32)] + [jax.ShapeDtypeStruct((rows, LANES), BF16)] * 3
        return shapes, [pl.BlockSpec((TILE, LANES), lambda *i: (row_of(*i), 0))] * 4
    shapes = [jax.ShapeDtypeStruct((2, rows, half), BF16)] * 2 + [
        jax.ShapeDtypeStruct((rows, LANES), F32), jax.ShapeDtypeStruct((rows, half), F32),
        jax.ShapeDtypeStruct((rows, half), F32)]
    specs = [pl.BlockSpec((2, TILE, half), lambda *i: (0, row_of(*i), 0))] * 2 + [
        pl.BlockSpec((TILE, width), lambda *i: (row_of(*i), 0)) for width in (LANES, half, half)]
    return shapes, specs


def fixed(shape):
    return pl.BlockSpec(shape, lambda *i: (0,) * len(shape))


def outside(count):
    return [pl.BlockSpec(memory_space=pl.ANY)] * count


def params(size):
    return pltpu.CompilerParams(dimension_semantics=("arbitrary",), vmem_limit_bytes=size << 20)


def weight_scratch(width):
    return [pltpu.VMEM((width, 3 * LANES + width), BF16), pltpu.VMEM((LANES + width, width), BF16),
            pltpu.SemaphoreType.DMA((6,))]


def forward_layer(meta, lens, pieces, weights, tables, length, first_row, phased, carry=None):
    rows = pieces[0].shape[0]
    tiles, before = rows // TILE, first_row // TILE
    half, width = LANES // 2, 4 * LANES
    local = lambda t, *_: t
    there = lambda t, *_: before + t
    by_row = lambda n, row_of: pl.BlockSpec((TILE, n), lambda *i: (row_of(*i), 0))
    (gain, bias, mix_hi, mix_lo, feat_w), mine, other = weights
    small = (gain, bias, mix_hi, mix_lo, feat_w)
    shapes, specs = partial_outs(rows, phased, local)
    extra = [(width, BF16), (LANES, F32), (half, F32)] + [(LANES, BF16)] * 5 + [
        (LANES + width, BF16), (width, BF16), (LANES, F32), (LANES, F32)]
    shapes += [jax.ShapeDtypeStruct((length, n), d) for n, d in extra]
    specs += [by_row(n, there) for n, _ in extra]
    shapes += [jax.ShapeDtypeStruct((length // TILE, LANES, LANES), F32), jax.ShapeDtypeStruct((length // TILE, 8, LANES), F32)]
    specs += [pl.BlockSpec((1, n, LANES), lambda *i: (there(*i), 0, 0)) for n in (LANES, 8)]
    states = [(LANES, LANES), (8, LANES)]
    shapes += [jax.ShapeDtypeStruct(s, F32) for s in states]
    specs += [fixed(s) for s in states]
    operands = [meta, jnp.stack([lens[0], jnp.int32(first_row)]), *pieces, *small, *tables, *mine, *other]
    in_specs = [by_row(p.shape[1], local) for p in pieces] + [fixed(w.shape) for w in small] + [by_row(half, there)] * 2 + outside(8)
    aliases = {}
    if carry is not None:
        state, saved = carry
        operands += [*state, *saved]
        in_specs += [fixed(s) for s in states] + outside(SAVED)
        aliases = {len(operands) - SAVED + i: len(shapes) - 2 - SAVED + i for i in range(SAVED)}
    outs = pl.pallas_call(
        functools.partial(forward_kernel, carry is not None, phased),
        name="layer_forward",
        out_shape=shapes,
        grid_spec=pltpu.PrefetchScalarGridSpec(
            num_scalar_prefetch=2, grid=(tiles,), in_specs=in_specs, out_specs=specs, scratch_shapes=weight_scratch(width)),
        input_output_aliases=aliases,
        compiler_params=params(56),
        cost_estimate=pl.CostEstimate(flops=rows * 20_000_000, transcendentals=rows * 5000, bytes_accessed=24 << 20),
    )(*operands)
    count = 5 if phased else 4
    return outs[:count], outs[count:count + SAVED], outs[count + SAVED:]


def backward_layer(meta, pieces, saved, weights, tables, length, first_row, phased, carry=None):
    rows = pieces[0].shape[0]
    tiles, before = rows // TILE, first_row // TILE
    half, width = LANES // 2, 4 * LANES
    local = lambda t, *_: tiles - 1 - t
    there = lambda t, *_: before + tiles - 1 - t
    by_row = lambda n, row_of=there: pl.BlockSpec((TILE, n), lambda *i: (row_of(*i), 0))
    normed, rq, rk, qf, kf, value, hcat, dgelu, invz, attended, prior_s, prior_k = saved
    (gain, bias, mix_hi, mix_lo, feat_w), mine, other = weights
    shapes, specs = partial_outs(rows, phased, local)
    shapes += [jax.ShapeDtypeStruct((8, length), F32), jax.ShapeDtypeStruct((length, 3 * LANES + width), BF16)]
    specs += [pl.BlockSpec((8, TILE), lambda *i: (0, there(*i))), by_row(3 * LANES + width)]
    states = [(LANES, LANES), (8, LANES)] * 2
    shapes += [jax.ShapeDtypeStruct(s, F32) for s in states]
    specs += [fixed(s) for s in states]
    operands = [meta, *pieces, normed, rq, rk, qf, kf, value, attended, dgelu, invz, prior_s, prior_k, gain, bias, mix_hi, *tables,
                *mine, *other]
    in_specs = [by_row(p.shape[1], local) for p in pieces] + [by_row(width)] + [by_row(LANES)] * 6 + [by_row(width), by_row(LANES)] + [
        pl.BlockSpec((1, n, LANES), lambda *i: (there(*i), 0, 0)) for n in (LANES, 8)] + [
        fixed(w.shape) for w in (gain, bias, mix_hi)] + [by_row(half)] * 2 + outside(8)
    aliases = {}
    if carry is not None:
        state, arrays = carry
        operands += [*state, *arrays]
        in_specs += [fixed(s) for s in states] + outside(2)
        aliases = {len(operands) - 2 + i: len(shapes) - 6 + i for i in range(2)}
    outs = pl.pallas_call(
        functools.partial(backward_kernel, carry is not None, phased),
        name="layer_backward",
        out_shape=shapes,
        grid_spec=pltpu.PrefetchScalarGridSpec(
            num_scalar_prefetch=1, grid=(tiles,), in_specs=in_specs, out_specs=specs,
            scratch_shapes=weight_scratch(width) + [pltpu.VMEM((TILE, width), BF16)]),
        input_output_aliases=aliases,
        compiler_params=params(56),
        cost_estimate=pl.CostEstimate(flops=rows * 25_000_000, transcendentals=0, bytes_accessed=24 << 20),
    )(*operands)
    count = 5 if phased else 4
    return outs[:count], outs[count:count + 2], outs[count + 2:]


def swap(value, axis, by):
    return lax.ppermute(value, axis, [(k, k ^ by) for k in range(lax.axis_size(axis))])


def gather_pieces(shard, meanwhile=()):
    from_x, from_y = after((swap(shard, "mp", 1), swap(shard, "mp", 2)), *meanwhile)
    return (shard, from_x, from_y) + last_pieces(from_x, from_y)


def last_pieces(from_x, from_y):
    half = from_x.shape[1] // 2
    return tuple(lax.optimization_barrier((swap(from_x[:, :half], "mp", 2), swap(from_y[:, half:], "mp", 1))))


def after(values, *others):
    if not others:
        return values
    return lax.optimization_barrier((values, others))[0]


def direct_sends(parts):
    return parts[0], [swap(part, "mp", r) for r, part in enumerate(parts) if r > 0]


def scatter_start(parts):
    return swap(parts[0], "mp", 1), swap(parts[1], "mp", 2)


def scatter_turn(parts, arrived):
    _, _, _, ka, kb = parts
    in_x, in_y = arrived
    return (ka + in_x[1].astype(F32)).astype(BF16), (kb + in_y[1].astype(F32)).astype(BF16)


def scatter_end(parts, arrived, to_y, to_x):
    _, _, k0, ka, _ = parts
    in_x, in_y = arrived
    half = ka.shape[1]
    last_y, last_x = swap(to_y, "mp", 2), swap(to_x, "mp", 1)
    return jnp.concatenate(
        [k0[:, :half] + in_x[0].astype(F32) + last_y.astype(F32), k0[:, half:] + in_y[0].astype(F32) + last_x.astype(F32)],
        axis=1)


def scatter_sum(parts):
    arrived = scatter_start(parts)
    return scatter_end(parts, arrived, *scatter_turn(parts, arrived))


def mp_total(values):
    return values + swap(values, "mp", 1) + swap(values, "mp", 2) + swap(values, "mp", 3)


def ring_scatter(block_of, axis, meanwhile=()):
    count = lax.axis_size(axis)
    rank = lax.axis_index(axis)
    pairs = [(k, (k + 1) % count) for k in range(count)]
    total = block_of((rank + count - 1) % count)
    for step in range(2, count + 1):
        arrived = lax.ppermute(total, axis, pairs)
        if step in (2, count):
            arrived = after(arrived, *meanwhile)
        total = (arrived.astype(F32) + block_of((rank + count - step) % count).astype(F32)).astype(BF16)
        yield arrived, total


def dp_sends(values):
    count = lax.axis_size("dp")
    if count > 8:
        return [lax.psum(values, "dp")]
    return [values] + [lax.ppermute(values, "dp", [(i, (i + k) % count) for i in range(count)]) for k in range(1, count)]


def block_sends(block_of, axis):
    count = lax.axis_size(axis)
    rank = lax.axis_index(axis)
    if count > 8:
        return [list(ring_scatter(block_of, axis))[-1][1]]
    return [block_of(rank)] + [
        lax.ppermute(block_of((rank + k) % count), axis, [(i, (i + k) % count) for i in range(count)]) for k in range(1, count)]


def sum_blocks(blocks):
    total = blocks[0].astype(F32)
    for block in blocks[1:]:
        total = total + block.astype(F32)
    return total.astype(BF16)


def weight_gradient(left, rights, section, place):
    rows = left.shape[0]
    whole = len(rights) == 1
    block = 256 if whole else 128
    m = left.shape[1] // (1 if whole else 2)
    n = rights[0].shape[1] // 2 if whole else 4 * LANES
    steps = m // block
    half_at = lambda i, meta: jnp.where(i < steps, 1 - meta[0], meta[0])
    if whole:
        left_at = lambda i, meta: (0, i % steps)
        right_specs = [pl.BlockSpec((rows, n), lambda i, meta: (0, half_at(i, meta)))]
    else:
        left_at = lambda i, meta: (0, half_at(i, meta) * steps + i % steps)
        right_specs = [fixed(p.shape) for p in rights]
    other, own = pl.pallas_call(
        functools.partial(product_kernel, steps),
        name="weight_gradient",
        out_shape=[jax.ShapeDtypeStruct((m, n), BF16)] * 2,
        grid_spec=pltpu.PrefetchScalarGridSpec(
            num_scalar_prefetch=1, grid=(2 * steps,),
            in_specs=[pl.BlockSpec((rows, block), left_at)] + right_specs,
            out_specs=[pl.BlockSpec((block, n), lambda i, meta: (jnp.minimum(i, steps - 1), 0)),
                       pl.BlockSpec((block, n), lambda i, meta: (jnp.maximum(i - steps, 0), 0))],
            scratch_shapes=[] if whole else [pltpu.VMEM((rows, n), BF16)]),
        compiler_params=params(20),
        cost_estimate=pl.CostEstimate(flops=4 * rows * m * n, transcendentals=0, bytes_accessed=4 * (rows * (m + n) + m * n)),
    )(jnp.stack([section, place]).astype(jnp.int32), left, *rights)
    return own, other


def dct_table(order):
    row_index = jnp.arange(order, dtype=F32)[:, None]
    col_index = jnp.arange(order, dtype=F32)[None, :]
    cosines = jnp.sqrt(2.0 / order) * jnp.cos(math.pi * (row_index + 0.5) * col_index / order)
    return cosines * jnp.where(col_index == 0, math.sqrt(0.5), 1.0)


def rotary_tables(length):
    column = jnp.arange(LANES // 2, dtype=jnp.int32) % HEAD
    half = ROT // 2
    index = (column % half).astype(F32)
    angles = jnp.arange(length, dtype=F32)[:, None] * (10000.0 ** (-index * 2.0 / ROT))[None, :]
    turned = (column < ROT)[None, :]
    sign = jnp.where(column < half, -1.0, 1.0)[None, :]
    return jnp.where(turned, jnp.cos(angles), 1.0), jnp.where(turned, sign * jnp.sin(angles), 0.0)


def shards(block_input, cotangent, lengths, ln_gain, ln_bias, w_qkv, w_out, w_up, w_down, freq_table, feat_weight):
    section = lax.axis_index("section")
    place = lax.axis_index("mp")
    group = lax.axis_index("dp")
    groups = lax.axis_size("dp")
    local_slots, length, shard_width = block_input.shape
    width = ln_gain.shape[1]
    heads = freq_table.shape[1]
    is_first = section == 0
    lens = lax.dynamic_slice_in_dim(lengths, section, 1, 0)
    metas = [jnp.stack([place, (section == l).astype(jnp.int32)]).astype(jnp.int32) for l in range(2)]

    def own(values):
        return lax.dynamic_index_in_dim(values, section, 0, keepdims=False)

    shard0 = own(block_input)

    small = jnp.concatenate([ln_gain[0], ln_bias[0], feat_weight.reshape(-1), freq_table.astype(F32).reshape(-1)])
    small_other = swap(small, "section", 1)
    mine = (w_qkv, w_up, w_out, w_down)
    other = tuple(swap(w, "section", 1) for w in mine)
    pieces0 = gather_pieces(shard0, [small_other, other[2]])

    def both(mine, other):
        return jnp.where(is_first, mine, other), jnp.where(is_first, other, mine)

    layers_small = both(small, small_other)
    table = dct_table(HEAD)
    eye = jnp.eye(heads, dtype=F32)

    def layer_weights(l):
        vec = layers_small[l]
        gain, bias = vec[:width].reshape(1, width), vec[width:2 * width].reshape(1, width)
        feat = vec[2 * width:2 * width + LANES].reshape(1, LANES)
        freq = vec[2 * width + LANES:].reshape(heads, HEAD, HEAD)
        mixed = jnp.einsum("nk,hkm->hnm", table, freq, precision=lax.Precision.HIGHEST)
        mixed = (eye[:, None, :, None] * mixed[:, :, None, :]).reshape(LANES, LANES)
        high = lax.reduce_precision(mixed, 8, 7)
        return (gain, bias, high.astype(BF16), (mixed - high).astype(BF16), feat), mine, other

    weights0, weights1 = layer_weights(0), layer_weights(1)
    tables = rotary_tables(length)

    cot = after(own(cotangent), pieces0[3], pieces0[4])
    cot_x, cot_y = swap(cot, "mp", 1), swap(cot, "mp", 2)
    part0, all0, _ = forward_layer(metas[0], lens, pieces0, weights0, tables, length, 0, True)
    part0 = after(part0, cot_x, cot_y)
    hidden = (shard0.astype(F32) + scatter_sum(part0)).astype(BF16)
    pieces1 = gather_pieces(hidden)
    cot_x, cot_y = after((cot_x, cot_y), pieces1[3], pieces1[4])
    pieces_g = (cot, cot_x, cot_y) + last_pieces(cot_x, cot_y)
    part1, all1, _ = forward_layer(metas[1], lens, pieces1, weights1, tables, length, 0, False)
    out_kept, out_sent = direct_sends(part1)

    def saved_of(arrays):
        return (arrays[0],) + tuple(arrays[3:])

    def in_block(mine, arrived):
        n = mine.shape[0] // groups
        cut = lambda v, i: lax.dynamic_slice_in_dim(v, i * n, n, 0)
        return lambda i: (cut(mine, i).astype(F32) + cut(arrived, i).astype(F32)).astype(BF16)

    def out_block(mine, arrived):
        n = mine.shape[1] // groups
        cut = lambda v, i: lax.dynamic_slice_in_dim(v, i * n, n, 1)
        return lambda i: (cut(mine, i).astype(F32) + cut(arrived, i).astype(F32)).astype(BF16)

    def run_backward(meta, grad, saved, weights, phased):
        parts, (stats, dcat), (_, _, dmix, fsum) = backward_layer(meta, grad, saved, weights, tables, length, 0, phased)
        return parts, stats, dcat, dmix, fsum

    def norm_backward(grad_shard, d_normed, sums, norm, gain_all):
        xhat, rstd = norm
        gain = lax.dynamic_slice_in_dim(gain_all, place * shard_width, shard_width, 1)
        mean_d = (sums[0] * (1.0 / width))[:, None]
        mean_dx = (sums[1] * (1.0 / width))[:, None]
        return grad_shard.astype(F32) + rstd[:, :1] * (d_normed * gain - mean_d - xhat * mean_dx)

    def small_gradients(d_normed, norm, dmix, fsum):
        gain_part = jnp.sum(d_normed * norm[0], axis=0)
        bias_part = jnp.sum(d_normed, axis=0)
        diagonal = jnp.stack([dmix[h * HEAD:(h + 1) * HEAD, h * HEAD:(h + 1) * HEAD] for h in range(heads)])
        return jnp.concatenate([gain_part, bias_part, fsum[0], diagonal.reshape(-1)])

    saved1, saved0 = saved_of(all1), saved_of(all0)
    own, other = weight_gradient(saved1[6], pieces_g, section, place)
    out_blocks1 = block_sends(out_block(own, swap(other, "section", 1)), "dp")
    grad1_b = after(pieces_g, out_blocks1[0])
    parts, stats, dcat1, dmix1, fsum1 = run_backward(metas[1], grad1_b, saved1, weights1, True)
    parts, stats, dcat1, dmix1, fsum1 = after((parts, stats, dcat1, dmix1, fsum1), *out_blocks1, *out_sent[:2])
    arrived, own, other = lax.optimization_barrier(
        (scatter_start(parts), *weight_gradient(saved1[0], (dcat1,), section, place)))
    turn = scatter_turn(parts, arrived)
    steps1 = list(ring_scatter(in_block(own, swap(other, "section", 1)), "dp"))
    arrivals1, red_in1 = [arrival for arrival, _ in steps1], steps1[-1][1]
    d_normed = scatter_end(parts, arrived, *turn)
    sums = mp_total(after(stats, *turn))
    g0 = norm_backward(cot, d_normed, sums, all1[1:3], weights1[0][0]).astype(BF16)
    small1 = small_gradients(d_normed, all1[1:3], dmix1, fsum1)
    pieces_g0 = gather_pieces(after(g0, arrivals1[0]), arrivals1[1:2])
    pieces_g0 = after(pieces_g0, *arrivals1[2:3])
    out = hidden.astype(F32) + out_kept + out_sent[0].astype(F32) + out_sent[1].astype(F32) + out_sent[2].astype(F32)

    own, other = weight_gradient(saved0[6], pieces_g0, section, place)
    out_blocks0 = block_sends(out_block(own, swap(other, "section", 1)), "dp")
    grad0_b = after(pieces_g0, out_blocks0[0])
    parts, stats, dcat0, dmix0, fsum0 = run_backward(metas[0], grad0_b, saved0, weights0, False)
    parts, stats, dcat0, dmix0, fsum0 = after((parts, stats, dcat0, dmix0, fsum0), *out_blocks0, out_sent[2])
    out_blocks1 = after(out_blocks1, dcat0)
    kept, sent = direct_sends(parts)
    sent[:2], own, other = lax.optimization_barrier((sent[:2], *weight_gradient(saved0[0], (dcat0,), section, place)))
    block0 = in_block(own, swap(other, "section", 1))
    meanwhile = sent[2:]
    ring0 = ring_scatter(block0, "dp", meanwhile)
    steps0 = [next(ring0)]
    meanwhile.clear()
    sums = mp_total(after(stats, steps0[0][1]))
    sent, dmix0, out_blocks0, out_blocks1 = after((sent, dmix0, out_blocks0, out_blocks1), steps0[0][1])
    d_normed = kept + sent[0].astype(F32) + sent[1].astype(F32) + sent[2].astype(F32)
    d_input = norm_backward(g0, d_normed, sums, all0[1:3], weights0[0][0])
    small0 = small_gradients(d_normed, all0[1:3], dmix0, fsum0)

    def to_owner(first, second, axis):
        mine, other = both(first, second)
        arrived = swap(other, "section", 1)
        return jnp.where(is_first, jnp.concatenate([mine, arrived], axis), jnp.concatenate([arrived, mine], axis)).astype(F32)

    grads_out = to_owner(sum_blocks(out_blocks0), sum_blocks(out_blocks1), 0)
    small_mine, small_send = both(small0, small1)
    small_sum = small_mine + swap(small_send, "section", 1)
    small_parts = dp_sends(small_sum)
    keep, send = both(d_input, out)
    arrived = swap(send, "section", 1)
    boundary = jnp.where(is_first, jnp.stack([keep, arrived]), jnp.stack([arrived, keep]))
    meanwhile.append(arrived)
    steps0 += list(ring0)
    grads_in = to_owner(steps0[-1][1], red_in1, 1)
    small_sum = sum(after(small_parts, steps0[-1][0]))
    feat_grad = small_sum[2 * shard_width:2 * shard_width + LANES].reshape(heads, HEAD) / feat_weight[0]
    freq_grad = jnp.einsum("nk,hnm->hkm", table, small_sum[2 * shard_width + LANES:].reshape(heads, HEAD, HEAD),
                           precision=lax.Precision.HIGHEST)
    qkv_grad = jnp.stack([grads_in[:, t * shard_width:(t + 1) * shard_width] for t in range(3)])
    return (
        boundary[None],
        small_sum[None, :shard_width],
        small_sum[None, shard_width:2 * shard_width],
        qkv_grad[None],
        grads_out[None, :shard_width],
        grads_in[None, :, 3 * shard_width:],
        grads_out[None, shard_width:],
        freq_grad[None],
        feat_grad[None],
    )


def solution(mesh):
    placed = (
        P("dp", None, "mp"), P("dp", None, "mp"), P("dp"), P("section", None), P("section", None),
        P("section", None, None, "mp"), P("section", "mp", None), P("section", None, "mp"), P("section", "mp", None),
        P("section", "mp", None, None), P("section", "mp", None),
    )
    return jax.shard_map(
        shards,
        mesh=mesh,
        in_specs=placed,
        out_specs=(
            P("section", "dp", None, "mp"), P("section", "mp"), P("section", "mp"), P("section", None, "dp", "mp"),
            P("section", "mp", "dp"), P("section", "dp", "mp"), P("section", "mp", "dp"), P("section", "mp", None, None),
            P("section", "mp", None),
        ),
        check_vma=False,
    )
```

```python
import functools
import math

import jax
import jax.numpy as jnp
from jax import lax
from jax.experimental import pallas as pl
from jax.experimental.pallas import tpu as pltpu
from jax.sharding import PartitionSpec as P

ROT = 16
TILE = 256
HEAD = 64
LANES = 256
EPS = 1e-05
F32 = jnp.float32
BF16 = jnp.bfloat16
RSQRT2 = math.sqrt(0.5)
RSQRT2PI = 1.0 / math.sqrt(2.0 * math.pi)
SAVED = 14


def dot_nn(a, b):
    return lax.dot_general(a, b, (((1,), (0,)), ((), ())), preferred_element_type=F32)


def dot_nt(a, b):
    return lax.dot_general(a, b, (((1,), (1,)), ((), ())), preferred_element_type=F32)


def dot_tn(a, b):
    return lax.dot_general(a, b, (((0,), (0,)), ((), ())), preferred_element_type=F32)


def split(values):
    high = values.astype(BF16)
    return high, (values - high.astype(F32)).astype(BF16)


def iota(shape, dim):
    return lax.broadcasted_iota(jnp.int32, shape, dim)


def partner(values):
    later = pltpu.roll(values, LANES - ROT // 2, 1)
    earlier = pltpu.roll(values, ROT // 2, 1)
    lower = iota(values.shape, 1) % HEAD < ROT // 2
    return jnp.where(lower, later, earlier)


def twice(table):
    return jnp.concatenate([table, table], axis=1)


def head_of(shape, dim):
    return iota(shape, dim) // HEAD


def weight_copies(refs, w_in, w_out, sems, which):
    qkv, up, out, down = refs
    ends = [(qkv.at[0, t], w_in.at[:, t * LANES:(t + 1) * LANES]) for t in range(3)] + [
        (up.at[0], w_in.at[:, 3 * LANES:]), (out.at[0], w_out.at[0:LANES, :]), (down.at[0], w_out.at[LANES:, :])]
    return [pltpu.make_async_copy(*ends[i], sems.at[i]) for i in which]


def start_weights(meta, mine, other, w_in, w_out, sems, order):
    def start(refs):
        for copy in weight_copies(refs, w_in, w_out, sems, order):
            copy.start()

    @pl.when(meta[1] == 1)
    def _():
        start(mine)

    @pl.when(meta[1] != 1)
    def _():
        start(other)


def wait_weights(step, refs, w_in, w_out, sems, which):
    @pl.when(step == 0)
    def _():
        for copy in weight_copies(refs, w_in, w_out, sems, which):
            copy.wait()


def forward_kernel(carried, phased, *refs):
    refs = list(refs)
    take = lambda n: [refs.pop(0) for _ in range(n)]
    meta, lens = take(2)
    p0, p1, p2, p3a, p3b, gain, bias, mix_hi, mix_lo, feat_w, cos_t, sin_t = take(12)
    mine, other = take(4), take(4)
    if carried:
        state_in, ksum_in = take(2)
        take(SAVED)
    parts = take(5 if phased else 4)
    normed, xhat, rstd, rq_o, rk_o, qf_o, kf_o, v_o, hcat, dgelu, invz, att_o, prior_s, prior_k = take(SAVED)
    state, ksum, w_in, w_out, sems = take(5)
    tile = pl.program_id(0)
    rank = meta[0]
    half = LANES // 2

    @pl.when(tile == 0)
    def _():
        start_weights(meta, mine, other, w_in, w_out, sems, (0, 1, 2, 3, 4, 5))
        if carried:
            state[...] = state_in[...]
            ksum[...] = ksum_in[...]
        else:
            state[...] = jnp.zeros_like(state)
            ksum[...] = jnp.zeros_like(ksum)

    pieces = [p0[...].astype(F32), p1[...].astype(F32), p2[...].astype(F32),
              jnp.concatenate([p3a[...], p3b[...]], axis=1).astype(F32)]
    width = 4 * LANES
    mean = jnp.sum(pieces[0] + pieces[1] + pieces[2] + pieces[3], axis=1, keepdims=True) * (1.0 / width)
    pieces = [piece - mean for piece in pieces]
    squares = sum(piece * piece for piece in pieces)
    factor = lax.rsqrt(jnp.sum(squares, axis=1, keepdims=True) * (1.0 / width) + EPS)
    for r in range(4):
        at = pl.ds(pl.multiple_of((rank ^ r) * LANES, LANES), LANES)
        hat = pieces[r] * factor
        if r == 0:
            xhat[...] = hat
        normed[:, at] = (hat * gain[:, at] + bias[:, at]).astype(BF16)
    rstd[...] = jnp.broadcast_to(factor, (TILE, half))
    tokens = normed[...]

    wait_weights(tile, mine, w_in, w_out, sems, (0, 1, 2))
    cosine, sine = twice(cos_t[...]), twice(sin_t[...])
    query = dot_nn(tokens, w_in[:, 0:LANES])
    key = dot_nn(tokens, w_in[:, LANES:2 * LANES])
    value = dot_nn(tokens, w_in[:, 2 * LANES:3 * LANES]).astype(BF16)
    rq = query * cosine + partner(query) * sine
    rk = key * cosine + partner(key) * sine
    weight = feat_w[...]

    def logits(rows):
        high, low = split(rows)
        return dot_nn(high, mix_hi[...]) + dot_nn(low, mix_hi[...]) + dot_nn(high, mix_lo[...])

    positions = lens[1] + tile * TILE + iota((TILE, LANES), 0)
    real = (positions < lens[0]).astype(F32)
    qf = (weight * jnp.exp(logits(rq))).astype(BF16)
    kf = (weight * jnp.exp(logits(rk)) * real).astype(BF16)
    rq_o[...] = rq.astype(BF16)
    rk_o[...] = rk.astype(BF16)
    qf_o[...] = qf
    kf_o[...] = kf
    v_o[...] = value

    square = (TILE, TILE)
    lower = iota(square, 0) >= iota(square, 1)
    same = head_of(square, 0) == head_of(square, 1)
    cumulative = dot_nn(lower.astype(BF16), kf) + ksum[0:1, :]
    high, low = split(qf.astype(F32) * cumulative)
    ones = same.astype(BF16)
    inverse = 1.0 / (dot_nn(high, ones) + dot_nn(low, ones))
    prior = jnp.where(same, state[...], 0.0)
    prior_hi, prior_lo = split(prior)
    numer = dot_nn(qf, prior_hi) + dot_nn(qf, prior_lo)
    lane_head = head_of((TILE, LANES), 1)
    zero = jnp.zeros((TILE, LANES), BF16)
    for h in range(LANES // HEAD):
        here = lane_head == h
        scores = dot_nt(qf, jnp.where(here, kf, zero))
        scores = jnp.where(lower, scores, 0.0).astype(BF16)
        numer = numer + dot_nn(scores, jnp.where(here, value, zero))
    prior_s[0] = prior
    prior_k[0] = ksum[...]
    state[...] = state[...] + dot_tn(kf, value)
    ksum[...] = jnp.broadcast_to(cumulative[TILE - 1:TILE, :], ksum.shape)
    invz[...] = inverse
    attended = numer * inverse
    att_o[...] = attended
    hcat[:, 0:LANES] = attended.astype(BF16)

    wait_weights(tile, mine, w_in, w_out, sems, (3,))
    for c in range(4):
        cols = slice(c * LANES, (c + 1) * LANES)
        up = dot_nn(tokens, w_in[:, (3 + c) * LANES:(4 + c) * LANES])
        cdf = 0.5 * (1.0 + lax.erf(up * RSQRT2))
        hcat[:, (1 + c) * LANES:(2 + c) * LANES] = (up * cdf).astype(BF16)
        dgelu[:, cols] = (cdf + up * (RSQRT2PI * jnp.exp(-0.5 * up * up))).astype(BF16)

    wait_weights(tile, mine, w_in, w_out, sems, (4, 5))
    hidden = hcat[...]
    emit(rank, lambda at: dot_nn(hidden, w_out[:, at]), parts)


def emit(rank, product, parts):
    half = LANES // 2
    for r in range(4):
        at = pl.ds(pl.multiple_of((rank ^ r) * LANES, LANES), LANES)
        part = product(at)
        if len(parts) == 4:
            parts[r][...] = part.astype(parts[r].dtype)
            continue
        sx, sy, k0, ka, kb = parts
        if r == 0:
            k0[...] = part
        elif r == 1:
            sx[0] = part[:, :half].astype(BF16)
            kb[...] = part[:, half:]
        elif r == 2:
            ka[...] = part[:, :half]
            sy[0] = part[:, half:].astype(BF16)
        else:
            sx[1] = part[:, :half].astype(BF16)
            sy[1] = part[:, half:].astype(BF16)


def backward_kernel(carried, phased, *refs):
    refs = list(refs)
    take = lambda n: [refs.pop(0) for _ in range(n)]
    meta, = take(1)
    pieces = take(5)
    normed, rq, rk, qf_i, kf_i, v_i, att_i, dgelu, invz, prior_s, prior_k, gain, bias, mix_hi, cos_t, sin_t = take(16)
    mine, other = take(4), take(4)
    if carried:
        state_in, gsum_in, dmix_in, fsum_in = take(4)
        take(2)
    parts = take(5 if phased else 4)
    stats, dcat, state, gsum, dmix, fsum = take(6)
    w_in, w_out, sems, grad = take(4)
    step = pl.program_id(0)
    rank = meta[0]

    @pl.when(step == 0)
    def _():
        start_weights(meta, mine, other, w_in, w_out, sems, (4, 5, 0, 1, 2, 3))
        if carried:
            state[...] = state_in[...]
            gsum[...] = gsum_in[...]
            dmix[...] = dmix_in[...]
            fsum[...] = fsum_in[...]
        else:
            state[...] = jnp.zeros_like(state)
            gsum[...] = jnp.zeros_like(gsum)
            dmix[...] = jnp.zeros_like(dmix)
            fsum[...] = jnp.zeros_like(fsum)

    wait_weights(step, mine, w_in, w_out, sems, (4, 5))
    assemble(rank, pieces, grad)
    g = grad[...]
    d_att = dot_nt(g, w_out[0:LANES, :]).astype(BF16).astype(F32)
    square = (TILE, TILE)
    same = head_of(square, 0) == head_of(square, 1)
    ones = same.astype(BF16)
    inverse = invz[...]
    dn = (d_att * inverse).astype(BF16)
    dn32 = dn.astype(F32)
    high, low = split(dn32 * att_i[...])
    dden = -(dot_nn(high, ones) + dot_nn(low, ones))
    den_hi = dden.astype(BF16).astype(F32)
    roll_hi = pltpu.roll(den_hi, HEAD, 1)
    roll_lo = pltpu.roll(dden - den_hi, HEAD, 1)
    qf, kf, value = qf_i[...], kf_i[...], v_i[...]
    zero = jnp.zeros((TILE, LANES), BF16)
    one = jnp.ones((TILE, LANES), BF16)
    lane = iota((TILE, LANES), 1)
    lane_head = lane // HEAD
    below = iota(square, 0) >= iota(square, 1)
    above = iota(square, 0) <= iota(square, 1)
    prior_hi, prior_lo = split(prior_s[0])
    later_hi, later_lo = split(jnp.where(same, state[...], 0.0))
    d_qf = dot_nt(dn, prior_hi) + dot_nt(dn, prior_lo) + prior_k[0, 0:1, :] * dden
    d_kf = dot_nt(value, later_hi) + dot_nt(value, later_lo) + gsum[0:1, :]
    d_v = dot_nn(kf, later_hi)
    heads = LANES // HEAD
    for h in range(heads):
        here = lane_head == h
        spare = HEAD * ((h + 1) % heads)
        left = jnp.where(lane == spare, roll_hi, jnp.where(lane == spare + 1, roll_lo, dn32)).astype(BF16)
        right = jnp.where(here, value, jnp.where((lane == spare) | (lane == spare + 1), one, zero))
        k_here = jnp.where(here, kf, zero)
        q_here = jnp.where(here, qf, zero)
        d_here = jnp.where(here, dn, zero)
        scores_t = jnp.where(above, dot_nt(k_here, qf), 0.0).astype(BF16)
        ds = jnp.where(below, dot_nt(left, right), 0.0).astype(BF16)
        ds_t = jnp.where(above, dot_nt(right, left), 0.0).astype(BF16)
        d_qf = d_qf + dot_nn(ds, k_here)
        d_kf = d_kf + dot_nn(ds_t, q_here)
        d_v = d_v + dot_nn(scores_t, d_here)
    state[...] = state[...] + dot_tn(qf, dn)
    gsum[...] = gsum[...] + jnp.sum(qf.astype(F32) * dden, axis=0, keepdims=True)
    dlq = d_qf * qf.astype(F32)
    dlk = d_kf * kf.astype(F32)
    fsum[...] = fsum[...] + jnp.sum(dlq + dlk, axis=0, keepdims=True)
    dlq, dlk = dlq.astype(BF16), dlk.astype(BF16)
    dmix[...] = dmix[...] + dot_tn(rq[...], dlq) + dot_tn(rk[...], dlk)
    cosine, sine = twice(cos_t[...]), twice(sin_t[...])
    for c, dl in ((0, dlq), (1, dlk)):
        dr = dot_nt(dl, mix_hi[...])
        dcat[:, c * LANES:(c + 1) * LANES] = (dr * cosine - partner(dr) * sine).astype(BF16)
    dcat[:, 2 * LANES:3 * LANES] = d_v.astype(BF16)
    for c in range(4):
        cols = slice(c * LANES, (c + 1) * LANES)
        d_act = dot_nt(g, w_out[(1 + c) * LANES:(2 + c) * LANES, :])
        dcat[:, (3 + c) * LANES:(4 + c) * LANES] = (d_act * dgelu[:, cols].astype(F32)).astype(BF16)
    wait_weights(step, mine, w_in, w_out, sems, (0, 1, 2, 3))
    wide = dcat[...]
    row = iota((8, LANES), 0)
    first, second = (row == 0).astype(BF16), (row == 1).astype(BF16)
    totals = []

    def product(at):
        part = dot_nt(wide, w_in[at, :])
        one_side = (part * gain[:, at]).astype(BF16)
        other = (part * (normed[:, at].astype(F32) - bias[:, at])).astype(BF16)
        totals.append(dot_nt(first, one_side) + dot_nt(second, other))
        return part

    emit(rank, product, parts)
    stats[...] = totals[0] + totals[1] + totals[2] + totals[3]


def assemble(rank, pieces, whole):
    half = LANES // 2
    for r in range(3):
        whole[:, pl.ds(pl.multiple_of((rank ^ r) * LANES, LANES), LANES)] = pieces[r][...]
    at = pl.multiple_of((rank ^ 3) * LANES, LANES)
    whole[:, pl.ds(at, half)] = pieces[3][...]
    whole[:, pl.ds(pl.multiple_of(at + half, half), half)] = pieces[4][...]


def product_kernel(steps, meta, left, *refs):
    *rights, out_other, out_own = refs[:-1] if len(refs) > 3 else refs
    step = pl.program_id(0)
    if len(rights) == 1:
        right = rights[0]
    else:
        right = refs[-1]

        @pl.when(step == 0)
        def _():
            assemble(meta[1], rights, right)

    product = dot_tn(left[...], right[...]).astype(BF16)

    @pl.when(step < steps)
    def _():
        out_other[...] = product

    @pl.when(step >= steps)
    def _():
        out_own[...] = product


def partial_outs(rows, phased, row_of):
    half = LANES // 2
    if not phased:
        shapes = [jax.ShapeDtypeStruct((rows, LANES), F32)] + [jax.ShapeDtypeStruct((rows, LANES), BF16)] * 3
        return shapes, [pl.BlockSpec((TILE, LANES), lambda *i: (row_of(*i), 0))] * 4
    shapes = [jax.ShapeDtypeStruct((2, rows, half), BF16)] * 2 + [
        jax.ShapeDtypeStruct((rows, LANES), F32), jax.ShapeDtypeStruct((rows, half), F32),
        jax.ShapeDtypeStruct((rows, half), F32)]
    specs = [pl.BlockSpec((2, TILE, half), lambda *i: (0, row_of(*i), 0))] * 2 + [
        pl.BlockSpec((TILE, width), lambda *i: (row_of(*i), 0)) for width in (LANES, half, half)]
    return shapes, specs


def fixed(shape):
    return pl.BlockSpec(shape, lambda *i: (0,) * len(shape))


def outside(count):
    return [pl.BlockSpec(memory_space=pl.ANY)] * count


def params(size):
    return pltpu.CompilerParams(dimension_semantics=("arbitrary",), vmem_limit_bytes=size << 20)


def weight_scratch(width):
    return [pltpu.VMEM((width, 3 * LANES + width), BF16), pltpu.VMEM((LANES + width, width), BF16),
            pltpu.SemaphoreType.DMA((6,))]


def forward_layer(meta, lens, pieces, weights, tables, length, first_row, phased, carry=None):
    rows = pieces[0].shape[0]
    tiles, before = rows // TILE, first_row // TILE
    half, width = LANES // 2, 4 * LANES
    local = lambda t, *_: t
    there = lambda t, *_: before + t
    by_row = lambda n, row_of: pl.BlockSpec((TILE, n), lambda *i: (row_of(*i), 0))
    (gain, bias, mix_hi, mix_lo, feat_w), mine, other = weights
    small = (gain, bias, mix_hi, mix_lo, feat_w)
    shapes, specs = partial_outs(rows, phased, local)
    extra = [(width, BF16), (LANES, F32), (half, F32)] + [(LANES, BF16)] * 5 + [
        (LANES + width, BF16), (width, BF16), (LANES, F32), (LANES, F32)]
    shapes += [jax.ShapeDtypeStruct((length, n), d) for n, d in extra]
    specs += [by_row(n, there) for n, _ in extra]
    shapes += [jax.ShapeDtypeStruct((length // TILE, LANES, LANES), F32), jax.ShapeDtypeStruct((length // TILE, 8, LANES), F32)]
    specs += [pl.BlockSpec((1, n, LANES), lambda *i: (there(*i), 0, 0)) for n in (LANES, 8)]
    states = [(LANES, LANES), (8, LANES)]
    shapes += [jax.ShapeDtypeStruct(s, F32) for s in states]
    specs += [fixed(s) for s in states]
    operands = [meta, jnp.stack([lens[0], jnp.int32(first_row)]), *pieces, *small, *tables, *mine, *other]
    in_specs = [by_row(p.shape[1], local) for p in pieces] + [fixed(w.shape) for w in small] + [by_row(half, there)] * 2 + outside(8)
    aliases = {}
    if carry is not None:
        state, saved = carry
        operands += [*state, *saved]
        in_specs += [fixed(s) for s in states] + outside(SAVED)
        aliases = {len(operands) - SAVED + i: len(shapes) - 2 - SAVED + i for i in range(SAVED)}
    outs = pl.pallas_call(
        functools.partial(forward_kernel, carry is not None, phased),
        name="layer_forward",
        out_shape=shapes,
        grid_spec=pltpu.PrefetchScalarGridSpec(
            num_scalar_prefetch=2, grid=(tiles,), in_specs=in_specs, out_specs=specs, scratch_shapes=weight_scratch(width)),
        input_output_aliases=aliases,
        compiler_params=params(56),
        cost_estimate=pl.CostEstimate(flops=rows * 20_000_000, transcendentals=rows * 5000, bytes_accessed=24 << 20),
    )(*operands)
    count = 5 if phased else 4
    return outs[:count], outs[count:count + SAVED], outs[count + SAVED:]


def backward_layer(meta, pieces, saved, weights, tables, length, first_row, phased, carry=None):
    rows = pieces[0].shape[0]
    tiles, before = rows // TILE, first_row // TILE
    half, width = LANES // 2, 4 * LANES
    local = lambda t, *_: tiles - 1 - t
    there = lambda t, *_: before + tiles - 1 - t
    by_row = lambda n, row_of=there: pl.BlockSpec((TILE, n), lambda *i: (row_of(*i), 0))
    normed, rq, rk, qf, kf, value, hcat, dgelu, invz, attended, prior_s, prior_k = saved
    (gain, bias, mix_hi, mix_lo, feat_w), mine, other = weights
    shapes, specs = partial_outs(rows, phased, local)
    shapes += [jax.ShapeDtypeStruct((8, length), F32), jax.ShapeDtypeStruct((length, 3 * LANES + width), BF16)]
    specs += [pl.BlockSpec((8, TILE), lambda *i: (0, there(*i))), by_row(3 * LANES + width)]
    states = [(LANES, LANES), (8, LANES)] * 2
    shapes += [jax.ShapeDtypeStruct(s, F32) for s in states]
    specs += [fixed(s) for s in states]
    operands = [meta, *pieces, normed, rq, rk, qf, kf, value, attended, dgelu, invz, prior_s, prior_k, gain, bias, mix_hi, *tables,
                *mine, *other]
    in_specs = [by_row(p.shape[1], local) for p in pieces] + [by_row(width)] + [by_row(LANES)] * 6 + [by_row(width), by_row(LANES)] + [
        pl.BlockSpec((1, n, LANES), lambda *i: (there(*i), 0, 0)) for n in (LANES, 8)] + [
        fixed(w.shape) for w in (gain, bias, mix_hi)] + [by_row(half)] * 2 + outside(8)
    aliases = {}
    if carry is not None:
        state, arrays = carry
        operands += [*state, *arrays]
        in_specs += [fixed(s) for s in states] + outside(2)
        aliases = {len(operands) - 2 + i: len(shapes) - 6 + i for i in range(2)}
    outs = pl.pallas_call(
        functools.partial(backward_kernel, carry is not None, phased),
        name="layer_backward",
        out_shape=shapes,
        grid_spec=pltpu.PrefetchScalarGridSpec(
            num_scalar_prefetch=1, grid=(tiles,), in_specs=in_specs, out_specs=specs,
            scratch_shapes=weight_scratch(width) + [pltpu.VMEM((TILE, width), BF16)]),
        input_output_aliases=aliases,
        compiler_params=params(56),
        cost_estimate=pl.CostEstimate(flops=rows * 25_000_000, transcendentals=0, bytes_accessed=24 << 20),
    )(*operands)
    count = 5 if phased else 4
    return outs[:count], outs[count:count + 2], outs[count + 2:]


def swap(value, axis, by):
    return lax.ppermute(value, axis, [(k, k ^ by) for k in range(lax.axis_size(axis))])


def gather_pieces(shard, meanwhile=()):
    from_x, from_y = after((swap(shard, "mp", 1), swap(shard, "mp", 2)), *meanwhile)
    return (shard, from_x, from_y) + last_pieces(from_x, from_y)


def last_pieces(from_x, from_y):
    half = from_x.shape[1] // 2
    return tuple(lax.optimization_barrier((swap(from_x[:, :half], "mp", 2), swap(from_y[:, half:], "mp", 1))))


def after(values, *others):
    if not others:
        return values
    return lax.optimization_barrier((values, others))[0]


def direct_sends(parts):
    return parts[0], [swap(part, "mp", r) for r, part in enumerate(parts) if r > 0]


def scatter_start(parts):
    return swap(parts[0], "mp", 1), swap(parts[1], "mp", 2)


def scatter_turn(parts, arrived):
    _, _, _, ka, kb = parts
    in_x, in_y = arrived
    return (ka + in_x[1].astype(F32)).astype(BF16), (kb + in_y[1].astype(F32)).astype(BF16)


def scatter_end(parts, arrived, to_y, to_x):
    _, _, k0, ka, _ = parts
    in_x, in_y = arrived
    half = ka.shape[1]
    last_y, last_x = swap(to_y, "mp", 2), swap(to_x, "mp", 1)
    return jnp.concatenate(
        [k0[:, :half] + in_x[0].astype(F32) + last_y.astype(F32), k0[:, half:] + in_y[0].astype(F32) + last_x.astype(F32)],
        axis=1)


def scatter_sum(parts):
    arrived = scatter_start(parts)
    return scatter_end(parts, arrived, *scatter_turn(parts, arrived))


def ring_scatter(block_of, axis, meanwhile=()):
    count = lax.axis_size(axis)
    rank = lax.axis_index(axis)
    pairs = [(k, (k + 1) % count) for k in range(count)]
    total = block_of((rank + count - 1) % count)
    for step in range(2, count + 1):
        arrived = lax.ppermute(total, axis, pairs)
        if step in (2, count):
            arrived = after(arrived, *meanwhile)
        total = (arrived.astype(F32) + block_of((rank + count - step) % count).astype(F32)).astype(BF16)
        yield arrived, total


def dp_sends(values):
    count = lax.axis_size("dp")
    if count > 8:
        return [lax.psum(values, "dp")]
    return [values] + [lax.ppermute(values, "dp", [(i, (i + k) % count) for i in range(count)]) for k in range(1, count)]


def block_sends(block_of, axis):
    count = lax.axis_size(axis)
    rank = lax.axis_index(axis)
    if count > 8:
        return [list(ring_scatter(block_of, axis))[-1][1]]
    return [block_of(rank)] + [
        lax.ppermute(block_of((rank + k) % count), axis, [(i, (i + k) % count) for i in range(count)]) for k in range(1, count)]


def sum_blocks(blocks):
    total = blocks[0].astype(F32)
    for block in blocks[1:]:
        total = total + block.astype(F32)
    return total.astype(BF16)


def weight_gradient(left, rights, section, place):
    rows = left.shape[0]
    whole = len(rights) == 1
    block = 256 if whole else 128
    m = left.shape[1] // (1 if whole else 2)
    n = rights[0].shape[1] // 2 if whole else 4 * LANES
    steps = m // block
    half_at = lambda i, meta: jnp.where(i < steps, 1 - meta[0], meta[0])
    if whole:
        left_at = lambda i, meta: (0, i % steps)
        right_specs = [pl.BlockSpec((rows, n), lambda i, meta: (0, half_at(i, meta)))]
    else:
        left_at = lambda i, meta: (0, half_at(i, meta) * steps + i % steps)
        right_specs = [fixed(p.shape) for p in rights]
    other, own = pl.pallas_call(
        functools.partial(product_kernel, steps),
        name="weight_gradient",
        out_shape=[jax.ShapeDtypeStruct((m, n), BF16)] * 2,
        grid_spec=pltpu.PrefetchScalarGridSpec(
            num_scalar_prefetch=1, grid=(2 * steps,),
            in_specs=[pl.BlockSpec((rows, block), left_at)] + right_specs,
            out_specs=[pl.BlockSpec((block, n), lambda i, meta: (jnp.minimum(i, steps - 1), 0)),
                       pl.BlockSpec((block, n), lambda i, meta: (jnp.maximum(i - steps, 0), 0))],
            scratch_shapes=[] if whole else [pltpu.VMEM((rows, n), BF16)]),
        compiler_params=params(20),
        cost_estimate=pl.CostEstimate(flops=4 * rows * m * n, transcendentals=0, bytes_accessed=4 * (rows * (m + n) + m * n)),
    )(jnp.stack([section, place]).astype(jnp.int32), left, *rights)
    return own, other


def dct_table(order):
    row_index = jnp.arange(order, dtype=F32)[:, None]
    col_index = jnp.arange(order, dtype=F32)[None, :]
    cosines = jnp.sqrt(2.0 / order) * jnp.cos(math.pi * (row_index + 0.5) * col_index / order)
    return cosines * jnp.where(col_index == 0, math.sqrt(0.5), 1.0)


def rotary_tables(length):
    column = jnp.arange(LANES // 2, dtype=jnp.int32) % HEAD
    half = ROT // 2
    index = (column % half).astype(F32)
    angles = jnp.arange(length, dtype=F32)[:, None] * (10000.0 ** (-index * 2.0 / ROT))[None, :]
    turned = (column < ROT)[None, :]
    sign = jnp.where(column < half, -1.0, 1.0)[None, :]
    return jnp.where(turned, jnp.cos(angles), 1.0), jnp.where(turned, sign * jnp.sin(angles), 0.0)


def shards(block_input, cotangent, lengths, ln_gain, ln_bias, w_qkv, w_out, w_up, w_down, freq_table, feat_weight):
    section = lax.axis_index("section")
    place = lax.axis_index("mp")
    group = lax.axis_index("dp")
    groups = lax.axis_size("dp")
    local_slots, length, shard_width = block_input.shape
    width = ln_gain.shape[1]
    heads = freq_table.shape[1]
    is_first = section == 0
    lens = lax.dynamic_slice_in_dim(lengths, section, 1, 0)
    metas = [jnp.stack([place, (section == l).astype(jnp.int32)]).astype(jnp.int32) for l in range(2)]

    def own(values):
        return lax.dynamic_index_in_dim(values, section, 0, keepdims=False)

    shard0 = own(block_input)

    small = jnp.concatenate([ln_gain[0], ln_bias[0], feat_weight.reshape(-1), freq_table.astype(F32).reshape(-1)])
    small_other = swap(small, "section", 1)
    mine = (w_qkv, w_up, w_out, w_down)
    other = tuple(swap(w, "section", 1) for w in mine)
    pieces0 = gather_pieces(shard0, [small_other, other[2]])

    def both(mine, other):
        return jnp.where(is_first, mine, other), jnp.where(is_first, other, mine)

    layers_small = both(small, small_other)
    table = dct_table(HEAD)
    eye = jnp.eye(heads, dtype=F32)

    def layer_weights(l):
        vec = layers_small[l]
        gain, bias = vec[:width].reshape(1, width), vec[width:2 * width].reshape(1, width)
        feat = vec[2 * width:2 * width + LANES].reshape(1, LANES)
        freq = vec[2 * width + LANES:].reshape(heads, HEAD, HEAD)
        mixed = jnp.einsum("nk,hkm->hnm", table, freq, precision=lax.Precision.HIGHEST)
        mixed = (eye[:, None, :, None] * mixed[:, :, None, :]).reshape(LANES, LANES)
        high = lax.reduce_precision(mixed, 8, 7)
        return (gain, bias, high.astype(BF16), (mixed - high).astype(BF16), feat), mine, other

    weights0, weights1 = layer_weights(0), layer_weights(1)
    tables = rotary_tables(length)

    cot = after(own(cotangent), pieces0[3], pieces0[4])
    cot_x, cot_y = swap(cot, "mp", 1), swap(cot, "mp", 2)
    part0, all0, _ = forward_layer(metas[0], lens, pieces0, weights0, tables, length, 0, True)
    part0 = after(part0, cot_x, cot_y)
    hidden = (shard0.astype(F32) + scatter_sum(part0)).astype(BF16)
    pieces1 = gather_pieces(hidden)
    cot_x, cot_y = after((cot_x, cot_y), pieces1[3], pieces1[4])
    pieces_g = (cot, cot_x, cot_y) + last_pieces(cot_x, cot_y)
    part1, all1, _ = forward_layer(metas[1], lens, pieces1, weights1, tables, length, 0, False)
    out_kept, out_sent = direct_sends(part1)

    def saved_of(arrays):
        return (arrays[0],) + tuple(arrays[3:])

    def in_block(mine, arrived):
        n = mine.shape[0] // groups
        cut = lambda v, i: lax.dynamic_slice_in_dim(v, i * n, n, 0)
        return lambda i: (cut(mine, i).astype(F32) + cut(arrived, i).astype(F32)).astype(BF16)

    def out_block(mine, arrived):
        n = mine.shape[1] // groups
        cut = lambda v, i: lax.dynamic_slice_in_dim(v, i * n, n, 1)
        return lambda i: (cut(mine, i).astype(F32) + cut(arrived, i).astype(F32)).astype(BF16)

    def run_backward(meta, grad, saved, weights, phased):
        parts, (stats, dcat), (_, _, dmix, fsum) = backward_layer(meta, grad, saved, weights, tables, length, 0, phased)
        return parts, stats, dcat, dmix, fsum

    def norm_backward(grad_shard, d_normed, sums, norm, gain_all):
        xhat, rstd = norm
        gain = lax.dynamic_slice_in_dim(gain_all, place * shard_width, shard_width, 1)
        mean_d = (sums[0] * (1.0 / width))[:, None]
        mean_dx = (sums[1] * (1.0 / width))[:, None]
        return grad_shard.astype(F32) + rstd[:, :1] * (d_normed * gain - mean_d - xhat * mean_dx)

    def small_gradients(d_normed, norm, dmix, fsum):
        gain_part = jnp.sum(d_normed * norm[0], axis=0)
        bias_part = jnp.sum(d_normed, axis=0)
        diagonal = jnp.stack([dmix[h * HEAD:(h + 1) * HEAD, h * HEAD:(h + 1) * HEAD] for h in range(heads)])
        return jnp.concatenate([gain_part, bias_part, fsum[0], diagonal.reshape(-1)])

    saved1, saved0 = saved_of(all1), saved_of(all0)
    own, other = weight_gradient(saved1[6], pieces_g, section, place)
    out_blocks1 = block_sends(out_block(own, swap(other, "section", 1)), "dp")
    grad1_b = after(pieces_g, out_blocks1[0])
    parts, stats, dcat1, dmix1, fsum1 = run_backward(metas[1], grad1_b, saved1, weights1, True)
    parts, stats, dcat1, dmix1, fsum1 = after((parts, stats, dcat1, dmix1, fsum1), *out_blocks1, *out_sent[:2])
    row_sums = [swap(stats, "mp", r) for r in (1, 2, 3)]
    arrived, row_sums, own, other = lax.optimization_barrier(
        (scatter_start(parts), row_sums, *weight_gradient(saved1[0], (dcat1,), section, place)))
    sums = sum(row_sums, stats)
    turn = scatter_turn(parts, arrived)
    steps1 = list(ring_scatter(in_block(own, swap(other, "section", 1)), "dp"))
    arrivals1, red_in1 = [arrival for arrival, _ in steps1], steps1[-1][1]
    d_normed = scatter_end(parts, arrived, *turn)
    g0 = norm_backward(cot, d_normed, sums, all1[1:3], weights1[0][0]).astype(BF16)
    small1 = small_gradients(d_normed, all1[1:3], dmix1, fsum1)
    pieces_g0 = gather_pieces(after(g0, arrivals1[0]), arrivals1[1:2])
    pieces_g0 = after(pieces_g0, *arrivals1[2:3])
    out = hidden.astype(F32) + out_kept + out_sent[0].astype(F32) + out_sent[1].astype(F32) + out_sent[2].astype(F32)

    own, other = weight_gradient(saved0[6], pieces_g0, section, place)
    out_blocks0 = block_sends(out_block(own, swap(other, "section", 1)), "dp")
    grad0_b = after(pieces_g0, out_blocks0[0])
    parts, stats, dcat0, dmix0, fsum0 = run_backward(metas[0], grad0_b, saved0, weights0, False)
    parts, stats, dcat0, dmix0, fsum0 = after((parts, stats, dcat0, dmix0, fsum0), *out_blocks0, out_sent[2])
    out_blocks1 = after(out_blocks1, dcat0)
    kept, sent = direct_sends(parts)
    row_sums = [swap(stats, "mp", r) for r in (1, 2, 3)]
    sent[:2], row_sums, own, other = lax.optimization_barrier(
        (sent[:2], row_sums, *weight_gradient(saved0[0], (dcat0,), section, place)))
    sums = sum(row_sums, stats)
    block0 = in_block(own, swap(other, "section", 1))
    meanwhile = sent[2:]
    ring0 = ring_scatter(block0, "dp", meanwhile)
    steps0 = [next(ring0)]
    meanwhile.clear()
    sent, dmix0, out_blocks0, out_blocks1 = after((sent, dmix0, out_blocks0, out_blocks1), steps0[0][1])
    d_normed = kept + sent[0].astype(F32) + sent[1].astype(F32) + sent[2].astype(F32)
    d_input = norm_backward(g0, d_normed, sums, all0[1:3], weights0[0][0])
    small0 = small_gradients(d_normed, all0[1:3], dmix0, fsum0)

    def to_owner(first, second, axis):
        mine, other = both(first, second)
        arrived = swap(other, "section", 1)
        return jnp.where(is_first, jnp.concatenate([mine, arrived], axis), jnp.concatenate([arrived, mine], axis)).astype(F32)

    grads_out = to_owner(sum_blocks(out_blocks0), sum_blocks(out_blocks1), 0)
    small_mine, small_send = both(small0, small1)
    small_sum = small_mine + swap(small_send, "section", 1)
    small_parts = dp_sends(small_sum)
    keep, send = both(d_input, out)
    arrived = swap(send, "section", 1)
    boundary = jnp.where(is_first, jnp.stack([keep, arrived]), jnp.stack([arrived, keep]))
    meanwhile.append(arrived)
    steps0 += list(ring0)
    grads_in = to_owner(steps0[-1][1], red_in1, 1)
    small_sum = sum(after(small_parts, steps0[-1][0]))
    feat_grad = small_sum[2 * shard_width:2 * shard_width + LANES].reshape(heads, HEAD) / feat_weight[0]
    freq_grad = jnp.einsum("nk,hnm->hkm", table, small_sum[2 * shard_width + LANES:].reshape(heads, HEAD, HEAD),
                           precision=lax.Precision.HIGHEST)
    qkv_grad = jnp.stack([grads_in[:, t * shard_width:(t + 1) * shard_width] for t in range(3)])
    return (
        boundary[None],
        small_sum[None, :shard_width],
        small_sum[None, shard_width:2 * shard_width],
        qkv_grad[None],
        grads_out[None, :shard_width],
        grads_in[None, :, 3 * shard_width:],
        grads_out[None, shard_width:],
        freq_grad[None],
        feat_grad[None],
    )


def solution(mesh):
    placed = (
        P("dp", None, "mp"), P("dp", None, "mp"), P("dp"), P("section", None), P("section", None),
        P("section", None, None, "mp"), P("section", "mp", None), P("section", None, "mp"), P("section", "mp", None),
        P("section", "mp", None, None), P("section", "mp", None),
    )
    return jax.shard_map(
        shards,
        mesh=mesh,
        in_specs=placed,
        out_specs=(
            P("section", "dp", None, "mp"), P("section", "mp"), P("section", "mp"), P("section", None, "dp", "mp"),
            P("section", "mp", "dp"), P("section", "dp", "mp"), P("section", "mp", "dp"), P("section", "mp", None, None),
            P("section", "mp", None),
        ),
        check_vma=False,
    )
```

```python
import functools
import math

import jax
import jax.numpy as jnp
from jax import lax
from jax.experimental import pallas as pl
from jax.experimental.pallas import tpu as pltpu
from jax.sharding import PartitionSpec as P

ROT = 16
TILE = 256
HEAD = 64
LANES = 256
EPS = 1e-05
F32 = jnp.float32
BF16 = jnp.bfloat16
RSQRT2 = math.sqrt(0.5)
RSQRT2PI = 1.0 / math.sqrt(2.0 * math.pi)
SAVED = 14


def dot_nn(a, b):
    return lax.dot_general(a, b, (((1,), (0,)), ((), ())), preferred_element_type=F32)


def dot_nt(a, b):
    return lax.dot_general(a, b, (((1,), (1,)), ((), ())), preferred_element_type=F32)


def dot_tn(a, b):
    return lax.dot_general(a, b, (((0,), (0,)), ((), ())), preferred_element_type=F32)


def split(values):
    high = values.astype(BF16)
    return high, (values - high.astype(F32)).astype(BF16)


def iota(shape, dim):
    return lax.broadcasted_iota(jnp.int32, shape, dim)


def partner(values):
    later = pltpu.roll(values, LANES - ROT // 2, 1)
    earlier = pltpu.roll(values, ROT // 2, 1)
    lower = iota(values.shape, 1) % HEAD < ROT // 2
    return jnp.where(lower, later, earlier)


def twice(table):
    return jnp.concatenate([table, table], axis=1)


def head_of(shape, dim):
    return iota(shape, dim) // HEAD


def weight_copies(refs, w_in, w_out, sems, which):
    qkv, up, out, down = refs
    ends = [(qkv.at[0, t], w_in.at[:, t * LANES:(t + 1) * LANES]) for t in range(3)] + [
        (up.at[0], w_in.at[:, 3 * LANES:]), (out.at[0], w_out.at[0:LANES, :]), (down.at[0], w_out.at[LANES:, :])]
    return [pltpu.make_async_copy(*ends[i], sems.at[i]) for i in which]


def start_weights(meta, mine, other, w_in, w_out, sems, order):
    def start(refs):
        for copy in weight_copies(refs, w_in, w_out, sems, order):
            copy.start()

    @pl.when(meta[1] == 1)
    def _():
        start(mine)

    @pl.when(meta[1] != 1)
    def _():
        start(other)


def wait_weights(step, refs, w_in, w_out, sems, which):
    @pl.when(step == 0)
    def _():
        for copy in weight_copies(refs, w_in, w_out, sems, which):
            copy.wait()


def forward_kernel(carried, phased, *refs):
    refs = list(refs)
    take = lambda n: [refs.pop(0) for _ in range(n)]
    meta, lens = take(2)
    p0, p1, p2, p3a, p3b, gain, bias, mix_hi, mix_lo, feat_w, cos_t, sin_t = take(12)
    mine, other = take(4), take(4)
    if carried:
        state_in, ksum_in = take(2)
        take(SAVED)
    parts = take(5 if phased else 4)
    normed, xhat, rstd, rq_o, rk_o, qf_o, kf_o, v_o, hcat, dgelu, invz, att_o, prior_s, prior_k = take(SAVED)
    state, ksum, w_in, w_out, sems = take(5)
    tile = pl.program_id(0)
    rank = meta[0]
    half = LANES // 2

    @pl.when(tile == 0)
    def _():
        start_weights(meta, mine, other, w_in, w_out, sems, (0, 1, 2, 3, 4, 5))
        if carried:
            state[...] = state_in[...]
            ksum[...] = ksum_in[...]
        else:
            state[...] = jnp.zeros_like(state)
            ksum[...] = jnp.zeros_like(ksum)

    pieces = [p0[...].astype(F32), p1[...].astype(F32), p2[...].astype(F32),
              jnp.concatenate([p3a[...], p3b[...]], axis=1).astype(F32)]
    width = 4 * LANES
    mean = jnp.sum(pieces[0] + pieces[1] + pieces[2] + pieces[3], axis=1, keepdims=True) * (1.0 / width)
    pieces = [piece - mean for piece in pieces]
    squares = sum(piece * piece for piece in pieces)
    factor = lax.rsqrt(jnp.sum(squares, axis=1, keepdims=True) * (1.0 / width) + EPS)
    for r in range(4):
        at = pl.ds(pl.multiple_of((rank ^ r) * LANES, LANES), LANES)
        hat = pieces[r] * factor
        if r == 0:
            xhat[...] = hat
        normed[:, at] = (hat * gain[:, at] + bias[:, at]).astype(BF16)
    rstd[...] = jnp.broadcast_to(factor, (TILE, half))
    tokens = normed[...]

    wait_weights(tile, mine, w_in, w_out, sems, (0, 1, 2))
    cosine, sine = twice(cos_t[...]), twice(sin_t[...])
    query = dot_nn(tokens, w_in[:, 0:LANES])
    key = dot_nn(tokens, w_in[:, LANES:2 * LANES])
    value = dot_nn(tokens, w_in[:, 2 * LANES:3 * LANES]).astype(BF16)
    rq = query * cosine + partner(query) * sine
    rk = key * cosine + partner(key) * sine
    weight = feat_w[...]

    def logits(rows):
        high, low = split(rows)
        return dot_nn(high, mix_hi[...]) + dot_nn(low, mix_hi[...]) + dot_nn(high, mix_lo[...])

    positions = lens[1] + tile * TILE + iota((TILE, LANES), 0)
    real = (positions < lens[0]).astype(F32)
    qf = (weight * jnp.exp(logits(rq))).astype(BF16)
    kf = (weight * jnp.exp(logits(rk)) * real).astype(BF16)
    rq_o[...] = rq.astype(BF16)
    rk_o[...] = rk.astype(BF16)
    qf_o[...] = qf
    kf_o[...] = kf
    v_o[...] = value

    square = (TILE, TILE)
    lower = iota(square, 0) >= iota(square, 1)
    same = head_of(square, 0) == head_of(square, 1)
    cumulative = dot_nn(lower.astype(BF16), kf) + ksum[0:1, :]
    high, low = split(qf.astype(F32) * cumulative)
    ones = same.astype(BF16)
    inverse = 1.0 / (dot_nn(high, ones) + dot_nn(low, ones))
    prior = jnp.where(same, state[...], 0.0)
    prior_hi, prior_lo = split(prior)
    numer = dot_nn(qf, prior_hi) + dot_nn(qf, prior_lo)
    lane_head = head_of((TILE, LANES), 1)
    zero = jnp.zeros((TILE, LANES), BF16)
    for h in range(LANES // HEAD):
        here = lane_head == h
        scores = dot_nt(qf, jnp.where(here, kf, zero))
        scores = jnp.where(lower, scores, 0.0).astype(BF16)
        numer = numer + dot_nn(scores, jnp.where(here, value, zero))
    prior_s[0] = prior
    prior_k[0] = ksum[...]
    state[...] = state[...] + dot_tn(kf, value)
    ksum[...] = jnp.broadcast_to(cumulative[TILE - 1:TILE, :], ksum.shape)
    invz[...] = inverse
    attended = numer * inverse
    att_o[...] = attended
    hcat[:, 0:LANES] = attended.astype(BF16)

    wait_weights(tile, mine, w_in, w_out, sems, (3,))
    for c in range(4):
        cols = slice(c * LANES, (c + 1) * LANES)
        up = dot_nn(tokens, w_in[:, (3 + c) * LANES:(4 + c) * LANES])
        cdf = 0.5 * (1.0 + lax.erf(up * RSQRT2))
        hcat[:, (1 + c) * LANES:(2 + c) * LANES] = (up * cdf).astype(BF16)
        dgelu[:, cols] = (cdf + up * (RSQRT2PI * jnp.exp(-0.5 * up * up))).astype(BF16)

    wait_weights(tile, mine, w_in, w_out, sems, (4, 5))
    hidden = hcat[...]
    emit(rank, lambda at: dot_nn(hidden, w_out[:, at]), parts)


def emit(rank, product, parts):
    half = LANES // 2
    for r in range(4):
        at = pl.ds(pl.multiple_of((rank ^ r) * LANES, LANES), LANES)
        part = product(at)
        if len(parts) == 4:
            parts[r][...] = part.astype(parts[r].dtype)
            continue
        sx, sy, k0, ka, kb = parts
        if r == 0:
            k0[...] = part
        elif r == 1:
            sx[0] = part[:, :half].astype(BF16)
            kb[...] = part[:, half:]
        elif r == 2:
            ka[...] = part[:, :half]
            sy[0] = part[:, half:].astype(BF16)
        else:
            sx[1] = part[:, :half].astype(BF16)
            sy[1] = part[:, half:].astype(BF16)


def backward_kernel(carried, phased, *refs):
    refs = list(refs)
    take = lambda n: [refs.pop(0) for _ in range(n)]
    meta, = take(1)
    pieces = take(5)
    normed, rq, rk, qf_i, kf_i, v_i, att_i, dgelu, invz, prior_s, prior_k, gain, bias, mix_hi, cos_t, sin_t = take(16)
    mine, other = take(4), take(4)
    if carried:
        state_in, gsum_in, dmix_in, fsum_in = take(4)
        take(2)
    parts = take(5 if phased else 4)
    stats, dcat, state, gsum, dmix, fsum = take(6)
    w_in, w_out, sems, grad = take(4)
    step = pl.program_id(0)
    rank = meta[0]

    @pl.when(step == 0)
    def _():
        start_weights(meta, mine, other, w_in, w_out, sems, (4, 5, 0, 1, 2, 3))
        if carried:
            state[...] = state_in[...]
            gsum[...] = gsum_in[...]
            dmix[...] = dmix_in[...]
            fsum[...] = fsum_in[...]
        else:
            state[...] = jnp.zeros_like(state)
            gsum[...] = jnp.zeros_like(gsum)
            dmix[...] = jnp.zeros_like(dmix)
            fsum[...] = jnp.zeros_like(fsum)

    wait_weights(step, mine, w_in, w_out, sems, (4, 5))
    assemble(rank, pieces, grad)
    g = grad[...]
    d_att = dot_nt(g, w_out[0:LANES, :]).astype(BF16).astype(F32)
    square = (TILE, TILE)
    same = head_of(square, 0) == head_of(square, 1)
    ones = same.astype(BF16)
    inverse = invz[...]
    dn = (d_att * inverse).astype(BF16)
    dn32 = dn.astype(F32)
    high, low = split(dn32 * att_i[...])
    dden = -(dot_nn(high, ones) + dot_nn(low, ones))
    den_hi = dden.astype(BF16).astype(F32)
    roll_hi = pltpu.roll(den_hi, HEAD, 1)
    roll_lo = pltpu.roll(dden - den_hi, HEAD, 1)
    qf, kf, value = qf_i[...], kf_i[...], v_i[...]
    zero = jnp.zeros((TILE, LANES), BF16)
    one = jnp.ones((TILE, LANES), BF16)
    lane = iota((TILE, LANES), 1)
    lane_head = lane // HEAD
    below = iota(square, 0) >= iota(square, 1)
    above = iota(square, 0) <= iota(square, 1)
    prior_hi, prior_lo = split(prior_s[0])
    later_hi, later_lo = split(jnp.where(same, state[...], 0.0))
    d_qf = dot_nt(dn, prior_hi) + dot_nt(dn, prior_lo) + prior_k[0, 0:1, :] * dden
    d_kf = dot_nt(value, later_hi) + dot_nt(value, later_lo) + gsum[0:1, :]
    d_v = dot_nn(kf, later_hi)
    heads = LANES // HEAD
    for h in range(heads):
        here = lane_head == h
        spare = HEAD * ((h + 1) % heads)
        left = jnp.where(lane == spare, roll_hi, jnp.where(lane == spare + 1, roll_lo, dn32)).astype(BF16)
        right = jnp.where(here, value, jnp.where((lane == spare) | (lane == spare + 1), one, zero))
        k_here = jnp.where(here, kf, zero)
        q_here = jnp.where(here, qf, zero)
        d_here = jnp.where(here, dn, zero)
        scores_t = jnp.where(above, dot_nt(k_here, qf), 0.0).astype(BF16)
        ds = jnp.where(below, dot_nt(left, right), 0.0).astype(BF16)
        ds_t = jnp.where(above, dot_nt(right, left), 0.0).astype(BF16)
        d_qf = d_qf + dot_nn(ds, k_here)
        d_kf = d_kf + dot_nn(ds_t, q_here)
        d_v = d_v + dot_nn(scores_t, d_here)
    state[...] = state[...] + dot_tn(qf, dn)
    gsum[...] = gsum[...] + jnp.sum(qf.astype(F32) * dden, axis=0, keepdims=True)
    dlq = d_qf * qf.astype(F32)
    dlk = d_kf * kf.astype(F32)
    fsum[...] = fsum[...] + jnp.sum(dlq + dlk, axis=0, keepdims=True)
    dlq, dlk = dlq.astype(BF16), dlk.astype(BF16)
    dmix[...] = dmix[...] + dot_tn(rq[...], dlq) + dot_tn(rk[...], dlk)
    cosine, sine = twice(cos_t[...]), twice(sin_t[...])
    for c, dl in ((0, dlq), (1, dlk)):
        dr = dot_nt(dl, mix_hi[...])
        dcat[:, c * LANES:(c + 1) * LANES] = (dr * cosine - partner(dr) * sine).astype(BF16)
    dcat[:, 2 * LANES:3 * LANES] = d_v.astype(BF16)
    for c in range(4):
        cols = slice(c * LANES, (c + 1) * LANES)
        d_act = dot_nt(g, w_out[(1 + c) * LANES:(2 + c) * LANES, :])
        dcat[:, (3 + c) * LANES:(4 + c) * LANES] = (d_act * dgelu[:, cols].astype(F32)).astype(BF16)
    wait_weights(step, mine, w_in, w_out, sems, (0, 1, 2, 3))
    wide = dcat[...]
    row = iota((8, LANES), 0)
    first, second = (row == 0).astype(BF16), (row == 1).astype(BF16)
    totals = []

    def product(at):
        part = dot_nt(wide, w_in[at, :])
        one_side = (part * gain[:, at]).astype(BF16)
        other = (part * (normed[:, at].astype(F32) - bias[:, at])).astype(BF16)
        totals.append(dot_nt(first, one_side) + dot_nt(second, other))
        return part

    emit(rank, product, parts)
    stats[...] = totals[0] + totals[1] + totals[2] + totals[3]


def assemble(rank, pieces, whole):
    half = LANES // 2
    for r in range(3):
        whole[:, pl.ds(pl.multiple_of((rank ^ r) * LANES, LANES), LANES)] = pieces[r][...]
    at = pl.multiple_of((rank ^ 3) * LANES, LANES)
    whole[:, pl.ds(at, half)] = pieces[3][...]
    whole[:, pl.ds(pl.multiple_of(at + half, half), half)] = pieces[4][...]


def product_kernel(steps, meta, left, *refs):
    *rights, out_other, out_own = refs[:-1] if len(refs) > 3 else refs
    step = pl.program_id(0)
    if len(rights) == 1:
        right = rights[0]
    else:
        right = refs[-1]

        @pl.when(step == 0)
        def _():
            assemble(meta[1], rights, right)

    product = dot_tn(left[...], right[...]).astype(BF16)

    @pl.when(step < steps)
    def _():
        out_other[...] = product

    @pl.when(step >= steps)
    def _():
        out_own[...] = product


def partial_outs(rows, phased, row_of):
    half = LANES // 2
    if not phased:
        shapes = [jax.ShapeDtypeStruct((rows, LANES), F32)] + [jax.ShapeDtypeStruct((rows, LANES), BF16)] * 3
        return shapes, [pl.BlockSpec((TILE, LANES), lambda *i: (row_of(*i), 0))] * 4
    shapes = [jax.ShapeDtypeStruct((2, rows, half), BF16)] * 2 + [
        jax.ShapeDtypeStruct((rows, LANES), F32), jax.ShapeDtypeStruct((rows, half), F32),
        jax.ShapeDtypeStruct((rows, half), F32)]
    specs = [pl.BlockSpec((2, TILE, half), lambda *i: (0, row_of(*i), 0))] * 2 + [
        pl.BlockSpec((TILE, width), lambda *i: (row_of(*i), 0)) for width in (LANES, half, half)]
    return shapes, specs


def fixed(shape):
    return pl.BlockSpec(shape, lambda *i: (0,) * len(shape))


def outside(count):
    return [pl.BlockSpec(memory_space=pl.ANY)] * count


def params(size):
    return pltpu.CompilerParams(dimension_semantics=("arbitrary",), vmem_limit_bytes=size << 20)


def weight_scratch(width):
    return [pltpu.VMEM((width, 3 * LANES + width), BF16), pltpu.VMEM((LANES + width, width), BF16),
            pltpu.SemaphoreType.DMA((6,))]


def forward_layer(meta, lens, pieces, weights, tables, length, first_row, phased, carry=None):
    rows = pieces[0].shape[0]
    tiles, before = rows // TILE, first_row // TILE
    half, width = LANES // 2, 4 * LANES
    local = lambda t, *_: t
    there = lambda t, *_: before + t
    by_row = lambda n, row_of: pl.BlockSpec((TILE, n), lambda *i: (row_of(*i), 0))
    (gain, bias, mix_hi, mix_lo, feat_w), mine, other = weights
    small = (gain, bias, mix_hi, mix_lo, feat_w)
    shapes, specs = partial_outs(rows, phased, local)
    extra = [(width, BF16), (LANES, F32), (half, F32)] + [(LANES, BF16)] * 5 + [
        (LANES + width, BF16), (width, BF16), (LANES, F32), (LANES, F32)]
    shapes += [jax.ShapeDtypeStruct((length, n), d) for n, d in extra]
    specs += [by_row(n, there) for n, _ in extra]
    shapes += [jax.ShapeDtypeStruct((length // TILE, LANES, LANES), F32), jax.ShapeDtypeStruct((length // TILE, 8, LANES), F32)]
    specs += [pl.BlockSpec((1, n, LANES), lambda *i: (there(*i), 0, 0)) for n in (LANES, 8)]
    states = [(LANES, LANES), (8, LANES)]
    shapes += [jax.ShapeDtypeStruct(s, F32) for s in states]
    specs += [fixed(s) for s in states]
    operands = [meta, jnp.stack([lens[0], jnp.int32(first_row)]), *pieces, *small, *tables, *mine, *other]
    in_specs = [by_row(p.shape[1], local) for p in pieces] + [fixed(w.shape) for w in small] + [by_row(half, there)] * 2 + outside(8)
    aliases = {}
    if carry is not None:
        state, saved = carry
        operands += [*state, *saved]
        in_specs += [fixed(s) for s in states] + outside(SAVED)
        aliases = {len(operands) - SAVED + i: len(shapes) - 2 - SAVED + i for i in range(SAVED)}
    outs = pl.pallas_call(
        functools.partial(forward_kernel, carry is not None, phased),
        name="layer_forward",
        out_shape=shapes,
        grid_spec=pltpu.PrefetchScalarGridSpec(
            num_scalar_prefetch=2, grid=(tiles,), in_specs=in_specs, out_specs=specs, scratch_shapes=weight_scratch(width)),
        input_output_aliases=aliases,
        compiler_params=params(56),
        cost_estimate=pl.CostEstimate(flops=rows * 20_000_000, transcendentals=rows * 5000, bytes_accessed=24 << 20),
    )(*operands)
    count = 5 if phased else 4
    return outs[:count], outs[count:count + SAVED], outs[count + SAVED:]


def backward_layer(meta, pieces, saved, weights, tables, length, first_row, phased, carry=None):
    rows = pieces[0].shape[0]
    tiles, before = rows // TILE, first_row // TILE
    half, width = LANES // 2, 4 * LANES
    local = lambda t, *_: tiles - 1 - t
    there = lambda t, *_: before + tiles - 1 - t
    by_row = lambda n, row_of=there: pl.BlockSpec((TILE, n), lambda *i: (row_of(*i), 0))
    normed, rq, rk, qf, kf, value, hcat, dgelu, invz, attended, prior_s, prior_k = saved
    (gain, bias, mix_hi, mix_lo, feat_w), mine, other = weights
    shapes, specs = partial_outs(rows, phased, local)
    shapes += [jax.ShapeDtypeStruct((8, length), F32), jax.ShapeDtypeStruct((length, 3 * LANES + width), BF16)]
    specs += [pl.BlockSpec((8, TILE), lambda *i: (0, there(*i))), by_row(3 * LANES + width)]
    states = [(LANES, LANES), (8, LANES)] * 2
    shapes += [jax.ShapeDtypeStruct(s, F32) for s in states]
    specs += [fixed(s) for s in states]
    operands = [meta, *pieces, normed, rq, rk, qf, kf, value, attended, dgelu, invz, prior_s, prior_k, gain, bias, mix_hi, *tables,
                *mine, *other]
    in_specs = [by_row(p.shape[1], local) for p in pieces] + [by_row(width)] + [by_row(LANES)] * 6 + [by_row(width), by_row(LANES)] + [
        pl.BlockSpec((1, n, LANES), lambda *i: (there(*i), 0, 0)) for n in (LANES, 8)] + [
        fixed(w.shape) for w in (gain, bias, mix_hi)] + [by_row(half)] * 2 + outside(8)
    aliases = {}
    if carry is not None:
        state, arrays = carry
        operands += [*state, *arrays]
        in_specs += [fixed(s) for s in states] + outside(2)
        aliases = {len(operands) - 2 + i: len(shapes) - 6 + i for i in range(2)}
    outs = pl.pallas_call(
        functools.partial(backward_kernel, carry is not None, phased),
        name="layer_backward",
        out_shape=shapes,
        grid_spec=pltpu.PrefetchScalarGridSpec(
            num_scalar_prefetch=1, grid=(tiles,), in_specs=in_specs, out_specs=specs,
            scratch_shapes=weight_scratch(width) + [pltpu.VMEM((TILE, width), BF16)]),
        input_output_aliases=aliases,
        compiler_params=params(56),
        cost_estimate=pl.CostEstimate(flops=rows * 25_000_000, transcendentals=0, bytes_accessed=24 << 20),
    )(*operands)
    count = 5 if phased else 4
    return outs[:count], outs[count:count + 2], outs[count + 2:]


def swap(value, axis, by):
    return lax.ppermute(value, axis, [(k, k ^ by) for k in range(lax.axis_size(axis))])


def gather_pieces(shard, meanwhile=()):
    from_x, from_y = after((swap(shard, "mp", 1), swap(shard, "mp", 2)), *meanwhile)
    return (shard, from_x, from_y) + last_pieces(from_x, from_y)


def last_pieces(from_x, from_y):
    half = from_x.shape[1] // 2
    return tuple(lax.optimization_barrier((swap(from_x[:, :half], "mp", 2), swap(from_y[:, half:], "mp", 1))))


def after(values, *others):
    if not others:
        return values
    return lax.optimization_barrier((values, others))[0]


def direct_sends(parts):
    return parts[0], [swap(part, "mp", r) for r, part in enumerate(parts) if r > 0]


def scatter_start(parts):
    return swap(parts[0], "mp", 1), swap(parts[1], "mp", 2)


def scatter_turn(parts, arrived):
    _, _, _, ka, kb = parts
    in_x, in_y = arrived
    return (ka + in_x[1].astype(F32)).astype(BF16), (kb + in_y[1].astype(F32)).astype(BF16)


def scatter_end(parts, arrived, to_y, to_x):
    _, _, k0, ka, _ = parts
    in_x, in_y = arrived
    half = ka.shape[1]
    last_y, last_x = swap(to_y, "mp", 2), swap(to_x, "mp", 1)
    return jnp.concatenate(
        [k0[:, :half] + in_x[0].astype(F32) + last_y.astype(F32), k0[:, half:] + in_y[0].astype(F32) + last_x.astype(F32)],
        axis=1)


def scatter_sum(parts):
    arrived = scatter_start(parts)
    return scatter_end(parts, arrived, *scatter_turn(parts, arrived))


def mp_total(values):
    return values + swap(values, "mp", 1) + swap(values, "mp", 2) + swap(values, "mp", 3)


def ring_scatter(block_of, axis, meanwhile=()):
    count = lax.axis_size(axis)
    rank = lax.axis_index(axis)
    pairs = [(k, (k + 1) % count) for k in range(count)]
    total = block_of((rank + count - 1) % count)
    for step in range(2, count + 1):
        arrived = lax.ppermute(total, axis, pairs)
        if step in (2, count):
            arrived = after(arrived, *meanwhile)
        total = (arrived.astype(F32) + block_of((rank + count - step) % count).astype(F32)).astype(BF16)
        yield arrived, total


def dp_sends(values):
    count = lax.axis_size("dp")
    if count > 8:
        return [lax.psum(values, "dp")]
    return [values] + [lax.ppermute(values, "dp", [(i, (i + k) % count) for i in range(count)]) for k in range(1, count)]


def block_sends(block_of, axis):
    count = lax.axis_size(axis)
    rank = lax.axis_index(axis)
    if count > 8:
        return [list(ring_scatter(block_of, axis))[-1][1]]
    return [block_of(rank)] + [
        lax.ppermute(block_of((rank + k) % count), axis, [(i, (i + k) % count) for i in range(count)]) for k in range(1, count)]


def sum_blocks(blocks):
    total = blocks[0].astype(F32)
    for block in blocks[1:]:
        total = total + block.astype(F32)
    return total.astype(BF16)


def weight_gradient(left, rights, section, place):
    rows = left.shape[0]
    whole = len(rights) == 1
    block = 256 if whole else 128
    m = left.shape[1] // (1 if whole else 2)
    n = rights[0].shape[1] // 2 if whole else 4 * LANES
    steps = m // block
    half_at = lambda i, meta: jnp.where(i < steps, 1 - meta[0], meta[0])
    if whole:
        left_at = lambda i, meta: (0, i % steps)
        right_specs = [pl.BlockSpec((rows, n), lambda i, meta: (0, half_at(i, meta)))]
    else:
        left_at = lambda i, meta: (0, half_at(i, meta) * steps + i % steps)
        right_specs = [fixed(p.shape) for p in rights]
    other, own = pl.pallas_call(
        functools.partial(product_kernel, steps),
        name="weight_gradient",
        out_shape=[jax.ShapeDtypeStruct((m, n), BF16)] * 2,
        grid_spec=pltpu.PrefetchScalarGridSpec(
            num_scalar_prefetch=1, grid=(2 * steps,),
            in_specs=[pl.BlockSpec((rows, block), left_at)] + right_specs,
            out_specs=[pl.BlockSpec((block, n), lambda i, meta: (jnp.minimum(i, steps - 1), 0)),
                       pl.BlockSpec((block, n), lambda i, meta: (jnp.maximum(i - steps, 0), 0))],
            scratch_shapes=[] if whole else [pltpu.VMEM((rows, n), BF16)]),
        compiler_params=params(58 if whole else 20),
        cost_estimate=pl.CostEstimate(flops=4 * rows * m * n, transcendentals=0, bytes_accessed=4 * (rows * (m + n) + m * n)),
    )(jnp.stack([section, place]).astype(jnp.int32), left, *rights)
    return own, other


def dct_table(order):
    row_index = jnp.arange(order, dtype=F32)[:, None]
    col_index = jnp.arange(order, dtype=F32)[None, :]
    cosines = jnp.sqrt(2.0 / order) * jnp.cos(math.pi * (row_index + 0.5) * col_index / order)
    return cosines * jnp.where(col_index == 0, math.sqrt(0.5), 1.0)


def rotary_tables(length):
    column = jnp.arange(LANES // 2, dtype=jnp.int32) % HEAD
    half = ROT // 2
    index = (column % half).astype(F32)
    angles = jnp.arange(length, dtype=F32)[:, None] * (10000.0 ** (-index * 2.0 / ROT))[None, :]
    turned = (column < ROT)[None, :]
    sign = jnp.where(column < half, -1.0, 1.0)[None, :]
    return jnp.where(turned, jnp.cos(angles), 1.0), jnp.where(turned, sign * jnp.sin(angles), 0.0)


def shards(block_input, cotangent, lengths, ln_gain, ln_bias, w_qkv, w_out, w_up, w_down, freq_table, feat_weight):
    section = lax.axis_index("section")
    place = lax.axis_index("mp")
    group = lax.axis_index("dp")
    groups = lax.axis_size("dp")
    local_slots, length, shard_width = block_input.shape
    width = ln_gain.shape[1]
    heads = freq_table.shape[1]
    is_first = section == 0
    lens = lax.dynamic_slice_in_dim(lengths, section, 1, 0)
    metas = [jnp.stack([place, (section == l).astype(jnp.int32)]).astype(jnp.int32) for l in range(2)]

    def own(values):
        return lax.dynamic_index_in_dim(values, section, 0, keepdims=False)

    shard0 = own(block_input)

    small = jnp.concatenate([ln_gain[0], ln_bias[0], feat_weight.reshape(-1), freq_table.astype(F32).reshape(-1)])
    small_other = swap(small, "section", 1)
    mine = (w_qkv, w_up, w_out, w_down)
    other = tuple(swap(w, "section", 1) for w in mine)
    pieces0 = gather_pieces(shard0, [small_other, other[2]])

    def both(mine, other):
        return jnp.where(is_first, mine, other), jnp.where(is_first, other, mine)

    layers_small = both(small, small_other)
    table = dct_table(HEAD)
    eye = jnp.eye(heads, dtype=F32)

    def layer_weights(l):
        vec = layers_small[l]
        gain, bias = vec[:width].reshape(1, width), vec[width:2 * width].reshape(1, width)
        feat = vec[2 * width:2 * width + LANES].reshape(1, LANES)
        freq = vec[2 * width + LANES:].reshape(heads, HEAD, HEAD)
        mixed = jnp.einsum("nk,hkm->hnm", table, freq, precision=lax.Precision.HIGHEST)
        mixed = (eye[:, None, :, None] * mixed[:, :, None, :]).reshape(LANES, LANES)
        high = lax.reduce_precision(mixed, 8, 7)
        return (gain, bias, high.astype(BF16), (mixed - high).astype(BF16), feat), mine, other

    weights0, weights1 = layer_weights(0), layer_weights(1)
    tables = rotary_tables(length)

    cot = after(own(cotangent), pieces0[3], pieces0[4])
    cot_x, cot_y = swap(cot, "mp", 1), swap(cot, "mp", 2)
    part0, all0, _ = forward_layer(metas[0], lens, pieces0, weights0, tables, length, 0, True)
    part0 = after(part0, cot_x, cot_y)
    hidden = (shard0.astype(F32) + scatter_sum(part0)).astype(BF16)
    pieces1 = gather_pieces(hidden)
    cot_x, cot_y = after((cot_x, cot_y), pieces1[3], pieces1[4])
    pieces_g = (cot, cot_x, cot_y) + last_pieces(cot_x, cot_y)
    part1, all1, _ = forward_layer(metas[1], lens, pieces1, weights1, tables, length, 0, False)
    out_kept, out_sent = direct_sends(part1)

    def saved_of(arrays):
        return (arrays[0],) + tuple(arrays[3:])

    def in_block(mine, arrived):
        n = mine.shape[0] // groups
        cut = lambda v, i: lax.dynamic_slice_in_dim(v, i * n, n, 0)
        return lambda i: (cut(mine, i).astype(F32) + cut(arrived, i).astype(F32)).astype(BF16)

    def out_block(mine, arrived):
        n = mine.shape[1] // groups
        cut = lambda v, i: lax.dynamic_slice_in_dim(v, i * n, n, 1)
        return lambda i: (cut(mine, i).astype(F32) + cut(arrived, i).astype(F32)).astype(BF16)

    def run_backward(meta, grad, saved, weights, phased):
        parts, (stats, dcat), (_, _, dmix, fsum) = backward_layer(meta, grad, saved, weights, tables, length, 0, phased)
        return parts, stats, dcat, dmix, fsum

    def norm_backward(grad_shard, d_normed, sums, norm, gain_all):
        xhat, rstd = norm
        gain = lax.dynamic_slice_in_dim(gain_all, place * shard_width, shard_width, 1)
        mean_d = (sums[0] * (1.0 / width))[:, None]
        mean_dx = (sums[1] * (1.0 / width))[:, None]
        return grad_shard.astype(F32) + rstd[:, :1] * (d_normed * gain - mean_d - xhat * mean_dx)

    def small_gradients(d_normed, norm, dmix, fsum):
        gain_part = jnp.sum(d_normed * norm[0], axis=0)
        bias_part = jnp.sum(d_normed, axis=0)
        diagonal = jnp.stack([dmix[h * HEAD:(h + 1) * HEAD, h * HEAD:(h + 1) * HEAD] for h in range(heads)])
        return jnp.concatenate([gain_part, bias_part, fsum[0], diagonal.reshape(-1)])

    saved1, saved0 = saved_of(all1), saved_of(all0)
    own, other = weight_gradient(saved1[6], pieces_g, section, place)
    out_blocks1 = block_sends(out_block(own, swap(other, "section", 1)), "dp")
    grad1_b = after(pieces_g, out_blocks1[0])
    parts, stats, dcat1, dmix1, fsum1 = run_backward(metas[1], grad1_b, saved1, weights1, True)
    parts, stats, dcat1, dmix1, fsum1 = after((parts, stats, dcat1, dmix1, fsum1), *out_blocks1, *out_sent[:2])
    arrived, own, other = lax.optimization_barrier(
        (scatter_start(parts), *weight_gradient(saved1[0], (dcat1,), section, place)))
    turn = scatter_turn(parts, arrived)
    steps1 = list(ring_scatter(in_block(own, swap(other, "section", 1)), "dp"))
    arrivals1, red_in1 = [arrival for arrival, _ in steps1], steps1[-1][1]
    d_normed = scatter_end(parts, arrived, *turn)
    sums = mp_total(after(stats, *turn))
    g0 = norm_backward(cot, d_normed, sums, all1[1:3], weights1[0][0]).astype(BF16)
    small1 = small_gradients(d_normed, all1[1:3], dmix1, fsum1)
    pieces_g0 = gather_pieces(after(g0, arrivals1[0]), arrivals1[1:2])
    pieces_g0 = after(pieces_g0, *arrivals1[2:3])
    out = hidden.astype(F32) + out_kept + out_sent[0].astype(F32) + out_sent[1].astype(F32) + out_sent[2].astype(F32)

    own, other = weight_gradient(saved0[6], pieces_g0, section, place)
    out_blocks0 = block_sends(out_block(own, swap(other, "section", 1)), "dp")
    grad0_b = after(pieces_g0, out_blocks0[0])
    parts, stats, dcat0, dmix0, fsum0 = run_backward(metas[0], grad0_b, saved0, weights0, False)
    parts, stats, dcat0, dmix0, fsum0 = after((parts, stats, dcat0, dmix0, fsum0), *out_blocks0, out_sent[2])
    out_blocks1 = after(out_blocks1, dcat0)
    kept, sent = direct_sends(parts)
    sent[:2], own, other = lax.optimization_barrier((sent[:2], *weight_gradient(saved0[0], (dcat0,), section, place)))
    block0 = in_block(own, swap(other, "section", 1))
    meanwhile = sent[2:]
    ring0 = ring_scatter(block0, "dp", meanwhile)
    steps0 = [next(ring0)]
    meanwhile.clear()
    sums = mp_total(after(stats, steps0[0][1]))
    sent, dmix0, out_blocks0, out_blocks1 = after((sent, dmix0, out_blocks0, out_blocks1), steps0[0][1])
    d_normed = kept + sent[0].astype(F32) + sent[1].astype(F32) + sent[2].astype(F32)
    d_input = norm_backward(g0, d_normed, sums, all0[1:3], weights0[0][0])
    small0 = small_gradients(d_normed, all0[1:3], dmix0, fsum0)

    def to_owner(first, second, axis):
        mine, other = both(first, second)
        arrived = swap(other, "section", 1)
        return jnp.where(is_first, jnp.concatenate([mine, arrived], axis), jnp.concatenate([arrived, mine], axis)).astype(F32)

    grads_out = to_owner(sum_blocks(out_blocks0), sum_blocks(out_blocks1), 0)
    small_mine, small_send = both(small0, small1)
    small_sum = small_mine + swap(small_send, "section", 1)
    small_parts = dp_sends(small_sum)
    keep, send = both(d_input, out)
    arrived = swap(send, "section", 1)
    boundary = jnp.where(is_first, jnp.stack([keep, arrived]), jnp.stack([arrived, keep]))
    meanwhile.append(arrived)
    steps0 += list(ring0)
    grads_in = to_owner(steps0[-1][1], red_in1, 1)
    small_sum = sum(after(small_parts, steps0[-1][0]))
    feat_grad = small_sum[2 * shard_width:2 * shard_width + LANES].reshape(heads, HEAD) / feat_weight[0]
    freq_grad = jnp.einsum("nk,hnm->hkm", table, small_sum[2 * shard_width + LANES:].reshape(heads, HEAD, HEAD),
                           precision=lax.Precision.HIGHEST)
    qkv_grad = jnp.stack([grads_in[:, t * shard_width:(t + 1) * shard_width] for t in range(3)])
    return (
        boundary[None],
        small_sum[None, :shard_width],
        small_sum[None, shard_width:2 * shard_width],
        qkv_grad[None],
        grads_out[None, :shard_width],
        grads_in[None, :, 3 * shard_width:],
        grads_out[None, shard_width:],
        freq_grad[None],
        feat_grad[None],
    )


def solution(mesh):
    placed = (
        P("dp", None, "mp"), P("dp", None, "mp"), P("dp"), P("section", None), P("section", None),
        P("section", None, None, "mp"), P("section", "mp", None), P("section", None, "mp"), P("section", "mp", None),
        P("section", "mp", None, None), P("section", "mp", None),
    )
    return jax.shard_map(
        shards,
        mesh=mesh,
        in_specs=placed,
        out_specs=(
            P("section", "dp", None, "mp"), P("section", "mp"), P("section", "mp"), P("section", None, "dp", "mp"),
            P("section", "mp", "dp"), P("section", "dp", "mp"), P("section", "mp", "dp"), P("section", "mp", None, None),
            P("section", "mp", None),
        ),
        check_vma=False,
    )
```
